32 devices in a mesh: section: 2 (over x), dp: 4 (over z), tensor: 4 (over y, core).
Axes of the slice: x: 2, y: 2, z: 4, core: 2. Of those that a mesh axis runs over, the one named last changes fastest.
Arguments:
- section_input: bfloat16 [2, 4, 736, 1152], P(None, 'dp', 'tensor'), may hold values from -6 to 6
- final_cotangent: bfloat16 [2, 4, 736, 1152], P(None, 'dp', 'tensor'), may hold values from -6 to 6
- lengths: int32 [2, 4], P(None, 'dp'), may hold values from 368 to 736, as said below
- qkv_weight: bfloat16 [2, 3, 1152, 1152], P('section', None, 'dp', 'tensor'), may hold values from -0.1875 to 0.1875
- out_weight: bfloat16 [2, 1152, 1152], P('section', 'tensor', 'dp'), may hold values from -2.5 to 2.5
- up_weight: bfloat16 [2, 1152, 4304], P('section', 'dp', 'tensor'), may hold values from -0.1875 to 0.1875
- down_weight: bfloat16 [2, 4304, 1152], P('section', 'tensor', 'dp'), may hold values from -0.09375 to 0.09375
- norm_gains: float32 [2, 2, 1152], P('section', None, ('dp', 'tensor')), may hold values from 0.1 to 1.9
- biases: float32 [2, 6, 1152], P('section', None, ('dp', 'tensor')), may hold values from -3 to 3
- up_bias: float32 [2, 4304], P('section', 'tensor'), may hold values from -3 to 3
Outputs:
- section_output: bfloat16 [2, 2, 4, 736, 1152], P('section', None, 'dp', 'tensor')
- input_grad: bfloat16 [2, 2, 4, 736, 1152], P('section', None, 'dp', 'tensor')
- qkv_grad: float32 [2, 3, 1152, 1152], P('section', None, 'dp', 'tensor')
- out_grad: float32 [2, 1152, 1152], P('section', 'tensor', 'dp')
- up_grad: float32 [2, 1152, 4304], P('section', 'dp', 'tensor')
- down_grad: float32 [2, 4304, 1152], P('section', 'tensor', 'dp')
- gains_grad: float32 [2, 2, 1152], P('section', None, ('dp', 'tensor'))
- biases_grad: float32 [2, 6, 1152], P('section', None, ('dp', 'tensor'))
- up_bias_grad: float32 [2, 4304], P('section', 'tensor')
The draws below stay inside these ranges and needn't reach their ends.
Inputs may be any that keep to these rules, and one draw needn't show every extreme that they name: `lengths`: in every micro-batch at least one image has all 736 token slots valid; every image has 368 valid slots or more.
All inputs are finite; a program needn't handle non-finite values.
Results may differ from the reference program's by a relative error of at most 0.018.
Values may be sent and summed in bfloat16 or wider, within the bound.
A program may use at most 192 MiB of HBM per device.

```python
import math
import jax
import jax.numpy as jnp
from jax import lax

D = 1152
HEADS = 16
HEAD = 72
FF = 4304
SEQ = 736
MB = 2
IMAGES = 4
LAYERS = 2


def draw_lengths(key, part):
    key_values, key_chosen = jax.random.split(jax.random.fold_in(key, 17))
    values = jax.random.randint(key_values, (MB, IMAGES), SEQ // 2, SEQ + 1)
    chosen = jax.random.randint(key_chosen, (MB, 1), 0, IMAGES)
    places = jnp.arange(IMAGES, dtype=jnp.int32)[None, :]
    return jnp.where(places == chosen, SEQ, values).astype(jnp.int32)


def shard_levels(rng, extent, cuts, low, largest):
    loudness = 1.0
    for axis_at, shards_of in cuts:
        draws = jax.random.uniform(jax.random.fold_in(jax.random.fold_in(rng, 6), axis_at), (shards_of,), jnp.float32, low / len(cuts), largest / len(cuts))
        loudness = loudness * jnp.repeat(jnp.exp(draws), extent[axis_at] // shards_of).reshape((-1,) + (1,) * (len(extent) - 1 - axis_at))
    return loudness


def normal_values(stream_key, dims, width, bound, shards=(), held_as=jnp.bfloat16):
    entries = width * jax.random.normal(stream_key, dims, jnp.float32)
    if shards:
        entries = entries * shard_levels(stream_key, dims, shards, -0.22, 0.18)
    return jnp.clip(entries, -bound, bound).astype(held_as)


def setup_inputs(seed: int = 0) -> dict:
    seeds = jax.random.split(jax.random.key(seed), 11)
    section_input = normal_values(seeds[0], (MB, IMAGES, SEQ, D), 1.0, 6.0, ((1, 4), (2, 4)))
    final_cotangent = normal_values(seeds[1], (MB, IMAGES, SEQ, D), 1.0, 6.0, ((1, 4), (2, 4)))
    lengths = draw_lengths(jax.random.fold_in(seeds[10], 71), 0)
    qkv_weight = normal_values(seeds[3], (LAYERS, 3, D, D), D ** -0.5, 0.1875, ((0, 2), (2, 4), (3, 4)))
    out_weight = normal_values(seeds[4], (LAYERS, D, D), (max(4 * D // SEQ, 1)) ** -0.5, 2.5, ((0, 2), (1, 4), (2, 4)))
    up_weight = normal_values(seeds[5], (LAYERS, D, FF), D ** -0.5, 0.1875, ((0, 2), (1, 4), (2, 4)))
    down_weight = normal_values(seeds[6], (LAYERS, FF, D), FF ** -0.5, 0.09375, ((0, 2), (1, 4), (2, 4)))
    norm_gains = jnp.clip(1.0 + 0.18 * jax.random.normal(seeds[7], (LAYERS, 2, D), jnp.float32), 0.1, 1.9)
    biases = normal_values(seeds[8], (LAYERS, 6, D), 0.5, 3.0, ((0, 2), (2, 16)), jnp.float32)
    up_bias = normal_values(seeds[9], (LAYERS, FF), 0.5, 3.0, ((0, 2), (1, 4)), jnp.float32)
    return {"section_input": section_input, "final_cotangent": final_cotangent, "lengths": lengths, "qkv_weight": qkv_weight, "out_weight": out_weight, "up_weight": up_weight, "down_weight": down_weight, "norm_gains": norm_gains, "biases": biases, "up_bias": up_bias}


@jax.custom_vjp
def low(v):
    return lax.optimization_barrier(v.astype(jnp.bfloat16)).astype(jnp.float32)

@jax.custom_vjp
def low_back(v):
    return v

def low_keep(v):
    return (low(v), None)

def low_pass(kept, grad):
    return (grad,)

def back_keep(v):
    return (v, None)

def back_low(kept, grad):
    return (low(grad),)
low.defvjp(low_keep, low_pass)
low_back.defvjp(back_keep, back_low)
norm_eps = 1e-06
masked_score = -1000000000.0
highest = lax.Precision.HIGHEST

def layer_norm(rows, gain_vec, shift_vec):
    centred = rows - lax.optimization_barrier(jnp.mean(rows, axis=-1, keepdims=True))
    spread = lax.optimization_barrier(jnp.mean(centred * centred, axis=-1, keepdims=True))
    return centred * lax.rsqrt(spread + norm_eps) * gain_vec + shift_vec

def both_ways(value):
    return low(low_back(value))

def matmul(left, right):
    return jnp.matmul(left, right, precision=highest)

def gelu_tanh(value):
    return jax.nn.gelu(value, approximate=True)

def encoder_layer(inputs, params, lengths_here):
    qkv_part, out_part, up_part, down_part, gains, shifts, up_bias_here = params
    group = inputs.shape[0]
    normed = low(layer_norm(inputs, gains[0], shifts[0]))
    queries = both_ways(matmul(normed, qkv_part[0]) + shifts[1])
    keys_all = both_ways(matmul(normed, qkv_part[1]))
    values = both_ways(matmul(normed, qkv_part[2]) + shifts[2])
    split = (group, SEQ, HEADS, HEAD)
    scores = jnp.einsum('gqhe,gkhe->ghqk', queries.reshape(split), keys_all.reshape(split), precision=highest) / math.sqrt(HEAD)
    valid = jnp.arange(SEQ, dtype=jnp.int32)[None, None, None, :] < lengths_here[:, None, None, None]
    scores = low_back(jnp.where(valid, scores, masked_score))
    probs = low(jax.nn.softmax(scores, axis=-1))
    mixed = jnp.einsum('ghqk,gkhe->gqhe', probs, values.reshape(split), precision=highest).reshape(group, SEQ, D)
    mixed = both_ways(mixed)
    hidden = inputs + low_back(matmul(mixed, out_part) + shifts[3])
    normed_two = low(layer_norm(hidden, gains[1], shifts[4]))
    upper = low_back(matmul(normed_two, up_part) + up_bias_here)
    active = low(gelu_tanh(upper))
    return hidden + low_back(matmul(active, down_part) + shifts[5])

def reference(section_input, final_cotangent, lengths, qkv_weight, out_weight, up_weight, down_weight, norm_gains, biases, up_bias):
    float_params = tuple((item.astype(jnp.float32) for item in (qkv_weight, out_weight, up_weight, down_weight, norm_gains, biases, up_bias)))
    total_images = MB * IMAGES
    group = math.gcd(total_images, 4)
    rounds = total_images // group
    shaped = section_input.astype(jnp.float32).reshape(rounds, group, SEQ, D)
    padding = jnp.zeros_like(shaped)
    length_groups = lengths.reshape(rounds, group)

    def whole(shaped_in, padding_in, params):

        def one_group(pieces):
            block_in, block_pad, block_len = pieces
            layer_zero = tuple((item[0] for item in params))
            layer_one = tuple((item[1] for item in params))
            first_out = encoder_layer(block_in, layer_zero, block_len)
            passed = low(low_back(first_out + block_pad))
            second_out = encoder_layer(passed, layer_one, block_len)
            return (passed, second_out)
        return lax.map(jax.checkpoint(one_group), (shaped_in, padding_in, length_groups))
    (passed, final), back_fn = jax.vjp(whole, shaped, padding, float_params)
    cotangent = final_cotangent.astype(jnp.float32).reshape(rounds, group, SEQ, D)
    grad_in, grad_pad, grad_params = back_fn((jnp.zeros_like(passed), cotangent))
    full_shape = (MB, IMAGES, SEQ, D)
    section_output = jnp.stack([passed.reshape(full_shape), final.reshape(full_shape)]).astype(jnp.bfloat16)
    input_grad = jnp.stack([grad_in.reshape(full_shape), grad_pad.reshape(full_shape)]).astype(jnp.bfloat16)
    return (section_output, input_grad, grad_params[0], grad_params[1], grad_params[2], grad_params[3], grad_params[4], grad_params[5], grad_params[6])
```

```python
import math

import jax
import jax.numpy as jnp
from jax import lax
from jax.experimental import pallas as pl
from jax.experimental.pallas import tpu as pltpu
from jax.sharding import PartitionSpec as P

HEAD = 72
LANES = 128
norm_eps = 1e-06
masked_score = -1000000000.0
score_scale = 1.0 / math.sqrt(HEAD)
SWAP = [(0, 1), (1, 0)]
GELU_A = math.sqrt(2.0 / math.pi)
GELU_B = 0.044715
EVERY = ("section", "dp", "tensor")


def round_up(value, step):
    return -(-value // step) * step


def dot(left, right, left_dim, right_dim):
    return lax.dot_general(
        left, right, (((left_dim,), (right_dim,)), ((), ())), preferred_element_type=jnp.float32
    )


def low(value):
    return value.astype(jnp.bfloat16)


def layer_norm(rows, gain_vec, shift_vec):
    centred = rows - jnp.mean(rows, axis=-1, keepdims=True)
    spread = jnp.mean(centred * centred, axis=-1, keepdims=True)
    return centred * lax.rsqrt(spread + norm_eps) * gain_vec + shift_vec


def norm_back(rows, gain_vec, grads):
    centred = rows - jnp.mean(rows, axis=-1, keepdims=True)
    spread = jnp.mean(centred * centred, axis=-1, keepdims=True)
    inverse = lax.rsqrt(spread + norm_eps)
    xhat = centred * inverse
    e = grads * gain_vec
    back = inverse * (
        e
        - jnp.mean(e, axis=-1, keepdims=True)
        - xhat * jnp.mean(e * xhat, axis=-1, keepdims=True)
    )
    return back, grads * xhat


def gelu_tanh(value):
    return jax.nn.gelu(value, approximate=True)


def pad_heads(flat, heads):
    split = flat.reshape(flat.shape[:-1] + (heads, HEAD))
    padded = jnp.pad(split, [(0, 0)] * (split.ndim - 1) + [(0, LANES - HEAD)])
    return padded.reshape(flat.shape[:-1] + (heads * LANES,))


def drop_heads(padded):
    heads = padded.shape[-1] // LANES
    split = padded.reshape(padded.shape[:-1] + (heads, LANES))[..., :HEAD]
    return split.reshape(padded.shape[:-1] + (heads * HEAD,))


MESH = pl.DeviceIdType.MESH
VMEM_BYTES = 64_000_000
LOG2E = 1.0 / math.log(2.0)
TILE = 256


class Slab:
    def __init__(self, half_rows):
        self.half_rows = half_rows
        section = lax.axis_index("section")
        tensor = lax.axis_index("tensor")
        core = lax.rem(tensor, 2)
        self.mine = self.around(section, tensor, core)
        self.theirs = self.around(section, tensor + 1 - 2 * core, 1 - core)
        self.mate = self.theirs[0]

    @staticmethod
    def around(section, tensor, core):
        over = lax.rem(tensor + 2, 4)
        turn = 1 - 2 * section
        first = (section + (1 - core) * turn, tensor + core * (over - tensor))
        second = (section + core * turn, tensor + (1 - core) * (over - tensor))
        return [(section, tensor), first, second, (1 - section, over)]

    def rows(self, ref, at):
        start = pl.multiple_of((2 * at[1] + at[0]) * self.half_rows, self.half_rows)
        return ref.at[pl.ds(start, self.half_rows)]

    def greet(self):
        barrier = pltpu.get_barrier_semaphore()
        for peer in (self.mine[1], self.mine[2], self.mate):
            pl.semaphore_signal(barrier, inc=1, device_id=named(peer), device_id_type=MESH)
        pl.semaphore_wait(barrier, 3)


def named(at):
    return {"section": at[0], "tensor": at[1]}


class Moves:
    def __init__(self, slab, send_sems, recv_sems):
        self.slab, self.send_sems, self.recv_sems = slab, send_sems, recv_sems
        self.sent = []

    def copy(self, src, dst, role, peer):
        return pltpu.make_async_remote_copy(
            src_ref=src,
            dst_ref=dst,
            send_sem=self.send_sems.at[role],
            recv_sem=self.recv_sems.at[role],
            device_id=named(peer),
            device_id_type=MESH,
        )

    def send(self, src, dst, role, peer):
        copy = self.copy(src, dst, role, peer)
        copy.start()
        self.sent.append(copy)

    def arrived(self, dst, role):
        self.copy(dst, dst, role, self.slab.mate).wait_recv()

    def drain(self):
        for copy in self.sent:
            copy.wait_send()


class Gather(Moves):
    def __init__(self, slab, whole, send_sems, recv_sems):
        super().__init__(slab, send_sems, recv_sems)
        self.whole = whole

    def pass_on(self, at, role, peer):
        part = self.slab.rows(self.whole, at)
        self.send(part, part, role, peer)

    def arrive(self, at, role):
        self.arrived(self.slab.rows(self.whole, at), role)

    def start(self):
        mine = self.slab.mine
        self.pass_on(mine[0], 0, mine[1])
        self.pass_on(mine[0], 1, mine[2])
        self.pass_on(mine[0], 3, self.slab.mate)

    def forward(self):
        mine, mate = self.slab.mine, self.slab.mate
        self.arrive(mine[1], 0)
        self.pass_on(mine[1], 2, mine[2])
        self.pass_on(mine[1], 4, mate)

    def to_mate(self):
        mine, mate = self.slab.mine, self.slab.mate
        self.arrive(mine[2], 1)
        self.pass_on(mine[2], 5, mate)
        self.arrive(mine[3], 2)
        self.pass_on(mine[3], 6, mate)

    def finish(self):
        for k in range(4):
            self.arrive(self.slab.theirs[k], 3 + k)
        self.drain()


class Scatter(Moves):
    def __init__(self, slab, terms, from_mate, outgoing, from_second, from_first, send_sems, recv_sems):
        super().__init__(slab, send_sems, recv_sems)
        self.terms, self.from_mate, self.outgoing = terms, from_mate, outgoing
        self.from_second, self.from_first = from_second, from_first

    def start(self):
        for k in (3, 2, 1, 0):
            part = self.slab.rows(self.terms, self.slab.theirs[k])
            self.send(part, self.from_mate.at[k], k, self.slab.mate)

    def chip_sum(self, k, rows):
        part = self.slab.rows(self.terms, self.slab.mine[k])
        return part[rows].astype(jnp.float32) + self.from_mate[k, rows].astype(jnp.float32)

    def blocks(self):
        return [pl.ds(start, 32) for start in range(0, self.slab.half_rows, 32)]

    def second_hop(self):
        second = self.slab.mine[2]
        for k, slot in ((3, 1), (2, 0)):
            self.arrived(self.from_mate.at[k], k)
            for rows in self.blocks():
                self.outgoing[slot, rows] = low(self.chip_sum(k, rows))
            self.send(self.outgoing.at[slot], self.from_second.at[slot], 4 + slot, second)

    def first_hop(self):
        self.arrived(self.from_mate.at[1], 1)
        self.arrived(self.from_second.at[1], 5)
        for rows in self.blocks():
            term = self.from_second[1, rows].astype(jnp.float32)
            self.outgoing[2, rows] = low(self.chip_sum(1, rows) + term)
        self.send(self.outgoing.at[2], self.from_first, 6, self.slab.mine[1])

    def finish(self):
        self.arrived(self.from_mate.at[0], 0)
        self.arrived(self.from_second.at[0], 4)
        self.arrived(self.from_first, 6)
        self.drain()

    def total(self, rows):
        other = self.from_second[0, rows].astype(jnp.float32)
        last = self.from_first[rows].astype(jnp.float32)
        return self.chip_sum(0, rows) + other + last


def scatter_scratch(micro, seq, half_rows, width):
    return [
        pltpu.VMEM((micro, seq, width), jnp.bfloat16),
        pltpu.VMEM((micro, 4, half_rows, width), jnp.bfloat16),
        pltpu.VMEM((micro, 3, half_rows, width), jnp.bfloat16),
        pltpu.VMEM((micro, 2, half_rows, width), jnp.bfloat16),
        pltpu.VMEM((micro, half_rows, width), jnp.bfloat16),
        pltpu.SemaphoreType.DMA((micro, 7)),
        pltpu.SemaphoreType.DMA((micro, 7)),
    ]


def gather_scratch(micro, seq, width):
    return [
        pltpu.VMEM((micro, seq, width), jnp.bfloat16),
        pltpu.SemaphoreType.DMA((micro, 7)),
        pltpu.SemaphoreType.DMA((micro, 7)),
    ]


def make_scatters(slab, refs, micro):
    terms, from_mate, outgoing, from_second, from_first, send_sems, recv_sems = refs
    return [
        Scatter(
            slab,
            terms.at[m],
            from_mate.at[m],
            outgoing.at[m],
            from_second.at[m],
            from_first.at[m],
            send_sems.at[m],
            recv_sems.at[m],
        )
        for m in range(micro)
    ]


def make_gathers(slab, refs, micro):
    whole, send_sems, recv_sems = refs
    return [
        Gather(slab, whole.at[m], send_sems.at[m], recv_sems.at[m]) for m in range(micro)
    ]


def step_rows(i, size):
    return pl.ds(pl.multiple_of(i * size, size), size)


def repeat(count, body):
    def one(i, carry):
        body(i)
        return carry

    lax.fori_loop(0, count, one, 0)


def widen(packed, wide):
    heads = packed.shape[1] // HEAD

    def block(i):
        rows = step_rows(i, 128)
        for h in range(heads):
            piece = packed[rows, h * HEAD : (h + 1) * HEAD]
            blank = jnp.zeros((128, LANES - HEAD), jnp.bfloat16)
            wide[rows, h * LANES : (h + 1) * LANES] = jnp.concatenate([piece, blank], axis=1)

    repeat(packed.shape[0] // 128, block)


def attn_forward_kernel(
    rows_ref, vec, bias, mask, packed_hbm, hidden_ref, lse_ref, normed_hbm, qkv_hbm, mixed_hbm, *rest
):
    micro, half_rows, width = rows_ref.shape
    gathered, gather_refs = rest[0], rest[0:3]
    scatter_refs = rest[3:10]
    terms = rest[3]
    packed, wide, qkv, mixed, load_sem, keep_sems = rest[10:]
    seq = qkv.shape[1]
    pair = mixed.shape[2]
    heads = pair // LANES
    load = pltpu.make_async_copy(packed_hbm, packed, load_sem)
    load.start()
    slab = Slab(half_rows)
    gathers = make_gathers(slab, gather_refs, micro)
    scatters = make_scatters(slab, scatter_refs, micro)
    slab.greet()
    for m in range(micro):
        own = slab.rows(gathered.at[m], slab.mine[0])
        for start in range(0, half_rows, 32):
            block = rows_ref[m, pl.ds(start, 32)].astype(jnp.float32)
            own[pl.ds(start, 32)] = low(layer_norm(block, vec[0:1], vec[2:3]))
        gathers[m].start()
    load.wait()
    widen(packed, wide)
    keeps = []

    def keep(src, dst, i):
        copy = pltpu.make_async_copy(src, dst, keep_sems.at[i])
        copy.start()
        keeps.append(copy)

    def project(m):
        def block(i):
            rows = step_rows(i, TILE)
            out = dot(gathered[m, rows], wide[:, : 3 * pair], 1, 0)
            qkv[m, rows] = low(out + bias[...])

        repeat(seq // TILE, block)

    def attend(m, h):
        def block(i):
            rows = step_rows(i, LANES)
            q = qkv[m, rows, h * LANES : (h + 1) * LANES]
            k = qkv[m, :, pair + h * LANES : pair + (h + 1) * LANES]
            v = qkv[m, :, 2 * pair + h * LANES : 2 * pair + (h + 1) * LANES]
            scores = dot(q, k, 1, 1) * (score_scale * LOG2E) + mask[m : m + 1]
            top = jnp.max(scores, axis=-1, keepdims=True)
            exp_scores = jnp.exp2(scores - top)
            total = jnp.sum(exp_scores, axis=-1, keepdims=True)
            probs = low(exp_scores * (1.0 / total))
            mixed[m, rows, h * LANES : (h + 1) * LANES] = low(dot(probs, v, 1, 0))
            lse = jnp.broadcast_to(top + jnp.log(total) * LOG2E, (LANES, LANES)).T
            lse_ref[m, h : h + 1, rows] = lse[0:1]

        repeat(seq // LANES, block)

    def output(m):
        def block(i):
            rows = step_rows(i, TILE)
            terms[m, rows] = low(dot(mixed[m, rows], wide[:, 3 * pair :], 1, 1))

        repeat(seq // TILE, block)

    def close(m):
        scatters[m].finish()
        for rows in scatters[m].blocks():
            start = rows_ref[m, rows].astype(jnp.float32)
            hidden_ref[m, rows] = start + scatters[m].total(rows) + vec[5:6]

    gathers[0].forward()
    gathers[0].to_mate()
    gathers[1].forward()
    gathers[0].finish()
    keep(gathered.at[0], normed_hbm.at[0], 0)
    project(0)
    gathers[1].to_mate()
    attend(0, 0)
    gathers[1].finish()
    keep(gathered.at[1], normed_hbm.at[1], 1)
    for h in range(1, heads):
        attend(0, h)
    output(0)
    scatters[0].start()
    keep(qkv.at[0], qkv_hbm.at[0], 2)
    keep(mixed.at[0], mixed_hbm.at[0], 3)
    project(1)
    scatters[0].second_hop()
    for h in range(heads):
        attend(1, h)
        if h == 0:
            scatters[0].first_hop()
    output(1)
    scatters[1].start()
    keep(qkv.at[1], qkv_hbm.at[1], 4)
    keep(mixed.at[1], mixed_hbm.at[1], 5)
    close(0)
    scatters[1].second_hop()
    scatters[1].first_hop()
    close(1)
    for copy in keeps:
        copy.wait()


def ffn_forward_kernel(
    hidden_ref, vec, up_bias, packed_hbm, out_ref, second_hbm, upper_hbm, *rest
):
    micro, half_rows, width = hidden_ref.shape
    gathered, gather_refs = rest[0], rest[0:3]
    scatter_refs = rest[3:10]
    terms = rest[3]
    packed, upper, load_sem, keep_sems = rest[10:]
    seq, ff = upper.shape[1:]
    load = pltpu.make_async_copy(packed_hbm, packed, load_sem)
    load.start()
    slab = Slab(half_rows)
    gathers = make_gathers(slab, gather_refs, micro)
    scatters = make_scatters(slab, scatter_refs, micro)
    slab.greet()
    for m in range(micro):
        own = slab.rows(gathered.at[m], slab.mine[0])
        for start in range(0, half_rows, 32):
            block = hidden_ref[m, pl.ds(start, 32)]
            own[pl.ds(start, 32)] = low(layer_norm(block, vec[1:2], vec[6:7]))
        gathers[m].start()
    load.wait()
    keeps = []

    def keep(src, dst, i):
        copy = pltpu.make_async_copy(src, dst, keep_sems.at[i])
        copy.start()
        keeps.append(copy)

    def compute(m, i):
        rows = step_rows(i, TILE)
        value = dot(gathered[m, rows], packed[:, :ff], 1, 0) + up_bias[...]
        upper[m, rows] = value
        active = low(gelu_tanh(value))
        terms[m, rows] = low(dot(active, packed[:, ff:], 1, 1))

    def close(m):
        scatters[m].finish()
        for rows in scatters[m].blocks():
            out_ref[m, rows] = low(hidden_ref[m, rows] + scatters[m].total(rows) + vec[7:8])

    count = seq // TILE
    gathers[0].forward()
    gathers[0].to_mate()
    gathers[1].forward()
    gathers[0].finish()
    keep(gathered.at[0], second_hbm.at[0], 0)
    repeat(count, lambda i: compute(0, i))
    scatters[0].start()
    keep(upper.at[0], upper_hbm.at[0], 1)
    gathers[1].to_mate()
    gathers[1].finish()
    keep(gathered.at[1], second_hbm.at[1], 2)
    scatters[0].second_hop()
    repeat(count, lambda i: compute(1, i))
    scatters[1].start()
    keep(upper.at[1], upper_hbm.at[1], 3)
    scatters[0].first_hop()
    scatters[1].second_hop()
    close(0)
    scatters[1].first_hop()
    close(1)
    for copy in keeps:
        copy.wait()


def ffn_backward_kernel(
    grad_ref, hidden_ref, vec, second_hbm, upper_hbm, packed_hbm,
    out_ref, grads_ref, small_ref, up_bias_ref, *rest
):
    micro, half_rows, width = hidden_ref.shape
    gathered, gather_refs = rest[0], rest[0:3]
    scatter_refs = rest[3:10]
    terms = rest[3]
    packed, second, upper, grad_upper, active, sums, load_sems = rest[10:]
    seq, ff = upper.shape[1:]
    loads = [pltpu.make_async_copy(packed_hbm, packed, load_sems.at[0])]
    for m in range(micro):
        loads.append(pltpu.make_async_copy(upper_hbm.at[m], upper.at[m], load_sems.at[1 + 2 * m]))
        loads.append(pltpu.make_async_copy(second_hbm.at[m], second.at[m], load_sems.at[2 + 2 * m]))
    for load in loads:
        load.start()
    slab = Slab(half_rows)
    gathers = make_gathers(slab, gather_refs, micro)
    scatters = make_scatters(slab, scatter_refs, micro)
    slab.greet()
    for m in range(micro):
        own = slab.rows(gathered.at[m], slab.mine[0])
        for start in range(0, half_rows, 32):
            own[pl.ds(start, 32)] = grad_ref[m, pl.ds(start, 32)]
        gathers[m].start()
    small_ref[...] = jnp.zeros_like(small_ref)
    up_bias_ref[...] = jnp.zeros_like(up_bias_ref)
    for load in loads:
        load.wait()

    def compute(m, i):
        rows = step_rows(i, TILE)
        value = upper[m, rows]
        square = value * value
        bent = jnp.tanh(GELU_A * value * (1.0 + GELU_B * square))
        half = 0.5 * (1.0 + bent)
        active[m, rows] = low(value * half)
        slope = half + (0.5 * GELU_A) * value * (1.0 - bent * bent) * (1.0 + 3.0 * GELU_B * square)
        grad_active = dot(gathered[m, rows], packed[:, ff:], 1, 0)
        grad = low(grad_active * slope)
        grad_upper[m, rows] = grad
        up_bias_ref[0:1] += jnp.sum(grad.astype(jnp.float32), axis=0, keepdims=True)
        terms[m, rows] = low(dot(grad, packed[:, :ff], 1, 1))

    def weight_grads(m):
        def block(i):
            cols = step_rows(i, LANES)
            up = dot(second[m, :, cols], grad_upper[m], 0, 0)
            down = dot(gathered[m, :, cols], active[m], 0, 0)
            if m == 0:
                sums[cols, :ff] = up
                sums[cols, ff:] = down
            else:
                grads_ref[cols, :ff] = low(sums[cols, :ff] + up)
                grads_ref[cols, ff:] = low(sums[cols, ff:] + down)

        repeat(width // LANES, block)

    def close(m):
        scatters[m].finish()
        for rows in scatters[m].blocks():
            grad_normed = scatters[m].total(rows)
            back, gain_terms = norm_back(hidden_ref[m, rows], vec[1:2], grad_normed)
            grad_rows = grad_ref[m, rows].astype(jnp.float32)
            grad_hidden = grad_rows + back
            out_ref[m, rows] = grad_hidden
            branch = low(grad_hidden).astype(jnp.float32)
            for j, item in enumerate((gain_terms, grad_normed, grad_rows, branch)):
                small_ref[j : j + 1] += jnp.sum(item, axis=0, keepdims=True)

    count = seq // TILE
    gathers[0].forward()
    gathers[0].to_mate()
    gathers[1].forward()
    gathers[0].finish()
    repeat(count, lambda i: compute(0, i))
    scatters[0].start()
    gathers[1].to_mate()
    gathers[1].finish()
    scatters[0].second_hop()
    repeat(count, lambda i: compute(1, i))
    scatters[1].start()
    scatters[0].first_hop()
    weight_grads(0)
    scatters[1].second_hop()
    close(0)
    scatters[1].first_hop()
    weight_grads(1)
    close(1)


def attn_backward_kernel(
    grad_ref, rows_ref, vec, lse, mask, normed_hbm, qkv_hbm, mixed_hbm, packed_hbm,
    out_ref, grads_ref, small_ref, bias_ref, *rest
):
    micro, half_rows, width = grad_ref.shape
    gathered, gather_refs = rest[0], rest[0:3]
    scatter_refs = rest[3:10]
    terms = rest[3]
    packed, wide, normed, qkv, mixed, grad_mixed, grad_qkv, turned, sums, load_sems = rest[10:]
    seq, pair = mixed.shape[1:]
    heads = pair // LANES
    loads = [pltpu.make_async_copy(packed_hbm, packed, load_sems.at[0])]
    for m in range(micro):
        loads.append(pltpu.make_async_copy(qkv_hbm.at[m], qkv.at[m], load_sems.at[1 + 3 * m]))
        loads.append(pltpu.make_async_copy(mixed_hbm.at[m], mixed.at[m], load_sems.at[2 + 3 * m]))
        loads.append(pltpu.make_async_copy(normed_hbm.at[m], normed.at[m], load_sems.at[3 + 3 * m]))
    for load in loads:
        load.start()
    slab = Slab(half_rows)
    gathers = make_gathers(slab, gather_refs, micro)
    scatters = make_scatters(slab, scatter_refs, micro)
    slab.greet()
    for m in range(micro):
        own = slab.rows(gathered.at[m], slab.mine[0])
        for start in range(0, half_rows, 32):
            own[pl.ds(start, 32)] = low(grad_ref[m, pl.ds(start, 32)])
        gathers[m].start()
    small_ref[...] = jnp.zeros_like(small_ref)
    bias_ref[...] = jnp.zeros_like(bias_ref)
    for load in loads:
        load.wait()
    widen(packed, wide)

    def head(h, part=0):
        return slice(part * pair + h * LANES, part * pair + (h + 1) * LANES)

    for m in range(micro):
        for h in range(heads):
            turned[m, h] = low(qkv[m, :, head(h, 1)].astype(jnp.float32).T)

    def mix_grads(m):
        def block(i):
            rows = step_rows(i, TILE)
            grad_mixed[m, rows] = low(dot(gathered[m, rows], wide[:, 3 * pair :], 1, 0))

        repeat(seq // TILE, block)

    def attend(m, h):
        keys, values = qkv[m, :, head(h, 1)], qkv[m, :, head(h, 2)]
        shut = mask[m]

        def block(i, carry):
            grad_keys, grad_values = carry
            rows = step_rows(i, LANES)
            queries = qkv[m, rows, head(h)]
            grads = grad_mixed[m, rows, head(h)]
            scores = dot(keys, queries, 1, 1) * (score_scale * LOG2E) + shut
            probs = jnp.exp2(scores - lse[m, h : h + 1, rows])
            grad_probs = dot(values, grads, 1, 1)
            inner = jnp.sum(grad_probs * probs, axis=0, keepdims=True)
            grad_scores = low(probs * (grad_probs - inner))
            turn = dot(turned[m, h], grad_scores, 1, 0).T
            grad_qkv[m, rows, head(h)] = low(turn * score_scale)
            grad_values = grad_values + dot(low(probs), grads, 1, 0)
            grad_keys = grad_keys + dot(grad_scores, queries, 1, 0)
            return grad_keys, grad_values

        zero = jnp.zeros((seq, LANES), jnp.float32)
        grad_keys, grad_values = lax.fori_loop(0, seq // LANES, block, (zero, zero))
        grad_qkv[m, :, head(h, 1)] = low(grad_keys * score_scale)
        grad_qkv[m, :, head(h, 2)] = low(grad_values)

    def back_project(m):
        def block(i):
            rows = step_rows(i, TILE)
            grads = grad_qkv[m, rows]
            terms[m, rows] = low(dot(grads, wide[:, : 3 * pair], 1, 1))
            for j, part in enumerate((0, 2)):
                piece = grads[:, part * pair : (part + 1) * pair].astype(jnp.float32)
                bias_ref[j : j + 1] += jnp.sum(piece, axis=0, keepdims=True)

        repeat(seq // TILE, block)

    def weight_grads(m):
        def block(i):
            cols = step_rows(i, LANES)
            first = dot(normed[m, :, cols], grad_qkv[m], 0, 0)
            last = dot(gathered[m, :, cols], mixed[m], 0, 0)
            if m == 0:
                sums[cols, : 3 * pair] = first
                sums[cols, 3 * pair :] = last
            else:
                total = low(
                    jnp.concatenate(
                        [sums[cols, : 3 * pair] + first, sums[cols, 3 * pair :] + last], axis=1
                    )
                )
                pieces = [
                    total[:, h * LANES : h * LANES + HEAD] for h in range(4 * heads)
                ]
                grads_ref[cols] = jnp.concatenate(pieces, axis=1)

        repeat(width // LANES, block)

    def close(m):
        scatters[m].finish()
        for rows in scatters[m].blocks():
            grad_normed = scatters[m].total(rows)
            back, gain_terms = norm_back(
                rows_ref[m, rows].astype(jnp.float32), vec[0:1], grad_normed
            )
            out_ref[m, rows] = low(grad_ref[m, rows] + back)
            for j, item in enumerate((gain_terms, grad_normed)):
                small_ref[j : j + 1] += jnp.sum(item, axis=0, keepdims=True)

    gathers[0].forward()
    gathers[0].to_mate()
    gathers[1].forward()
    gathers[0].finish()
    mix_grads(0)
    attend(0, 0)
    gathers[1].to_mate()
    for h in range(1, heads):
        attend(0, h)
    gathers[1].finish()
    back_project(0)
    scatters[0].start()
    mix_grads(1)
    attend(1, 0)
    scatters[0].second_hop()
    for h in range(1, heads):
        attend(1, h)
        if h == 1:
            scatters[0].first_hop()
    back_project(1)
    scatters[1].start()
    weight_grads(0)
    scatters[1].second_hop()
    close(0)
    scatters[1].first_hop()
    weight_grads(1)
    close(1)


def any_spec():
    return pl.BlockSpec(memory_space=pl.ANY)


def vmem_spec():
    return pl.BlockSpec(memory_space=pltpu.VMEM)


def shape_of(shape, dtype):
    return jax.ShapeDtypeStruct(shape, dtype)


def params(collective):
    return pltpu.CompilerParams(
        collective_id=collective, has_side_effects=True, vmem_limit_bytes=VMEM_BYTES
    )


def attn_forward(rows_low, vec, bias_qv, packed, mask):
    micro, half_rows, width = rows_low.shape
    seq = mask.shape[1]
    pair = bias_qv.shape[1]
    heads = pair // LANES
    bias = jnp.concatenate([bias_qv[0], jnp.zeros((pair,), jnp.float32), bias_qv[1]])[None]
    low_type, high_type = jnp.bfloat16, jnp.float32
    hidden, lse, normed, qkv, mixed = pl.pallas_call(
        attn_forward_kernel,
        out_shape=[
            shape_of((micro, half_rows, width), high_type),
            shape_of((micro, heads, seq), high_type),
            shape_of((micro, seq, width), low_type),
            shape_of((micro, seq, 3 * pair), low_type),
            shape_of((micro, seq, pair), low_type),
        ],
        in_specs=[vmem_spec()] * 4 + [any_spec()],
        out_specs=[vmem_spec()] * 2 + [any_spec()] * 3,
        scratch_shapes=gather_scratch(micro, seq, width)
        + scatter_scratch(micro, seq, half_rows, width)
        + [
            pltpu.VMEM(packed.shape, low_type),
            pltpu.VMEM((width, 4 * pair), low_type),
            pltpu.VMEM((micro, seq, 3 * pair), low_type),
            pltpu.VMEM((micro, seq, pair), low_type),
            pltpu.SemaphoreType.DMA,
            pltpu.SemaphoreType.DMA((6,)),
        ],
        compiler_params=params(0),
        name="attn_forward",
    )(rows_low, vec, bias, mask, packed)
    return hidden, (normed, qkv, lse, mixed)


def ffn_forward(hidden, vec, up_bias, packed, seq):
    micro, half_rows, width = hidden.shape
    ff = up_bias.shape[0]
    low_type, high_type = jnp.bfloat16, jnp.float32
    out, second, upper = pl.pallas_call(
        ffn_forward_kernel,
        out_shape=[
            shape_of((micro, half_rows, width), low_type),
            shape_of((micro, seq, width), low_type),
            shape_of((micro, seq, ff), high_type),
        ],
        in_specs=[vmem_spec()] * 3 + [any_spec()],
        out_specs=[vmem_spec()] + [any_spec()] * 2,
        scratch_shapes=gather_scratch(micro, seq, width)
        + scatter_scratch(micro, seq, half_rows, width)
        + [
            pltpu.VMEM(packed.shape, low_type),
            pltpu.VMEM((micro, seq, ff), high_type),
            pltpu.SemaphoreType.DMA,
            pltpu.SemaphoreType.DMA((4,)),
        ],
        compiler_params=params(1),
        name="ffn_forward",
    )(hidden, vec, up_bias[None], packed)
    return out, (second, upper)


def ffn_backward(grad_low, hidden, kept, vec, packed):
    second, upper = kept
    micro, half_rows, width = hidden.shape
    seq, ff = upper.shape[1:]
    low_type, high_type = jnp.bfloat16, jnp.float32
    grad_hidden, grads, small, up_bias = pl.pallas_call(
        ffn_backward_kernel,
        out_shape=[
            shape_of((micro, half_rows, width), high_type),
            shape_of((width, 2 * ff), low_type),
            shape_of((8, width), high_type),
            shape_of((8, ff), high_type),
        ],
        in_specs=[vmem_spec()] * 3 + [any_spec()] * 3,
        out_specs=[vmem_spec()] * 4,
        scratch_shapes=gather_scratch(micro, seq, width)
        + scatter_scratch(micro, seq, half_rows, width)
        + [
            pltpu.VMEM(packed.shape, low_type),
            pltpu.VMEM((micro, seq, width), low_type),
            pltpu.VMEM((micro, seq, ff), high_type),
            pltpu.VMEM((micro, seq, ff), low_type),
            pltpu.VMEM((micro, seq, ff), low_type),
            pltpu.VMEM((width, 2 * ff), high_type),
            pltpu.SemaphoreType.DMA((1 + 2 * micro,)),
        ],
        compiler_params=params(2),
        name="ffn_backward",
    )(grad_low, hidden, vec, second, upper, packed)
    return grad_hidden, grads, small, up_bias[0]


def attn_backward(grad_hidden, rows_low, kept, vec, packed, mask):
    normed, qkv, lse, mixed = kept
    micro, half_rows, width = grad_hidden.shape
    seq, pair = mixed.shape[1:]
    heads = pair // LANES
    low_type, high_type = jnp.bfloat16, jnp.float32
    out, grads, small, bias = pl.pallas_call(
        attn_backward_kernel,
        out_shape=[
            shape_of((micro, half_rows, width), low_type),
            shape_of(packed.shape, low_type),
            shape_of((8, width), high_type),
            shape_of((8, pair), high_type),
        ],
        in_specs=[vmem_spec()] * 5 + [any_spec()] * 4,
        out_specs=[vmem_spec()] * 4,
        scratch_shapes=gather_scratch(micro, seq, width)
        + scatter_scratch(micro, seq, half_rows, width)
        + [
            pltpu.VMEM(packed.shape, low_type),
            pltpu.VMEM((width, 4 * pair), low_type),
            pltpu.VMEM((micro, seq, width), low_type),
            pltpu.VMEM((micro, seq, 3 * pair), low_type),
            pltpu.VMEM((micro, seq, pair), low_type),
            pltpu.VMEM((micro, seq, pair), low_type),
            pltpu.VMEM((micro, seq, 3 * pair), low_type),
            pltpu.VMEM((micro, heads, LANES, seq), low_type),
            pltpu.VMEM((width, 4 * pair), high_type),
            pltpu.SemaphoreType.DMA((1 + 3 * micro,)),
        ],
        compiler_params=params(3),
        name="attn_backward",
    )(grad_hidden, rows_low, vec, lse, mask, normed, qkv, mixed, packed)
    return out, grads, small, bias[:2]


def shards(
    section_input,
    final_cotangent,
    lengths,
    qkv_weight,
    out_weight,
    up_weight,
    down_weight,
    norm_gains,
    biases,
    up_bias,
):
    here = lax.axis_index("section")
    tensor = lax.axis_index("tensor")
    sections = lax.axis_size("section")
    micro, _, own_rows, width = section_input.shape
    head_cols = qkv_weight.shape[3]
    pair_cols = head_cols // sections
    heads = pair_cols // HEAD
    ff_cols = up_weight.shape[2]
    half_ff = ff_cols // sections
    ff_wide = round_up(half_ff, LANES)
    half_rows = round_up(-(-own_rows // sections), 32)
    full_rows = half_rows * sections
    seq = full_rows * lax.axis_size("tensor")

    def pick(two, index):
        return lax.dynamic_index_in_dim(two, index, 0, keepdims=False)

    def by_layer(mine, other):
        return [jnp.where(here == 0, mine, other), jnp.where(here == 0, other, mine)]

    def swap(value):
        return lax.ppermute(value, "section", SWAP)

    part_rows = qkv_weight.shape[2]
    heads_first = jnp.concatenate([jnp.moveaxis(qkv_weight[0], 1, 0), out_weight[0].T[:, None]], 1)
    halves = heads_first.reshape(part_rows, 4, sections, pair_cols)
    attn_parts = jnp.moveaxis(halves, 2, 0).reshape(sections, part_rows, 4 * pair_cols)
    ff_parts = jnp.stack([up_weight[0], down_weight[0].T], 1)
    ff_parts = ff_parts.reshape(part_rows, 2, sections, half_ff)
    ff_parts = jnp.pad(ff_parts, [(0, 0)] * 3 + [(0, ff_wide - half_ff)])
    ff_parts = jnp.moveaxis(ff_parts, 2, 0).reshape(sections, part_rows, 2 * ff_wide)
    attn_layers = by_layer(pick(attn_parts, here), swap(pick(attn_parts, 1 - here)))
    ff_layers = by_layer(pick(ff_parts, here), swap(pick(ff_parts, 1 - here)))
    attn_packed, ff_packed = [], []
    for layer in range(2):
        attn_packed.append(lax.all_gather(attn_layers[layer], "dp", axis=0, tiled=True))
        ff_packed.append(lax.all_gather(ff_layers[layer], "dp", axis=0, tiled=True))

    small = jnp.concatenate([norm_gains[0], biases[0]], 0)
    vectors = lax.all_gather(small, EVERY, axis=0, tiled=False)
    vectors = vectors.reshape((sections, -1) + small.shape)
    vectors = jnp.moveaxis(vectors, 1, 2).reshape(sections, small.shape[0], width)
    up_biases = lax.all_gather(up_bias[0], "section", axis=0, tiled=False)
    up_biases = lax.dynamic_slice_in_dim(up_biases, here * half_ff, half_ff, 1)
    up_biases = jnp.pad(up_biases, [(0, 0), (0, ff_wide - half_ff)])
    head_start = tensor * head_cols + here * pair_cols
    bias_qv = lax.dynamic_slice_in_dim(vectors[:, 3:5], head_start, pair_cols, 2)
    bias_qv = pad_heads(bias_qv, heads)

    place = jnp.arange(seq, dtype=jnp.int32)
    within = place % full_rows
    token = (place // full_rows) * own_rows + within
    live = (within < own_rows)[None] & (token[None] < lengths)
    mask = jnp.where(live, 0.0, masked_score).astype(jnp.float32)
    mask_columns = jnp.broadcast_to(mask[:, :, None], (micro, seq, LANES))

    def my_rows(value):
        padded = jnp.pad(value[:, 0], [(0, 0), (0, full_rows - own_rows), (0, 0)])
        return lax.dynamic_slice_in_dim(padded, here * half_rows, half_rows, 1)

    def whole_rows(first, second):
        mine, other = jnp.where(here == 0, first, second), jnp.where(here == 0, second, first)
        got = swap(other)
        low_half, high_half = by_layer(mine, got)
        return jnp.concatenate([low_half, high_half], 1)[:, None, :own_rows]

    rows = my_rows(section_input)
    inputs, hiddens, attn_kept, ff_kept, outputs = [], [], [], [], []
    for layer in range(2):
        inputs.append(rows)
        hidden, kept = attn_forward(
            rows, vectors[layer], bias_qv[layer], attn_packed[layer], mask
        )
        hiddens.append(hidden)
        attn_kept.append(kept)
        rows, kept = ffn_forward(
            hidden, vectors[layer], up_biases[layer], ff_packed[layer], seq
        )
        ff_kept.append(kept)
        outputs.append(rows)
    section_output = whole_rows(outputs[0], outputs[1])

    grads = my_rows(final_cotangent)
    zero_row = jnp.zeros((width,), jnp.float32)
    attn_sums, ff_sums, small_sums, up_sums, input_grads = {}, {}, {}, {}, {}
    for layer in (1, 0):
        grad_hidden, ff_grad, small_two, up_sums[layer] = ffn_backward(
            grads, hiddens[layer], ff_kept[layer], vectors[layer], ff_packed[layer]
        )
        ff_sums[layer] = lax.psum_scatter(ff_grad, "dp", scatter_dimension=0, tiled=True)
        grads, attn_grad, small_one, bias_grad = attn_backward(
            grad_hidden,
            inputs[layer],
            attn_kept[layer],
            vectors[layer],
            attn_packed[layer],
            mask_columns,
        )
        attn_sums[layer] = lax.psum_scatter(attn_grad, "dp", scatter_dimension=0, tiled=True)
        input_grads[layer] = grads
        bias_grad = drop_heads(bias_grad)
        bias_rows = [
            lax.dynamic_update_slice_in_dim(zero_row, bias_grad[i], head_start, 0) for i in (0, 1)
        ]
        small_sums[layer] = jnp.stack(
            [
                small_one[0],
                small_two[0],
                small_one[1],
                bias_rows[0],
                bias_rows[1],
                small_two[3],
                small_two[1],
                small_two[2],
            ]
        )
    input_grad = whole_rows(input_grads[0], input_grads[1])

    def own_layer(sums):
        mine, other = by_layer(sums[0], sums[1])
        return jnp.stack(by_layer(mine, swap(other)), 1)

    attn_total = own_layer(attn_sums).astype(jnp.float32)
    attn_total = attn_total.reshape(part_rows, sections, 4, pair_cols)
    attn_total = jnp.moveaxis(attn_total, 2, 0).reshape(4, part_rows, head_cols)
    ff_total = own_layer(ff_sums).astype(jnp.float32)
    ff_total = ff_total.reshape(part_rows, sections, 2, ff_wide)[..., :half_ff]
    ff_total = jnp.moveaxis(ff_total, 2, 0).reshape(2, part_rows, ff_cols)

    small_all = jnp.stack([small_sums[0], small_sums[1]])
    small_all = small_all.reshape(small_all.shape[:2] + (-1, small.shape[1]))
    small_all = jnp.moveaxis(small_all, 2, 1).reshape((-1,) + small.shape)
    small_mine = lax.psum_scatter(small_all, EVERY, scatter_dimension=0, tiled=True)
    up_all = lax.psum(jnp.stack([up_sums[0], up_sums[1]])[:, :half_ff], "dp")
    up_mine, up_other = by_layer(up_all[0], up_all[1])
    up_total = jnp.stack(by_layer(up_mine, swap(up_other))).reshape(1, ff_cols)
    gains = norm_gains.shape[1]
    return (
        section_output[None],
        input_grad[None],
        attn_total[None, :3],
        attn_total[3].T[None],
        ff_total[0][None],
        ff_total[1].T[None],
        small_mine[:, :gains],
        small_mine[:, gains:],
        up_total,
    )


def solution(mesh):
    in_specs = (
        P(None, "dp", "tensor", None),
        P(None, "dp", "tensor", None),
        P(None, "dp"),
        P("section", None, "dp", "tensor"),
        P("section", "tensor", "dp"),
        P("section", "dp", "tensor"),
        P("section", "tensor", "dp"),
        P("section", None, ("dp", "tensor")),
        P("section", None, ("dp", "tensor")),
        P("section", "tensor"),
    )
    out_specs = (
        P("section", None, "dp", "tensor", None),
        P("section", None, "dp", "tensor", None),
        P("section", None, "dp", "tensor"),
        P("section", "tensor", "dp"),
        P("section", "dp", "tensor"),
        P("section", "tensor", "dp"),
        P("section", None, ("dp", "tensor")),
        P("section", None, ("dp", "tensor")),
        P("section", "tensor"),
    )
    return jax.shard_map(shards, mesh=mesh, in_specs=in_specs, out_specs=out_specs, check_vma=False)
```

```python
import functools
import math

import jax
import jax.numpy as jnp
from jax import lax
from jax.experimental import pallas as pl
from jax.experimental.pallas import tpu as pltpu
from jax.sharding import PartitionSpec as P


HEAD = 72
LANES = 128
norm_eps = 1e-06
masked_score = -1000000000.0
score_scale = 1.0 / math.sqrt(HEAD)
GELU_A = math.sqrt(2.0 / math.pi)
GELU_B = 0.044715


def round_up(value, step):
    return -(-value // step) * step


def dot(left, right, left_dim, right_dim):
    return lax.dot_general(
        left, right, (((left_dim,), (right_dim,)), ((), ())), preferred_element_type=jnp.float32
    )


def low(value):
    return value.astype(jnp.bfloat16)


def layer_norm(rows, gain_vec, shift_vec):
    centred = rows - jnp.mean(rows, axis=-1, keepdims=True)
    spread = jnp.mean(centred * centred, axis=-1, keepdims=True)
    return centred * lax.rsqrt(spread + norm_eps) * gain_vec + shift_vec


def norm_back(rows, gain_vec, grads):
    centred = rows - jnp.mean(rows, axis=-1, keepdims=True)
    spread = jnp.mean(centred * centred, axis=-1, keepdims=True)
    inverse = lax.rsqrt(spread + norm_eps)
    xhat = centred * inverse
    e = grads * gain_vec
    back = inverse * (
        e
        - jnp.mean(e, axis=-1, keepdims=True)
        - xhat * jnp.mean(e * xhat, axis=-1, keepdims=True)
    )
    return back, grads * xhat


def gelu_tanh(value):
    return jax.nn.gelu(value, approximate=True)


MESH = pl.DeviceIdType.MESH
VMEM_BYTES = 64_000_000
COST = pl.CostEstimate(flops=20_000_000_000, transcendentals=0, bytes_accessed=100_000_000)
LOG2E = 1.0 / math.log(2.0)
TILE = 256


class Slab:
    def __init__(self, half_rows):
        self.half_rows = half_rows
        section = lax.axis_index("section")
        tensor = lax.axis_index("tensor")
        core = lax.rem(tensor, 2)
        self.core = core
        self.mine = self.around(section, tensor, core)
        self.theirs = self.around(section, tensor + 1 - 2 * core, 1 - core)
        self.mate = self.theirs[0]
        over = lax.rem(tensor + 2, 4)
        self.near, self.far = tensor, over
        self.mate_near, self.mate_far = self.mate[1], lax.rem(self.mate[1] + 2, 4)
        self.grid = self.places(section, self.near, self.far)
        self.mate_grid = self.places(section, self.mate_near, self.mate_far)
        self.across_y = self.grid[2]
        self.first, self.second = self.mine[1], self.mine[2]

    @staticmethod
    def places(section, near, far):
        flip = 1 - section
        return [(section, near), (flip, near), (section, far), (flip, far)]

    @staticmethod
    def around(section, tensor, core):
        over = lax.rem(tensor + 2, 4)
        turn = 1 - 2 * section
        first = (section + (1 - core) * turn, tensor + core * (over - tensor))
        second = (section + core * turn, tensor + (1 - core) * (over - tensor))
        return [(section, tensor), first, second, (1 - section, over)]

    def rows(self, ref, at):
        start = pl.multiple_of((2 * at[1] + at[0]) * self.half_rows, self.half_rows)
        return ref.at[pl.ds(start, self.half_rows)]

    def tile(self, tensor):
        size = 2 * self.half_rows
        return pl.ds(pl.multiple_of(tensor * size, size), size)

    def chip_tiles(self, far):
        return (self.mate_far, self.far) if far else (self.mate_near, self.near)

    def greet(self):
        barrier = pltpu.get_barrier_semaphore()
        for peer in (self.first, self.second, self.mate):
            pl.semaphore_signal(barrier, inc=1, device_id=named(peer), device_id_type=MESH)
        pl.semaphore_wait(barrier, 3)


def named(at):
    return {"section": at[0], "tensor": at[1]}


class Moves:
    def __init__(self, slab, send_sems, recv_sems):
        self.slab, self.send_sems, self.recv_sems = slab, send_sems, recv_sems
        self.sent = []

    def copy(self, src, dst, role, peer):
        return pltpu.make_async_remote_copy(
            src_ref=src,
            dst_ref=dst,
            send_sem=self.send_sems.at[role],
            recv_sem=self.recv_sems.at[role],
            device_id=named(peer),
            device_id_type=MESH,
        )

    def send(self, src, dst, role, peer):
        copy = self.copy(src, dst, role, peer)
        copy.start()
        self.sent.append(copy)

    def arrived(self, dst, role):
        self.copy(dst, dst, role, self.slab.mate).wait_recv()

    def drain(self):
        for copy in self.sent:
            copy.wait_send()


class Gather(Moves):
    def __init__(self, slab, whole, send_sems, recv_sems):
        super().__init__(slab, send_sems, recv_sems)
        self.whole = whole

    def pass_on(self, at, role, peer):
        part = self.slab.rows(self.whole, at)
        self.send(part, part, role, peer)

    def arrive(self, at, role):
        self.arrived(self.slab.rows(self.whole, at), role)

    def start(self):
        mine = self.slab.mine
        self.pass_on(mine[0], 0, mine[1])
        self.pass_on(mine[0], 3, self.slab.mate)

    def second(self):
        self.sent.pop(0).wait_send()
        self.pass_on(self.slab.mine[0], 1, self.slab.mine[2])

    def forward(self):
        mine, mate = self.slab.mine, self.slab.mate
        self.arrive(mine[1], 0)
        self.pass_on(mine[1], 2, mine[2])
        self.pass_on(mine[1], 4, mate)

    def to_mate(self):
        mine, mate = self.slab.mine, self.slab.mate
        self.arrive(mine[2], 1)
        self.pass_on(mine[2], 5, mate)
        self.arrive(mine[3], 2)
        self.pass_on(mine[3], 6, mate)

    def finish(self):
        for k in range(4):
            self.arrive(self.slab.theirs[k], 3 + k)
        self.drain()


class TileGather:
    def __init__(self, whole, send_sems, recv_sems):
        self.whole, self.send_sems, self.recv_sems = whole, send_sems, recv_sems
        self.tensor = lax.axis_index("tensor")
        self.over = lax.rem(self.tensor + 2, 4)
        self.mate = self.tensor + 1 - 2 * lax.rem(self.tensor, 2)
        self.micro, rows = whole.shape[0], whole.shape[1] // 4
        self.tile_rows = rows
        self.sent = []

    def tile(self, m, index):
        start = pl.multiple_of(index * self.tile_rows, self.tile_rows)
        return self.whole.at[m, pl.ds(start, self.tile_rows)]

    def copy(self, m, index, role, peer):
        part = self.tile(m, index)
        return remote(
            part, part, self.send_sems.at[m, role], self.recv_sems.at[m, role], {"tensor": peer}
        )

    def send(self, m, index, role, peer):
        copy = self.copy(m, index, role, peer)
        copy.start()
        self.sent.append(copy)

    def start(self):
        for m in range(self.micro):
            self.send(m, self.tensor, 0, self.over)
            self.send(m, self.tensor, 1, self.mate)

    def pass_on(self):
        for m in range(self.micro):
            self.copy(m, self.over, 0, self.over).wait_recv()
            self.send(m, self.over, 2, self.mate)

    def finish(self):
        for m in range(self.micro):
            self.copy(m, self.mate, 1, self.mate).wait_recv()
            self.copy(m, lax.rem(self.mate + 2, 4), 2, self.mate).wait_recv()

    def drain(self):
        for copy in self.sent:
            copy.wait_send()


class Scatter(Moves):
    def __init__(self, slab, terms, from_mate, outgoing, arrivals, send_sems, recv_sems):
        super().__init__(slab, send_sems, recv_sems)
        self.terms, self.from_mate, self.outgoing = terms, from_mate, outgoing
        self.relay, self.from_second, self.from_first = (arrivals.at[k] for k in range(3))

    def to_mate(self, at, role):
        self.send(self.slab.rows(self.terms, at), self.from_mate.at[role], role, self.slab.mate)

    def mate_far(self):
        self.to_mate(self.slab.mate_grid[3], 3)
        self.to_mate(self.slab.mate_grid[2], 1 + self.slab.core)

    def mate_near(self):
        self.to_mate(self.slab.mate_grid[1], 2 - self.slab.core)
        self.to_mate(self.slab.mate_grid[0], 0)

    def chip_sum(self, k, rows):
        part = self.slab.rows(self.terms, self.slab.mine[k])
        return part[rows].astype(jnp.float32) + self.from_mate[k, rows].astype(jnp.float32)

    def blocks(self):
        return [pl.ds(start, 32) for start in range(0, self.slab.half_rows, 32)]

    def hop(self, k, slot, dst, role, peer, ride=None):
        self.arrived(self.from_mate.at[k], k)
        if ride is not None:
            self.arrived(ride, 4)
        for rows in self.blocks():
            value = self.chip_sum(k, rows)
            if ride is not None:
                value = value + ride[rows].astype(jnp.float32)
            self.outgoing[slot, rows] = low(value)
        self.send(self.outgoing.at[slot], dst, role, peer)

    def far_hop(self):
        self.hop(3, 0, self.relay, 4, self.slab.second)

    def second_hop(self):
        self.hop(2, 1, self.from_second, 5, self.slab.second)

    def first_hop(self):
        self.hop(1, 2, self.from_first, 6, self.slab.first, self.relay)

    def finish(self):
        self.arrived(self.from_mate.at[0], 0)
        self.arrived(self.from_second, 5)
        self.arrived(self.from_first, 6)
        self.drain()

    def total(self, rows):
        other = self.from_second[rows].astype(jnp.float32) + self.from_first[rows].astype(
            jnp.float32
        )
        return self.chip_sum(0, rows) + other


def scatter_scratch(micro, seq, half_rows, width):
    return [
        pltpu.VMEM((micro, seq, width), jnp.bfloat16),
        pltpu.VMEM((micro, 4, half_rows, width), jnp.bfloat16),
        pltpu.VMEM((micro, 3, half_rows, width), jnp.bfloat16),
        pltpu.VMEM((micro, 3, half_rows, width), jnp.bfloat16),
        pltpu.SemaphoreType.DMA((micro, 7)),
        pltpu.SemaphoreType.DMA((micro, 7)),
    ]


def gather_scratch(micro, seq, width):
    return [
        pltpu.VMEM((micro, seq, width), jnp.bfloat16),
        pltpu.SemaphoreType.DMA((micro, 7)),
        pltpu.SemaphoreType.DMA((micro, 7)),
    ]


def make_scatters(slab, refs, micro):
    terms, from_mate, outgoing, arrivals, send_sems, recv_sems = refs
    return [
        Scatter(
            slab,
            terms.at[m],
            from_mate.at[m],
            outgoing.at[m],
            arrivals.at[m],
            send_sems.at[m],
            recv_sems.at[m],
        )
        for m in range(micro)
    ]


def make_gathers(slab, refs, micro):
    whole, send_sems, recv_sems = refs
    return [
        Gather(slab, whole.at[m], send_sems.at[m], recv_sems.at[m]) for m in range(micro)
    ]


def step_rows(i, size):
    return pl.ds(pl.multiple_of(i * size, size), size)


def repeat(count, body):
    def one(i, carry):
        body(i)
        return carry

    lax.fori_loop(0, count, one, 0)


def shut_keys(length, own_rows, full_rows, shape, dimension):
    place = lax.broadcasted_iota(jnp.int32, shape, dimension)
    step = jnp.zeros(shape, jnp.int32)
    for t in range(1, 4):
        step += (place >= t * full_rows).astype(jnp.int32)
    live = (place - step * full_rows < own_rows) & (
        place - step * (full_rows - own_rows) < length
    )
    return jnp.where(live, 0.0, masked_score)


def chip_rows(slab, far, compute):
    first, last = slab.chip_tiles(far)
    repeat(2, lambda i: compute(slab.tile(first + i * (last - first))))


def open_gathers(gathers, fill):
    fill(0)
    gathers[0].start()
    fill(1)
    gathers[0].second()
    gathers[1].start()
    gathers[0].forward()
    gathers[1].second()


def widen(packed, wide):
    heads = packed.shape[1] // HEAD

    def block(i):
        rows = step_rows(i, 128)
        for h in range(heads):
            piece = packed[rows, h * HEAD : (h + 1) * HEAD]
            blank = jnp.zeros((128, LANES - HEAD), jnp.bfloat16)
            wide[rows, h * LANES : (h + 1) * LANES] = jnp.concatenate([piece, blank], axis=1)

    repeat(packed.shape[0] // 128, block)


def split_tail(packed, tails, up_cols):
    start = packed.shape[1] - LANES

    def block(i):
        rows = step_rows(i, 128)
        for j in range(2):
            piece = packed[rows, start + j * up_cols : start + (j + 1) * up_cols]
            blank = jnp.zeros((128, LANES - up_cols), jnp.bfloat16)
            tails[rows, j * LANES : (j + 1) * LANES] = jnp.concatenate([piece, blank], axis=1)

    repeat(packed.shape[0] // 128, block)


def up_dot(rows, packed, tails):
    main = (packed.shape[1] - LANES) // 2
    first = dot(rows, packed[:, :main], 1, 0)
    return jnp.concatenate([first, dot(rows, tails[:, :LANES], 1, 0)], axis=1)


def up_back(grads, packed, tails):
    main = (packed.shape[1] - LANES) // 2
    return dot(grads[:, :main], packed[:, :main], 1, 1) + dot(
        grads[:, main:], tails[:, :LANES], 1, 1
    )


def down_dot(active, packed, tails):
    main = (packed.shape[1] - LANES) // 2
    return dot(active[:, :main], packed[:, main : 2 * main], 1, 1) + dot(
        active[:, main:], tails[:, LANES:], 1, 1
    )


def down_back(rows, packed, tails):
    main = (packed.shape[1] - LANES) // 2
    first = dot(rows, packed[:, main : 2 * main], 1, 0)
    return jnp.concatenate([first, dot(rows, tails[:, LANES:], 1, 0)], axis=1)


def attn_forward_kernel(
    ready, at, layer, own_rows, rows_ref, vectors, bias_ref, lengths, packed_hbm, given_hbm, grads_ref,
    hidden_ref, lse_ref, normed_hbm, qkv_hbm, mixed_hbm, *rest
):
    micro, half_rows, width = rows_ref.shape
    gathered, gather_refs = rest[0], rest[0:3]
    scatter_refs = rest[3:9]
    terms = rest[3]
    packed, wide, qkv, mixed, load_sem, keep_sems, given_sems, all_grads, tile_send, tile_recv = rest[9:]
    vec, bias = vectors.at[layer], bias_ref[layer]
    seq = qkv.shape[1]
    pair = mixed.shape[2]
    heads = pair // LANES
    load = pltpu.make_async_copy(
        packed_hbm.at[:, at : at + packed.shape[1]], packed, load_sem
    )
    load.start()
    slab = Slab(half_rows)
    gathers = make_gathers(slab, gather_refs, micro)
    scatters = make_scatters(slab, scatter_refs, micro)
    given = [
        pltpu.make_async_copy(given_hbm.at[m], gathered.at[m], given_sems.at[m])
        for m in range(micro if ready else 0)
    ]
    for copy in given:
        copy.start()
    slab.greet()
    if ready:
        tiles = TileGather(all_grads, tile_send, tile_recv)
        for m in range(micro):
            own = tiles.tile(m, tiles.tensor)
            count = grads_ref.shape[1]
            own[:count] = grads_ref[m]
            own[count:] = jnp.zeros((tiles.tile_rows - count, width), jnp.bfloat16)
        tiles.start()

    def fill(m):
        own = slab.rows(gathered.at[m], slab.mine[0])
        for start in range(0, half_rows, 32):
            block = rows_ref[m, pl.ds(start, 32)].astype(jnp.float32)
            own[pl.ds(start, 32)] = low(layer_norm(block, vec[0:1], vec[2:3]))

    if not ready:
        open_gathers(gathers, fill)
    load.wait()
    widen(packed, wide)
    keeps = []

    def keep(src, dst, i):
        copy = pltpu.make_async_copy(src, dst, keep_sems.at[i])
        copy.start()
        keeps.append(copy)

    def project(m):
        def block(i):
            rows = step_rows(i, TILE)
            out = dot(gathered[m, rows], wide[:, : 3 * pair], 1, 0)
            qkv[m, rows] = low(out + bias)

        repeat(seq // TILE, block)

    def attend(m, rows):
        shut = shut_keys(lengths[m], own_rows, 2 * half_rows, (1, seq), 1)
        for h in range(heads):
            cols = slice(h * LANES, (h + 1) * LANES)
            q = qkv[m, rows, cols]
            k = qkv[m, :, pair + h * LANES : pair + (h + 1) * LANES]
            v = qkv[m, :, 2 * pair + h * LANES : 2 * pair + (h + 1) * LANES]
            scores = dot(q, k, 1, 1) * (score_scale * LOG2E) + shut
            top = jnp.max(scores, axis=-1, keepdims=True)
            exp_scores = jnp.exp2(scores - top)
            total = jnp.sum(exp_scores, axis=-1, keepdims=True)
            probs = low(exp_scores * (1.0 / total))
            mixed[m, rows, cols] = low(dot(probs, v, 1, 0))
            lse_ref[m, h, rows] = jnp.broadcast_to(
                top + jnp.log(total) * LOG2E, (2 * half_rows, LANES)
            )
        terms[m, rows] = low(dot(mixed[m, rows], wide[:, 3 * pair :], 1, 1))

    def close(m):
        scatters[m].finish()
        for rows in scatters[m].blocks():
            start = rows_ref[m, rows].astype(jnp.float32)
            hidden_ref[m, rows] = start + scatters[m].total(rows) + vec[5:6]

    def gathered_rows(m):
        if ready:
            given[m].wait()
            return
        gathers[m].to_mate()
        gathers[m].finish()
        keep(gathered.at[m], normed_hbm.at[m], m)

    gathered_rows(0)
    project(0)
    if not ready:
        gathers[1].forward()
    chip_rows(slab, True, lambda rows: attend(0, rows))
    scatters[0].mate_far()
    gathered_rows(1)
    scatters[0].far_hop()
    chip_rows(slab, False, lambda rows: attend(0, rows))
    scatters[0].mate_near()
    keep(qkv.at[0], qkv_hbm.at[0], 2)
    keep(mixed.at[0], mixed_hbm.at[0], 3)
    project(1)
    scatters[0].second_hop()
    scatters[0].first_hop()
    if ready:
        tiles.pass_on()
    chip_rows(slab, True, lambda rows: attend(1, rows))
    scatters[1].mate_far()
    close(0)
    scatters[1].far_hop()
    if ready:
        tiles.finish()
        for m in range(micro):
            keep(all_grads.at[m], normed_hbm.at[m], m)
    chip_rows(slab, False, lambda rows: attend(1, rows))
    scatters[1].mate_near()
    keep(qkv.at[1], qkv_hbm.at[1], 4)
    keep(mixed.at[1], mixed_hbm.at[1], 5)
    scatters[1].second_hop()
    scatters[1].first_hop()
    close(1)
    if ready:
        tiles.drain()
    for copy in keeps:
        copy.wait()


def ffn_forward_kernel(
    half_ff, at, layer, hidden_ref, vectors, up_biases, packed_hbm, out_ref, second_hbm, upper_hbm, *rest
):
    micro, half_rows, _ = hidden_ref.shape
    gathered, gather_refs = rest[0], rest[0:3]
    scatter_refs = rest[3:9]
    terms = rest[3]
    packed, tails, upper, load_sem, keep_sems = rest[9:]
    vec, up_bias = vectors.at[layer], up_biases.at[layer]
    _, ff = upper.shape[1:]
    load = pltpu.make_async_copy(
        packed_hbm.at[:, at : at + packed.shape[1]], packed, load_sem
    )
    load.start()
    slab = Slab(half_rows)
    gathers = make_gathers(slab, gather_refs, micro)
    scatters = make_scatters(slab, scatter_refs, micro)
    slab.greet()

    def fill(m):
        own = slab.rows(gathered.at[m], slab.mine[0])
        for start in range(0, half_rows, 32):
            block = hidden_ref[m, pl.ds(start, 32)]
            own[pl.ds(start, 32)] = low(layer_norm(block, vec[1:2], vec[6:7]))

    open_gathers(gathers, fill)
    load.wait()
    split_tail(packed, tails, half_ff - ff + LANES)
    keeps = []

    def keep(src, dst, i):
        copy = pltpu.make_async_copy(src, dst, keep_sems.at[i])
        copy.start()
        keeps.append(copy)

    def compute(m, rows):
        value = up_dot(gathered[m, rows], packed, tails) + up_bias[...]
        upper[m, rows] = value
        active = low(gelu_tanh(value))
        terms[m, rows] = low(down_dot(active, packed, tails))

    def close(m):
        scatters[m].finish()
        for rows in scatters[m].blocks():
            out_ref[m, rows] = low(hidden_ref[m, rows] + scatters[m].total(rows) + vec[7:8])

    gathers[0].to_mate()
    gathers[0].finish()
    keep(gathered.at[0], second_hbm.at[0], 0)
    chip_rows(slab, True, lambda rows: compute(0, rows))
    scatters[0].mate_far()
    gathers[1].forward()
    scatters[0].far_hop()
    chip_rows(slab, False, lambda rows: compute(0, rows))
    scatters[0].mate_near()
    keep(upper.at[0], upper_hbm.at[0], 1)
    gathers[1].to_mate()
    scatters[0].second_hop()
    gathers[1].finish()
    keep(gathered.at[1], second_hbm.at[1], 2)
    chip_rows(slab, True, lambda rows: compute(1, rows))
    scatters[1].mate_far()
    scatters[0].first_hop()
    scatters[1].far_hop()
    chip_rows(slab, False, lambda rows: compute(1, rows))
    scatters[1].mate_near()
    keep(upper.at[1], upper_hbm.at[1], 3)
    scatters[1].second_hop()
    close(0)
    scatters[1].first_hop()
    close(1)
    for copy in keeps:
        copy.wait()


def ffn_backward_kernel(
    half_ff, at, layer, grad_ref, hidden_ref, vectors, second_hbm, upper_hbm, packed_hbm,
    out_ref, grads_ref, small_ref, up_bias_ref, *rest
):
    micro, half_rows, width = hidden_ref.shape
    gathered, gather_refs = rest[0], rest[0:3]
    scatter_refs = rest[3:9]
    terms = rest[3]
    packed, tails, second, upper, grad_upper, active, load_sems = rest[9:]
    vec = vectors.at[layer]
    seq, ff = upper.shape[1:]
    main = ff - LANES
    extra = half_ff - main
    load_packed = pltpu.make_async_copy(
        packed_hbm.at[:, at : at + packed.shape[1]], packed, load_sems.at[0]
    )
    load_packed.start()
    load_upper, load_second = [], []
    for m in range(micro):
        load_upper.append(
            pltpu.make_async_copy(upper_hbm.at[m], upper.at[m], load_sems.at[1 + m])
        )
        load_upper[m].start()
    for m in range(micro):
        load_second.append(
            pltpu.make_async_copy(second_hbm.at[m], second.at[m], load_sems.at[1 + micro + m])
        )
        load_second[m].start()
    slab = Slab(half_rows)
    gathers = make_gathers(slab, gather_refs, micro)
    scatters = make_scatters(slab, scatter_refs, micro)
    slab.greet()

    def fill(m):
        own = slab.rows(gathered.at[m], slab.mine[0])
        for start in range(0, half_rows, 32):
            own[pl.ds(start, 32)] = grad_ref[m, pl.ds(start, 32)]

    open_gathers(gathers, fill)
    small_ref[...] = jnp.zeros_like(small_ref)
    up_bias_ref[...] = jnp.zeros_like(up_bias_ref)
    load_packed.wait()
    split_tail(packed, tails, extra)

    def compute(m, rows):
        value = upper[m, rows]
        square = value * value
        bent = jnp.tanh(GELU_A * value * (1.0 + GELU_B * square))
        half = 0.5 * (1.0 + bent)
        active[m, rows] = low(value * half)
        slope = half + (0.5 * GELU_A) * value * (1.0 - bent * bent) * (1.0 + 3.0 * GELU_B * square)
        grad_active = down_back(gathered[m, rows], packed, tails)
        grad = low(grad_active * slope)
        grad_upper[m, rows] = grad
        up_bias_ref[0:1] += jnp.sum(grad.astype(jnp.float32), axis=0, keepdims=True)
        terms[m, rows] = low(up_back(grad, packed, tails))

    def stacked(ref, cols=slice(None)):
        return ref[:, :, cols].reshape(micro * seq, -1)

    def weight_grads(first, last):
        def block(i):
            cols = step_rows(i, LANES)
            up = dot(stacked(second, cols), stacked(grad_upper), 0, 0)
            down = dot(stacked(gathered, cols), stacked(active), 0, 0)
            grads_ref[cols, :main] = low(up[:, :main])
            grads_ref[cols, main : 2 * main] = low(down[:, :main])
            blank = jnp.zeros((LANES, LANES - 2 * extra), jnp.float32)
            rest_cols = [up[:, main : main + extra], down[:, main : main + extra], blank]
            grads_ref[cols, 2 * main :] = low(jnp.concatenate(rest_cols, axis=1))

        repeat(last - first, lambda i: block(first + i))

    def close(m):
        scatters[m].finish()
        for rows in scatters[m].blocks():
            grad_normed = scatters[m].total(rows)
            back, gain_terms = norm_back(hidden_ref[m, rows], vec[1:2], grad_normed)
            grad_rows = grad_ref[m, rows].astype(jnp.float32)
            grad_hidden = grad_rows + back
            out_ref[m, rows] = grad_hidden
            branch = low(grad_hidden).astype(jnp.float32)
            for j, item in enumerate((gain_terms, grad_normed, grad_rows, branch)):
                small_ref[j : j + 1] += jnp.sum(item, axis=0, keepdims=True)

    gathers[0].to_mate()
    gathers[0].finish()
    load_upper[0].wait()
    chip_rows(slab, True, lambda rows: compute(0, rows))
    scatters[0].mate_far()
    gathers[1].forward()
    scatters[0].far_hop()
    chip_rows(slab, False, lambda rows: compute(0, rows))
    scatters[0].mate_near()
    gathers[1].to_mate()
    scatters[0].second_hop()
    gathers[1].finish()
    load_upper[1].wait()
    chip_rows(slab, True, lambda rows: compute(1, rows))
    scatters[1].mate_far()
    scatters[0].first_hop()
    scatters[1].far_hop()
    chip_rows(slab, False, lambda rows: compute(1, rows))
    scatters[1].mate_near()
    scatters[1].second_hop()
    for load in load_second:
        load.wait()
    blocks = width // LANES
    weight_grads(0, blocks // 3)
    scatters[1].first_hop()
    close(0)
    weight_grads(blocks // 3, blocks)
    close(1)


def ffn_turn_kernel(
    half_ff, at, layer, hidden_ref, grad_ref, vectors, up_biases, given_hbm, packed_hbm,
    out_ref, grad_out_ref, grads_ref, small_ref, up_bias_ref, *rest
):
    micro, half_rows, width = hidden_ref.shape
    gathered, gather_refs = rest[0], rest[0:3]
    terms, back_terms = rest[3], rest[9]
    packed, tails, given, grad_upper, active, load_sem, given_sems = rest[15:]
    vec, up_bias = vectors.at[layer], up_biases.at[layer]
    seq, ff = active.shape[1:]
    main = ff - LANES
    extra = half_ff - main
    load = pltpu.make_async_copy(
        packed_hbm.at[:, at : at + packed.shape[1]], packed, load_sem
    )
    load.start()
    loads = [
        pltpu.make_async_copy(given_hbm.at[m], given.at[m], given_sems.at[m]) for m in range(micro)
    ]
    for copy in loads:
        copy.start()
    slab = Slab(half_rows)
    gathers = make_gathers(slab, gather_refs, micro)
    scatters = make_scatters(slab, rest[3:9], micro)
    backs = make_scatters(slab, rest[9:15], micro)
    slab.greet()

    def fill(m):
        own = slab.rows(gathered.at[m], slab.mine[0])
        for start in range(0, half_rows, 32):
            block = hidden_ref[m, pl.ds(start, 32)]
            own[pl.ds(start, 32)] = low(layer_norm(block, vec[1:2], vec[6:7]))

    open_gathers(gathers, fill)
    small_ref[...] = jnp.zeros_like(small_ref)
    up_bias_ref[...] = jnp.zeros_like(up_bias_ref)
    load.wait()
    split_tail(packed, tails, extra)

    def compute(m, rows):
        value = up_dot(gathered[m, rows], packed, tails) + up_bias[...]
        square = value * value
        bent = jnp.tanh(GELU_A * value * (1.0 + GELU_B * square))
        half = 0.5 * (1.0 + bent)
        shown = low(value * half)
        active[m, rows] = shown
        slope = half + (0.5 * GELU_A) * value * (1.0 - bent * bent) * (1.0 + 3.0 * GELU_B * square)
        grad = low(down_back(given[m, rows], packed, tails) * slope)
        grad_upper[m, rows] = grad
        up_bias_ref[0:1] += jnp.sum(grad.astype(jnp.float32), axis=0, keepdims=True)
        back_terms[m, rows] = low(up_back(grad, packed, tails))
        terms[m, rows] = low(down_dot(shown, packed, tails))

    def stacked(ref, cols=slice(None)):
        return ref[:, :, cols].reshape(micro * seq, -1)

    def weight_grads(first, last):
        def block(i):
            cols = step_rows(i, LANES)
            up = dot(stacked(gathered, cols), stacked(grad_upper), 0, 0)
            down = dot(stacked(given, cols), stacked(active), 0, 0)
            grads_ref[cols, :main] = low(up[:, :main])
            grads_ref[cols, main : 2 * main] = low(down[:, :main])
            blank = jnp.zeros((LANES, LANES - 2 * extra), jnp.float32)
            rest_cols = [up[:, main : main + extra], down[:, main : main + extra], blank]
            grads_ref[cols, 2 * main :] = low(jnp.concatenate(rest_cols, axis=1))

        repeat(last - first, lambda i: block(first + i))

    def close_back(m):
        backs[m].finish()
        for rows in backs[m].blocks():
            grad_normed = backs[m].total(rows)
            back, gain_terms = norm_back(hidden_ref[m, rows], vec[1:2], grad_normed)
            grad_rows = grad_ref[m, rows].astype(jnp.float32)
            grad_hidden = grad_rows + back
            grad_out_ref[m, rows] = grad_hidden
            branch = low(grad_hidden).astype(jnp.float32)
            for j, item in enumerate((gain_terms, grad_normed, grad_rows, branch)):
                small_ref[j : j + 1] += jnp.sum(item, axis=0, keepdims=True)

    def close(m):
        scatters[m].finish()
        for rows in scatters[m].blocks():
            out_ref[m, rows] = low(hidden_ref[m, rows] + scatters[m].total(rows) + vec[7:8])

    gathers[0].to_mate()
    gathers[0].finish()
    loads[0].wait()
    chip_rows(slab, True, lambda rows: compute(0, rows))
    backs[0].mate_far()
    scatters[0].mate_far()
    gathers[1].forward()
    backs[0].far_hop()
    chip_rows(slab, False, lambda rows: compute(0, rows))
    backs[0].mate_near()
    scatters[0].mate_near()
    gathers[1].to_mate()
    backs[0].second_hop()
    gathers[1].finish()
    loads[1].wait()
    chip_rows(slab, True, lambda rows: compute(1, rows))
    backs[1].mate_far()
    scatters[1].mate_far()
    backs[0].first_hop()
    backs[1].far_hop()
    chip_rows(slab, False, lambda rows: compute(1, rows))
    backs[1].mate_near()
    scatters[1].mate_near()
    backs[1].second_hop()
    for scatter in scatters:
        scatter.far_hop()
        scatter.second_hop()
    blocks = width // LANES
    weight_grads(0, blocks // 3)
    backs[1].first_hop()
    for scatter in scatters:
        scatter.first_hop()
    close_back(0)
    weight_grads(blocks // 3, blocks)
    close_back(1)
    for m in range(micro):
        close(m)


def attn_backward_kernel(
    at, layer, own_rows, grad_ref, rows_ref, vectors, lse, lengths, normed_hbm, qkv_hbm, mixed_hbm, packed_hbm,
    out_ref, grads_ref, small_ref, bias_ref, *rest
):
    micro, half_rows, width = grad_ref.shape
    gathered, gather_refs = rest[0], rest[0:3]
    scatter_refs = rest[3:9]
    terms = rest[3]
    packed, wide, normed, qkv, mixed, grad_mixed, grad_qkv, turned, shut = rest[9:18]
    low_probs, grad_scores, load_sems = rest[18:]
    vec = vectors.at[layer]
    seq, pair = mixed.shape[1:]
    heads = pair // LANES
    load_packed = pltpu.make_async_copy(
        packed_hbm.at[:, at : at + packed.shape[1]], packed, load_sems.at[0]
    )
    load_packed.start()
    load_qkv, load_rest = [], []
    for m in range(micro):
        load_qkv.append(pltpu.make_async_copy(qkv_hbm.at[m], qkv.at[m], load_sems.at[1 + 3 * m]))
        load_qkv[m].start()
    for m in range(micro):
        for k, (src, dst) in enumerate(((mixed_hbm, mixed), (normed_hbm, normed))):
            load = pltpu.make_async_copy(src.at[m], dst.at[m], load_sems.at[2 + k + 3 * m])
            load.start()
            load_rest.append(load)
    slab = Slab(half_rows)
    gathers = make_gathers(slab, gather_refs, micro)
    scatters = make_scatters(slab, scatter_refs, micro)
    slab.greet()

    def fill(m):
        own = slab.rows(gathered.at[m], slab.mine[0])
        for start in range(0, half_rows, 32):
            own[pl.ds(start, 32)] = low(grad_ref[m, pl.ds(start, 32)])

    open_gathers(gathers, fill)
    small_ref[...] = jnp.zeros_like(small_ref)
    bias_ref[...] = jnp.zeros_like(bias_ref)
    load_packed.wait()
    widen(packed, wide)

    def head(h, part=0):
        return slice(part * pair + h * LANES, part * pair + (h + 1) * LANES)

    for m in range(micro):
        load_qkv[m].wait()
        shut[m] = shut_keys(lengths[m], own_rows, 2 * half_rows, (seq, LANES), 0)
        for h in range(heads):
            turned[m, h] = low(qkv[m, :, head(h, 1)].astype(jnp.float32).T)

    def mix_grads(m):
        def block(i):
            rows = step_rows(i, TILE)
            grad_mixed[m, rows] = low(dot(gathered[m, rows], wide[:, 3 * pair :], 1, 0))

        repeat(seq // TILE, block)

    def attend(m, h):
        def block(i):
            rows = step_rows(i, LANES)
            queries = qkv[m, rows, head(h)]
            grads = grad_mixed[m, rows, head(h)]
            scores = dot(qkv[m, :, head(h, 1)], queries, 1, 1) * (score_scale * LOG2E) + shut[m]
            probs = jnp.exp2(scores - lse[m, h, rows].T[0:1])
            grad_probs = dot(qkv[m, :, head(h, 2)], grads, 1, 1)
            inner = jnp.sum(grad_probs * probs, axis=0, keepdims=True)
            low_probs[:, rows] = low(probs)
            grad_scores[:, rows] = low(probs * (grad_probs - inner))

        repeat(seq // LANES, block)
        grad_keys = dot(grad_scores[...], qkv[m, :, head(h)], 1, 0)
        grad_qkv[m, :, head(h, 1)] = low(grad_keys * score_scale)
        grad_qkv[m, :, head(h, 2)] = low(dot(low_probs[...], grad_mixed[m, :, head(h)], 1, 0))
        turn = dot(turned[m, h], grad_scores[...], 1, 0).T
        grad_qkv[m, :, head(h)] = low(turn * score_scale)

    def back_project(m, rows):
        grads = grad_qkv[m, rows]
        terms[m, rows] = low(dot(grads, wide[:, : 3 * pair], 1, 1))
        for j, part in enumerate((0, 2)):
            piece = grads[:, part * pair : (part + 1) * pair].astype(jnp.float32)
            bias_ref[j : j + 1] += jnp.sum(piece, axis=0, keepdims=True)

    def stacked(ref, cols=slice(None)):
        return ref[:, :, cols].reshape(micro * seq, -1)

    def weight_grads(first, last):
        def block(i):
            cols = step_rows(i, LANES)
            front = dot(stacked(normed, cols), stacked(grad_qkv), 0, 0)
            back = dot(stacked(gathered, cols), stacked(mixed), 0, 0)
            total = low(jnp.concatenate([front, back], axis=1))
            pieces = [total[:, h * LANES : h * LANES + HEAD] for h in range(4 * heads)]
            grads_ref[cols] = jnp.concatenate(pieces, axis=1)

        repeat(last - first, lambda i: block(first + i))

    def close(m):
        scatters[m].finish()
        for rows in scatters[m].blocks():
            grad_normed = scatters[m].total(rows)
            back, gain_terms = norm_back(
                rows_ref[m, rows].astype(jnp.float32), vec[0:1], grad_normed
            )
            out_ref[m, rows] = low(grad_ref[m, rows] + back)
            for j, item in enumerate((gain_terms, grad_normed)):
                small_ref[j : j + 1] += jnp.sum(item, axis=0, keepdims=True)

    gathers[0].to_mate()
    gathers[0].finish()
    mix_grads(0)
    attend(0, 0)
    gathers[1].forward()
    for h in range(1, heads):
        attend(0, h)
    gathers[1].to_mate()
    chip_rows(slab, True, lambda rows: back_project(0, rows))
    scatters[0].mate_far()
    scatters[0].far_hop()
    chip_rows(slab, False, lambda rows: back_project(0, rows))
    scatters[0].mate_near()
    gathers[1].finish()
    scatters[0].second_hop()
    mix_grads(1)
    scatters[0].first_hop()
    for h in range(heads):
        attend(1, h)
    chip_rows(slab, True, lambda rows: back_project(1, rows))
    scatters[1].mate_far()
    scatters[1].far_hop()
    chip_rows(slab, False, lambda rows: back_project(1, rows))
    scatters[1].mate_near()
    close(0)
    scatters[1].second_hop()
    for load in load_rest:
        load.wait()
    blocks = width // LANES
    weight_grads(0, blocks // 3)
    scatters[1].first_hop()
    weight_grads(blocks // 3, blocks)
    close(1)


def any_spec():
    return pl.BlockSpec(memory_space=pl.ANY)


def vmem_spec():
    return pl.BlockSpec(memory_space=pltpu.VMEM)


def shape_of(shape, dtype):
    return jax.ShapeDtypeStruct(shape, dtype)


def params(collective):
    return pltpu.CompilerParams(
        collective_id=collective, has_side_effects=True, vmem_limit_bytes=VMEM_BYTES
    )


def smem_spec():
    return pl.BlockSpec(memory_space=pltpu.SMEM)


def attn_forward(rows_low, vectors, bias, packed, at, layer, lengths, own_rows, given=None, grads=None):
    micro, half_rows, width = rows_low.shape
    seq = 8 * half_rows
    pair = bias.shape[2] // 3
    heads = pair // LANES
    low_type, high_type = jnp.bfloat16, jnp.float32
    hidden, lse, normed, qkv, mixed = pl.pallas_call(
        functools.partial(attn_forward_kernel, given is not None, at, layer, own_rows),
        out_shape=[
            shape_of((micro, half_rows, width), high_type),
            shape_of((micro, heads, seq, LANES), high_type),
            shape_of((micro, seq, width), low_type),
            shape_of((micro, seq, 3 * pair), low_type),
            shape_of((micro, seq, pair), low_type),
        ],
        in_specs=[vmem_spec()] * 3 + [smem_spec(), any_spec(), any_spec(), vmem_spec()],
        out_specs=[vmem_spec()] * 2 + [any_spec()] * 3,
        scratch_shapes=gather_scratch(micro, seq, width)
        + scatter_scratch(micro, seq, half_rows, width)
        + [
            pltpu.VMEM((width, 4 * heads * HEAD), low_type),
            pltpu.VMEM((width, 4 * pair), low_type),
            pltpu.VMEM((micro, seq, 3 * pair), low_type),
            pltpu.VMEM((micro, seq, pair), low_type),
            pltpu.SemaphoreType.DMA,
            pltpu.SemaphoreType.DMA((6,)),
            pltpu.SemaphoreType.DMA((micro,)),
            pltpu.VMEM((micro, seq if given is not None else 32, width), low_type),
            pltpu.SemaphoreType.DMA((micro, 3)),
            pltpu.SemaphoreType.DMA((micro, 3)),
        ],
        compiler_params=params(0 if given is None else 6),
        cost_estimate=COST,
        name="attn_forward",
    )(
        rows_low,
        vectors,
        bias,
        lengths,
        packed,
        packed if given is None else given,
        rows_low if grads is None else grads,
    )
    if given is None:
        return hidden, (normed, qkv, lse, mixed)
    return hidden, (given, qkv, lse, mixed), normed


def ffn_forward(hidden, vectors, up_biases, packed, at, layer, half_ff):
    micro, half_rows, width = hidden.shape
    seq = 8 * half_rows
    ff = up_biases.shape[2]
    packed_cols = 2 * ff - LANES
    low_type, high_type = jnp.bfloat16, jnp.float32
    out, second, upper = pl.pallas_call(
        functools.partial(ffn_forward_kernel, half_ff, at, layer),
        out_shape=[
            shape_of((micro, half_rows, width), low_type),
            shape_of((micro, seq, width), low_type),
            shape_of((micro, seq, ff), high_type),
        ],
        in_specs=[vmem_spec()] * 3 + [any_spec()],
        out_specs=[vmem_spec()] + [any_spec()] * 2,
        scratch_shapes=gather_scratch(micro, seq, width)
        + scatter_scratch(micro, seq, half_rows, width)
        + [
            pltpu.VMEM((width, packed_cols), low_type),
            pltpu.VMEM((width, 2 * LANES), low_type),
            pltpu.VMEM((micro, seq, ff), high_type),
            pltpu.SemaphoreType.DMA,
            pltpu.SemaphoreType.DMA((4,)),
        ],
        compiler_params=params(1),
        cost_estimate=COST,
        name="ffn_forward",
    )(hidden, vectors, up_biases, packed)
    return out, (second, upper)


def ffn_turn(hidden, grad_low, given, vectors, up_biases, packed, at, layer, half_ff):
    micro, half_rows, width = hidden.shape
    seq = 8 * half_rows
    ff = up_biases.shape[2]
    low_type, high_type = jnp.bfloat16, jnp.float32
    out, grad_hidden, grads, small, up_bias = pl.pallas_call(
        functools.partial(ffn_turn_kernel, half_ff, at, layer),
        out_shape=[
            shape_of((micro, half_rows, width), low_type),
            shape_of((micro, half_rows, width), high_type),
            shape_of((width, 2 * ff - LANES), low_type),
            shape_of((8, width), high_type),
            shape_of((8, ff), high_type),
        ],
        in_specs=[vmem_spec()] * 4 + [any_spec()] * 2,
        out_specs=[vmem_spec()] * 5,
        scratch_shapes=gather_scratch(micro, seq, width)
        + scatter_scratch(micro, seq, half_rows, width)
        + scatter_scratch(micro, seq, half_rows, width)
        + [
            pltpu.VMEM((width, 2 * ff - LANES), low_type),
            pltpu.VMEM((width, 2 * LANES), low_type),
            pltpu.VMEM((micro, seq, width), low_type),
            pltpu.VMEM((micro, seq, ff), low_type),
            pltpu.VMEM((micro, seq, ff), low_type),
            pltpu.SemaphoreType.DMA,
            pltpu.SemaphoreType.DMA((micro,)),
        ],
        compiler_params=params(7),
        cost_estimate=COST,
        name="ffn_turn",
    )(hidden, grad_low, vectors, up_biases, given, packed)
    return out, grad_hidden, grads, small, up_bias[:1]


def ffn_backward(grad_low, hidden, kept, vectors, packed, at, layer, half_ff):
    second, upper = kept
    micro, half_rows, width = hidden.shape
    seq, ff = upper.shape[1:]
    low_type, high_type = jnp.bfloat16, jnp.float32
    grad_hidden, grads, small, up_bias = pl.pallas_call(
        functools.partial(ffn_backward_kernel, half_ff, at, layer),
        out_shape=[
            shape_of((micro, half_rows, width), high_type),
            shape_of((width, 2 * ff - LANES), low_type),
            shape_of((8, width), high_type),
            shape_of((8, ff), high_type),
        ],
        in_specs=[vmem_spec()] * 3 + [any_spec()] * 3,
        out_specs=[vmem_spec()] * 4,
        scratch_shapes=gather_scratch(micro, seq, width)
        + scatter_scratch(micro, seq, half_rows, width)
        + [
            pltpu.VMEM((width, 2 * ff - LANES), low_type),
            pltpu.VMEM((width, 2 * LANES), low_type),
            pltpu.VMEM((micro, seq, width), low_type),
            pltpu.VMEM((micro, seq, ff), high_type),
            pltpu.VMEM((micro, seq, ff), low_type),
            pltpu.VMEM((micro, seq, ff), low_type),
            pltpu.SemaphoreType.DMA((1 + 2 * micro,)),
        ],
        compiler_params=params(2),
        cost_estimate=COST,
        name="ffn_backward",
    )(grad_low, hidden, vectors, second, upper, packed)
    return grad_hidden, grads, small, up_bias[:1]


def attn_backward(grad_hidden, rows_low, kept, vectors, packed, at, layer, lengths, own_rows):
    normed, qkv, lse, mixed = kept
    micro, half_rows, width = grad_hidden.shape
    seq, pair = mixed.shape[1:]
    heads = pair // LANES
    low_type, high_type = jnp.bfloat16, jnp.float32
    out, grads, small, bias = pl.pallas_call(
        functools.partial(attn_backward_kernel, at, layer, own_rows),
        out_shape=[
            shape_of((micro, half_rows, width), low_type),
            shape_of((width, 4 * heads * HEAD), low_type),
            shape_of((8, width), high_type),
            shape_of((8, pair), high_type),
        ],
        in_specs=[vmem_spec()] * 4 + [smem_spec()] + [any_spec()] * 4,
        out_specs=[vmem_spec()] * 4,
        scratch_shapes=gather_scratch(micro, seq, width)
        + scatter_scratch(micro, seq, half_rows, width)
        + [
            pltpu.VMEM((width, 4 * heads * HEAD), low_type),
            pltpu.VMEM((width, 4 * pair), low_type),
            pltpu.VMEM((micro, seq, width), low_type),
            pltpu.VMEM((micro, seq, 3 * pair), low_type),
            pltpu.VMEM((micro, seq, pair), low_type),
            pltpu.VMEM((micro, seq, pair), low_type),
            pltpu.VMEM((micro, seq, 3 * pair), low_type),
            pltpu.VMEM((micro, heads, LANES, seq), low_type),
            pltpu.VMEM((micro, seq, LANES), high_type),
            pltpu.VMEM((seq, seq), low_type),
            pltpu.VMEM((seq, seq), low_type),
            pltpu.SemaphoreType.DMA((1 + 3 * micro,)),
        ],
        compiler_params=params(3 + 5 * layer),
        cost_estimate=COST,
        name="attn_backward",
    )(grad_hidden, rows_low, vectors, lse, lengths, normed, qkv, mixed, packed)
    return out, grads, small, bias


def slab_peers():
    section, tensor = lax.axis_index("section"), lax.axis_index("tensor")
    peers = []
    for role in range(1, 8):
        far, step = role // 4, role % 4
        other = section + far * (1 - 2 * section)
        to = (other, lax.rem(tensor + step, 4))
        source = (other, lax.rem(tensor + 4 - step, 4))
        peers.append((role, to, source))
    return peers


def column_peers(count):
    here = lax.axis_index("dp")
    return [
        (step, lax.rem(here + step, count), lax.rem(here + count - step, count))
        for step in range(1, count)
    ]


def greet_all(count):
    barrier = pltpu.get_barrier_semaphore()
    for _, to, _ in slab_peers():
        pl.semaphore_signal(barrier, inc=1, device_id=named(to), device_id_type=MESH)
    for _, to, _ in column_peers(count):
        pl.semaphore_signal(barrier, inc=1, device_id={"dp": to}, device_id_type=MESH)
    pl.semaphore_wait(barrier, 7 + count - 1)


def remote(src, dst, send_sem, recv_sem, peer):
    return pltpu.make_async_remote_copy(
        src_ref=src,
        dst_ref=dst,
        send_sem=send_sem,
        recv_sem=recv_sem,
        device_id=peer,
        device_id_type=MESH,
    )


def prologue_kernel(
    count, heads, qkv_ref, out_ref_t, up_ref_in, down_ref_t, gains_ref, shifts_ref, up_bias, rows_ref,
    first_hbm, normed_hbm, attn_ref, ff_hbm, out_ref, up_ref, bias_ref,
    attn_parts, ff_parts, up_halves, mine_ref, all_rows, line, ff_line, column, slab, up_got,
    rows_send, rows_recv, column_send, column_recv, slab_send, slab_recv, swap_send, swap_recv,
    right_send, right_recv, left_send, left_recv, out_sems,
):
    section, tensor, here = (lax.axis_index(name) for name in ("section", "tensor", "dp"))
    width = out_ref.shape[2]
    chunk = width // (4 * count)
    rows = attn_parts.shape[1]
    micro, own_rows = rows_ref.shape[:2]
    pieces = swap_send.shape[0] - 2
    size = rows // pieces
    other = {"section": 1 - section}
    pair = heads * LANES
    pair_cols = heads * HEAD
    half_ff = up_ref_in.shape[1] // 2
    main = half_ff // LANES * LANES
    extra = half_ff - main
    greet_all(count)
    for half in range(2):
        span = slice(half * pair_cols, (half + 1) * pair_cols)
        parts = [qkv_ref[k, :, span] for k in range(3)] + [out_ref_t[:, span]]
        attn_parts[half] = jnp.concatenate(parts, axis=1)
    keep_slot = jnp.where(section == 0, here, count)
    send_slot = jnp.where(section == 0, here, count)
    got_slot = jnp.where(section == 0, count, here)
    sent = []
    for p in range(pieces):
        span = pl.ds(p * size, size)
        copy = remote(
            attn_parts.at[1 - section, span],
            line.at[send_slot, span],
            swap_send.at[p],
            swap_recv.at[p],
            other,
        )
        copy.start()
        sent.append(copy)
    line[keep_slot] = attn_parts[section]
    mine_ref[...] = jnp.zeros_like(mine_ref)
    gains = gains_ref.shape[0]
    mine_ref[:gains, :chunk] = gains_ref[...]
    mine_ref[gains:, :chunk] = shifts_ref[...]
    column[here] = mine_ref[...]
    for step, to, _ in column_peers(count):
        copy = remote(
            mine_ref, column.at[here], column_send.at[step], column_recv.at[step], {"dp": to}
        )
        copy.start()
        sent.append(copy)

    def swapped(p):
        got = line.at[got_slot, pl.ds(p * size, size)]
        remote(got, got, swap_send.at[p], swap_recv.at[p], other).wait_recv()

    def hop(step, p, way, finish=False):
        origin = here - way * step
        sends, recvs = (right_send, right_recv) if way == 1 else (left_send, left_recv)
        inside = (origin >= 0) if way == 1 else (origin < count)
        onward = (here + 1 < count) if way == 1 else (here > 0)
        slot = line.at[jnp.clip(origin, 0, count - 1), pl.ds(p * size, size)]
        target = jnp.clip(here + way, 0, count - 1)
        if step > 0 and not finish:

            @pl.when(inside)
            def _():
                remote(slot, slot, sends.at[step, p], recvs.at[step, p], {"dp": target}).wait_recv()

        if step + 1 < count:

            @pl.when(inside & onward)
            def _():
                copy = remote(
                    slot, slot, sends.at[step, p], recvs.at[step + 1, p], {"dp": target}
                )
                if finish:
                    copy.wait_send()
                else:
                    copy.start()

    def hops(step):
        for p in range(pieces):
            for way in (1, -1):
                hop(step, p, way)

    for p in range(pieces):

        @pl.when(section == 1)
        def _():
            swapped(p)

        for way in (1, -1):
            hop(0, p, way)
    for step, _, source in column_peers(count):
        slot = column.at[source]
        remote(slot, slot, column_send.at[step], column_recv.at[step], {"dp": source}).wait_recv()
    for role, to, _ in slab_peers():
        copy = remote(
            column, slab.at[section, tensor], slab_send.at[role], slab_recv.at[role], named(to)
        )
        copy.start()
        sent.append(copy)
    slab[section, tensor] = column[...]
    blank = jnp.zeros((rows, LANES - 2 * extra), jnp.bfloat16)
    up_halves[...] = jnp.zeros_like(up_halves)
    for half in range(2):
        start = half * half_ff
        up_halves[half, :, :half_ff] = up_bias[:, start : start + half_ff]
        ff_parts[half, :, :main] = up_ref_in[:, start : start + main]
        ff_parts[half, :, main : 2 * main] = down_ref_t[:, start : start + main]
        span = slice(start + main, start + half_ff)
        ff_parts[half, :, 2 * main :] = jnp.concatenate(
            [up_ref_in[:, span], down_ref_t[:, span], blank], axis=1
        )
    ff_swap = remote(
        ff_parts.at[1 - section],
        ff_line.at[section],
        swap_send.at[pieces],
        swap_recv.at[pieces],
        other,
    )
    up_swap = remote(
        up_halves.at[1 - section],
        up_got.at[section],
        swap_send.at[pieces + 1],
        swap_recv.at[pieces + 1],
        other,
    )
    up_swap.start()
    for role, _, source in slab_peers():
        slot = slab.at[source[0], source[1]]
        remote(slot, slot, slab_send.at[role], slab_recv.at[role], named(source)).wait_recv()
    ff_swap.start()
    for layer in range(2):
        for part in range(4 * count):
            piece = slab[layer, part % 4, part // 4]
            out_ref[layer, :, part * chunk : (part + 1) * chunk] = piece[:, :chunk]
    tiles = TileGather(all_rows, rows_send, rows_recv)
    for m in range(micro):
        own = tiles.tile(m, tensor)
        for begin in range(0, own_rows, 32):
            end = min(begin + 32, own_rows)
            block = rows_ref[m, begin:end].astype(jnp.float32)
            own[begin:end] = low(layer_norm(block, out_ref[0, 0:1], out_ref[0, 2:3]))
        own[own_rows:] = jnp.zeros((tiles.tile_rows - own_rows, width), jnp.bfloat16)
    tiles.start()
    hops(1)
    start = (2 * tensor + section) * pair_cols
    for layer in range(2):
        turned = pltpu.roll(out_ref[layer], lax.rem(width - start, width), 1)
        empty = jnp.zeros((1, LANES - HEAD), jnp.float32)
        for part, row in ((0, 3), (2, 4)):
            for h in range(heads):
                at = part * pair + h * LANES
                piece = turned[row : row + 1, h * HEAD : (h + 1) * HEAD]
                bias_ref[layer, :, at : at + LANES] = jnp.concatenate([piece, empty], 1)
        bias_ref[layer, :, pair : 2 * pair] = jnp.zeros((1, pair), jnp.float32)
    up_ref[section] = up_halves[section]
    outs = []

    def put(src, dst, i):
        copy = pltpu.make_async_copy(src, dst, out_sems.at[i])
        copy.start()
        outs.append(copy)

    ff_line_out = ff_hbm.at[section]
    put(ff_parts.at[section], ff_line_out, count)
    for step in range(2, count):
        hops(step)
        if step == 2:
            tiles.pass_on()
    if count <= 2:
        tiles.pass_on()
    for p in range(pieces):

        @pl.when(section == 0)
        def _():
            swapped(p)

    for at in range(count):
        put(line.at[at], first_hbm.at[pl.ds(at * rows, rows)], at)
    attn_ref[...] = line[count]
    got = up_got.at[1 - section]
    remote(got, got, swap_send.at[pieces + 1], swap_recv.at[pieces + 1], other).wait_recv()
    up_ref[1 - section] = up_got[1 - section]
    tiles.finish()
    put(all_rows, normed_hbm, count + 2)
    ff_got = ff_line.at[1 - section]
    remote(ff_got, ff_got, swap_send.at[pieces], swap_recv.at[pieces], other).wait_recv()
    put(ff_got, ff_hbm.at[1 - section], count + 1)
    for step in range(count):
        for p in range(pieces):
            for way in (1, -1):
                hop(step, p, way, True)
    for copy in sent + [ff_swap, up_swap]:
        copy.wait_send()
    tiles.drain()
    for copy in outs:
        copy.wait()


def prologue(qkv, out_t, up, down_t, gains, shifts, up_bias, rows_low, count, heads, tile_rows):
    part_rows = qkv.shape[1]
    micro, _, width = rows_low.shape
    vector_rows = gains.shape[0] + shifts.shape[0]
    half_ff = up.shape[1] // 2
    ff_wide = round_up(half_ff, LANES)
    attn_shape = (part_rows, 4 * heads * HEAD)
    ff_shape = (2, part_rows, 2 * ff_wide - LANES)
    all_rows = (micro, 4 * tile_rows, width)
    pieces = 3 if part_rows % 96 == 0 else 1
    low_type, high_type = jnp.bfloat16, jnp.float32
    dma = pltpu.SemaphoreType.DMA
    return pl.pallas_call(
        functools.partial(prologue_kernel, count, heads),
        out_shape=[
            shape_of((count * part_rows, attn_shape[1]), low_type),
            shape_of(all_rows, low_type),
            shape_of(attn_shape, low_type),
            shape_of(ff_shape, low_type),
            shape_of((2, vector_rows, width), high_type),
            shape_of((2, 1, ff_wide), high_type),
            shape_of((2, 1, 3 * heads * LANES), high_type),
        ],
        in_specs=[vmem_spec()] * 8,
        out_specs=[any_spec()] * 2 + [vmem_spec(), any_spec()] + [vmem_spec()] * 3,
        scratch_shapes=[
            pltpu.VMEM((2,) + attn_shape, low_type),
            pltpu.VMEM(ff_shape, low_type),
            pltpu.VMEM((2, 1, ff_wide), high_type),
            pltpu.VMEM((vector_rows, LANES), high_type),
            pltpu.VMEM(all_rows, low_type),
            pltpu.VMEM((count + 1,) + attn_shape, low_type),
            pltpu.VMEM(ff_shape, low_type),
            pltpu.VMEM((count, vector_rows, LANES), high_type),
            pltpu.VMEM((2, 4, count, vector_rows, LANES), high_type),
            pltpu.VMEM((2, 1, ff_wide), high_type),
            dma((micro, 3)),
            dma((micro, 3)),
            dma((count,)),
            dma((count,)),
            dma((8,)),
            dma((8,)),
            dma((pieces + 2,)),
            dma((pieces + 2,)),
            dma((count, pieces)),
            dma((count, pieces)),
            dma((count, pieces)),
            dma((count, pieces)),
            dma((count + 3,)),
        ],
        compiler_params=params(4),
        cost_estimate=COST,
        name="prologue",
    )(qkv, out_t, up, down_t, gains, shifts, up_bias, rows_low)


def home_kernel(
    count, chunk, attn_zero, attn_one, ff_zero, ff_one, biases_in, ups_in,
    ff_sums_hbm, attn_sum_hbm, rows_hbm,
    out_ref, up_ref, ff_got_hbm, attn_got_hbm, rows_got_hbm,
    parts, ups, slab, column, up_pair, up_column, total,
    column_send, column_recv, slab_send, slab_recv, up_sems, up_column_send, up_column_recv, far_send, far_recv,
):
    section, tensor, here = (lax.axis_index(name) for name in ("section", "tensor", "dp"))
    width = attn_zero.shape[1]
    heads = biases_in.shape[2] // LANES
    other = {"section": 1 - section}
    greet_all(count)
    parts[...] = jnp.zeros_like(parts)
    start = (2 * tensor + section) * (heads * HEAD)
    for layer, (attn, ff) in enumerate(((attn_zero, ff_zero), (attn_one, ff_one))):
        bias = biases_in[layer]
        blank = jnp.zeros((8, width - heads * HEAD), jnp.float32)
        pieces = [bias[:, h * LANES : h * LANES + HEAD] for h in range(heads)]
        placed = pltpu.roll(jnp.concatenate(pieces + [blank], 1), start, 1)
        whole = jnp.concatenate(
            [attn[0:1], ff[0:1], attn[1:2], placed[0:2], ff[3:4], ff[1:2], ff[2:3]], axis=0
        )
        for part in range(4 * count):
            piece = whole[:, part * chunk : (part + 1) * chunk]
            parts[layer, part % 4, part // 4, :, :chunk] = piece
        ups[layer] = ups_in[layer]
    sent = []

    def send(src, dst, send_sem, recv_sem, peer):
        copy = remote(src, dst, send_sem, recv_sem, peer)
        copy.start()
        sent.append(copy)

    send(ups.at[1 - section], up_pair.at[section], up_sems.at[0], up_sems.at[1], other)
    for role, to, _ in slab_peers():
        send(
            parts.at[to[0], to[1]], slab.at[role], slab_send.at[role], slab_recv.at[role], named(to)
        )
    up_pair[section] = ups[section]
    value = parts[section, tensor]
    for role, _, source in slab_peers():
        slot = slab.at[role]
        remote(slot, slot, slab_send.at[role], slab_recv.at[role], named(source)).wait_recv()
        value = value + slab[role]
    total[...] = value
    for step, to, _ in column_peers(count):
        send(total.at[to], column.at[step], column_send.at[step], column_recv.at[step], {"dp": to})
    got = up_pair.at[1 - section]
    remote(got, got, up_sems.at[0], up_sems.at[1], other).wait_recv()
    for step, to, _ in column_peers(count):
        send(
            up_pair, up_column.at[here], up_column_send.at[step], up_column_recv.at[step], {"dp": to}
        )
    far = (
        (ff_sums_hbm.at[1 - section], ff_got_hbm),
        (rows_hbm.at[1 - section], rows_got_hbm),
    )
    for k, (src, dst) in enumerate(far):
        send(src, dst, far_send.at[k], far_recv.at[k], other)

    @pl.when(section == 0)
    def _():
        remote(attn_sum_hbm, attn_got_hbm, far_send.at[2], far_recv.at[2], other).start()

    up_column[here] = up_pair[...]
    result = total[here]
    for step, _, source in column_peers(count):
        slot = column.at[step]
        remote(slot, slot, column_send.at[step], column_recv.at[step], {"dp": source}).wait_recv()
        result = result + column[step]
    out_ref[...] = result
    for step, _, source in column_peers(count):
        slot = up_column.at[source]
        remote(
            slot, slot, up_column_send.at[step], up_column_recv.at[step], {"dp": source}
        ).wait_recv()
    value = up_column[0]
    for at in range(1, count):
        value = value + up_column[at]
    up_ref[...] = value
    for k, (_, dst) in enumerate(far):
        remote(dst, dst, far_send.at[k], far_recv.at[k], other).wait_recv()
    last = remote(attn_sum_hbm, attn_got_hbm, far_send.at[2], far_recv.at[2], other)

    @pl.when(section == 0)
    def _():
        last.wait_send()

    @pl.when(section == 1)
    def _():
        last.wait_recv()

    for copy in sent:
        copy.wait_send()


def home(attn_small, ff_small, bias_grads, up_grads, ff_sums, attn_sum, rows, count, chunk):
    vector_rows, lanes = 8, LANES
    up_shape = up_grads.shape[1:]
    dma = pltpu.SemaphoreType.DMA
    high_type = jnp.float32
    return pl.pallas_call(
        functools.partial(home_kernel, count, chunk),
        out_shape=[
            shape_of((vector_rows, lanes), high_type),
            shape_of((2,) + up_shape, high_type),
            shape_of(ff_sums.shape[1:], ff_sums.dtype),
            shape_of(attn_sum.shape, attn_sum.dtype),
            shape_of(rows.shape[1:], rows.dtype),
        ],
        in_specs=[vmem_spec()] * 6 + [any_spec()] * 3,
        out_specs=[vmem_spec()] * 2 + [any_spec()] * 3,
        scratch_shapes=[
            pltpu.VMEM((2, 4, count, vector_rows, lanes), high_type),
            pltpu.VMEM((2,) + up_shape, high_type),
            pltpu.VMEM((8, count, vector_rows, lanes), high_type),
            pltpu.VMEM((count, vector_rows, lanes), high_type),
            pltpu.VMEM((2,) + up_shape, high_type),
            pltpu.VMEM((count, 2) + up_shape, high_type),
            pltpu.VMEM((count, vector_rows, lanes), high_type),
            dma((count,)),
            dma((count,)),
            dma((8,)),
            dma((8,)),
            dma((2,)),
            dma((count,)),
            dma((count,)),
            dma((3,)),
            dma((3,)),
        ],
        compiler_params=params(5),
        cost_estimate=COST,
        name="home",
    )(*attn_small, *ff_small, bias_grads, up_grads, ff_sums, attn_sum, rows)


def shards(
    section_input,
    final_cotangent,
    lengths,
    qkv_weight,
    out_weight,
    up_weight,
    down_weight,
    norm_gains,
    biases,
    up_bias,
):
    here = lax.axis_index("section")
    sections = lax.axis_size("section")
    micro, _, own_rows, _ = section_input.shape
    head_cols = qkv_weight.shape[3]
    pair_cols = head_cols // sections
    heads = pair_cols // HEAD
    ff_cols = up_weight.shape[2]
    half_ff = ff_cols // sections
    half_rows = round_up(-(-own_rows // sections), 32)
    full_rows = half_rows * sections

    def by_layer(mine, other):
        return [jnp.where(here == 0, mine, other), jnp.where(here == 0, other, mine)]

    part_rows = qkv_weight.shape[2]
    count = lax.axis_size("dp")
    chunk = norm_gains.shape[2]
    main = half_ff // LANES * LANES
    first, normed, attn_part, ff_two, vectors, up_biases, bias_qv = prologue(
        qkv_weight[0],
        out_weight[0].T,
        up_weight[0],
        down_weight[0].T,
        norm_gains[0],
        biases[0],
        up_bias,
        section_input[:, 0],
        count,
        heads,
        full_rows,
    )

    def gather_column(part):
        return lax.all_gather(part, "dp", axis=0, tiled=True)

    ff_first = gather_column(ff_two[0])
    attn_packed = [(first, 0), (gather_column(attn_part), 0)]
    ff_packed = [(ff_first, 0), (gather_column(ff_two[1]), 0)]
    lengths_here = lengths.reshape(micro)

    def my_rows(value):
        padded = jnp.pad(value[:, 0], [(0, 0), (0, full_rows - own_rows), (0, 0)])
        return lax.dynamic_slice_in_dim(padded, here * half_rows, half_rows, 1)

    def whole_rows(first, second, got):
        low_half, high_half = by_layer(jnp.where(here == 0, first, second), got)
        return jnp.concatenate([low_half, high_half], 1)[:, None, :own_rows]

    def send_home(value, layer):
        return lax.ppermute(value, "section", [(1 - layer, layer)])

    rows = my_rows(section_input)
    inputs, hiddens, attn_kept = [], [], []
    for layer in range(2):
        inputs.append(rows)
        operands = (rows, vectors, bias_qv, *attn_packed[layer], layer, lengths_here, own_rows)
        if layer == 0:
            hidden, kept, grads_all = attn_forward(*operands, normed, final_cotangent[:, 0])
        else:
            hidden, kept = attn_forward(*operands)
        hiddens.append(hidden)
        attn_kept.append(kept)
        if layer == 0:
            rows, ff_kept = ffn_forward(hidden, vectors, up_biases, *ff_packed[0], 0, half_ff)

    attn_sums, ff_sums, up_sums, input_grads = {}, {}, {}, {}
    attn_small, ff_small, bias_grads = {}, {}, {}
    for layer in (1, 0):
        if layer == 1:
            last, grad_hidden, ff_grad, ff_small[1], up_sums[1] = ffn_turn(
                hiddens[1],
                my_rows(final_cotangent),
                grads_all,
                vectors,
                up_biases,
                *ff_packed[1],
                1,
                half_ff,
            )
        else:
            grad_hidden, ff_grad, ff_small[0], up_sums[0] = ffn_backward(
                grads, hiddens[0], ff_kept, vectors, *ff_packed[0], 0, half_ff
            )
        ff_sums[layer] = lax.psum_scatter(ff_grad, "dp", scatter_dimension=0, tiled=True)
        grads, attn_grad, attn_small[layer], bias_grads[layer] = attn_backward(
            grad_hidden,
            inputs[layer],
            attn_kept[layer],
            vectors,
            *attn_packed[layer],
            layer,
            lengths_here,
            own_rows,
        )
        attn_sums[layer] = lax.psum_scatter(attn_grad, "dp", scatter_dimension=0, tiled=True)
        input_grads[layer] = grads

    out_got = [send_home(rows, 0), send_home(last, 1)]
    section_output = whole_rows(rows, last, jnp.where(here == 0, out_got[0], out_got[1]))
    small_mine, up_total, ff_got, attn_got, rows_got = home(
        [attn_small[0], attn_small[1]],
        [ff_small[0], ff_small[1]],
        jnp.stack([bias_grads[0], bias_grads[1]]),
        jnp.stack([up_sums[0], up_sums[1]]),
        jnp.stack([ff_sums[0], ff_sums[1]]),
        attn_sums[1],
        jnp.stack([input_grads[0], input_grads[1]]),
        count,
        chunk,
    )
    small_mine = small_mine[None, :, :chunk]
    up_total = up_total[:, :, :half_ff].reshape(1, ff_cols)
    input_grad = whole_rows(input_grads[0], input_grads[1], rows_got)

    def own_layer(sums, got):
        return by_layer(jnp.where(here == 0, sums[0], sums[1]), got)

    attn_got = jnp.where(here == 0, send_home(attn_sums[0], 0), attn_got)
    attn_total = jnp.stack(own_layer(attn_sums, attn_got), 1).astype(jnp.float32)
    attn_total = attn_total.reshape(part_rows, sections, 4, pair_cols)
    attn_total = jnp.moveaxis(attn_total, 2, 0).reshape(4, part_rows, head_cols)
    ff_halves = own_layer(ff_sums, ff_got)
    rest_cols = half_ff - main

    def ff_piece(index):
        pieces = []
        for half in ff_halves:
            pieces.append(half[:, index * main : (index + 1) * main])
            start = 2 * main + index * rest_cols
            pieces.append(half[:, start : start + rest_cols])
        return jnp.concatenate(pieces, 1).astype(jnp.float32)

    ff_total = [ff_piece(0), ff_piece(1)]

    gains = norm_gains.shape[1]
    return (
        section_output[None],
        input_grad[None],
        attn_total[None, :3],
        attn_total[3].T[None],
        ff_total[0][None],
        ff_total[1].T[None],
        small_mine[:, :gains],
        small_mine[:, gains:],
        up_total,
    )


def solution(mesh):
    in_specs = (
        P(None, "dp", "tensor", None),
        P(None, "dp", "tensor", None),
        P(None, "dp"),
        P("section", None, "dp", "tensor"),
        P("section", "tensor", "dp"),
        P("section", "dp", "tensor"),
        P("section", "tensor", "dp"),
        P("section", None, ("dp", "tensor")),
        P("section", None, ("dp", "tensor")),
        P("section", "tensor"),
    )
    out_specs = (
        P("section", None, "dp", "tensor", None),
        P("section", None, "dp", "tensor", None),
        P("section", None, "dp", "tensor"),
        P("section", "tensor", "dp"),
        P("section", "dp", "tensor"),
        P("section", "tensor", "dp"),
        P("section", None, ("dp", "tensor")),
        P("section", None, ("dp", "tensor")),
        P("section", "tensor"),
    )
    return jax.shard_map(shards, mesh=mesh, in_specs=in_specs, out_specs=out_specs, check_vma=False)
```

```python
import functools
import math

import jax
import jax.numpy as jnp
from jax import lax
from jax.experimental import pallas as pl
from jax.experimental.pallas import tpu as pltpu
from jax.sharding import PartitionSpec as P


HEAD = 72
LANES = 128
norm_eps = 1e-06
masked_score = -1000000000.0
score_scale = 1.0 / math.sqrt(HEAD)
GELU_A = math.sqrt(2.0 / math.pi)
GELU_B = 0.044715


def round_up(value, step):
    return -(-value // step) * step


def dot(left, right, left_dim, right_dim):
    return lax.dot_general(
        left, right, (((left_dim,), (right_dim,)), ((), ())), preferred_element_type=jnp.float32
    )


def low(value):
    return value.astype(jnp.bfloat16)


def layer_norm(rows, gain_vec, shift_vec):
    centred = rows - jnp.mean(rows, axis=-1, keepdims=True)
    spread = jnp.mean(centred * centred, axis=-1, keepdims=True)
    return centred * lax.rsqrt(spread + norm_eps) * gain_vec + shift_vec


def norm_back(rows, gain_vec, grads):
    centred = rows - jnp.mean(rows, axis=-1, keepdims=True)
    spread = jnp.mean(centred * centred, axis=-1, keepdims=True)
    inverse = lax.rsqrt(spread + norm_eps)
    xhat = centred * inverse
    e = grads * gain_vec
    back = inverse * (
        e
        - jnp.mean(e, axis=-1, keepdims=True)
        - xhat * jnp.mean(e * xhat, axis=-1, keepdims=True)
    )
    return back, grads * xhat


def gelu_tanh(value):
    return jax.nn.gelu(value, approximate=True)


MESH = pl.DeviceIdType.MESH
VMEM_BYTES = 64_000_000
COST = pl.CostEstimate(flops=20_000_000_000, transcendentals=0, bytes_accessed=100_000_000)
LOG2E = 1.0 / math.log(2.0)
TILE = 256
WIDE = 384


class Slab:
    def __init__(self, half_rows):
        self.half_rows = half_rows
        section = lax.axis_index("section")
        tensor = lax.axis_index("tensor")
        core = lax.rem(tensor, 2)
        self.core = core
        self.mine = self.around(section, tensor, core)
        self.theirs = self.around(section, tensor + 1 - 2 * core, 1 - core)
        self.mate = self.theirs[0]
        over = lax.rem(tensor + 2, 4)
        self.near, self.far = tensor, over
        self.mate_near, self.mate_far = self.mate[1], lax.rem(self.mate[1] + 2, 4)
        self.grid = self.places(section, self.near, self.far)
        self.mate_grid = self.places(section, self.mate_near, self.mate_far)
        self.across_y = self.grid[2]
        self.first, self.second = self.mine[1], self.mine[2]

    @staticmethod
    def places(section, near, far):
        flip = 1 - section
        return [(section, near), (flip, near), (section, far), (flip, far)]

    @staticmethod
    def around(section, tensor, core):
        over = lax.rem(tensor + 2, 4)
        turn = 1 - 2 * section
        first = (section + (1 - core) * turn, tensor + core * (over - tensor))
        second = (section + core * turn, tensor + (1 - core) * (over - tensor))
        return [(section, tensor), first, second, (1 - section, over)]

    def rows(self, ref, at):
        start = pl.multiple_of((2 * at[1] + at[0]) * self.half_rows, self.half_rows)
        return ref.at[pl.ds(start, self.half_rows)]

    def greet(self):
        barrier = pltpu.get_barrier_semaphore()
        for peer in (self.first, self.second, self.mate):
            pl.semaphore_signal(barrier, inc=1, device_id=named(peer), device_id_type=MESH)
        pl.semaphore_wait(barrier, 3)


def named(at):
    return {"section": at[0], "tensor": at[1]}


class Moves:
    def __init__(self, slab, send_sems, recv_sems):
        self.slab, self.send_sems, self.recv_sems = slab, send_sems, recv_sems
        self.sent = []

    def copy(self, src, dst, role, peer):
        return pltpu.make_async_remote_copy(
            src_ref=src,
            dst_ref=dst,
            send_sem=self.send_sems.at[role],
            recv_sem=self.recv_sems.at[role],
            device_id=named(peer),
            device_id_type=MESH,
        )

    def send(self, src, dst, role, peer):
        copy = self.copy(src, dst, role, peer)
        copy.start()
        self.sent.append(copy)

    def arrived(self, dst, role):
        self.copy(dst, dst, role, self.slab.mate).wait_recv()

    def drain(self):
        for copy in self.sent:
            copy.wait_send()


class Gather(Moves):
    def __init__(self, slab, whole, send_sems, recv_sems):
        super().__init__(slab, send_sems, recv_sems)
        self.whole = whole

    def pass_on(self, at, role, peer):
        part = self.slab.rows(self.whole, at)
        self.send(part, part, role, peer)

    def arrive(self, at, role):
        self.arrived(self.slab.rows(self.whole, at), role)

    def start(self):
        mine = self.slab.mine
        self.pass_on(mine[0], 0, mine[1])
        self.pass_on(mine[0], 3, self.slab.mate)

    def second(self):
        self.sent.pop(0).wait_send()
        self.pass_on(self.slab.mine[0], 1, self.slab.mine[2])

    def forward(self):
        mine, mate = self.slab.mine, self.slab.mate
        self.arrive(mine[1], 0)
        self.pass_on(mine[1], 2, mine[2])
        self.pass_on(mine[1], 4, mate)

    def to_mate(self):
        mine, mate = self.slab.mine, self.slab.mate
        self.arrive(mine[2], 1)
        self.pass_on(mine[2], 5, mate)
        self.arrive(mine[3], 2)
        self.pass_on(mine[3], 6, mate)

    def finish(self):
        for k in range(4):
            self.arrive(self.slab.theirs[k], 3 + k)
        self.drain()


class TileGather:
    def __init__(self, whole, send_sems, recv_sems):
        self.whole, self.send_sems, self.recv_sems = whole, send_sems, recv_sems
        self.tensor = lax.axis_index("tensor")
        self.over = lax.rem(self.tensor + 2, 4)
        self.mate = self.tensor + 1 - 2 * lax.rem(self.tensor, 2)
        self.micro, rows = whole.shape[0], whole.shape[1] // 4
        self.tile_rows = rows
        self.sent = []

    def tile(self, m, index):
        start = pl.multiple_of(index * self.tile_rows, self.tile_rows)
        return self.whole.at[m, pl.ds(start, self.tile_rows)]

    def copy(self, m, index, role, peer):
        part = self.tile(m, index)
        return remote(
            part, part, self.send_sems.at[m, role], self.recv_sems.at[m, role], {"tensor": peer}
        )

    def send(self, m, index, role, peer):
        copy = self.copy(m, index, role, peer)
        copy.start()
        self.sent.append(copy)

    def start(self):
        for m in range(self.micro):
            self.send(m, self.tensor, 0, self.over)
            self.send(m, self.tensor, 1, self.mate)

    def pass_on(self):
        for m in range(self.micro):
            self.copy(m, self.over, 0, self.over).wait_recv()
            self.send(m, self.over, 2, self.mate)

    def finish(self):
        for m in range(self.micro):
            self.copy(m, self.mate, 1, self.mate).wait_recv()
            self.copy(m, lax.rem(self.mate + 2, 4), 2, self.mate).wait_recv()

    def drain(self):
        for copy in self.sent:
            copy.wait_send()


class Scatter(Moves):
    def __init__(self, slab, terms, from_mate, outgoing, arrivals, send_sems, recv_sems):
        super().__init__(slab, send_sems, recv_sems)
        self.terms, self.from_mate, self.outgoing = terms, from_mate, outgoing
        self.relay, self.from_second, self.from_first = (arrivals.at[k] for k in range(3))

    def to_mate(self, at, role):
        self.send(self.slab.rows(self.terms, at), self.from_mate.at[role], role, self.slab.mate)

    def mate_far(self):
        self.to_mate(self.slab.mate_grid[3], 3)
        self.to_mate(self.slab.mate_grid[2], 1 + self.slab.core)

    def mate_near(self):
        self.to_mate(self.slab.mate_grid[1], 2 - self.slab.core)
        self.to_mate(self.slab.mate_grid[0], 0)

    def chip_sum(self, k, rows):
        part = self.slab.rows(self.terms, self.slab.mine[k])
        return part[rows].astype(jnp.float32) + self.from_mate[k, rows].astype(jnp.float32)

    def blocks(self):
        return [pl.ds(start, 32) for start in range(0, self.slab.half_rows, 32)]

    def hop(self, k, slot, dst, role, peer, ride=None):
        self.arrived(self.from_mate.at[k], k)
        if ride is not None:
            self.arrived(ride, 4)
        for rows in self.blocks():
            value = self.chip_sum(k, rows)
            if ride is not None:
                value = value + ride[rows].astype(jnp.float32)
            self.outgoing[slot, rows] = low(value)
        self.send(self.outgoing.at[slot], dst, role, peer)

    def far_hop(self):
        self.hop(3, 0, self.relay, 4, self.slab.second)

    def second_hop(self):
        self.hop(2, 1, self.from_second, 5, self.slab.second)

    def first_hop(self):
        self.hop(1, 2, self.from_first, 6, self.slab.first, self.relay)

    def finish(self):
        self.arrived(self.from_mate.at[0], 0)
        self.arrived(self.from_second, 5)
        self.arrived(self.from_first, 6)
        self.drain()

    def total(self, rows):
        other = self.from_second[rows].astype(jnp.float32) + self.from_first[rows].astype(
            jnp.float32
        )
        return self.chip_sum(0, rows) + other


def scatter_scratch(micro, seq, half_rows, width):
    return [
        pltpu.VMEM((micro, seq, width), jnp.bfloat16),
        pltpu.VMEM((micro, 4, half_rows, width), jnp.bfloat16),
        pltpu.VMEM((micro, 3, half_rows, width), jnp.bfloat16),
        pltpu.VMEM((micro, 3, half_rows, width), jnp.bfloat16),
        pltpu.SemaphoreType.DMA((micro, 7)),
        pltpu.SemaphoreType.DMA((micro, 7)),
    ]


def gather_scratch(micro, seq, width):
    return [
        pltpu.VMEM((micro, seq, width), jnp.bfloat16),
        pltpu.SemaphoreType.DMA((micro, 7)),
        pltpu.SemaphoreType.DMA((micro, 7)),
    ]


def make_scatters(slab, refs, micro):
    terms, from_mate, outgoing, arrivals, send_sems, recv_sems = refs
    return [
        Scatter(
            slab,
            terms.at[m],
            from_mate.at[m],
            outgoing.at[m],
            arrivals.at[m],
            send_sems.at[m],
            recv_sems.at[m],
        )
        for m in range(micro)
    ]


def make_gathers(slab, refs, micro):
    whole, send_sems, recv_sems = refs
    return [
        Gather(slab, whole.at[m], send_sems.at[m], recv_sems.at[m]) for m in range(micro)
    ]


def step_rows(i, size):
    return pl.ds(pl.multiple_of(i * size, size), size)


def repeat(count, body):
    def one(i, carry):
        body(i)
        return carry

    lax.fori_loop(0, count, one, 0)


def shut_keys(length, own_rows, full_rows, shape, dimension):
    place = lax.broadcasted_iota(jnp.int32, shape, dimension)
    step = jnp.zeros(shape, jnp.int32)
    for t in range(1, 4):
        step += (place >= t * full_rows).astype(jnp.int32)
    live = (place - step * full_rows < own_rows) & (
        place - step * (full_rows - own_rows) < length
    )
    return jnp.where(live, 0.0, masked_score)


def chip_rows(slab, far, compute, parts=1):
    tensor = (slab.far if far else slab.near) - slab.core
    size = 4 * slab.half_rows // parts

    def one(i):
        start = tensor * (2 * slab.half_rows) + i * size
        compute(pl.ds(pl.multiple_of(start, 2 * slab.half_rows), size))

    repeat(parts, one)


def open_gathers(gathers, fill, prepare):
    fill(0)
    gathers[0].start()
    fill(1)
    gathers[0].second()
    gathers[1].start()
    prepare()
    gathers[0].forward()
    gathers[1].second()


def widen(packed, wide):
    heads = packed.shape[1] // HEAD

    def block(i):
        rows = step_rows(i, 128)
        for h in range(heads):
            piece = packed[rows, h * HEAD : (h + 1) * HEAD]
            blank = jnp.zeros((128, LANES - HEAD), jnp.bfloat16)
            wide[rows, h * LANES : (h + 1) * LANES] = jnp.concatenate([piece, blank], axis=1)

    repeat(packed.shape[0] // 128, block)


def split_tail(packed, tails, up_cols):
    start = packed.shape[1] - LANES

    def block(i):
        rows = step_rows(i, 128)
        for j in range(2):
            piece = packed[rows, start + j * up_cols : start + (j + 1) * up_cols]
            blank = jnp.zeros((128, LANES - up_cols), jnp.bfloat16)
            tails[rows, j * LANES : (j + 1) * LANES] = jnp.concatenate([piece, blank], axis=1)

    repeat(packed.shape[0] // 128, block)


def up_dot(rows, packed, tails):
    main = (packed.shape[1] - LANES) // 2
    first = dot(rows, packed[:, :main], 1, 0)
    return jnp.concatenate([first, dot(rows, tails[:, :LANES], 1, 0)], axis=1)


def up_back(grads, packed, tails):
    main = (packed.shape[1] - LANES) // 2
    return dot(grads[:, :main], packed[:, :main], 1, 1) + dot(
        grads[:, main:], tails[:, :LANES], 1, 1
    )


def down_dot(active, packed, tails):
    main = (packed.shape[1] - LANES) // 2
    return dot(active[:, :main], packed[:, main : 2 * main], 1, 1) + dot(
        active[:, main:], tails[:, LANES:], 1, 1
    )


def down_back(rows, packed, tails):
    main = (packed.shape[1] - LANES) // 2
    first = dot(rows, packed[:, main : 2 * main], 1, 0)
    return jnp.concatenate([first, dot(rows, tails[:, LANES:], 1, 0)], axis=1)


def attn_forward_kernel(
    ready, at, layer, own_rows, rows_ref, vectors, bias_ref, lengths, packed_hbm, given_hbm, grads_ref,
    hidden_ref, lse_ref, normed_hbm, qkv_hbm, mixed_hbm, *rest
):
    micro, half_rows, width = rows_ref.shape
    gathered, gather_refs = rest[0], rest[0:3]
    scatter_refs = rest[3:9]
    terms = rest[3]
    packed, wide, qkv, mixed, load_sem, keep_sems, given_sems, all_grads, tile_send, tile_recv = rest[9:]
    vec, bias = vectors.at[layer], bias_ref[layer]
    seq = qkv.shape[1]
    pair = mixed.shape[2]
    heads = pair // LANES
    load = pltpu.make_async_copy(
        packed_hbm.at[:, at : at + packed.shape[1]], packed, load_sem
    )
    load.start()
    slab = Slab(half_rows)
    gathers = make_gathers(slab, gather_refs, micro)
    scatters = make_scatters(slab, scatter_refs, micro)
    given = [
        pltpu.make_async_copy(given_hbm.at[m], gathered.at[m], given_sems.at[m])
        for m in range(micro if ready else 0)
    ]
    for copy in given:
        copy.start()
    slab.greet()
    if ready:
        tiles = TileGather(all_grads, tile_send, tile_recv)
        for m in range(micro):
            own = tiles.tile(m, tiles.tensor)
            count = grads_ref.shape[1]
            own[:count] = grads_ref[m]
            own[count:] = jnp.zeros((tiles.tile_rows - count, width), jnp.bfloat16)
        tiles.start()

    def fill(m):
        own = slab.rows(gathered.at[m], slab.mine[0])
        for start in range(0, half_rows, 32):
            block = rows_ref[m, pl.ds(start, 32)].astype(jnp.float32)
            own[pl.ds(start, 32)] = low(layer_norm(block, vec[0:1], vec[2:3]))

    def prepare():
        load.wait()
        widen(packed, wide)

    if ready:
        prepare()
    else:
        open_gathers(gathers, fill, prepare)
    keeps = []

    def keep(src, dst, i):
        copy = pltpu.make_async_copy(src, dst, keep_sems.at[i])
        copy.start()
        keeps.append(copy)

    def project(m):
        def block(i):
            rows = step_rows(i, 4 * half_rows)
            out = dot(gathered[m, rows], wide[:, : 3 * pair], 1, 0)
            qkv[m, rows] = low(out + bias)

        repeat(seq // (4 * half_rows), block)

    def attend(m, rows):
        shut = shut_keys(lengths[m], own_rows, 2 * half_rows, (1, seq), 1)
        for h in range(heads):
            cols = slice(h * LANES, (h + 1) * LANES)
            q = qkv[m, rows, cols]
            k = qkv[m, :, pair + h * LANES : pair + (h + 1) * LANES]
            v = qkv[m, :, 2 * pair + h * LANES : 2 * pair + (h + 1) * LANES]
            scores = dot(q, k, 1, 1) * (score_scale * LOG2E) + shut
            top = jnp.max(scores, axis=-1, keepdims=True)
            exp_scores = jnp.exp2(scores - top)
            total = jnp.sum(exp_scores, axis=-1, keepdims=True)
            probs = low(exp_scores * (1.0 / total))
            mixed[m, rows, cols] = low(dot(probs, v, 1, 0))
            lse_ref[m, h, rows] = jnp.broadcast_to(
                top + jnp.log(total) * LOG2E, (2 * half_rows, LANES)
            )

    def output(m, rows):
        terms[m, rows] = low(dot(mixed[m, rows], wide[:, 3 * pair :], 1, 1))

    def close(m):
        scatters[m].finish()
        for rows in scatters[m].blocks():
            start = rows_ref[m, rows].astype(jnp.float32)
            hidden_ref[m, rows] = start + scatters[m].total(rows) + vec[5:6]

    def gathered_rows(m):
        if ready:
            given[m].wait()
            return
        gathers[m].to_mate()
        gathers[m].finish()
        keep(gathered.at[m], normed_hbm.at[m], m)

    gathered_rows(0)
    project(0)
    if not ready:
        gathers[1].forward()
    chip_rows(slab, True, lambda rows: attend(0, rows), 2)
    chip_rows(slab, True, lambda rows: output(0, rows))
    scatters[0].mate_far()
    gathered_rows(1)
    scatters[0].far_hop()
    chip_rows(slab, False, lambda rows: attend(0, rows), 2)
    chip_rows(slab, False, lambda rows: output(0, rows))
    scatters[0].mate_near()
    keep(qkv.at[0], qkv_hbm.at[0], 2)
    keep(mixed.at[0], mixed_hbm.at[0], 3)
    project(1)
    scatters[0].second_hop()
    scatters[0].first_hop()
    if ready:
        tiles.pass_on()
    chip_rows(slab, True, lambda rows: attend(1, rows), 2)
    chip_rows(slab, True, lambda rows: output(1, rows))
    scatters[1].mate_far()
    close(0)
    scatters[1].far_hop()
    if ready:
        tiles.finish()
        for m in range(micro):
            keep(all_grads.at[m], normed_hbm.at[m], m)
    chip_rows(slab, False, lambda rows: attend(1, rows), 2)
    chip_rows(slab, False, lambda rows: output(1, rows))
    scatters[1].mate_near()
    keep(qkv.at[1], qkv_hbm.at[1], 4)
    keep(mixed.at[1], mixed_hbm.at[1], 5)
    scatters[1].second_hop()
    scatters[1].first_hop()
    close(1)
    if ready:
        tiles.drain()
    for copy in keeps:
        copy.wait()


def ffn_forward_kernel(
    half_ff, at, layer, hidden_ref, vectors, up_biases, packed_hbm, out_ref, second_hbm, upper_hbm, *rest
):
    micro, half_rows, _ = hidden_ref.shape
    gathered, gather_refs = rest[0], rest[0:3]
    scatter_refs = rest[3:9]
    terms = rest[3]
    packed, tails, upper, load_sem, keep_sems = rest[9:]
    vec, up_bias = vectors.at[layer], up_biases.at[layer]
    _, ff = upper.shape[1:]
    load = pltpu.make_async_copy(
        packed_hbm.at[:, at : at + packed.shape[1]], packed, load_sem
    )
    load.start()
    slab = Slab(half_rows)
    gathers = make_gathers(slab, gather_refs, micro)
    scatters = make_scatters(slab, scatter_refs, micro)
    slab.greet()

    def fill(m):
        own = slab.rows(gathered.at[m], slab.mine[0])
        for start in range(0, half_rows, 32):
            block = hidden_ref[m, pl.ds(start, 32)]
            own[pl.ds(start, 32)] = low(layer_norm(block, vec[1:2], vec[6:7]))

    def prepare():
        load.wait()
        split_tail(packed, tails, half_ff - ff + LANES)

    open_gathers(gathers, fill, prepare)
    keeps = []

    def keep(src, dst, i):
        copy = pltpu.make_async_copy(src, dst, keep_sems.at[i])
        copy.start()
        keeps.append(copy)

    def compute(m, rows):
        value = up_dot(gathered[m, rows], packed, tails) + up_bias[...]
        upper[m, rows] = value
        active = low(gelu_tanh(value))
        terms[m, rows] = low(down_dot(active, packed, tails))

    def close(m):
        scatters[m].finish()
        for rows in scatters[m].blocks():
            out_ref[m, rows] = low(hidden_ref[m, rows] + scatters[m].total(rows) + vec[7:8])

    gathers[0].to_mate()
    gathers[0].finish()
    keep(gathered.at[0], second_hbm.at[0], 0)
    chip_rows(slab, True, lambda rows: compute(0, rows))
    scatters[0].mate_far()
    gathers[1].forward()
    scatters[0].far_hop()
    chip_rows(slab, False, lambda rows: compute(0, rows))
    scatters[0].mate_near()
    keep(upper.at[0], upper_hbm.at[0], 1)
    gathers[1].to_mate()
    scatters[0].second_hop()
    gathers[1].finish()
    keep(gathered.at[1], second_hbm.at[1], 2)
    chip_rows(slab, True, lambda rows: compute(1, rows))
    scatters[1].mate_far()
    scatters[0].first_hop()
    scatters[1].far_hop()
    chip_rows(slab, False, lambda rows: compute(1, rows))
    scatters[1].mate_near()
    keep(upper.at[1], upper_hbm.at[1], 3)
    scatters[1].second_hop()
    close(0)
    scatters[1].first_hop()
    close(1)
    for copy in keeps:
        copy.wait()


def ffn_backward_kernel(
    half_ff, at, layer, grad_ref, hidden_ref, vectors, second_hbm, upper_hbm, packed_hbm,
    out_ref, grads_ref, small_ref, up_bias_ref, *rest
):
    micro, half_rows, width = hidden_ref.shape
    gathered, gather_refs = rest[0], rest[0:3]
    scatter_refs = rest[3:9]
    terms = rest[3]
    packed, tails, second, upper, grad_upper, active, load_sems = rest[9:]
    vec = vectors.at[layer]
    seq, ff = upper.shape[1:]
    main = ff - LANES
    extra = half_ff - main
    load_packed = pltpu.make_async_copy(
        packed_hbm.at[:, at : at + packed.shape[1]], packed, load_sems.at[0]
    )
    load_packed.start()
    load_upper, load_second = [], []
    for m in range(micro):
        load_upper.append(
            pltpu.make_async_copy(upper_hbm.at[m], upper.at[m], load_sems.at[1 + m])
        )
        load_upper[m].start()
    for m in range(micro):
        load_second.append(
            pltpu.make_async_copy(second_hbm.at[m], second.at[m], load_sems.at[1 + micro + m])
        )
        load_second[m].start()
    slab = Slab(half_rows)
    gathers = make_gathers(slab, gather_refs, micro)
    scatters = make_scatters(slab, scatter_refs, micro)
    slab.greet()

    def fill(m):
        own = slab.rows(gathered.at[m], slab.mine[0])
        for start in range(0, half_rows, 32):
            own[pl.ds(start, 32)] = grad_ref[m, pl.ds(start, 32)]

    def prepare():
        small_ref[...] = jnp.zeros_like(small_ref)
        up_bias_ref[...] = jnp.zeros_like(up_bias_ref)
        load_packed.wait()
        split_tail(packed, tails, extra)

    open_gathers(gathers, fill, prepare)

    def compute(m, rows):
        value = upper[m, rows]
        square = value * value
        bent = jnp.tanh(GELU_A * value * (1.0 + GELU_B * square))
        half = 0.5 * (1.0 + bent)
        active[m, rows] = low(value * half)
        slope = half + (0.5 * GELU_A) * value * (1.0 - bent * bent) * (1.0 + 3.0 * GELU_B * square)
        grad_active = down_back(gathered[m, rows], packed, tails)
        grad = low(grad_active * slope)
        grad_upper[m, rows] = grad
        up_bias_ref[0:1] += jnp.sum(grad.astype(jnp.float32), axis=0, keepdims=True)
        terms[m, rows] = low(up_back(grad, packed, tails))

    def stacked(ref, cols=slice(None)):
        return ref[:, :, cols].reshape(micro * seq, -1)

    def weight_grads(first, last):
        def block(i):
            cols = step_rows(i, WIDE)
            up = dot(stacked(second, cols), stacked(grad_upper), 0, 0)
            down = dot(stacked(gathered, cols), stacked(active), 0, 0)
            grads_ref[cols, :main] = low(up[:, :main])
            grads_ref[cols, main : 2 * main] = low(down[:, :main])
            blank = jnp.zeros((WIDE, LANES - 2 * extra), jnp.float32)
            rest_cols = [up[:, main : main + extra], down[:, main : main + extra], blank]
            grads_ref[cols, 2 * main :] = low(jnp.concatenate(rest_cols, axis=1))

        repeat(last - first, lambda i: block(first + i))

    def close(m):
        scatters[m].finish()
        for rows in scatters[m].blocks():
            grad_normed = scatters[m].total(rows)
            back, gain_terms = norm_back(hidden_ref[m, rows], vec[1:2], grad_normed)
            grad_rows = grad_ref[m, rows].astype(jnp.float32)
            grad_hidden = grad_rows + back
            out_ref[m, rows] = grad_hidden
            branch = low(grad_hidden).astype(jnp.float32)
            for j, item in enumerate((gain_terms, grad_normed, grad_rows, branch)):
                small_ref[j : j + 1] += jnp.sum(item, axis=0, keepdims=True)

    gathers[0].to_mate()
    gathers[0].finish()
    load_upper[0].wait()
    chip_rows(slab, True, lambda rows: compute(0, rows))
    scatters[0].mate_far()
    gathers[1].forward()
    scatters[0].far_hop()
    chip_rows(slab, False, lambda rows: compute(0, rows))
    scatters[0].mate_near()
    gathers[1].to_mate()
    scatters[0].second_hop()
    gathers[1].finish()
    load_upper[1].wait()
    chip_rows(slab, True, lambda rows: compute(1, rows))
    scatters[1].mate_far()
    scatters[0].first_hop()
    scatters[1].far_hop()
    chip_rows(slab, False, lambda rows: compute(1, rows))
    scatters[1].mate_near()
    scatters[1].second_hop()
    for load in load_second:
        load.wait()
    blocks = width // WIDE
    weight_grads(0, blocks // 3)
    scatters[1].first_hop()
    close(0)
    weight_grads(blocks // 3, blocks)
    close(1)


def ffn_turn_kernel(
    half_ff, at, layer, hidden_ref, grad_ref, vectors, up_biases, given_hbm, packed_hbm,
    out_ref, grad_out_ref, grads_ref, small_ref, up_bias_ref, *rest
):
    micro, half_rows, width = hidden_ref.shape
    gathered, gather_refs = rest[0], rest[0:3]
    terms, back_terms = rest[3], rest[9]
    packed, tails, given, grad_upper, active, load_sem, given_sems = rest[15:]
    vec, up_bias = vectors.at[layer], up_biases.at[layer]
    seq, ff = active.shape[1:]
    main = ff - LANES
    extra = half_ff - main
    load = pltpu.make_async_copy(
        packed_hbm.at[:, at : at + packed.shape[1]], packed, load_sem
    )
    load.start()
    loads = [
        pltpu.make_async_copy(given_hbm.at[m], given.at[m], given_sems.at[m]) for m in range(micro)
    ]
    for copy in loads:
        copy.start()
    slab = Slab(half_rows)
    gathers = make_gathers(slab, gather_refs, micro)
    scatters = make_scatters(slab, rest[3:9], micro)
    backs = make_scatters(slab, rest[9:15], micro)
    slab.greet()

    def fill(m):
        own = slab.rows(gathered.at[m], slab.mine[0])
        for start in range(0, half_rows, 32):
            block = hidden_ref[m, pl.ds(start, 32)]
            own[pl.ds(start, 32)] = low(layer_norm(block, vec[1:2], vec[6:7]))

    def prepare():
        small_ref[...] = jnp.zeros_like(small_ref)
        up_bias_ref[...] = jnp.zeros_like(up_bias_ref)
        load.wait()
        split_tail(packed, tails, extra)

    open_gathers(gathers, fill, prepare)

    def compute(m, rows):
        value = up_dot(gathered[m, rows], packed, tails) + up_bias[...]
        square = value * value
        bent = jnp.tanh(GELU_A * value * (1.0 + GELU_B * square))
        half = 0.5 * (1.0 + bent)
        shown = low(value * half)
        active[m, rows] = shown
        slope = half + (0.5 * GELU_A) * value * (1.0 - bent * bent) * (1.0 + 3.0 * GELU_B * square)
        grad = low(down_back(given[m, rows], packed, tails) * slope)
        grad_upper[m, rows] = grad
        up_bias_ref[0:1] += jnp.sum(grad.astype(jnp.float32), axis=0, keepdims=True)
        back_terms[m, rows] = low(up_back(grad, packed, tails))
        terms[m, rows] = low(down_dot(shown, packed, tails))

    def stacked(ref, cols=slice(None)):
        return ref[:, :, cols].reshape(micro * seq, -1)

    def weight_grads(first, last):
        def block(i):
            cols = step_rows(i, WIDE)
            up = dot(stacked(gathered, cols), stacked(grad_upper), 0, 0)
            down = dot(stacked(given, cols), stacked(active), 0, 0)
            grads_ref[cols, :main] = low(up[:, :main])
            grads_ref[cols, main : 2 * main] = low(down[:, :main])
            blank = jnp.zeros((WIDE, LANES - 2 * extra), jnp.float32)
            rest_cols = [up[:, main : main + extra], down[:, main : main + extra], blank]
            grads_ref[cols, 2 * main :] = low(jnp.concatenate(rest_cols, axis=1))

        repeat(last - first, lambda i: block(first + i))

    def close_back(m):
        backs[m].finish()
        for rows in backs[m].blocks():
            grad_normed = backs[m].total(rows)
            back, gain_terms = norm_back(hidden_ref[m, rows], vec[1:2], grad_normed)
            grad_rows = grad_ref[m, rows].astype(jnp.float32)
            grad_hidden = grad_rows + back
            grad_out_ref[m, rows] = grad_hidden
            branch = low(grad_hidden).astype(jnp.float32)
            for j, item in enumerate((gain_terms, grad_normed, grad_rows, branch)):
                small_ref[j : j + 1] += jnp.sum(item, axis=0, keepdims=True)

    def close(m):
        scatters[m].finish()
        for rows in scatters[m].blocks():
            out_ref[m, rows] = low(hidden_ref[m, rows] + scatters[m].total(rows) + vec[7:8])

    gathers[0].to_mate()
    gathers[0].finish()
    loads[0].wait()
    chip_rows(slab, True, lambda rows: compute(0, rows))
    backs[0].mate_far()
    scatters[0].mate_far()
    gathers[1].forward()
    backs[0].far_hop()
    chip_rows(slab, False, lambda rows: compute(0, rows))
    backs[0].mate_near()
    scatters[0].mate_near()
    gathers[1].to_mate()
    backs[0].second_hop()
    gathers[1].finish()
    scatters[0].far_hop()
    scatters[0].second_hop()
    loads[1].wait()
    chip_rows(slab, True, lambda rows: compute(1, rows))
    backs[1].mate_far()
    scatters[1].mate_far()
    backs[0].first_hop()
    backs[1].far_hop()
    scatters[0].first_hop()
    chip_rows(slab, False, lambda rows: compute(1, rows))
    backs[1].mate_near()
    scatters[1].mate_near()
    backs[1].second_hop()
    scatters[1].far_hop()
    scatters[1].second_hop()
    blocks = width // WIDE
    weight_grads(0, blocks // 3)
    backs[1].first_hop()
    scatters[1].first_hop()
    close_back(0)
    weight_grads(blocks // 3, blocks)
    close_back(1)
    for m in range(micro):
        close(m)


def attn_backward_kernel(
    at, layer, own_rows, both_ways, grad_ref, rows_ref, vectors, lse, lengths,
    normed_hbm, qkv_hbm, mixed_hbm, packed_hbm, errand_hbm,
    out_ref, grads_ref, small_ref, bias_ref, errand_got, *rest
):
    micro, half_rows, width = grad_ref.shape
    gathered, gather_refs = rest[0], rest[0:3]
    scatter_refs = rest[3:9]
    terms = rest[3]
    packed, wide, normed, qkv, mixed, grad_mixed, grad_qkv, turned, shut = rest[9:18]
    low_probs, grad_scores, high_probs, errand_sems, load_sems = rest[18:]
    vec = vectors.at[layer]
    seq, pair = mixed.shape[1:]
    heads = pair // LANES
    load_packed = pltpu.make_async_copy(
        packed_hbm.at[:, at : at + packed.shape[1]], packed, load_sems.at[0]
    )
    load_packed.start()
    load_qkv, load_rest = [], []
    for m in range(micro):
        load_qkv.append(pltpu.make_async_copy(qkv_hbm.at[m], qkv.at[m], load_sems.at[1 + 3 * m]))
        load_qkv[m].start()
    for m in range(micro):
        for k, (src, dst) in enumerate(((mixed_hbm, mixed), (normed_hbm, normed))):
            load = pltpu.make_async_copy(src.at[m], dst.at[m], load_sems.at[2 + k + 3 * m])
            load.start()
            load_rest.append(load)
    slab = Slab(half_rows)
    gathers = make_gathers(slab, gather_refs, micro)
    scatters = make_scatters(slab, scatter_refs, micro)
    slab.greet()

    def fill(m):
        own = slab.rows(gathered.at[m], slab.mine[0])
        for start in range(0, half_rows, 32):
            own[pl.ds(start, 32)] = low(grad_ref[m, pl.ds(start, 32)])

    def head(h, part=0):
        return slice(part * pair + h * LANES, part * pair + (h + 1) * LANES)

    def ready_qkv(m):
        load_qkv[m].wait()
        shut[...] = shut_keys(lengths[m], own_rows, 2 * half_rows, (seq, LANES), 0)
        for h in range(heads):
            turned[m, h] = low(qkv[m, :, head(h, 1)].astype(jnp.float32).T)

    def find_probs(m, h):
        def block(i):
            rows = step_rows(i, TILE)
            keys, queries = qkv[m, :, head(h, 1)], qkv[m, rows, head(h)]
            closed = jnp.concatenate([shut[...]] * (TILE // LANES), axis=1)
            scores = dot(keys, queries, 1, 1) * (score_scale * LOG2E) + closed
            high_probs[m, h, :, rows] = jnp.exp2(scores - lse[m, h, rows].T[0:1])

        repeat(seq // TILE, block)

    errand = remote(
        errand_hbm,
        errand_got,
        errand_sems.at[0],
        errand_sems.at[1],
        {"section": 1 - lax.axis_index("section")},
    )
    sends_errand = (lax.axis_index("section") == 0) | both_ways
    gets_errand = (lax.axis_index("section") == 1) | both_ways

    def prepare():
        small_ref[...] = jnp.zeros_like(small_ref)
        bias_ref[...] = jnp.zeros_like(bias_ref)
        ready_qkv(0)
        find_probs(0, 0)

    open_gathers(gathers, fill, prepare)

    def mix_grads(m):
        def block(i):
            rows = step_rows(i, 4 * half_rows)
            grad_mixed[m, rows] = low(dot(gathered[m, rows], wide[:, 3 * pair :], 1, 0))

        repeat(seq // (4 * half_rows), block)

    def attend(m, h):
        def block(i):
            rows = step_rows(i, TILE)
            grads = grad_mixed[m, rows, head(h)]
            probs = high_probs[m, h, :, rows]
            grad_probs = dot(qkv[m, :, head(h, 2)], grads, 1, 1)
            inner = jnp.sum(grad_probs * probs, axis=0, keepdims=True)
            low_probs[:, rows] = low(probs)
            grad_scores[:, rows] = low(probs * (grad_probs - inner))

        repeat(seq // TILE, block)
        grad_keys = dot(grad_scores[...], qkv[m, :, head(h)], 1, 0)
        grad_qkv[m, :, head(h, 1)] = low(grad_keys * score_scale)
        grad_qkv[m, :, head(h, 2)] = low(dot(low_probs[...], grad_mixed[m, :, head(h)], 1, 0))
        turn = dot(turned[m, h], grad_scores[...], 1, 0).T
        grad_qkv[m, :, head(h)] = low(turn * score_scale)

    def back_project(m, rows):
        grads = grad_qkv[m, rows]
        terms[m, rows] = low(dot(grads, wide[:, : 3 * pair], 1, 1))
        for j, part in enumerate((0, 2)):
            piece = grads[:, part * pair : (part + 1) * pair].astype(jnp.float32)
            bias_ref[j : j + 1] += jnp.sum(piece, axis=0, keepdims=True)

    def stacked(ref, cols=slice(None)):
        return ref[:, :, cols].reshape(micro * seq, -1)

    def weight_grads(first, last):
        def block(i):
            cols = step_rows(i, WIDE)
            front = dot(stacked(normed, cols), stacked(grad_qkv), 0, 0)
            back = dot(stacked(gathered, cols), stacked(mixed), 0, 0)
            total = low(jnp.concatenate([front, back], axis=1))
            pieces = [total[:, h * LANES : h * LANES + HEAD] for h in range(4 * heads)]
            grads_ref[cols] = jnp.concatenate(pieces, axis=1)

        repeat(last - first, lambda i: block(first + i))

    def close(m):
        scatters[m].finish()
        for rows in scatters[m].blocks():
            grad_normed = scatters[m].total(rows)
            back, gain_terms = norm_back(
                rows_ref[m, rows].astype(jnp.float32), vec[0:1], grad_normed
            )
            out_ref[m, rows] = low(grad_ref[m, rows] + back)
            for j, item in enumerate((gain_terms, grad_normed)):
                small_ref[j : j + 1] += jnp.sum(item, axis=0, keepdims=True)

    load_packed.wait()
    widen(packed, wide)
    gathers[1].forward()
    gathers[0].to_mate()

    @pl.when(sends_errand)
    def _():
        errand.start()

    for h in range(1, heads):
        find_probs(0, h)
    gathers[0].finish()
    mix_grads(0)
    attend(0, 0)
    gathers[1].to_mate()
    for h in range(1, heads):
        attend(0, h)
    chip_rows(slab, True, lambda rows: back_project(0, rows))
    scatters[0].mate_far()
    ready_qkv(1)
    find_probs(1, 0)
    scatters[0].far_hop()
    chip_rows(slab, False, lambda rows: back_project(0, rows))
    scatters[0].mate_near()
    gathers[1].finish()
    mix_grads(1)
    scatters[0].second_hop()
    for h in range(1, heads):
        find_probs(1, h)
    scatters[0].first_hop()
    for h in range(heads):
        attend(1, h)
    chip_rows(slab, True, lambda rows: back_project(1, rows))
    scatters[1].mate_far()
    scatters[1].far_hop()
    chip_rows(slab, False, lambda rows: back_project(1, rows))
    scatters[1].mate_near()
    close(0)
    scatters[1].second_hop()
    for load in load_rest:
        load.wait()
    blocks = width // WIDE
    weight_grads(0, blocks // 3)
    scatters[1].first_hop()
    weight_grads(blocks // 3, blocks)
    close(1)

    @pl.when(sends_errand)
    def _():
        errand.wait_send()

    @pl.when(gets_errand)
    def _():
        errand.wait_recv()


def any_spec():
    return pl.BlockSpec(memory_space=pl.ANY)


def vmem_spec():
    return pl.BlockSpec(memory_space=pltpu.VMEM)


def shape_of(shape, dtype):
    return jax.ShapeDtypeStruct(shape, dtype)


def params(collective):
    return pltpu.CompilerParams(
        collective_id=collective, has_side_effects=True, vmem_limit_bytes=VMEM_BYTES
    )


def smem_spec():
    return pl.BlockSpec(memory_space=pltpu.SMEM)


def attn_forward(rows_low, vectors, bias, packed, at, layer, lengths, own_rows, given=None, grads=None):
    micro, half_rows, width = rows_low.shape
    seq = 8 * half_rows
    pair = bias.shape[2] // 3
    heads = pair // LANES
    low_type, high_type = jnp.bfloat16, jnp.float32
    hidden, lse, normed, qkv, mixed = pl.pallas_call(
        functools.partial(attn_forward_kernel, given is not None, at, layer, own_rows),
        out_shape=[
            shape_of((micro, half_rows, width), high_type),
            shape_of((micro, heads, seq, LANES), high_type),
            shape_of((micro, seq, width), low_type),
            shape_of((micro, seq, 3 * pair), low_type),
            shape_of((micro, seq, pair), low_type),
        ],
        in_specs=[vmem_spec()] * 3 + [smem_spec(), any_spec(), any_spec(), vmem_spec()],
        out_specs=[vmem_spec()] * 2 + [any_spec()] * 3,
        scratch_shapes=gather_scratch(micro, seq, width)
        + scatter_scratch(micro, seq, half_rows, width)
        + [
            pltpu.VMEM((width, 4 * heads * HEAD), low_type),
            pltpu.VMEM((width, 4 * pair), low_type),
            pltpu.VMEM((micro, seq, 3 * pair), low_type),
            pltpu.VMEM((micro, seq, pair), low_type),
            pltpu.SemaphoreType.DMA,
            pltpu.SemaphoreType.DMA((6,)),
            pltpu.SemaphoreType.DMA((micro,)),
            pltpu.VMEM((micro, seq if given is not None else 32, width), low_type),
            pltpu.SemaphoreType.DMA((micro, 3)),
            pltpu.SemaphoreType.DMA((micro, 3)),
        ],
        compiler_params=params(0 if given is None else 6),
        cost_estimate=COST,
        name="attn_forward",
    )(
        rows_low,
        vectors,
        bias,
        lengths,
        packed,
        packed if given is None else given,
        rows_low if grads is None else grads,
    )
    if given is None:
        return hidden, (normed, qkv, lse, mixed)
    return hidden, (given, qkv, lse, mixed), normed


def ffn_forward(hidden, vectors, up_biases, packed, at, layer, half_ff):
    micro, half_rows, width = hidden.shape
    seq = 8 * half_rows
    ff = up_biases.shape[2]
    packed_cols = 2 * ff - LANES
    low_type, high_type = jnp.bfloat16, jnp.float32
    out, second, upper = pl.pallas_call(
        functools.partial(ffn_forward_kernel, half_ff, at, layer),
        out_shape=[
            shape_of((micro, half_rows, width), low_type),
            shape_of((micro, seq, width), low_type),
            shape_of((micro, seq, ff), high_type),
        ],
        in_specs=[vmem_spec()] * 3 + [any_spec()],
        out_specs=[vmem_spec()] + [any_spec()] * 2,
        scratch_shapes=gather_scratch(micro, seq, width)
        + scatter_scratch(micro, seq, half_rows, width)
        + [
            pltpu.VMEM((width, packed_cols), low_type),
            pltpu.VMEM((width, 2 * LANES), low_type),
            pltpu.VMEM((micro, seq, ff), high_type),
            pltpu.SemaphoreType.DMA,
            pltpu.SemaphoreType.DMA((4,)),
        ],
        compiler_params=params(1),
        cost_estimate=COST,
        name="ffn_forward",
    )(hidden, vectors, up_biases, packed)
    return out, (second, upper)


def ffn_turn(hidden, grad_low, given, vectors, up_biases, packed, at, layer, half_ff):
    micro, half_rows, width = hidden.shape
    seq = 8 * half_rows
    ff = up_biases.shape[2]
    low_type, high_type = jnp.bfloat16, jnp.float32
    out, grad_hidden, grads, small, up_bias = pl.pallas_call(
        functools.partial(ffn_turn_kernel, half_ff, at, layer),
        out_shape=[
            shape_of((micro, half_rows, width), low_type),
            shape_of((micro, half_rows, width), high_type),
            shape_of((width, 2 * ff - LANES), low_type),
            shape_of((8, width), high_type),
            shape_of((8, ff), high_type),
        ],
        in_specs=[vmem_spec()] * 4 + [any_spec()] * 2,
        out_specs=[vmem_spec()] * 5,
        scratch_shapes=gather_scratch(micro, seq, width)
        + scatter_scratch(micro, seq, half_rows, width)
        + scatter_scratch(micro, seq, half_rows, width)
        + [
            pltpu.VMEM((width, 2 * ff - LANES), low_type),
            pltpu.VMEM((width, 2 * LANES), low_type),
            pltpu.VMEM((micro, seq, width), low_type),
            pltpu.VMEM((micro, seq, ff), low_type),
            pltpu.VMEM((micro, seq, ff), low_type),
            pltpu.SemaphoreType.DMA,
            pltpu.SemaphoreType.DMA((micro,)),
        ],
        compiler_params=params(7),
        cost_estimate=COST,
        name="ffn_turn",
    )(hidden, grad_low, vectors, up_biases, given, packed)
    return out, grad_hidden, grads, small, up_bias[:1]


def ffn_backward(grad_low, hidden, kept, vectors, packed, at, layer, half_ff):
    second, upper = kept
    micro, half_rows, width = hidden.shape
    seq, ff = upper.shape[1:]
    low_type, high_type = jnp.bfloat16, jnp.float32
    grad_hidden, grads, small, up_bias = pl.pallas_call(
        functools.partial(ffn_backward_kernel, half_ff, at, layer),
        out_shape=[
            shape_of((micro, half_rows, width), high_type),
            shape_of((width, 2 * ff - LANES), low_type),
            shape_of((8, width), high_type),
            shape_of((8, ff), high_type),
        ],
        in_specs=[vmem_spec()] * 3 + [any_spec()] * 3,
        out_specs=[vmem_spec()] * 4,
        scratch_shapes=gather_scratch(micro, seq, width)
        + scatter_scratch(micro, seq, half_rows, width)
        + [
            pltpu.VMEM((width, 2 * ff - LANES), low_type),
            pltpu.VMEM((width, 2 * LANES), low_type),
            pltpu.VMEM((micro, seq, width), low_type),
            pltpu.VMEM((micro, seq, ff), high_type),
            pltpu.VMEM((micro, seq, ff), low_type),
            pltpu.VMEM((micro, seq, ff), low_type),
            pltpu.SemaphoreType.DMA((1 + 2 * micro,)),
        ],
        compiler_params=params(2),
        cost_estimate=COST,
        name="ffn_backward",
    )(grad_low, hidden, vectors, second, upper, packed)
    return grad_hidden, grads, small, up_bias[:1]


def attn_backward(
    grad_hidden, rows_low, kept, vectors, packed, at, layer, lengths, own_rows, errand, both_ways
):
    normed, qkv, lse, mixed = kept
    micro, half_rows, width = grad_hidden.shape
    seq, pair = mixed.shape[1:]
    heads = pair // LANES
    low_type, high_type = jnp.bfloat16, jnp.float32
    out, grads, small, bias, got = pl.pallas_call(
        functools.partial(attn_backward_kernel, at, layer, own_rows, both_ways),
        out_shape=[
            shape_of((micro, half_rows, width), low_type),
            shape_of((width, 4 * heads * HEAD), low_type),
            shape_of((8, width), high_type),
            shape_of((8, pair), high_type),
            shape_of(errand.shape, errand.dtype),
        ],
        in_specs=[vmem_spec()] * 4 + [smem_spec()] + [any_spec()] * 5,
        out_specs=[vmem_spec()] * 4 + [any_spec()],
        scratch_shapes=gather_scratch(micro, seq, width)
        + scatter_scratch(micro, seq, half_rows, width)
        + [
            pltpu.VMEM((width, 4 * heads * HEAD), low_type),
            pltpu.VMEM((width, 4 * pair), low_type),
            pltpu.VMEM((micro, seq, width), low_type),
            pltpu.VMEM((micro, seq, 3 * pair), low_type),
            pltpu.VMEM((micro, seq, pair), low_type),
            pltpu.VMEM((micro, seq, pair), low_type),
            pltpu.VMEM((micro, seq, 3 * pair), low_type),
            pltpu.VMEM((micro, heads, LANES, seq), low_type),
            pltpu.VMEM((seq, LANES), high_type),
            pltpu.VMEM((seq, seq), low_type),
            pltpu.VMEM((seq, seq), low_type),
            pltpu.VMEM((micro, heads, seq, seq), high_type),
            pltpu.SemaphoreType.DMA((2,)),
            pltpu.SemaphoreType.DMA((1 + 3 * micro,)),
        ],
        compiler_params=params(3 + 5 * layer),
        cost_estimate=COST,
        name="attn_backward",
    )(grad_hidden, rows_low, vectors, lse, lengths, normed, qkv, mixed, packed, errand)
    return out, grads, small, bias, got


def slab_peers():
    section, tensor = lax.axis_index("section"), lax.axis_index("tensor")
    peers = []
    for role in range(1, 8):
        far, step = role // 4, role % 4
        other = section + far * (1 - 2 * section)
        to = (other, lax.rem(tensor + step, 4))
        source = (other, lax.rem(tensor + 4 - step, 4))
        peers.append((role, to, source))
    return peers


def column_peers(count):
    here = lax.axis_index("dp")
    return [
        (step, lax.rem(here + step, count), lax.rem(here + count - step, count))
        for step in range(1, count)
    ]


def greet_all(count):
    barrier = pltpu.get_barrier_semaphore()
    for _, to, _ in slab_peers():
        pl.semaphore_signal(barrier, inc=1, device_id=named(to), device_id_type=MESH)
    for _, to, _ in column_peers(count):
        pl.semaphore_signal(barrier, inc=1, device_id={"dp": to}, device_id_type=MESH)
    pl.semaphore_wait(barrier, 7 + count - 1)


def remote(src, dst, send_sem, recv_sem, peer):
    return pltpu.make_async_remote_copy(
        src_ref=src,
        dst_ref=dst,
        send_sem=send_sem,
        recv_sem=recv_sem,
        device_id=peer,
        device_id_type=MESH,
    )


def prologue_kernel(
    count, heads, qkv_ref, out_ref_t, up_ref_in, down_ref_t, gains_ref, shifts_ref, up_bias, rows_ref,
    first_hbm, normed_hbm, attn_ref, ff_zero_hbm, ff_one_hbm, out_ref, up_ref, bias_ref,
    attn_parts, ff_parts, up_halves, mine_ref, all_rows, line, ff_line, column, slab, up_got,
    rows_send, rows_recv, column_send, column_recv, slab_send, slab_recv, swap_send, swap_recv,
    right_send, right_recv, left_send, left_recv, out_sems,
):
    section, tensor, here = (lax.axis_index(name) for name in ("section", "tensor", "dp"))
    width = out_ref.shape[2]
    chunk = width // (4 * count)
    rows = attn_parts.shape[1]
    micro, own_rows = rows_ref.shape[:2]
    pieces = swap_send.shape[0] - 2
    size = rows // pieces
    other = {"section": 1 - section}
    pair = heads * LANES
    pair_cols = heads * HEAD
    half_ff = up_ref_in.shape[1] // 2
    main = half_ff // LANES * LANES
    extra = half_ff - main
    greet_all(count)
    for half in range(2):
        span = slice(half * pair_cols, (half + 1) * pair_cols)
        parts = [qkv_ref[k, :, span] for k in range(3)] + [out_ref_t[:, span]]
        attn_parts[half] = jnp.concatenate(parts, axis=1)
    keep_slot = jnp.where(section == 0, here, count)
    send_slot = jnp.where(section == 0, here, count)
    got_slot = jnp.where(section == 0, count, here)
    sent = []
    for p in range(pieces):
        span = pl.ds(p * size, size)
        copy = remote(
            attn_parts.at[1 - section, span],
            line.at[send_slot, span],
            swap_send.at[p],
            swap_recv.at[p],
            other,
        )
        copy.start()
        sent.append(copy)
    line[keep_slot] = attn_parts[section]
    mine_ref[...] = jnp.zeros_like(mine_ref)
    gains = gains_ref.shape[0]
    mine_ref[:gains, :chunk] = gains_ref[...]
    mine_ref[gains:, :chunk] = shifts_ref[...]
    column[here] = mine_ref[...]
    for step, to, _ in column_peers(count):
        copy = remote(
            mine_ref, column.at[here], column_send.at[step], column_recv.at[step], {"dp": to}
        )
        copy.start()
        sent.append(copy)

    def swapped(p):
        got = line.at[got_slot, pl.ds(p * size, size)]
        remote(got, got, swap_send.at[p], swap_recv.at[p], other).wait_recv()

    def hop(step, p, way, finish=False):
        origin = here - way * step
        sends, recvs = (right_send, right_recv) if way == 1 else (left_send, left_recv)
        inside = (origin >= 0) if way == 1 else (origin < count)
        onward = (here + 1 < count) if way == 1 else (here > 0)
        slot = line.at[jnp.clip(origin, 0, count - 1), pl.ds(p * size, size)]
        target = jnp.clip(here + way, 0, count - 1)
        if step > 0 and not finish:

            @pl.when(inside)
            def _():
                remote(slot, slot, sends.at[step, p], recvs.at[step, p], {"dp": target}).wait_recv()

        if step + 1 < count:

            @pl.when(inside & onward)
            def _():
                copy = remote(
                    slot, slot, sends.at[step, p], recvs.at[step + 1, p], {"dp": target}
                )
                if finish:
                    copy.wait_send()
                else:
                    copy.start()

    def hops(step):
        for p in range(pieces):
            for way in (1, -1):
                hop(step, p, way)

    for step, _, source in column_peers(count):
        slot = column.at[source]
        remote(slot, slot, column_send.at[step], column_recv.at[step], {"dp": source}).wait_recv()
    for role, to, _ in slab_peers():
        copy = remote(
            column, slab.at[section, tensor], slab_send.at[role], slab_recv.at[role], named(to)
        )
        copy.start()
        sent.append(copy)
    slab[section, tensor] = column[...]
    for p in range(pieces):

        @pl.when(section == 1)
        def _():
            swapped(p)

        for way in (1, -1):
            hop(0, p, way)
    blank = jnp.zeros((rows, LANES - 2 * extra), jnp.bfloat16)
    up_halves[...] = jnp.zeros_like(up_halves)
    for half in range(2):
        start = half * half_ff
        up_halves[half, :, :half_ff] = up_bias[:, start : start + half_ff]
        ff_parts[half, :, :main] = up_ref_in[:, start : start + main]
        ff_parts[half, :, main : 2 * main] = down_ref_t[:, start : start + main]
        span = slice(start + main, start + half_ff)
        ff_parts[half, :, 2 * main :] = jnp.concatenate(
            [up_ref_in[:, span], down_ref_t[:, span], blank], axis=1
        )
    ff_swap = remote(
        ff_parts.at[1 - section],
        ff_line.at[section],
        swap_send.at[pieces],
        swap_recv.at[pieces],
        other,
    )
    up_swap = remote(
        up_halves.at[1 - section],
        up_got.at[section],
        swap_send.at[pieces + 1],
        swap_recv.at[pieces + 1],
        other,
    )
    up_swap.start()
    for role, _, source in slab_peers():
        slot = slab.at[source[0], source[1]]
        remote(slot, slot, slab_send.at[role], slab_recv.at[role], named(source)).wait_recv()
    ff_swap.start()
    for layer in range(2):
        for part in range(4 * count):
            piece = slab[layer, part % 4, part // 4]
            out_ref[layer, :, part * chunk : (part + 1) * chunk] = piece[:, :chunk]
    tiles = TileGather(all_rows, rows_send, rows_recv)
    for m in range(micro):
        own = tiles.tile(m, tensor)
        for begin in range(0, own_rows, 32):
            end = min(begin + 32, own_rows)
            block = rows_ref[m, begin:end].astype(jnp.float32)
            own[begin:end] = low(layer_norm(block, out_ref[0, 0:1], out_ref[0, 2:3]))
        own[own_rows:] = jnp.zeros((tiles.tile_rows - own_rows, width), jnp.bfloat16)
    tiles.start()
    hops(1)
    start = (2 * tensor + section) * pair_cols
    for layer in range(2):
        turned = pltpu.roll(out_ref[layer], lax.rem(width - start, width), 1)
        empty = jnp.zeros((1, LANES - HEAD), jnp.float32)
        for part, row in ((0, 3), (2, 4)):
            for h in range(heads):
                at = part * pair + h * LANES
                piece = turned[row : row + 1, h * HEAD : (h + 1) * HEAD]
                bias_ref[layer, :, at : at + LANES] = jnp.concatenate([piece, empty], 1)
        bias_ref[layer, :, pair : 2 * pair] = jnp.zeros((1, pair), jnp.float32)
    up_ref[section] = up_halves[section]
    outs = []

    def put(src, dst, i):
        copy = pltpu.make_async_copy(src, dst, out_sems.at[i])
        copy.start()
        outs.append(copy)

    def put_ff(src, section_of_first, i):
        for layer, dst in enumerate((ff_zero_hbm, ff_one_hbm)):
            here_too = layer if section_of_first == 0 else 1 - layer

            @pl.when(section == here_too)
            def _():
                pltpu.make_async_copy(src, dst, out_sems.at[i]).start()

        outs.append(pltpu.make_async_copy(src, ff_zero_hbm, out_sems.at[i]))

    put_ff(ff_parts.at[section], 0, count)
    for step in range(2, count):
        hops(step)
        if step == 2:
            tiles.pass_on()
    if count <= 2:
        tiles.pass_on()
    for p in range(pieces):

        @pl.when(section == 0)
        def _():
            swapped(p)

    for at in range(count):
        put(line.at[at], first_hbm.at[pl.ds(at * rows, rows)], at)
    attn_ref[...] = line[count]
    got = up_got.at[1 - section]
    remote(got, got, swap_send.at[pieces + 1], swap_recv.at[pieces + 1], other).wait_recv()
    up_ref[1 - section] = up_got[1 - section]
    tiles.finish()
    put(all_rows, normed_hbm, count + 2)
    ff_got = ff_line.at[1 - section]
    remote(ff_got, ff_got, swap_send.at[pieces], swap_recv.at[pieces], other).wait_recv()
    put_ff(ff_got, 1, count + 1)
    for step in range(count):
        for p in range(pieces):
            for way in (1, -1):
                hop(step, p, way, True)
    for copy in sent + [ff_swap, up_swap]:
        copy.wait_send()
    tiles.drain()
    for copy in outs:
        copy.wait()


def prologue(qkv, out_t, up, down_t, gains, shifts, up_bias, rows_low, count, heads, tile_rows):
    part_rows = qkv.shape[1]
    micro, _, width = rows_low.shape
    vector_rows = gains.shape[0] + shifts.shape[0]
    half_ff = up.shape[1] // 2
    ff_wide = round_up(half_ff, LANES)
    attn_shape = (part_rows, 4 * heads * HEAD)
    ff_shape = (2, part_rows, 2 * ff_wide - LANES)
    all_rows = (micro, 4 * tile_rows, width)
    pieces = 3 if part_rows % 96 == 0 else 1
    low_type, high_type = jnp.bfloat16, jnp.float32
    dma = pltpu.SemaphoreType.DMA
    return pl.pallas_call(
        functools.partial(prologue_kernel, count, heads),
        out_shape=[
            shape_of((count * part_rows, attn_shape[1]), low_type),
            shape_of(all_rows, low_type),
            shape_of(attn_shape, low_type),
            shape_of(ff_shape[1:], low_type),
            shape_of(ff_shape[1:], low_type),
            shape_of((2, vector_rows, width), high_type),
            shape_of((2, 1, ff_wide), high_type),
            shape_of((2, 1, 3 * heads * LANES), high_type),
        ],
        in_specs=[vmem_spec()] * 8,
        out_specs=[any_spec()] * 2 + [vmem_spec()] + [any_spec()] * 2 + [vmem_spec()] * 3,
        scratch_shapes=[
            pltpu.VMEM((2,) + attn_shape, low_type),
            pltpu.VMEM(ff_shape, low_type),
            pltpu.VMEM((2, 1, ff_wide), high_type),
            pltpu.VMEM((vector_rows, LANES), high_type),
            pltpu.VMEM(all_rows, low_type),
            pltpu.VMEM((count + 1,) + attn_shape, low_type),
            pltpu.VMEM(ff_shape, low_type),
            pltpu.VMEM((count, vector_rows, LANES), high_type),
            pltpu.VMEM((2, 4, count, vector_rows, LANES), high_type),
            pltpu.VMEM((2, 1, ff_wide), high_type),
            dma((micro, 3)),
            dma((micro, 3)),
            dma((count,)),
            dma((count,)),
            dma((8,)),
            dma((8,)),
            dma((pieces + 2,)),
            dma((pieces + 2,)),
            dma((count, pieces)),
            dma((count, pieces)),
            dma((count, pieces)),
            dma((count, pieces)),
            dma((count + 3,)),
        ],
        compiler_params=params(4),
        cost_estimate=COST,
        name="prologue",
    )(qkv, out_t, up, down_t, gains, shifts, up_bias, rows_low)


def home_kernel(
    count, chunk, attn_zero, attn_one, ff_zero, ff_one, biases_in, ups_in,
    ff_sum_hbm, attn_sum_hbm, rows_hbm,
    out_ref, up_ref, ff_got_hbm, attn_got_hbm, rows_got_hbm,
    parts, ups, slab, column, up_pair, up_column, total,
    column_send, column_recv, slab_send, slab_recv, up_sems, up_column_send, up_column_recv, far_send, far_recv,
):
    section, tensor, here = (lax.axis_index(name) for name in ("section", "tensor", "dp"))
    width = attn_zero.shape[1]
    heads = biases_in.shape[2] // LANES
    other = {"section": 1 - section}
    greet_all(count)
    parts[...] = jnp.zeros_like(parts)
    start = (2 * tensor + section) * (heads * HEAD)
    for layer, (attn, ff) in enumerate(((attn_zero, ff_zero), (attn_one, ff_one))):
        bias = biases_in[layer]
        blank = jnp.zeros((8, width - heads * HEAD), jnp.float32)
        pieces = [bias[:, h * LANES : h * LANES + HEAD] for h in range(heads)]
        placed = pltpu.roll(jnp.concatenate(pieces + [blank], 1), start, 1)
        whole = jnp.concatenate(
            [attn[0:1], ff[0:1], attn[1:2], placed[0:2], ff[3:4], ff[1:2], ff[2:3]], axis=0
        )
        for part in range(4 * count):
            piece = whole[:, part * chunk : (part + 1) * chunk]
            parts[layer, part % 4, part // 4, :, :chunk] = piece
        ups[layer] = ups_in[layer]
    sent = []

    def send(src, dst, send_sem, recv_sem, peer):
        copy = remote(src, dst, send_sem, recv_sem, peer)
        copy.start()
        sent.append(copy)

    send(ups.at[1 - section], up_pair.at[section], up_sems.at[0], up_sems.at[1], other)
    for role, to, _ in slab_peers():
        send(
            parts.at[to[0], to[1]], slab.at[role], slab_send.at[role], slab_recv.at[role], named(to)
        )
    far_rows = remote(rows_hbm, rows_got_hbm, far_send.at[0], far_recv.at[0], other)
    far_ff = remote(ff_sum_hbm, ff_got_hbm, far_send.at[1], far_recv.at[1], other)
    far_attn = remote(attn_sum_hbm, attn_got_hbm, far_send.at[2], far_recv.at[2], other)
    one_way = ((far_ff, 1), (far_attn, 0))
    far_rows.start()
    for copy, source in one_way:
        pl.when(section == source)(copy.start)
    up_pair[section] = ups[section]
    value = parts[section, tensor]
    for role, _, source in slab_peers():
        slot = slab.at[role]
        remote(slot, slot, slab_send.at[role], slab_recv.at[role], named(source)).wait_recv()
        value = value + slab[role]
    total[...] = value
    for step, to, _ in column_peers(count):
        send(total.at[to], column.at[step], column_send.at[step], column_recv.at[step], {"dp": to})
    got = up_pair.at[1 - section]
    remote(got, got, up_sems.at[0], up_sems.at[1], other).wait_recv()
    for step, to, _ in column_peers(count):
        send(
            up_pair, up_column.at[here], up_column_send.at[step], up_column_recv.at[step], {"dp": to}
        )
    up_column[here] = up_pair[...]
    result = total[here]
    for step, _, source in column_peers(count):
        slot = column.at[step]
        remote(slot, slot, column_send.at[step], column_recv.at[step], {"dp": source}).wait_recv()
        result = result + column[step]
    out_ref[...] = result
    for step, _, source in column_peers(count):
        slot = up_column.at[source]
        remote(
            slot, slot, up_column_send.at[step], up_column_recv.at[step], {"dp": source}
        ).wait_recv()
    value = up_column[0]
    for at in range(1, count):
        value = value + up_column[at]
    up_ref[...] = value
    far_rows.wait()
    for copy, source in one_way:
        pl.when(section == source)(copy.wait_send)
        pl.when(section != source)(copy.wait_recv)
    for copy in sent:
        copy.wait_send()


def home(attn_small, ff_small, bias_grads, up_grads, ff_sum, attn_sum, rows, count, chunk):
    vector_rows, lanes = 8, LANES
    up_shape = up_grads.shape[1:]
    dma = pltpu.SemaphoreType.DMA
    high_type = jnp.float32
    return pl.pallas_call(
        functools.partial(home_kernel, count, chunk),
        out_shape=[
            shape_of((vector_rows, lanes), high_type),
            shape_of((2,) + up_shape, high_type),
            shape_of(ff_sum.shape, ff_sum.dtype),
            shape_of(attn_sum.shape, attn_sum.dtype),
            shape_of(rows.shape, rows.dtype),
        ],
        in_specs=[vmem_spec()] * 6 + [any_spec()] * 3,
        out_specs=[vmem_spec()] * 2 + [any_spec()] * 3,
        scratch_shapes=[
            pltpu.VMEM((2, 4, count, vector_rows, lanes), high_type),
            pltpu.VMEM((2,) + up_shape, high_type),
            pltpu.VMEM((8, count, vector_rows, lanes), high_type),
            pltpu.VMEM((count, vector_rows, lanes), high_type),
            pltpu.VMEM((2,) + up_shape, high_type),
            pltpu.VMEM((count, 2) + up_shape, high_type),
            pltpu.VMEM((count, vector_rows, lanes), high_type),
            dma((count,)),
            dma((count,)),
            dma((8,)),
            dma((8,)),
            dma((2,)),
            dma((count,)),
            dma((count,)),
            dma((3,)),
            dma((3,)),
        ],
        compiler_params=params(5),
        cost_estimate=COST,
        name="home",
    )(*attn_small, *ff_small, bias_grads, up_grads, ff_sum, attn_sum, rows)


def finish_kernel(
    ff_zero, ff_one, ff_zero_got, ff_one_got, attn_zero, attn_one, attn_one_got,
    qkv_ref, out_ref, up_ref, down_ref, attn_zero_got, send_sem, recv_sem,
):
    section = lax.axis_index("section")
    first = section == 0
    other = {"section": 1 - section}
    barrier = pltpu.get_barrier_semaphore()
    pl.semaphore_signal(barrier, inc=1, device_id=other, device_id_type=MESH)
    pl.semaphore_wait(barrier, 1)
    copy = remote(attn_zero, attn_zero_got, send_sem, recv_sem, other)

    @pl.when(section == 1)
    def _():
        copy.start()
        attn_zero_got[...] = attn_zero[...]

    rows = up_ref.shape[0]
    half_ff = up_ref.shape[1] // 2
    main = half_ff // LANES * LANES
    extra = half_ff - main
    pair_cols = qkv_ref.shape[2] // 2
    size = 96 if rows % 96 == 0 else rows

    def ff_block(i):
        at = step_rows(i, size)
        halves = (
            jnp.where(first, ff_zero[at], ff_one_got[at]),
            jnp.where(first, ff_zero_got[at], ff_one[at]),
        )
        for k, ref in enumerate((up_ref, down_ref)):
            pieces = []
            for half in halves:
                start = 2 * main + k * extra
                pieces += [half[:, k * main : (k + 1) * main], half[:, start : start + extra]]
            ref[at] = jnp.concatenate(pieces, axis=1).astype(jnp.float32)

    repeat(rows // size, ff_block)

    @pl.when(first)
    def _():
        copy.wait_recv()

    def attn_block(i):
        at = step_rows(i, size)
        halves = (
            jnp.where(first, attn_zero[at], attn_one_got[at]),
            jnp.where(first, attn_zero_got[at], attn_one[at]),
        )
        for k in range(4):
            span = slice(k * pair_cols, (k + 1) * pair_cols)
            whole = jnp.concatenate([half[:, span] for half in halves], axis=1)
            whole = whole.astype(jnp.float32)
            if k < 3:
                qkv_ref[k, at] = whole
            else:
                out_ref[at] = whole

    repeat(rows // size, attn_block)

    @pl.when(section == 1)
    def _():
        copy.wait_send()


def finish(ff_sums, ff_got, attn_sums, attn_got, head_cols, ff_cols):
    rows = ff_sums[0].shape[0]
    high_type = jnp.float32
    return pl.pallas_call(
        finish_kernel,
        out_shape=[
            shape_of((3, rows, head_cols), high_type),
            shape_of((rows, head_cols), high_type),
            shape_of((rows, ff_cols), high_type),
            shape_of((rows, ff_cols), high_type),
        ],
        in_specs=[vmem_spec()] * 7,
        out_specs=[vmem_spec()] * 4,
        scratch_shapes=[
            pltpu.VMEM(attn_sums[0].shape, attn_sums[0].dtype),
            pltpu.SemaphoreType.DMA,
            pltpu.SemaphoreType.DMA,
        ],
        compiler_params=params(9),
        cost_estimate=COST,
        name="finish",
    )(*ff_sums, *ff_got, *attn_sums, attn_got)


def shards(
    section_input,
    final_cotangent,
    lengths,
    qkv_weight,
    out_weight,
    up_weight,
    down_weight,
    norm_gains,
    biases,
    up_bias,
):
    here = lax.axis_index("section")
    sections = lax.axis_size("section")
    micro, _, own_rows, _ = section_input.shape
    head_cols = qkv_weight.shape[3]
    pair_cols = head_cols // sections
    heads = pair_cols // HEAD
    ff_cols = up_weight.shape[2]
    half_ff = ff_cols // sections
    half_rows = round_up(-(-own_rows // sections), 32)
    full_rows = half_rows * sections

    def by_layer(mine, other):
        return [jnp.where(here == 0, mine, other), jnp.where(here == 0, other, mine)]

    count = lax.axis_size("dp")
    chunk = norm_gains.shape[2]
    first, normed, attn_part, ff_zero, ff_one, vectors, up_biases, bias_qv = prologue(
        qkv_weight[0],
        out_weight[0].T,
        up_weight[0],
        down_weight[0].T,
        norm_gains[0],
        biases[0],
        up_bias,
        section_input[:, 0],
        count,
        heads,
        full_rows,
    )

    def gather_column(part):
        return lax.all_gather(part, "dp", axis=0, tiled=True)

    ff_first = gather_column(ff_zero)
    attn_packed = [(first, 0), (gather_column(attn_part), 0)]
    ff_packed = [(ff_first, 0), (gather_column(ff_one), 0)]
    lengths_here = lengths.reshape(micro)

    def my_rows(value):
        padded = jnp.pad(value[:, 0], [(0, 0), (0, full_rows - own_rows), (0, 0)])
        return lax.dynamic_slice_in_dim(padded, here * half_rows, half_rows, 1)

    def whole_rows(first, second, got):
        low_half, high_half = by_layer(jnp.where(here == 0, first, second), got)
        return jnp.concatenate([low_half, high_half], 1)[:, None, :own_rows]

    rows = my_rows(section_input)
    inputs, hiddens, attn_kept = [], [], []
    for layer in range(2):
        inputs.append(rows)
        operands = (rows, vectors, bias_qv, *attn_packed[layer], layer, lengths_here, own_rows)
        if layer == 0:
            hidden, kept, grads_all = attn_forward(*operands, normed, final_cotangent[:, 0])
        else:
            hidden, kept = attn_forward(*operands)
        hiddens.append(hidden)
        attn_kept.append(kept)
        if layer == 0:
            rows, ff_kept = ffn_forward(hidden, vectors, up_biases, *ff_packed[0], 0, half_ff)

    attn_sums, ff_sums, up_sums, input_grads = {}, {}, {}, {}
    attn_small, ff_small, bias_grads, errands = {}, {}, {}, {}
    for layer in (1, 0):
        if layer == 1:
            last, grad_hidden, ff_grad, ff_small[1], up_sums[1] = ffn_turn(
                hiddens[1],
                my_rows(final_cotangent),
                grads_all,
                vectors,
                up_biases,
                *ff_packed[1],
                1,
                half_ff,
            )
        else:
            grad_hidden, ff_grad, ff_small[0], up_sums[0] = ffn_backward(
                grads, hiddens[0], ff_kept, vectors, *ff_packed[0], 0, half_ff
            )
        ff_sums[layer] = lax.psum_scatter(ff_grad, "dp", scatter_dimension=0, tiled=True)
        if layer == 1:
            errand, both_ways = jnp.where(here == 0, last, rows), True
        else:
            errand, both_ways = ff_sums[1], False
        grads, attn_grad, attn_small[layer], bias_grads[layer], got = attn_backward(
            grad_hidden,
            inputs[layer],
            attn_kept[layer],
            vectors,
            *attn_packed[layer],
            layer,
            lengths_here,
            own_rows,
            errand,
            both_ways,
        )
        errands[layer] = got
        attn_sums[layer] = lax.psum_scatter(attn_grad, "dp", scatter_dimension=0, tiled=True)
        input_grads[layer] = grads

    section_output = whole_rows(rows, last, errands[1])
    small_mine, up_total, ff_got, attn_got, rows_got = home(
        [attn_small[0], attn_small[1]],
        [ff_small[0], ff_small[1]],
        jnp.stack([bias_grads[0], bias_grads[1]]),
        jnp.stack([up_sums[0], up_sums[1]]),
        ff_sums[0],
        attn_sums[1],
        jnp.where(here == 0, input_grads[1], input_grads[0]),
        count,
        chunk,
    )
    small_mine = small_mine[None, :, :chunk]
    up_total = up_total[:, :, :half_ff].reshape(1, ff_cols)
    input_grad = whole_rows(input_grads[0], input_grads[1], rows_got)

    qkv_total, out_total, up_grad, down_grad = finish(
        [ff_sums[0], ff_sums[1]],
        [ff_got, errands[0]],
        [attn_sums[0], attn_sums[1]],
        attn_got,
        head_cols,
        ff_cols,
    )
    gains = norm_gains.shape[1]
    return (
        section_output[None],
        input_grad[None],
        qkv_total[None],
        out_total.T[None],
        up_grad[None],
        down_grad.T[None],
        small_mine[:, :gains],
        small_mine[:, gains:],
        up_total,
    )


def solution(mesh):
    in_specs = (
        P(None, "dp", "tensor", None),
        P(None, "dp", "tensor", None),
        P(None, "dp"),
        P("section", None, "dp", "tensor"),
        P("section", "tensor", "dp"),
        P("section", "dp", "tensor"),
        P("section", "tensor", "dp"),
        P("section", None, ("dp", "tensor")),
        P("section", None, ("dp", "tensor")),
        P("section", "tensor"),
    )
    out_specs = (
        P("section", None, "dp", "tensor", None),
        P("section", None, "dp", "tensor", None),
        P("section", None, "dp", "tensor"),
        P("section", "tensor", "dp"),
        P("section", "dp", "tensor"),
        P("section", "tensor", "dp"),
        P("section", None, ("dp", "tensor")),
        P("section", None, ("dp", "tensor")),
        P("section", "tensor"),
    )
    return jax.shard_map(shards, mesh=mesh, in_specs=in_specs, out_specs=out_specs, check_vma=False)
```

```python
import functools
import math

import jax
import jax.numpy as jnp
from jax import lax
from jax.experimental import pallas as pl
from jax.experimental.pallas import tpu as pltpu
from jax.sharding import PartitionSpec as P


HEAD = 72
LANES = 128
norm_eps = 1e-06
masked_score = -1000000000.0
score_scale = 1.0 / math.sqrt(HEAD)
GELU_A = math.sqrt(2.0 / math.pi)
GELU_B = 0.044715


def round_up(value, step):
    return -(-value // step) * step


def dot(left, right, left_dim, right_dim):
    return lax.dot_general(
        left, right, (((left_dim,), (right_dim,)), ((), ())), preferred_element_type=jnp.float32
    )


def low(value):
    return value.astype(jnp.bfloat16)


def layer_norm(rows, gain_vec, shift_vec):
    centred = rows - jnp.mean(rows, axis=-1, keepdims=True)
    spread = jnp.mean(centred * centred, axis=-1, keepdims=True)
    return centred * lax.rsqrt(spread + norm_eps) * gain_vec + shift_vec


def norm_back(rows, gain_vec, grads):
    centred = rows - jnp.mean(rows, axis=-1, keepdims=True)
    spread = jnp.mean(centred * centred, axis=-1, keepdims=True)
    inverse = lax.rsqrt(spread + norm_eps)
    xhat = centred * inverse
    e = grads * gain_vec
    back = inverse * (
        e
        - jnp.mean(e, axis=-1, keepdims=True)
        - xhat * jnp.mean(e * xhat, axis=-1, keepdims=True)
    )
    return back, grads * xhat


def gelu_tanh(value):
    return jax.nn.gelu(value, approximate=True)


MESH = pl.DeviceIdType.MESH
VMEM_BYTES = 64_000_000
COST = pl.CostEstimate(flops=20_000_000_000, transcendentals=0, bytes_accessed=100_000_000)
LOG2E = 1.0 / math.log(2.0)
TILE = 256
WIDE = 384


class Slab:
    def __init__(self, half_rows):
        self.half_rows = half_rows
        section = lax.axis_index("section")
        tensor = lax.axis_index("tensor")
        core = lax.rem(tensor, 2)
        self.core = core
        self.mine = self.around(section, tensor, core)
        self.theirs = self.around(section, tensor + 1 - 2 * core, 1 - core)
        self.far_role, self.near_role = 1 + core, 2 - core
        self.mate = self.theirs[0]
        over = lax.rem(tensor + 2, 4)
        self.near, self.far = tensor, over
        self.mate_near, self.mate_far = self.mate[1], lax.rem(self.mate[1] + 2, 4)
        self.grid = self.places(section, self.near, self.far)
        self.mate_grid = self.places(section, self.mate_near, self.mate_far)
        self.across_y = self.grid[2]
        self.first, self.second = self.mine[1], self.mine[2]

    def place(self, section, tensor):
        start = (2 * tensor + section) * self.half_rows
        return (section, tensor, pl.multiple_of(start, self.half_rows))

    def places(self, section, near, far):
        flip = 1 - section
        return [self.place(*at) for at in ((section, near), (flip, near), (section, far), (flip, far))]

    def around(self, section, tensor, core):
        over = lax.rem(tensor + 2, 4)
        turn = 1 - 2 * section
        first = (section + (1 - core) * turn, tensor + core * (over - tensor))
        second = (section + core * turn, tensor + (1 - core) * (over - tensor))
        places = ((section, tensor), first, second, (1 - section, over))
        return [self.place(*at) for at in places]

    def rows(self, ref, at):
        return ref.at[pl.ds(at[2], self.half_rows)]

    def greet(self):
        barrier = pltpu.get_barrier_semaphore()
        for peer in (self.first, self.second, self.mate):
            pl.semaphore_signal(barrier, inc=1, device_id=named(peer), device_id_type=MESH)
        pl.semaphore_wait(barrier, 3)


def named(at):
    return {"section": at[0], "tensor": at[1]}


class Moves:
    def __init__(self, slab, send_sems, recv_sems):
        self.slab, self.send_sems, self.recv_sems = slab, send_sems, recv_sems
        self.sent = []

    def copy(self, src, dst, role, peer):
        return pltpu.make_async_remote_copy(
            src_ref=src,
            dst_ref=dst,
            send_sem=self.send_sems.at[role],
            recv_sem=self.recv_sems.at[role],
            device_id=named(peer),
            device_id_type=MESH,
        )

    def send(self, ends, role, peer):
        self.copy(*ends(), role, peer).start()
        self.sent.append(lambda: self.copy(*ends(), role, peer))

    def arrived(self, dst, role):
        self.copy(dst, dst, role, self.slab.mate).wait_recv()

    def drain(self):
        for copy in self.sent:
            copy().wait_send()


class Gather(Moves):
    def __init__(self, slab, whole, send_sems, recv_sems):
        super().__init__(slab, send_sems, recv_sems)
        self.whole = whole

    def pass_on(self, at, role, peer):
        self.send(lambda: (self.slab.rows(self.whole, at),) * 2, role, peer)

    def arrive(self, at, role):
        self.arrived(self.slab.rows(self.whole, at), role)

    def start(self):
        mine = self.slab.mine
        self.pass_on(mine[0], 0, mine[1])
        self.pass_on(mine[0], 3, self.slab.mate)

    def second(self):
        self.sent.pop(0)().wait_send()
        self.pass_on(self.slab.mine[0], 1, self.slab.mine[2])

    def forward(self):
        mine, mate = self.slab.mine, self.slab.mate
        self.arrive(mine[1], 0)
        self.pass_on(mine[1], 2, mine[2])
        self.pass_on(mine[1], 4, mate)

    def to_mate(self):
        mine, mate = self.slab.mine, self.slab.mate
        self.arrive(mine[2], 1)
        self.pass_on(mine[2], 5, mate)
        self.arrive(mine[3], 2)
        self.pass_on(mine[3], 6, mate)

    def finish(self):
        for k in range(4):
            self.arrive(self.slab.theirs[k], 3 + k)
        self.drain()


class TileGather:
    def __init__(self, whole, send_sems, recv_sems):
        self.whole, self.send_sems, self.recv_sems = whole, send_sems, recv_sems
        self.tensor = lax.axis_index("tensor")
        self.over = lax.rem(self.tensor + 2, 4)
        self.mate = self.tensor + 1 - 2 * lax.rem(self.tensor, 2)
        self.micro, rows = whole.shape[0], whole.shape[1] // 4
        self.tile_rows = rows
        self.sent = []

    def tile(self, m, index):
        start = pl.multiple_of(index * self.tile_rows, self.tile_rows)
        return self.whole.at[m, pl.ds(start, self.tile_rows)]

    def copy(self, m, index, role, peer):
        part = self.tile(m, index)
        return remote(
            part, part, self.send_sems.at[m, role], self.recv_sems.at[m, role], {"tensor": peer}
        )

    def send(self, m, index, role, peer):
        self.copy(m, index, role, peer).start()
        self.sent.append(lambda: self.copy(m, index, role, peer))

    def start(self):
        for m in range(self.micro):
            self.send(m, self.tensor, 0, self.over)
            self.send(m, self.tensor, 1, self.mate)

    def pass_on(self):
        for m in range(self.micro):
            self.copy(m, self.over, 0, self.over).wait_recv()
            self.send(m, self.over, 2, self.mate)

    def finish(self):
        for m in range(self.micro):
            self.copy(m, self.mate, 1, self.mate).wait_recv()
            self.copy(m, lax.rem(self.mate + 2, 4), 2, self.mate).wait_recv()

    def drain(self):
        for copy in self.sent:
            copy().wait_send()


class Scatter(Moves):
    def __init__(self, slab, terms, from_mate, outgoing, arrivals, send_sems, recv_sems):
        super().__init__(slab, send_sems, recv_sems)
        self.terms, self.from_mate, self.outgoing = terms, from_mate, outgoing
        self.relay, self.from_second, self.from_first = (arrivals.at[k] for k in range(3))

    def to_mate(self, at, role):
        self.send(
            lambda: (self.slab.rows(self.terms, at), self.from_mate.at[role]), role, self.slab.mate
        )

    def mate_far(self):
        self.to_mate(self.slab.mate_grid[3], 3)
        self.to_mate(self.slab.mate_grid[2], self.slab.far_role)

    def mate_near(self):
        self.to_mate(self.slab.mate_grid[1], self.slab.near_role)
        self.to_mate(self.slab.mate_grid[0], 0)

    def chip_sum(self, k, rows):
        part = self.slab.rows(self.terms, self.slab.mine[k])
        return part[rows].astype(jnp.float32) + self.from_mate[k, rows].astype(jnp.float32)

    def blocks(self):
        return [pl.ds(start, 32) for start in range(0, self.slab.half_rows, 32)]

    def hop(self, k, slot, dst, role, peer, ride=None):
        self.arrived(self.from_mate.at[k], k)
        if ride is not None:
            self.arrived(ride, 4)
        for rows in self.blocks():
            value = self.chip_sum(k, rows)
            if ride is not None:
                value = value + ride[rows].astype(jnp.float32)
            self.outgoing[slot, rows] = low(value)
        self.send(lambda: (self.outgoing.at[slot], dst), role, peer)

    def far_hop(self):
        self.hop(3, 0, self.relay, 4, self.slab.second)

    def second_hop(self):
        self.hop(2, 1, self.from_second, 5, self.slab.second)

    def first_hop(self):
        self.hop(1, 2, self.from_first, 6, self.slab.first, self.relay)

    def finish(self):
        self.arrived(self.from_mate.at[0], 0)
        self.arrived(self.from_second, 5)
        self.arrived(self.from_first, 6)
        self.drain()

    def total(self, rows):
        other = self.from_second[rows].astype(jnp.float32) + self.from_first[rows].astype(
            jnp.float32
        )
        return self.chip_sum(0, rows) + other


def scatter_scratch(micro, seq, half_rows, width):
    return [
        pltpu.VMEM((micro, seq, width), jnp.bfloat16),
        pltpu.VMEM((micro, 4, half_rows, width), jnp.bfloat16),
        pltpu.VMEM((micro, 3, half_rows, width), jnp.bfloat16),
        pltpu.VMEM((micro, 3, half_rows, width), jnp.bfloat16),
        pltpu.SemaphoreType.DMA((micro, 7)),
        pltpu.SemaphoreType.DMA((micro, 7)),
    ]


def gather_scratch(micro, seq, width):
    return [
        pltpu.VMEM((micro, seq, width), jnp.bfloat16),
        pltpu.SemaphoreType.DMA((micro, 7)),
        pltpu.SemaphoreType.DMA((micro, 7)),
    ]


def make_scatters(slab, refs, micro):
    terms, from_mate, outgoing, arrivals, send_sems, recv_sems = refs
    return [
        Scatter(
            slab,
            terms.at[m],
            from_mate.at[m],
            outgoing.at[m],
            arrivals.at[m],
            send_sems.at[m],
            recv_sems.at[m],
        )
        for m in range(micro)
    ]


def make_gathers(slab, refs, micro):
    whole, send_sems, recv_sems = refs
    return [
        Gather(slab, whole.at[m], send_sems.at[m], recv_sems.at[m]) for m in range(micro)
    ]


def step_from(start, i, size):
    return pl.ds(pl.multiple_of(start + i * size, size), size)


def step_rows(i, size):
    return pl.ds(pl.multiple_of(i * size, size), size)


def repeat(count, body):
    def one(i, carry):
        body(i)
        return carry

    lax.fori_loop(0, count, one, 0)


def shut_keys(length, own_rows, full_rows, shape, dimension):
    place = lax.broadcasted_iota(jnp.int32, shape, dimension)
    step = jnp.zeros(shape, jnp.int32)
    for t in range(1, 4):
        step += (place >= t * full_rows).astype(jnp.int32)
    live = (place - step * full_rows < own_rows) & (
        place - step * (full_rows - own_rows) < length
    )
    return jnp.where(live, 0.0, masked_score)


def stages(count, work, hooks):
    def body(k):
        work(k)
        for at, steps in hooks.items():

            @pl.when(k == at)
            def _():
                for step in steps:
                    step()

    repeat(count, body)


def chip_rows(slab, k):
    far, near = slab.far - slab.core, slab.near - slab.core
    start = (far + lax.rem(k, 2) * (near - far)) * (2 * slab.half_rows)
    return pl.multiple_of(start, 2 * slab.half_rows)


def open_gathers(gathers, fill, prepare):
    fill(0)
    gathers[0].start()
    fill(1)
    gathers[0].second()
    gathers[1].start()
    prepare()
    gathers[0].forward()
    gathers[1].second()


def widen(packed, wide):
    heads = packed.shape[1] // HEAD

    def block(i):
        rows = step_rows(i, 128)
        for h in range(heads):
            piece = packed[rows, h * HEAD : (h + 1) * HEAD]
            blank = jnp.zeros((128, LANES - HEAD), jnp.bfloat16)
            wide[rows, h * LANES : (h + 1) * LANES] = jnp.concatenate([piece, blank], axis=1)

    repeat(packed.shape[0] // 128, block)


def split_tail(packed, tails, up_cols):
    start = packed.shape[1] - LANES

    def block(i):
        rows = step_rows(i, 128)
        for j in range(2):
            piece = packed[rows, start + j * up_cols : start + (j + 1) * up_cols]
            blank = jnp.zeros((128, LANES - up_cols), jnp.bfloat16)
            tails[rows, j * LANES : (j + 1) * LANES] = jnp.concatenate([piece, blank], axis=1)

    repeat(packed.shape[0] // 128, block)


def up_dot(rows, packed, tails):
    main = (packed.shape[1] - LANES) // 2
    first = dot(rows, packed[:, :main], 1, 0)
    return jnp.concatenate([first, dot(rows, tails[:, :LANES], 1, 0)], axis=1)


def up_back(grads, packed, tails):
    main = (packed.shape[1] - LANES) // 2
    return dot(grads[:, :main], packed[:, :main], 1, 1) + dot(
        grads[:, main:], tails[:, :LANES], 1, 1
    )


def down_dot(active, packed, tails):
    main = (packed.shape[1] - LANES) // 2
    return dot(active[:, :main], packed[:, main : 2 * main], 1, 1) + dot(
        active[:, main:], tails[:, LANES:], 1, 1
    )


def down_back(rows, packed, tails):
    main = (packed.shape[1] - LANES) // 2
    first = dot(rows, packed[:, main : 2 * main], 1, 0)
    return jnp.concatenate([first, dot(rows, tails[:, LANES:], 1, 0)], axis=1)


def attn_forward_kernel(
    ready, at, layer, own_rows, rows_ref, vectors, bias_ref, lengths, packed_hbm, given_hbm, grads_ref,
    hidden_ref, lse_ref, normed_hbm, qkv_hbm, mixed_hbm, *rest
):
    micro, half_rows, width = rows_ref.shape
    gathered, gather_refs = rest[0], rest[0:3]
    scatter_refs = rest[3:9]
    terms = rest[3]
    packed, wide, qkv, mixed, load_sem, keep_sems, given_sems, all_grads, tile_send, tile_recv = rest[9:]
    vec, bias = vectors.at[layer], bias_ref[layer]
    seq = qkv.shape[1]
    pair = mixed.shape[2]
    heads = pair // LANES
    load = pltpu.make_async_copy(
        packed_hbm.at[:, at : at + packed.shape[1]], packed, load_sem
    )
    load.start()
    slab = Slab(half_rows)
    gathers = make_gathers(slab, gather_refs, micro)
    scatters = make_scatters(slab, scatter_refs, micro)
    given = [
        pltpu.make_async_copy(given_hbm.at[m], gathered.at[m], given_sems.at[m])
        for m in range(micro if ready else 0)
    ]
    for copy in given:
        copy.start()
    slab.greet()
    if ready:
        tiles = TileGather(all_grads, tile_send, tile_recv)
        for m in range(micro):
            own = tiles.tile(m, tiles.tensor)
            count = grads_ref.shape[1]
            own[:count] = grads_ref[m]
            own[count:] = jnp.zeros((tiles.tile_rows - count, width), jnp.bfloat16)
        tiles.start()

    def fill(m):
        own = slab.rows(gathered.at[m], slab.mine[0])
        for start in range(0, half_rows, 32):
            block = rows_ref[m, pl.ds(start, 32)].astype(jnp.float32)
            own[pl.ds(start, 32)] = low(layer_norm(block, vec[0:1], vec[2:3]))

    def prepare():
        load.wait()
        widen(packed, wide)

    if ready:
        prepare()
    else:
        open_gathers(gathers, fill, prepare)
    keeps = []

    def keep(src, dst, m, i):
        def copy():
            return pltpu.make_async_copy(src.at[m], dst.at[m], keep_sems.at[i])

        copy().start()
        keeps.append(copy)

    def project(m):
        def block(i):
            rows = step_rows(i, 4 * half_rows)
            out = dot(gathered[m, rows], wide[:, : 3 * pair], 1, 0)
            qkv[m, rows] = low(out + bias)

        repeat(seq // (4 * half_rows), block)

    def attend(m, rows):
        shut = shut_keys(lengths[m], own_rows, 2 * half_rows, (1, seq), 1)
        for h in range(heads):
            cols = slice(h * LANES, (h + 1) * LANES)
            q = qkv[m, rows, cols]
            k = qkv[m, :, pair + h * LANES : pair + (h + 1) * LANES]
            v = qkv[m, :, 2 * pair + h * LANES : 2 * pair + (h + 1) * LANES]
            scores = dot(q, k, 1, 1) * (score_scale * LOG2E) + shut
            top = jnp.max(scores, axis=-1, keepdims=True)
            exp_scores = jnp.exp2(scores - top)
            total = jnp.sum(exp_scores, axis=-1, keepdims=True)
            probs = low(exp_scores * (1.0 / total))
            mixed[m, rows, cols] = low(dot(probs, v, 1, 0))
            lse_ref[m, h, rows] = jnp.broadcast_to(
                top + jnp.log(total) * LOG2E, (2 * half_rows, LANES)
            )

    def output(m, rows):
        terms[m, rows] = low(dot(mixed[m, rows], wide[:, 3 * pair :], 1, 1))

    def close(m):
        scatters[m].finish()
        for rows in scatters[m].blocks():
            start = rows_ref[m, rows].astype(jnp.float32)
            hidden_ref[m, rows] = start + scatters[m].total(rows) + vec[5:6]

    def gathered_rows(m):
        if ready:
            given[m].wait()
            return
        gathers[m].to_mate()
        gathers[m].finish()
        keep(gathered, normed_hbm, m, m)

    def work(k):
        m = lax.div(k, 2)
        start = chip_rows(slab, k)
        pl.when(lax.rem(k, 2) == 0)(lambda: project(m))

        def piece(i):
            attend(m, step_from(start, i, 2 * half_rows))

        repeat(2, piece)
        output(m, pl.ds(start, 4 * half_rows))

    def keep_two(m):
        keep(qkv, qkv_hbm, m, 2 + 2 * m)
        keep(mixed, mixed_hbm, m, 3 + 2 * m)

    def grads_on():
        if ready:
            tiles.pass_on()

    def grads_in():
        if ready:
            tiles.finish()
            for m in range(micro):
                keep(all_grads, normed_hbm, m, m)

    gathered_rows(0)
    if not ready:
        gathers[1].forward()
    zero, one = scatters
    stages(
        4,
        work,
        {
            0: [zero.mate_far, lambda: gathered_rows(1), zero.far_hop],
            1: [zero.mate_near, lambda: keep_two(0), zero.second_hop, zero.first_hop, grads_on],
            2: [one.mate_far, lambda: close(0), one.far_hop, grads_in],
            3: [one.mate_near, lambda: keep_two(1), one.second_hop, one.first_hop],
        },
    )
    close(1)
    if ready:
        tiles.drain()
    for copy in keeps:
        copy().wait()


def ffn_forward_kernel(
    half_ff, at, layer, hidden_ref, vectors, up_biases, packed_hbm, out_ref, second_hbm, upper_hbm, *rest
):
    micro, half_rows, _ = hidden_ref.shape
    gathered, gather_refs = rest[0], rest[0:3]
    scatter_refs = rest[3:9]
    terms = rest[3]
    packed, tails, upper, load_sem, keep_sems = rest[9:]
    vec, up_bias = vectors.at[layer], up_biases.at[layer]
    _, ff = upper.shape[1:]
    load = pltpu.make_async_copy(
        packed_hbm.at[:, at : at + packed.shape[1]], packed, load_sem
    )
    load.start()
    slab = Slab(half_rows)
    gathers = make_gathers(slab, gather_refs, micro)
    scatters = make_scatters(slab, scatter_refs, micro)
    slab.greet()

    def fill(m):
        own = slab.rows(gathered.at[m], slab.mine[0])
        for start in range(0, half_rows, 32):
            block = hidden_ref[m, pl.ds(start, 32)]
            own[pl.ds(start, 32)] = low(layer_norm(block, vec[1:2], vec[6:7]))

    def prepare():
        load.wait()
        split_tail(packed, tails, half_ff - ff + LANES)

    open_gathers(gathers, fill, prepare)
    keeps = []

    def keep(src, dst, m, i):
        def copy():
            return pltpu.make_async_copy(src.at[m], dst.at[m], keep_sems.at[i])

        copy().start()
        keeps.append(copy)

    def compute(m, rows):
        value = up_dot(gathered[m, rows], packed, tails) + up_bias[...]
        upper[m, rows] = value
        active = low(gelu_tanh(value))
        terms[m, rows] = low(down_dot(active, packed, tails))

    def close(m):
        scatters[m].finish()
        for rows in scatters[m].blocks():
            out_ref[m, rows] = low(hidden_ref[m, rows] + scatters[m].total(rows) + vec[7:8])

    def work(k):
        compute(lax.div(k, 2), pl.ds(chip_rows(slab, k), 4 * half_rows))

    gathers[0].to_mate()
    gathers[0].finish()
    keep(gathered, second_hbm, 0, 0)
    zero, one = scatters
    stages(
        4,
        work,
        {
            0: [zero.mate_far, gathers[1].forward, zero.far_hop],
            1: [
                zero.mate_near,
                lambda: keep(upper, upper_hbm, 0, 1),
                gathers[1].to_mate,
                zero.second_hop,
                gathers[1].finish,
                lambda: keep(gathered, second_hbm, 1, 2),
            ],
            2: [one.mate_far, zero.first_hop, one.far_hop],
            3: [one.mate_near, lambda: keep(upper, upper_hbm, 1, 3), one.second_hop],
        },
    )
    close(0)
    one.first_hop()
    close(1)
    for copy in keeps:
        copy().wait()


def ffn_backward_kernel(
    half_ff, at, layer, grad_ref, hidden_ref, vectors, second_hbm, upper_hbm, packed_hbm,
    out_ref, grads_ref, small_ref, up_bias_ref, *rest
):
    micro, half_rows, width = hidden_ref.shape
    gathered, gather_refs = rest[0], rest[0:3]
    scatter_refs = rest[3:9]
    terms = rest[3]
    packed, tails, second, upper, grad_upper, active, load_sems = rest[9:]
    vec = vectors.at[layer]
    seq, ff = upper.shape[1:]
    main = ff - LANES
    extra = half_ff - main
    load_packed = pltpu.make_async_copy(
        packed_hbm.at[:, at : at + packed.shape[1]], packed, load_sems.at[0]
    )
    load_packed.start()
    load_upper, load_second = [], []
    for m in range(micro):
        load_upper.append(
            pltpu.make_async_copy(upper_hbm.at[m], upper.at[m], load_sems.at[1 + m])
        )
        load_upper[m].start()
    for m in range(micro):
        load_second.append(
            pltpu.make_async_copy(second_hbm.at[m], second.at[m], load_sems.at[1 + micro + m])
        )
        load_second[m].start()
    slab = Slab(half_rows)
    gathers = make_gathers(slab, gather_refs, micro)
    scatters = make_scatters(slab, scatter_refs, micro)
    slab.greet()

    def fill(m):
        own = slab.rows(gathered.at[m], slab.mine[0])
        for start in range(0, half_rows, 32):
            own[pl.ds(start, 32)] = grad_ref[m, pl.ds(start, 32)]

    def prepare():
        small_ref[...] = jnp.zeros_like(small_ref)
        up_bias_ref[...] = jnp.zeros_like(up_bias_ref)
        load_packed.wait()
        split_tail(packed, tails, extra)

    open_gathers(gathers, fill, prepare)

    def compute(m, rows):
        value = upper[m, rows]
        square = value * value
        bent = jnp.tanh(GELU_A * value * (1.0 + GELU_B * square))
        half = 0.5 * (1.0 + bent)
        active[m, rows] = low(value * half)
        slope = half + (0.5 * GELU_A) * value * (1.0 - bent * bent) * (1.0 + 3.0 * GELU_B * square)
        grad_active = down_back(gathered[m, rows], packed, tails)
        grad = low(grad_active * slope)
        grad_upper[m, rows] = grad
        up_bias_ref[0:1] += jnp.sum(grad.astype(jnp.float32), axis=0, keepdims=True)
        terms[m, rows] = low(up_back(grad, packed, tails))

    def stacked(ref, cols=slice(None)):
        return ref[:, :, cols].reshape(micro * seq, -1)

    def weight_grads(hooks):
        def block(i):
            cols = step_rows(i, WIDE)
            up = dot(stacked(second, cols), stacked(grad_upper), 0, 0)
            down = dot(stacked(gathered, cols), stacked(active), 0, 0)
            grads_ref[cols, :main] = low(up[:, :main])
            grads_ref[cols, main : 2 * main] = low(down[:, :main])
            blank = jnp.zeros((WIDE, LANES - 2 * extra), jnp.float32)
            rest_cols = [up[:, main : main + extra], down[:, main : main + extra], blank]
            grads_ref[cols, 2 * main :] = low(jnp.concatenate(rest_cols, axis=1))

        stages(width // WIDE, block, hooks)

    def close(m):
        scatters[m].finish()
        for rows in scatters[m].blocks():
            grad_normed = scatters[m].total(rows)
            back, gain_terms = norm_back(hidden_ref[m, rows], vec[1:2], grad_normed)
            grad_rows = grad_ref[m, rows].astype(jnp.float32)
            grad_hidden = grad_rows + back
            out_ref[m, rows] = grad_hidden
            branch = low(grad_hidden).astype(jnp.float32)
            for j, item in enumerate((gain_terms, grad_normed, grad_rows, branch)):
                small_ref[j : j + 1] += jnp.sum(item, axis=0, keepdims=True)

    def work(k):
        compute(lax.div(k, 2), pl.ds(chip_rows(slab, k), 4 * half_rows))

    gathers[0].to_mate()
    gathers[0].finish()
    load_upper[0].wait()
    zero, one = scatters
    stages(
        4,
        work,
        {
            0: [zero.mate_far, gathers[1].forward, zero.far_hop],
            1: [
                zero.mate_near,
                gathers[1].to_mate,
                zero.second_hop,
                gathers[1].finish,
                load_upper[1].wait,
            ],
            2: [one.mate_far, zero.first_hop, one.far_hop],
            3: [one.mate_near, one.second_hop],
        },
    )
    for load in load_second:
        load.wait()
    weight_grads({0: [one.first_hop, lambda: close(0)]})
    close(1)


def ffn_turn_kernel(
    half_ff, at, layer, hidden_ref, grad_ref, vectors, up_biases, given_hbm, packed_hbm,
    out_ref, grad_out_ref, grads_ref, small_ref, up_bias_ref, *rest
):
    micro, half_rows, width = hidden_ref.shape
    gathered, gather_refs = rest[0], rest[0:3]
    terms, back_terms = rest[3], rest[9]
    packed, tails, given, grad_upper, active, load_sem, given_sems = rest[15:]
    vec, up_bias = vectors.at[layer], up_biases.at[layer]
    seq, ff = active.shape[1:]
    main = ff - LANES
    extra = half_ff - main
    load = pltpu.make_async_copy(
        packed_hbm.at[:, at : at + packed.shape[1]], packed, load_sem
    )
    load.start()
    loads = [
        pltpu.make_async_copy(given_hbm.at[m], given.at[m], given_sems.at[m]) for m in range(micro)
    ]
    for copy in loads:
        copy.start()
    slab = Slab(half_rows)
    gathers = make_gathers(slab, gather_refs, micro)
    scatters = make_scatters(slab, rest[3:9], micro)
    backs = make_scatters(slab, rest[9:15], micro)
    slab.greet()

    def fill(m):
        own = slab.rows(gathered.at[m], slab.mine[0])
        for start in range(0, half_rows, 32):
            block = hidden_ref[m, pl.ds(start, 32)]
            own[pl.ds(start, 32)] = low(layer_norm(block, vec[1:2], vec[6:7]))

    def prepare():
        small_ref[...] = jnp.zeros_like(small_ref)
        up_bias_ref[...] = jnp.zeros_like(up_bias_ref)
        load.wait()
        split_tail(packed, tails, extra)

    open_gathers(gathers, fill, prepare)

    def compute(m, rows):
        value = up_dot(gathered[m, rows], packed, tails) + up_bias[...]
        square = value * value
        bent = jnp.tanh(GELU_A * value * (1.0 + GELU_B * square))
        half = 0.5 * (1.0 + bent)
        shown = low(value * half)
        active[m, rows] = shown
        slope = half + (0.5 * GELU_A) * value * (1.0 - bent * bent) * (1.0 + 3.0 * GELU_B * square)
        grad = low(down_back(given[m, rows], packed, tails) * slope)
        grad_upper[m, rows] = grad
        up_bias_ref[0:1] += jnp.sum(grad.astype(jnp.float32), axis=0, keepdims=True)
        back_terms[m, rows] = low(up_back(grad, packed, tails))
        terms[m, rows] = low(down_dot(shown, packed, tails))

    def stacked(ref, cols=slice(None)):
        return ref[:, :, cols].reshape(micro * seq, -1)

    def weight_grads(hooks):
        def block(i):
            cols = step_rows(i, WIDE)
            up = dot(stacked(gathered, cols), stacked(grad_upper), 0, 0)
            down = dot(stacked(given, cols), stacked(active), 0, 0)
            grads_ref[cols, :main] = low(up[:, :main])
            grads_ref[cols, main : 2 * main] = low(down[:, :main])
            blank = jnp.zeros((WIDE, LANES - 2 * extra), jnp.float32)
            rest_cols = [up[:, main : main + extra], down[:, main : main + extra], blank]
            grads_ref[cols, 2 * main :] = low(jnp.concatenate(rest_cols, axis=1))

        stages(width // WIDE, block, hooks)

    def close_back(m):
        backs[m].finish()
        for rows in backs[m].blocks():
            grad_normed = backs[m].total(rows)
            back, gain_terms = norm_back(hidden_ref[m, rows], vec[1:2], grad_normed)
            grad_rows = grad_ref[m, rows].astype(jnp.float32)
            grad_hidden = grad_rows + back
            grad_out_ref[m, rows] = grad_hidden
            branch = low(grad_hidden).astype(jnp.float32)
            for j, item in enumerate((gain_terms, grad_normed, grad_rows, branch)):
                small_ref[j : j + 1] += jnp.sum(item, axis=0, keepdims=True)

    def close(m):
        scatters[m].finish()
        for rows in scatters[m].blocks():
            out_ref[m, rows] = low(hidden_ref[m, rows] + scatters[m].total(rows) + vec[7:8])

    def work(k):
        compute(lax.div(k, 2), pl.ds(chip_rows(slab, k), 4 * half_rows))

    gathers[0].to_mate()
    gathers[0].finish()
    loads[0].wait()
    zero, one = scatters
    back_zero, back_one = backs
    stages(
        4,
        work,
        {
            0: [back_zero.mate_far, zero.mate_far, gathers[1].forward, back_zero.far_hop],
            1: [
                back_zero.mate_near,
                zero.mate_near,
                gathers[1].to_mate,
                back_zero.second_hop,
                gathers[1].finish,
                zero.far_hop,
                zero.second_hop,
                loads[1].wait,
            ],
            2: [
                back_one.mate_far,
                one.mate_far,
                back_zero.first_hop,
                back_one.far_hop,
                zero.first_hop,
            ],
            3: [
                back_one.mate_near,
                one.mate_near,
                back_one.second_hop,
                one.far_hop,
                one.second_hop,
            ],
        },
    )
    weight_grads({0: [back_one.first_hop, one.first_hop, lambda: close_back(0)]})
    close_back(1)
    for m in range(micro):
        close(m)


def attn_backward_kernel(
    at, layer, own_rows, both_ways, grad_ref, rows_ref, vectors, lse, lengths,
    normed_hbm, qkv_hbm, mixed_hbm, packed_hbm, errand_hbm,
    out_ref, grads_ref, small_ref, bias_ref, errand_got, *rest
):
    micro, half_rows, width = grad_ref.shape
    gathered, gather_refs = rest[0], rest[0:3]
    scatter_refs = rest[3:9]
    terms = rest[3]
    packed, wide, normed, qkv, mixed, grad_mixed, grad_qkv, turned, shut = rest[9:18]
    low_probs, grad_scores, high_probs, errand_sems, load_sems = rest[18:]
    vec = vectors.at[layer]
    seq, pair = mixed.shape[1:]
    heads = pair // LANES
    load_packed = pltpu.make_async_copy(
        packed_hbm.at[:, at : at + packed.shape[1]], packed, load_sems.at[0]
    )
    load_packed.start()
    load_qkv, load_rest = [], []
    for m in range(micro):
        load_qkv.append(pltpu.make_async_copy(qkv_hbm.at[m], qkv.at[m], load_sems.at[1 + 3 * m]))
        load_qkv[m].start()
    for m in range(micro):
        for k, (src, dst) in enumerate(((mixed_hbm, mixed), (normed_hbm, normed))):
            load = pltpu.make_async_copy(src.at[m], dst.at[m], load_sems.at[2 + k + 3 * m])
            load.start()
            load_rest.append(load)
    slab = Slab(half_rows)
    gathers = make_gathers(slab, gather_refs, micro)
    scatters = make_scatters(slab, scatter_refs, micro)
    slab.greet()

    def fill(m):
        own = slab.rows(gathered.at[m], slab.mine[0])
        for start in range(0, half_rows, 32):
            own[pl.ds(start, 32)] = low(grad_ref[m, pl.ds(start, 32)])

    def head(h, part=0):
        return pl.ds(pl.multiple_of(part * pair + h * LANES, LANES), LANES)

    def ready_qkv(m):
        load_qkv[m].wait()
        shut[m] = shut_keys(lengths[m], own_rows, 2 * half_rows, (seq, LANES), 0)
        for h in range(heads):
            turned[m, h] = low(qkv[m, :, head(h, 1)].astype(jnp.float32).T)

    def find_probs(m, h):
        def block(i):
            rows = step_rows(i, TILE)
            keys, queries = qkv[m, :, head(h, 1)], qkv[m, rows, head(h)]
            closed = jnp.concatenate([shut[m]] * (TILE // LANES), axis=1)
            scores = dot(keys, queries, 1, 1) * (score_scale * LOG2E) + closed
            high_probs[m, h, :, rows] = jnp.exp2(scores - lse[m, h, rows].T[0:1])

        repeat(seq // TILE, block)

    def find_all(k):
        find_probs(lax.div(k, heads), lax.rem(k, heads))

    errand = remote(
        errand_hbm,
        errand_got,
        errand_sems.at[0],
        errand_sems.at[1],
        {"section": 1 - lax.axis_index("section")},
    )
    sends_errand = (lax.axis_index("section") == 0) | both_ways
    gets_errand = (lax.axis_index("section") == 1) | both_ways

    def prepare():
        small_ref[...] = jnp.zeros_like(small_ref)
        bias_ref[...] = jnp.zeros_like(bias_ref)
        load_packed.wait()
        widen(packed, wide)
        for m in range(micro):
            ready_qkv(m)

    fill(0)
    gathers[0].start()
    fill(1)
    gathers[0].second()
    gathers[1].start()
    prepare()

    def mix_grads(m):
        def block(i):
            rows = step_rows(i, 4 * half_rows)
            grad_mixed[m, rows] = low(dot(gathered[m, rows], wide[:, 3 * pair :], 1, 0))

        repeat(seq // (4 * half_rows), block)

    def attend(m, h):
        def block(i):
            rows = step_rows(i, TILE)
            grads = grad_mixed[m, rows, head(h)]
            probs = high_probs[m, h, :, rows]
            grad_probs = dot(qkv[m, :, head(h, 2)], grads, 1, 1)
            inner = jnp.sum(grad_probs * probs, axis=0, keepdims=True)
            low_probs[:, rows] = low(probs)
            grad_scores[:, rows] = low(probs * (grad_probs - inner))

        repeat(seq // TILE, block)
        grad_keys = dot(grad_scores[...], qkv[m, :, head(h)], 1, 0)
        grad_qkv[m, :, head(h, 1)] = low(grad_keys * score_scale)
        grad_qkv[m, :, head(h, 2)] = low(dot(low_probs[...], grad_mixed[m, :, head(h)], 1, 0))
        turn = dot(turned[m, h], grad_scores[...], 1, 0).T
        grad_qkv[m, :, head(h)] = low(turn * score_scale)

    def back_project(m, rows):
        grads = grad_qkv[m, rows]
        terms[m, rows] = low(dot(grads, wide[:, : 3 * pair], 1, 1))
        for j, part in enumerate((0, 2)):
            piece = grads[:, part * pair : (part + 1) * pair].astype(jnp.float32)
            bias_ref[j : j + 1] += jnp.sum(piece, axis=0, keepdims=True)

    def stacked(ref, cols=slice(None)):
        return ref[:, :, cols].reshape(micro * seq, -1)

    def weight_grads(hooks):
        def block(i):
            cols = step_rows(i, WIDE)
            front = dot(stacked(normed, cols), stacked(grad_qkv), 0, 0)
            back = dot(stacked(gathered, cols), stacked(mixed), 0, 0)
            total = low(jnp.concatenate([front, back], axis=1))
            pieces = [total[:, h * LANES : h * LANES + HEAD] for h in range(4 * heads)]
            grads_ref[cols] = jnp.concatenate(pieces, axis=1)

        stages(width // WIDE, block, hooks)

    def close(m):
        scatters[m].finish()
        for rows in scatters[m].blocks():
            grad_normed = scatters[m].total(rows)
            back, gain_terms = norm_back(
                rows_ref[m, rows].astype(jnp.float32), vec[0:1], grad_normed
            )
            out_ref[m, rows] = low(grad_ref[m, rows] + back)
            for j, item in enumerate((gain_terms, grad_normed)):
                small_ref[j : j + 1] += jnp.sum(item, axis=0, keepdims=True)

    def start_errand():
        pl.when(sends_errand)(errand.start)

    stages(
        2 * heads,
        find_all,
        {
            0: [gathers[0].forward, gathers[1].second],
            1: [gathers[1].forward, gathers[0].to_mate, start_errand],
        },
    )
    gathers[0].finish()
    zero, one = scatters
    attend_hooks = {
        0: [gathers[1].to_mate],
        heads - 1: [gathers[1].finish],
        heads: [zero.first_hop],
    }
    project_hooks = {
        0: [zero.mate_far, zero.far_hop],
        1: [zero.mate_near, zero.second_hop],
        2: [one.mate_far, one.far_hop],
        3: [one.mate_near, lambda: close(0), one.second_hop],
    }

    def hooked(at, hooks):
        for k, steps in hooks.items():

            @pl.when(at == k)
            def _():
                for step in steps:
                    step()

    def image(m):
        mix_grads(m)

        def one_head(h):
            attend(m, h)
            hooked(m * heads + h, attend_hooks)

        repeat(heads, one_head)

        def one_chip(i):
            back_project(m, pl.ds(chip_rows(slab, i), 4 * half_rows))
            hooked(2 * m + i, project_hooks)

        repeat(2, one_chip)

    repeat(micro, image)
    for load in load_rest:
        load.wait()
    weight_grads({0: [one.first_hop]})
    close(1)

    @pl.when(sends_errand)
    def _():
        errand.wait_send()

    @pl.when(gets_errand)
    def _():
        errand.wait_recv()


def any_spec():
    return pl.BlockSpec(memory_space=pl.ANY)


def vmem_spec():
    return pl.BlockSpec(memory_space=pltpu.VMEM)


def shape_of(shape, dtype):
    return jax.ShapeDtypeStruct(shape, dtype)


def params(collective):
    return pltpu.CompilerParams(
        collective_id=collective, has_side_effects=True, vmem_limit_bytes=VMEM_BYTES
    )


def smem_spec():
    return pl.BlockSpec(memory_space=pltpu.SMEM)


def attn_forward(rows_low, vectors, bias, packed, at, layer, lengths, own_rows, given=None, grads=None):
    micro, half_rows, width = rows_low.shape
    seq = 8 * half_rows
    pair = bias.shape[2] // 3
    heads = pair // LANES
    low_type, high_type = jnp.bfloat16, jnp.float32
    hidden, lse, normed, qkv, mixed = pl.pallas_call(
        functools.partial(attn_forward_kernel, given is not None, at, layer, own_rows),
        out_shape=[
            shape_of((micro, half_rows, width), high_type),
            shape_of((micro, heads, seq, LANES), high_type),
            shape_of((micro, seq, width), low_type),
            shape_of((micro, seq, 3 * pair), low_type),
            shape_of((micro, seq, pair), low_type),
        ],
        in_specs=[vmem_spec()] * 3 + [smem_spec(), any_spec(), any_spec(), vmem_spec()],
        out_specs=[vmem_spec()] * 2 + [any_spec()] * 3,
        scratch_shapes=gather_scratch(micro, seq, width)
        + scatter_scratch(micro, seq, half_rows, width)
        + [
            pltpu.VMEM((width, 4 * heads * HEAD), low_type),
            pltpu.VMEM((width, 4 * pair), low_type),
            pltpu.VMEM((micro, seq, 3 * pair), low_type),
            pltpu.VMEM((micro, seq, pair), low_type),
            pltpu.SemaphoreType.DMA,
            pltpu.SemaphoreType.DMA((6,)),
            pltpu.SemaphoreType.DMA((micro,)),
            pltpu.VMEM((micro, seq if given is not None else 32, width), low_type),
            pltpu.SemaphoreType.DMA((micro, 3)),
            pltpu.SemaphoreType.DMA((micro, 3)),
        ],
        compiler_params=params(0 if given is None else 6),
        cost_estimate=COST,
        name="attn_forward",
    )(
        rows_low,
        vectors,
        bias,
        lengths,
        packed,
        packed if given is None else given,
        rows_low if grads is None else grads,
    )
    if given is None:
        return hidden, (normed, qkv, lse, mixed)
    return hidden, (given, qkv, lse, mixed), normed


def ffn_forward(hidden, vectors, up_biases, packed, at, layer, half_ff):
    micro, half_rows, width = hidden.shape
    seq = 8 * half_rows
    ff = up_biases.shape[2]
    packed_cols = 2 * ff - LANES
    low_type, high_type = jnp.bfloat16, jnp.float32
    out, second, upper = pl.pallas_call(
        functools.partial(ffn_forward_kernel, half_ff, at, layer),
        out_shape=[
            shape_of((micro, half_rows, width), low_type),
            shape_of((micro, seq, width), low_type),
            shape_of((micro, seq, ff), high_type),
        ],
        in_specs=[vmem_spec()] * 3 + [any_spec()],
        out_specs=[vmem_spec()] + [any_spec()] * 2,
        scratch_shapes=gather_scratch(micro, seq, width)
        + scatter_scratch(micro, seq, half_rows, width)
        + [
            pltpu.VMEM((width, packed_cols), low_type),
            pltpu.VMEM((width, 2 * LANES), low_type),
            pltpu.VMEM((micro, seq, ff), high_type),
            pltpu.SemaphoreType.DMA,
            pltpu.SemaphoreType.DMA((4,)),
        ],
        compiler_params=params(1),
        cost_estimate=COST,
        name="ffn_forward",
    )(hidden, vectors, up_biases, packed)
    return out, (second, upper)


def ffn_turn(hidden, grad_low, given, vectors, up_biases, packed, at, layer, half_ff):
    micro, half_rows, width = hidden.shape
    seq = 8 * half_rows
    ff = up_biases.shape[2]
    low_type, high_type = jnp.bfloat16, jnp.float32
    out, grad_hidden, grads, small, up_bias = pl.pallas_call(
        functools.partial(ffn_turn_kernel, half_ff, at, layer),
        out_shape=[
            shape_of((micro, half_rows, width), low_type),
            shape_of((micro, half_rows, width), high_type),
            shape_of((width, 2 * ff - LANES), low_type),
            shape_of((8, width), high_type),
            shape_of((8, ff), high_type),
        ],
        in_specs=[vmem_spec()] * 4 + [any_spec()] * 2,
        out_specs=[vmem_spec()] * 5,
        scratch_shapes=gather_scratch(micro, seq, width)
        + scatter_scratch(micro, seq, half_rows, width)
        + scatter_scratch(micro, seq, half_rows, width)
        + [
            pltpu.VMEM((width, 2 * ff - LANES), low_type),
            pltpu.VMEM((width, 2 * LANES), low_type),
            pltpu.VMEM((micro, seq, width), low_type),
            pltpu.VMEM((micro, seq, ff), low_type),
            pltpu.VMEM((micro, seq, ff), low_type),
            pltpu.SemaphoreType.DMA,
            pltpu.SemaphoreType.DMA((micro,)),
        ],
        compiler_params=params(7),
        cost_estimate=COST,
        name="ffn_turn",
    )(hidden, grad_low, vectors, up_biases, given, packed)
    return out, grad_hidden, grads, small, up_bias[:1]


def ffn_backward(grad_low, hidden, kept, vectors, packed, at, layer, half_ff):
    second, upper = kept
    micro, half_rows, width = hidden.shape
    seq, ff = upper.shape[1:]
    low_type, high_type = jnp.bfloat16, jnp.float32
    grad_hidden, grads, small, up_bias = pl.pallas_call(
        functools.partial(ffn_backward_kernel, half_ff, at, layer),
        out_shape=[
            shape_of((micro, half_rows, width), high_type),
            shape_of((width, 2 * ff - LANES), low_type),
            shape_of((8, width), high_type),
            shape_of((8, ff), high_type),
        ],
        in_specs=[vmem_spec()] * 3 + [any_spec()] * 3,
        out_specs=[vmem_spec()] * 4,
        scratch_shapes=gather_scratch(micro, seq, width)
        + scatter_scratch(micro, seq, half_rows, width)
        + [
            pltpu.VMEM((width, 2 * ff - LANES), low_type),
            pltpu.VMEM((width, 2 * LANES), low_type),
            pltpu.VMEM((micro, seq, width), low_type),
            pltpu.VMEM((micro, seq, ff), high_type),
            pltpu.VMEM((micro, seq, ff), low_type),
            pltpu.VMEM((micro, seq, ff), low_type),
            pltpu.SemaphoreType.DMA((1 + 2 * micro,)),
        ],
        compiler_params=params(2),
        cost_estimate=COST,
        name="ffn_backward",
    )(grad_low, hidden, vectors, second, upper, packed)
    return grad_hidden, grads, small, up_bias[:1]


def attn_backward(
    grad_hidden, rows_low, kept, vectors, packed, at, layer, lengths, own_rows, errand, both_ways
):
    normed, qkv, lse, mixed = kept
    micro, half_rows, width = grad_hidden.shape
    seq, pair = mixed.shape[1:]
    heads = pair // LANES
    low_type, high_type = jnp.bfloat16, jnp.float32
    out, grads, small, bias, got = pl.pallas_call(
        functools.partial(attn_backward_kernel, at, layer, own_rows, both_ways),
        out_shape=[
            shape_of((micro, half_rows, width), low_type),
            shape_of((width, 4 * heads * HEAD), low_type),
            shape_of((8, width), high_type),
            shape_of((8, pair), high_type),
            shape_of(errand.shape, errand.dtype),
        ],
        in_specs=[vmem_spec()] * 4 + [smem_spec()] + [any_spec()] * 5,
        out_specs=[vmem_spec()] * 4 + [any_spec()],
        scratch_shapes=gather_scratch(micro, seq, width)
        + scatter_scratch(micro, seq, half_rows, width)
        + [
            pltpu.VMEM((width, 4 * heads * HEAD), low_type),
            pltpu.VMEM((width, 4 * pair), low_type),
            pltpu.VMEM((micro, seq, width), low_type),
            pltpu.VMEM((micro, seq, 3 * pair), low_type),
            pltpu.VMEM((micro, seq, pair), low_type),
            pltpu.VMEM((micro, seq, pair), low_type),
            pltpu.VMEM((micro, seq, 3 * pair), low_type),
            pltpu.VMEM((micro, heads, LANES, seq), low_type),
            pltpu.VMEM((micro, seq, LANES), high_type),
            pltpu.VMEM((seq, seq), low_type),
            pltpu.VMEM((seq, seq), low_type),
            pltpu.VMEM((micro, heads, seq, seq), high_type),
            pltpu.SemaphoreType.DMA((2,)),
            pltpu.SemaphoreType.DMA((1 + 3 * micro,)),
        ],
        compiler_params=params(3 + 5 * layer),
        cost_estimate=COST,
        name="attn_backward",
    )(grad_hidden, rows_low, vectors, lse, lengths, normed, qkv, mixed, packed, errand)
    return out, grads, small, bias, got


def slab_peers():
    section, tensor = lax.axis_index("section"), lax.axis_index("tensor")
    peers = []
    for role in range(1, 8):
        far, step = role // 4, role % 4
        other = section + far * (1 - 2 * section)
        to = (other, lax.rem(tensor + step, 4))
        source = (other, lax.rem(tensor + 4 - step, 4))
        peers.append((role, to, source))
    return peers


def column_peers(count):
    here = lax.axis_index("dp")
    return [
        (step, lax.rem(here + step, count), lax.rem(here + count - step, count))
        for step in range(1, count)
    ]


def greet_all(count):
    barrier = pltpu.get_barrier_semaphore()
    for _, to, _ in slab_peers():
        pl.semaphore_signal(barrier, inc=1, device_id=named(to), device_id_type=MESH)
    for _, to, _ in column_peers(count):
        pl.semaphore_signal(barrier, inc=1, device_id={"dp": to}, device_id_type=MESH)
    pl.semaphore_wait(barrier, 7 + count - 1)


def remote(src, dst, send_sem, recv_sem, peer):
    return pltpu.make_async_remote_copy(
        src_ref=src,
        dst_ref=dst,
        send_sem=send_sem,
        recv_sem=recv_sem,
        device_id=peer,
        device_id_type=MESH,
    )


def prologue_kernel(
    count, heads, qkv_ref, out_ref_t, up_ref_in, down_ref_t, gains_ref, shifts_ref, up_bias, rows_ref,
    first_hbm, normed_hbm, attn_ref, ff_zero_hbm, ff_one_hbm, out_ref, up_ref, bias_ref,
    attn_parts, ff_parts, up_halves, mine_ref, all_rows, line, ff_line, column, slab, up_got,
    rows_send, rows_recv, column_send, column_recv, slab_send, slab_recv, swap_send, swap_recv,
    right_send, right_recv, left_send, left_recv, out_sems,
):
    section, tensor, here = (lax.axis_index(name) for name in ("section", "tensor", "dp"))
    width = out_ref.shape[2]
    chunk = width // (4 * count)
    rows = attn_parts.shape[1]
    micro, own_rows = rows_ref.shape[:2]
    pieces = swap_send.shape[0] - 2
    size = rows // pieces
    other = {"section": 1 - section}
    pair = heads * LANES
    pair_cols = heads * HEAD
    half_ff = up_ref_in.shape[1] // 2
    main = half_ff // LANES * LANES
    extra = half_ff - main
    greet_all(count)
    for half in range(2):
        span = slice(half * pair_cols, (half + 1) * pair_cols)
        parts = [qkv_ref[k, :, span] for k in range(3)] + [out_ref_t[:, span]]
        attn_parts[half] = jnp.concatenate(parts, axis=1)
    keep_slot = jnp.where(section == 0, here, count)
    send_slot = jnp.where(section == 0, here, count)
    got_slot = jnp.where(section == 0, count, here)
    sent = []
    for p in range(pieces):
        span = pl.ds(p * size, size)
        copy = remote(
            attn_parts.at[1 - section, span],
            line.at[send_slot, span],
            swap_send.at[p],
            swap_recv.at[p],
            other,
        )
        copy.start()
        sent.append(copy)
    line[keep_slot] = attn_parts[section]
    mine_ref[...] = jnp.zeros_like(mine_ref)
    gains = gains_ref.shape[0]
    mine_ref[:gains, :chunk] = gains_ref[...]
    mine_ref[gains:, :chunk] = shifts_ref[...]
    column[here] = mine_ref[...]
    for step, to, _ in column_peers(count):
        copy = remote(
            mine_ref, column.at[here], column_send.at[step], column_recv.at[step], {"dp": to}
        )
        copy.start()
        sent.append(copy)

    def swapped(p):
        got = line.at[got_slot, pl.ds(p * size, size)]
        remote(got, got, swap_send.at[p], swap_recv.at[p], other).wait_recv()

    def hop(step, p, way, finish=False):
        origin = here - way * step
        sends, recvs = (right_send, right_recv) if way == 1 else (left_send, left_recv)
        inside = (origin >= 0) if way == 1 else (origin < count)
        onward = (here + 1 < count) if way == 1 else (here > 0)
        slot = line.at[jnp.clip(origin, 0, count - 1), pl.ds(p * size, size)]
        target = jnp.clip(here + way, 0, count - 1)
        if step > 0 and not finish:

            @pl.when(inside)
            def _():
                remote(slot, slot, sends.at[step, p], recvs.at[step, p], {"dp": target}).wait_recv()

        if step + 1 < count:

            @pl.when(inside & onward)
            def _():
                copy = remote(
                    slot, slot, sends.at[step, p], recvs.at[step + 1, p], {"dp": target}
                )
                if finish:
                    copy.wait_send()
                else:
                    copy.start()

    def hops(step):
        for p in range(pieces):
            for way in (1, -1):
                hop(step, p, way)

    for step, _, source in column_peers(count):
        slot = column.at[source]
        remote(slot, slot, column_send.at[step], column_recv.at[step], {"dp": source}).wait_recv()
    for role, to, _ in slab_peers():
        copy = remote(
            column, slab.at[section, tensor], slab_send.at[role], slab_recv.at[role], named(to)
        )
        copy.start()
        sent.append(copy)
    slab[section, tensor] = column[...]
    for p in range(pieces):

        @pl.when(section == 1)
        def _():
            swapped(p)

        for way in (1, -1):
            hop(0, p, way)
    blank = jnp.zeros((rows, LANES - 2 * extra), jnp.bfloat16)
    up_halves[...] = jnp.zeros_like(up_halves)
    for half in range(2):
        start = half * half_ff
        up_halves[half, :, :half_ff] = up_bias[:, start : start + half_ff]
        ff_parts[half, :, :main] = up_ref_in[:, start : start + main]
        ff_parts[half, :, main : 2 * main] = down_ref_t[:, start : start + main]
        span = slice(start + main, start + half_ff)
        ff_parts[half, :, 2 * main :] = jnp.concatenate(
            [up_ref_in[:, span], down_ref_t[:, span], blank], axis=1
        )
    ff_swap = remote(
        ff_parts.at[1 - section],
        ff_line.at[section],
        swap_send.at[pieces],
        swap_recv.at[pieces],
        other,
    )
    up_swap = remote(
        up_halves.at[1 - section],
        up_got.at[section],
        swap_send.at[pieces + 1],
        swap_recv.at[pieces + 1],
        other,
    )
    up_swap.start()
    for role, _, source in slab_peers():
        slot = slab.at[source[0], source[1]]
        remote(slot, slot, slab_send.at[role], slab_recv.at[role], named(source)).wait_recv()
    ff_swap.start()
    for layer in range(2):
        for part in range(4 * count):
            piece = slab[layer, part % 4, part // 4]
            out_ref[layer, :, part * chunk : (part + 1) * chunk] = piece[:, :chunk]
    tiles = TileGather(all_rows, rows_send, rows_recv)
    for m in range(micro):
        own = tiles.tile(m, tensor)
        for begin in range(0, own_rows, 32):
            end = min(begin + 32, own_rows)
            block = rows_ref[m, begin:end].astype(jnp.float32)
            own[begin:end] = low(layer_norm(block, out_ref[0, 0:1], out_ref[0, 2:3]))
        own[own_rows:] = jnp.zeros((tiles.tile_rows - own_rows, width), jnp.bfloat16)
    tiles.start()
    hops(1)
    start = (2 * tensor + section) * pair_cols
    for layer in range(2):
        turned = pltpu.roll(out_ref[layer], lax.rem(width - start, width), 1)
        empty = jnp.zeros((1, LANES - HEAD), jnp.float32)
        for part, row in ((0, 3), (2, 4)):
            for h in range(heads):
                at = part * pair + h * LANES
                piece = turned[row : row + 1, h * HEAD : (h + 1) * HEAD]
                bias_ref[layer, :, at : at + LANES] = jnp.concatenate([piece, empty], 1)
        bias_ref[layer, :, pair : 2 * pair] = jnp.zeros((1, pair), jnp.float32)
    up_ref[section] = up_halves[section]
    outs = []

    def put(src, dst, i):
        copy = pltpu.make_async_copy(src, dst, out_sems.at[i])
        copy.start()
        outs.append(copy)

    def put_ff(src, section_of_first, i):
        for layer, dst in enumerate((ff_zero_hbm, ff_one_hbm)):
            here_too = layer if section_of_first == 0 else 1 - layer

            @pl.when(section == here_too)
            def _():
                pltpu.make_async_copy(src, dst, out_sems.at[i]).start()

        outs.append(pltpu.make_async_copy(src, ff_zero_hbm, out_sems.at[i]))

    put_ff(ff_parts.at[section], 0, count)
    for step in range(2, count):
        hops(step)
        if step == 2:
            tiles.pass_on()
    if count <= 2:
        tiles.pass_on()
    for p in range(pieces):

        @pl.when(section == 0)
        def _():
            swapped(p)

    for at in range(count):
        put(line.at[at], first_hbm.at[pl.ds(at * rows, rows)], at)
    attn_ref[...] = line[count]
    got = up_got.at[1 - section]
    remote(got, got, swap_send.at[pieces + 1], swap_recv.at[pieces + 1], other).wait_recv()
    up_ref[1 - section] = up_got[1 - section]
    tiles.finish()
    put(all_rows, normed_hbm, count + 2)
    ff_got = ff_line.at[1 - section]
    remote(ff_got, ff_got, swap_send.at[pieces], swap_recv.at[pieces], other).wait_recv()
    put_ff(ff_got, 1, count + 1)
    for step in range(count):
        for p in range(pieces):
            for way in (1, -1):
                hop(step, p, way, True)
    for copy in sent + [ff_swap, up_swap]:
        copy.wait_send()
    tiles.drain()
    for copy in outs:
        copy.wait()


def prologue(qkv, out_t, up, down_t, gains, shifts, up_bias, rows_low, count, heads, tile_rows):
    part_rows = qkv.shape[1]
    micro, _, width = rows_low.shape
    vector_rows = gains.shape[0] + shifts.shape[0]
    half_ff = up.shape[1] // 2
    ff_wide = round_up(half_ff, LANES)
    attn_shape = (part_rows, 4 * heads * HEAD)
    ff_shape = (2, part_rows, 2 * ff_wide - LANES)
    all_rows = (micro, 4 * tile_rows, width)
    pieces = 3 if part_rows % 96 == 0 else 1
    low_type, high_type = jnp.bfloat16, jnp.float32
    dma = pltpu.SemaphoreType.DMA
    return pl.pallas_call(
        functools.partial(prologue_kernel, count, heads),
        out_shape=[
            shape_of((count * part_rows, attn_shape[1]), low_type),
            shape_of(all_rows, low_type),
            shape_of(attn_shape, low_type),
            shape_of(ff_shape[1:], low_type),
            shape_of(ff_shape[1:], low_type),
            shape_of((2, vector_rows, width), high_type),
            shape_of((2, 1, ff_wide), high_type),
            shape_of((2, 1, 3 * heads * LANES), high_type),
        ],
        in_specs=[vmem_spec()] * 8,
        out_specs=[any_spec()] * 2 + [vmem_spec()] + [any_spec()] * 2 + [vmem_spec()] * 3,
        scratch_shapes=[
            pltpu.VMEM((2,) + attn_shape, low_type),
            pltpu.VMEM(ff_shape, low_type),
            pltpu.VMEM((2, 1, ff_wide), high_type),
            pltpu.VMEM((vector_rows, LANES), high_type),
            pltpu.VMEM(all_rows, low_type),
            pltpu.VMEM((count + 1,) + attn_shape, low_type),
            pltpu.VMEM(ff_shape, low_type),
            pltpu.VMEM((count, vector_rows, LANES), high_type),
            pltpu.VMEM((2, 4, count, vector_rows, LANES), high_type),
            pltpu.VMEM((2, 1, ff_wide), high_type),
            dma((micro, 3)),
            dma((micro, 3)),
            dma((count,)),
            dma((count,)),
            dma((8,)),
            dma((8,)),
            dma((pieces + 2,)),
            dma((pieces + 2,)),
            dma((count, pieces)),
            dma((count, pieces)),
            dma((count, pieces)),
            dma((count, pieces)),
            dma((count + 3,)),
        ],
        compiler_params=params(4),
        cost_estimate=COST,
        name="prologue",
    )(qkv, out_t, up, down_t, gains, shifts, up_bias, rows_low)


def home_kernel(
    count, chunk, attn_zero, attn_one, ff_zero, ff_one, biases_in, ups_in,
    ff_sum_hbm, attn_sum_hbm, rows_hbm,
    out_ref, up_ref, ff_got_hbm, attn_got_hbm, rows_got_hbm,
    parts, ups, slab, column, up_pair, up_column, total,
    column_send, column_recv, slab_send, slab_recv, up_sems, up_column_send, up_column_recv, far_send, far_recv,
):
    section, tensor, here = (lax.axis_index(name) for name in ("section", "tensor", "dp"))
    width = attn_zero.shape[1]
    heads = biases_in.shape[2] // LANES
    other = {"section": 1 - section}
    greet_all(count)
    parts[...] = jnp.zeros_like(parts)
    start = (2 * tensor + section) * (heads * HEAD)
    for layer, (attn, ff) in enumerate(((attn_zero, ff_zero), (attn_one, ff_one))):
        bias = biases_in[layer]
        blank = jnp.zeros((8, width - heads * HEAD), jnp.float32)
        pieces = [bias[:, h * LANES : h * LANES + HEAD] for h in range(heads)]
        placed = pltpu.roll(jnp.concatenate(pieces + [blank], 1), start, 1)
        whole = jnp.concatenate(
            [attn[0:1], ff[0:1], attn[1:2], placed[0:2], ff[3:4], ff[1:2], ff[2:3]], axis=0
        )
        for part in range(4 * count):
            piece = whole[:, part * chunk : (part + 1) * chunk]
            parts[layer, part % 4, part // 4, :, :chunk] = piece
        ups[layer] = ups_in[layer]
    sent = []

    def send(src, dst, send_sem, recv_sem, peer):
        copy = remote(src, dst, send_sem, recv_sem, peer)
        copy.start()
        sent.append(copy)

    send(ups.at[1 - section], up_pair.at[section], up_sems.at[0], up_sems.at[1], other)
    for role, to, _ in slab_peers():
        send(
            parts.at[to[0], to[1]], slab.at[role], slab_send.at[role], slab_recv.at[role], named(to)
        )
    far_rows = remote(rows_hbm, rows_got_hbm, far_send.at[0], far_recv.at[0], other)
    far_ff = remote(ff_sum_hbm, ff_got_hbm, far_send.at[1], far_recv.at[1], other)
    far_attn = remote(attn_sum_hbm, attn_got_hbm, far_send.at[2], far_recv.at[2], other)
    one_way = ((far_ff, 1), (far_attn, 0))
    far_rows.start()
    for copy, source in one_way:
        pl.when(section == source)(copy.start)
    up_pair[section] = ups[section]
    value = parts[section, tensor]
    for role, _, source in slab_peers():
        slot = slab.at[role]
        remote(slot, slot, slab_send.at[role], slab_recv.at[role], named(source)).wait_recv()
        value = value + slab[role]
    total[...] = value
    for step, to, _ in column_peers(count):
        send(total.at[to], column.at[step], column_send.at[step], column_recv.at[step], {"dp": to})
    got = up_pair.at[1 - section]
    remote(got, got, up_sems.at[0], up_sems.at[1], other).wait_recv()
    for step, to, _ in column_peers(count):
        send(
            up_pair, up_column.at[here], up_column_send.at[step], up_column_recv.at[step], {"dp": to}
        )
    up_column[here] = up_pair[...]
    result = total[here]
    for step, _, source in column_peers(count):
        slot = column.at[step]
        remote(slot, slot, column_send.at[step], column_recv.at[step], {"dp": source}).wait_recv()
        result = result + column[step]
    out_ref[...] = result
    for step, _, source in column_peers(count):
        slot = up_column.at[source]
        remote(
            slot, slot, up_column_send.at[step], up_column_recv.at[step], {"dp": source}
        ).wait_recv()
    value = up_column[0]
    for at in range(1, count):
        value = value + up_column[at]
    up_ref[...] = value
    far_rows.wait()
    for copy, source in one_way:
        pl.when(section == source)(copy.wait_send)
        pl.when(section != source)(copy.wait_recv)
    for copy in sent:
        copy.wait_send()


def home(attn_small, ff_small, bias_grads, up_grads, ff_sum, attn_sum, rows, count, chunk):
    vector_rows, lanes = 8, LANES
    up_shape = up_grads.shape[1:]
    dma = pltpu.SemaphoreType.DMA
    high_type = jnp.float32
    return pl.pallas_call(
        functools.partial(home_kernel, count, chunk),
        out_shape=[
            shape_of((vector_rows, lanes), high_type),
            shape_of((2,) + up_shape, high_type),
            shape_of(ff_sum.shape, ff_sum.dtype),
            shape_of(attn_sum.shape, attn_sum.dtype),
            shape_of(rows.shape, rows.dtype),
        ],
        in_specs=[vmem_spec()] * 6 + [any_spec()] * 3,
        out_specs=[vmem_spec()] * 2 + [any_spec()] * 3,
        scratch_shapes=[
            pltpu.VMEM((2, 4, count, vector_rows, lanes), high_type),
            pltpu.VMEM((2,) + up_shape, high_type),
            pltpu.VMEM((8, count, vector_rows, lanes), high_type),
            pltpu.VMEM((count, vector_rows, lanes), high_type),
            pltpu.VMEM((2,) + up_shape, high_type),
            pltpu.VMEM((count, 2) + up_shape, high_type),
            pltpu.VMEM((count, vector_rows, lanes), high_type),
            dma((count,)),
            dma((count,)),
            dma((8,)),
            dma((8,)),
            dma((2,)),
            dma((count,)),
            dma((count,)),
            dma((3,)),
            dma((3,)),
        ],
        compiler_params=params(5),
        cost_estimate=COST,
        name="home",
    )(*attn_small, *ff_small, bias_grads, up_grads, ff_sum, attn_sum, rows)


def ff_finish_kernel(zero, one, zero_got, one_got, up_ref, down_ref):
    first = lax.axis_index("section") == 0
    halves = (
        jnp.where(first, zero[...], one_got[...]),
        jnp.where(first, zero_got[...], one[...]),
    )
    half_ff = up_ref.shape[1] // 2
    main = half_ff // LANES * LANES
    extra = half_ff - main
    for k in range(2):
        pieces = []
        for half in halves:
            start = 2 * main + k * extra
            pieces += [half[:, k * main : (k + 1) * main], half[:, start : start + extra]]
        whole = jnp.concatenate(pieces, axis=1).astype(jnp.float32)
        if k == 0:
            up_ref[...] = whole
        else:
            down_ref[...] = whole.T


def ff_finish(sums, got, ff_cols):
    rows = sums[0].shape[0]
    return pl.pallas_call(
        ff_finish_kernel,
        out_shape=[
            shape_of((rows, ff_cols), jnp.float32),
            shape_of((ff_cols, rows), jnp.float32),
        ],
        in_specs=[vmem_spec()] * 4,
        out_specs=[vmem_spec()] * 2,
        compiler_params=pltpu.CompilerParams(vmem_limit_bytes=VMEM_BYTES),
        cost_estimate=COST,
        name="ff_finish",
    )(*sums, *got)


def attn_finish_kernel(zero, one, zero_got, one_got, qkv_ref, out_ref):
    first = lax.axis_index("section") == 0
    halves = (
        jnp.where(first, zero[...], one_got[...]),
        jnp.where(first, zero_got[...], one[...]),
    )
    pair_cols = qkv_ref.shape[2] // 2
    for k in range(4):
        span = slice(k * pair_cols, (k + 1) * pair_cols)
        whole = jnp.concatenate([half[:, span] for half in halves], axis=1).astype(jnp.float32)
        if k < 3:
            qkv_ref[k] = whole
        else:
            out_ref[...] = whole.T


def attn_finish(sums, got, head_cols):
    rows = sums[0].shape[0]
    return pl.pallas_call(
        attn_finish_kernel,
        out_shape=[
            shape_of((3, rows, head_cols), jnp.float32),
            shape_of((head_cols, rows), jnp.float32),
        ],
        in_specs=[vmem_spec()] * 4,
        out_specs=[vmem_spec()] * 2,
        compiler_params=pltpu.CompilerParams(vmem_limit_bytes=VMEM_BYTES),
        name="attn_finish",
    )(*sums, *got)


def shards(
    section_input,
    final_cotangent,
    lengths,
    qkv_weight,
    out_weight,
    up_weight,
    down_weight,
    norm_gains,
    biases,
    up_bias,
):
    here = lax.axis_index("section")
    sections = lax.axis_size("section")
    micro, _, own_rows, _ = section_input.shape
    head_cols = qkv_weight.shape[3]
    pair_cols = head_cols // sections
    heads = pair_cols // HEAD
    ff_cols = up_weight.shape[2]
    half_ff = ff_cols // sections
    half_rows = round_up(-(-own_rows // sections), 32)
    full_rows = half_rows * sections

    def by_layer(mine, other):
        return [jnp.where(here == 0, mine, other), jnp.where(here == 0, other, mine)]

    count = lax.axis_size("dp")
    chunk = norm_gains.shape[2]
    first, normed, attn_part, ff_zero, ff_one, vectors, up_biases, bias_qv = prologue(
        qkv_weight[0],
        out_weight[0].T,
        up_weight[0],
        down_weight[0].T,
        norm_gains[0],
        biases[0],
        up_bias,
        section_input[:, 0],
        count,
        heads,
        full_rows,
    )

    def gather_column(part):
        return lax.all_gather(part, "dp", axis=0, tiled=True)

    ff_first = gather_column(ff_zero)
    attn_packed = [(first, 0), (gather_column(attn_part), 0)]
    ff_packed = [(ff_first, 0), (gather_column(ff_one), 0)]
    lengths_here = lengths.reshape(micro)

    def my_rows(value):
        padded = jnp.pad(value[:, 0], [(0, 0), (0, full_rows - own_rows), (0, 0)])
        return lax.dynamic_slice_in_dim(padded, here * half_rows, half_rows, 1)

    def whole_rows(first, second, got):
        low_half, high_half = by_layer(jnp.where(here == 0, first, second), got)
        return jnp.concatenate([low_half, high_half], 1)[:, None, :own_rows]

    rows = my_rows(section_input)
    inputs, hiddens, attn_kept = [], [], []
    for layer in range(2):
        inputs.append(rows)
        operands = (rows, vectors, bias_qv, *attn_packed[layer], layer, lengths_here, own_rows)
        if layer == 0:
            hidden, kept, grads_all = attn_forward(*operands, normed, final_cotangent[:, 0])
        else:
            hidden, kept = attn_forward(*operands)
        hiddens.append(hidden)
        attn_kept.append(kept)
        if layer == 0:
            rows, ff_kept = ffn_forward(hidden, vectors, up_biases, *ff_packed[0], 0, half_ff)

    attn_sums, ff_sums, up_sums, input_grads = {}, {}, {}, {}
    attn_small, ff_small, bias_grads, errands = {}, {}, {}, {}
    for layer in (1, 0):
        if layer == 1:
            last, grad_hidden, ff_grad, ff_small[1], up_sums[1] = ffn_turn(
                hiddens[1],
                my_rows(final_cotangent),
                grads_all,
                vectors,
                up_biases,
                *ff_packed[1],
                1,
                half_ff,
            )
        else:
            grad_hidden, ff_grad, ff_small[0], up_sums[0] = ffn_backward(
                grads, hiddens[0], ff_kept, vectors, *ff_packed[0], 0, half_ff
            )
        ff_sums[layer] = lax.psum_scatter(ff_grad, "dp", scatter_dimension=0, tiled=True)
        if layer == 1:
            errand, both_ways = jnp.where(here == 0, last, rows), True
        else:
            errand, both_ways = ff_sums[1], False
        grads, attn_grad, attn_small[layer], bias_grads[layer], got = attn_backward(
            grad_hidden,
            inputs[layer],
            attn_kept[layer],
            vectors,
            *attn_packed[layer],
            layer,
            lengths_here,
            own_rows,
            errand,
            both_ways,
        )
        errands[layer] = got
        attn_sums[layer] = lax.psum_scatter(attn_grad, "dp", scatter_dimension=0, tiled=True)
        input_grads[layer] = grads

    section_output = whole_rows(rows, last, errands[1])
    small_mine, up_total, ff_got, attn_got, rows_got = home(
        [attn_small[0], attn_small[1]],
        [ff_small[0], ff_small[1]],
        jnp.stack([bias_grads[0], bias_grads[1]]),
        jnp.stack([up_sums[0], up_sums[1]]),
        ff_sums[0],
        attn_sums[1],
        jnp.where(here == 0, input_grads[1], input_grads[0]),
        count,
        chunk,
    )
    small_mine = small_mine[None, :, :chunk]
    up_total = up_total[:, :, :half_ff].reshape(1, ff_cols)
    input_grad = whole_rows(input_grads[0], input_grads[1], rows_got)

    attn_zero_got = lax.ppermute(attn_sums[0], "section", [(1, 0)])
    up_grad, down_grad = ff_finish([ff_sums[0], ff_sums[1]], [ff_got, errands[0]], ff_cols)
    qkv_total, out_total = attn_finish(
        [attn_sums[0], attn_sums[1]], [attn_zero_got, attn_got], head_cols
    )
    gains = norm_gains.shape[1]
    return (
        section_output[None],
        input_grad[None],
        qkv_total[None],
        out_total[None],
        up_grad[None],
        down_grad[None],
        small_mine[:, :gains],
        small_mine[:, gains:],
        up_total,
    )


def solution(mesh):
    in_specs = (
        P(None, "dp", "tensor", None),
        P(None, "dp", "tensor", None),
        P(None, "dp"),
        P("section", None, "dp", "tensor"),
        P("section", "tensor", "dp"),
        P("section", "dp", "tensor"),
        P("section", "tensor", "dp"),
        P("section", None, ("dp", "tensor")),
        P("section", None, ("dp", "tensor")),
        P("section", "tensor"),
    )
    out_specs = (
        P("section", None, "dp", "tensor", None),
        P("section", None, "dp", "tensor", None),
        P("section", None, "dp", "tensor"),
        P("section", "tensor", "dp"),
        P("section", "dp", "tensor"),
        P("section", "tensor", "dp"),
        P("section", None, ("dp", "tensor")),
        P("section", None, ("dp", "tensor")),
        P("section", "tensor"),
    )
    return jax.shard_map(shards, mesh=mesh, in_specs=in_specs, out_specs=out_specs, check_vma=False)
```

```python
import functools
import math

import jax
import jax.numpy as jnp
from jax import lax
from jax.experimental import pallas as pl
from jax.experimental.pallas import tpu as pltpu
from jax.sharding import PartitionSpec as P


HEAD = 72
LANES = 128
norm_eps = 1e-06
masked_score = -1000000000.0
score_scale = 1.0 / math.sqrt(HEAD)
GELU_A = math.sqrt(2.0 / math.pi)
GELU_B = 0.044715


def round_up(value, step):
    return -(-value // step) * step


def dot(left, right, left_dim, right_dim):
    return lax.dot_general(
        left, right, (((left_dim,), (right_dim,)), ((), ())), preferred_element_type=jnp.float32
    )


def low(value):
    return value.astype(jnp.bfloat16)


def layer_norm(rows, gain_vec, shift_vec):
    centred = rows - jnp.mean(rows, axis=-1, keepdims=True)
    spread = jnp.mean(centred * centred, axis=-1, keepdims=True)
    return centred * lax.rsqrt(spread + norm_eps) * gain_vec + shift_vec


def norm_back(rows, gain_vec, grads):
    centred = rows - jnp.mean(rows, axis=-1, keepdims=True)
    spread = jnp.mean(centred * centred, axis=-1, keepdims=True)
    inverse = lax.rsqrt(spread + norm_eps)
    xhat = centred * inverse
    e = grads * gain_vec
    back = inverse * (
        e
        - jnp.mean(e, axis=-1, keepdims=True)
        - xhat * jnp.mean(e * xhat, axis=-1, keepdims=True)
    )
    return back, grads * xhat


def gelu_tanh(value):
    return jax.nn.gelu(value, approximate=True)


MESH = pl.DeviceIdType.MESH
VMEM_BYTES = 64_000_000
COST = pl.CostEstimate(flops=20_000_000_000, transcendentals=0, bytes_accessed=100_000_000)
LOG2E = 1.0 / math.log(2.0)
TILE = 256
WIDE = 384


class Slab:
    def __init__(self, half_rows):
        self.half_rows = half_rows
        section = lax.axis_index("section")
        tensor = lax.axis_index("tensor")
        core = lax.rem(tensor, 2)
        self.core = core
        self.mine = self.around(section, tensor, core)
        self.theirs = self.around(section, tensor + 1 - 2 * core, 1 - core)
        self.far_role, self.near_role = 1 + core, 2 - core
        self.mate = self.theirs[0]
        over = lax.rem(tensor + 2, 4)
        self.near, self.far = tensor, over
        self.mate_near, self.mate_far = self.mate[1], lax.rem(self.mate[1] + 2, 4)
        self.grid = self.places(section, self.near, self.far)
        self.mate_grid = self.places(section, self.mate_near, self.mate_far)
        self.across_y = self.grid[2]
        self.first, self.second = self.mine[1], self.mine[2]

    def place(self, section, tensor):
        start = (2 * tensor + section) * self.half_rows
        return (section, tensor, pl.multiple_of(start, self.half_rows))

    def places(self, section, near, far):
        flip = 1 - section
        return [self.place(*at) for at in ((section, near), (flip, near), (section, far), (flip, far))]

    def around(self, section, tensor, core):
        over = lax.rem(tensor + 2, 4)
        turn = 1 - 2 * section
        first = (section + (1 - core) * turn, tensor + core * (over - tensor))
        second = (section + core * turn, tensor + (1 - core) * (over - tensor))
        places = ((section, tensor), first, second, (1 - section, over))
        return [self.place(*at) for at in places]

    def rows(self, ref, at):
        return ref.at[pl.ds(at[2], self.half_rows)]

    def greet(self):
        barrier = pltpu.get_barrier_semaphore()
        for peer in (self.first, self.second, self.mate):
            pl.semaphore_signal(barrier, inc=1, device_id=named(peer), device_id_type=MESH)
        pl.semaphore_wait(barrier, 3)


def named(at):
    return {"section": at[0], "tensor": at[1]}


class Moves:
    def __init__(self, slab, send_sems, recv_sems):
        self.slab, self.send_sems, self.recv_sems = slab, send_sems, recv_sems
        self.sent = []

    def copy(self, src, dst, role, peer):
        return pltpu.make_async_remote_copy(
            src_ref=src,
            dst_ref=dst,
            send_sem=self.send_sems.at[role],
            recv_sem=self.recv_sems.at[role],
            device_id=named(peer),
            device_id_type=MESH,
        )

    def send(self, ends, role, peer):
        self.copy(*ends(), role, peer).start()
        self.sent.append(lambda: self.copy(*ends(), role, peer))

    def arrived(self, dst, role):
        self.copy(dst, dst, role, self.slab.mate).wait_recv()

    def drain(self):
        for copy in self.sent:
            copy().wait_send()


class Gather(Moves):
    def __init__(self, slab, whole, send_sems, recv_sems):
        super().__init__(slab, send_sems, recv_sems)
        self.whole = whole

    def pass_on(self, at, role, peer):
        self.send(lambda: (self.slab.rows(self.whole, at),) * 2, role, peer)

    def arrive(self, at, role):
        self.arrived(self.slab.rows(self.whole, at), role)

    def start(self):
        mine = self.slab.mine
        self.pass_on(mine[0], 0, mine[1])
        self.pass_on(mine[0], 3, self.slab.mate)

    def second(self):
        self.sent.pop(0)().wait_send()
        self.pass_on(self.slab.mine[0], 1, self.slab.mine[2])

    def forward(self):
        mine, mate = self.slab.mine, self.slab.mate
        self.arrive(mine[1], 0)
        self.pass_on(mine[1], 2, mine[2])
        self.pass_on(mine[1], 4, mate)

    def to_mate(self):
        mine, mate = self.slab.mine, self.slab.mate
        self.arrive(mine[2], 1)
        self.pass_on(mine[2], 5, mate)
        self.arrive(mine[3], 2)
        self.pass_on(mine[3], 6, mate)

    def finish(self):
        for k in range(4):
            self.arrive(self.slab.theirs[k], 3 + k)
        self.drain()


class TileGather:
    def __init__(self, whole, send_sems, recv_sems):
        self.whole, self.send_sems, self.recv_sems = whole, send_sems, recv_sems
        self.tensor = lax.axis_index("tensor")
        self.over = lax.rem(self.tensor + 2, 4)
        self.mate = self.tensor + 1 - 2 * lax.rem(self.tensor, 2)
        self.micro, rows = whole.shape[0], whole.shape[1] // 4
        self.tile_rows = rows
        self.sent = []

    def tile(self, m, index):
        start = pl.multiple_of(index * self.tile_rows, self.tile_rows)
        return self.whole.at[m, pl.ds(start, self.tile_rows)]

    def copy(self, m, index, role, peer):
        part = self.tile(m, index)
        return remote(
            part, part, self.send_sems.at[m, role], self.recv_sems.at[m, role], {"tensor": peer}
        )

    def send(self, m, index, role, peer):
        self.copy(m, index, role, peer).start()
        self.sent.append(lambda: self.copy(m, index, role, peer))

    def start(self):
        for m in range(self.micro):
            self.send(m, self.tensor, 0, self.over)
            self.send(m, self.tensor, 1, self.mate)

    def pass_on(self):
        for m in range(self.micro):
            self.copy(m, self.over, 0, self.over).wait_recv()
            self.send(m, self.over, 2, self.mate)

    def finish(self):
        for m in range(self.micro):
            self.copy(m, self.mate, 1, self.mate).wait_recv()
            self.copy(m, lax.rem(self.mate + 2, 4), 2, self.mate).wait_recv()

    def drain(self):
        for copy in self.sent:
            copy().wait_send()


class Scatter(Moves):
    def __init__(self, slab, terms, from_mate, outgoing, arrivals, send_sems, recv_sems):
        super().__init__(slab, send_sems, recv_sems)
        self.terms, self.from_mate, self.outgoing = terms, from_mate, outgoing
        self.relay, self.from_second, self.from_first = (arrivals.at[k] for k in range(3))

    def to_mate(self, at, role):
        self.send(
            lambda: (self.slab.rows(self.terms, at), self.from_mate.at[role]), role, self.slab.mate
        )

    def mate_far(self):
        self.to_mate(self.slab.mate_grid[3], 3)
        self.to_mate(self.slab.mate_grid[2], self.slab.far_role)

    def mate_near(self):
        self.to_mate(self.slab.mate_grid[1], self.slab.near_role)
        self.to_mate(self.slab.mate_grid[0], 0)

    def chip_sum(self, k, rows):
        part = self.slab.rows(self.terms, self.slab.mine[k])
        return part[rows].astype(jnp.float32) + self.from_mate[k, rows].astype(jnp.float32)

    def blocks(self):
        return [pl.ds(start, 32) for start in range(0, self.slab.half_rows, 32)]

    def hop(self, k, slot, dst, role, peer, ride=None):
        self.arrived(self.from_mate.at[k], k)
        if ride is not None:
            self.arrived(ride, 4)
        for rows in self.blocks():
            value = self.chip_sum(k, rows)
            if ride is not None:
                value = value + ride[rows].astype(jnp.float32)
            self.outgoing[slot, rows] = low(value)
        self.send(lambda: (self.outgoing.at[slot], dst), role, peer)

    def far_hop(self):
        self.hop(3, 0, self.relay, 4, self.slab.second)

    def second_hop(self):
        self.hop(2, 1, self.from_second, 5, self.slab.second)

    def first_hop(self):
        self.hop(1, 2, self.from_first, 6, self.slab.first, self.relay)

    def finish(self):
        self.arrived(self.from_mate.at[0], 0)
        self.arrived(self.from_second, 5)
        self.arrived(self.from_first, 6)
        self.drain()

    def total(self, rows):
        other = self.from_second[rows].astype(jnp.float32) + self.from_first[rows].astype(
            jnp.float32
        )
        return self.chip_sum(0, rows) + other


def scatter_scratch(micro, seq, half_rows, width):
    return [
        pltpu.VMEM((micro, seq, width), jnp.bfloat16),
        pltpu.VMEM((micro, 4, half_rows, width), jnp.bfloat16),
        pltpu.VMEM((micro, 3, half_rows, width), jnp.bfloat16),
        pltpu.VMEM((micro, 3, half_rows, width), jnp.bfloat16),
        pltpu.SemaphoreType.DMA((micro, 7)),
        pltpu.SemaphoreType.DMA((micro, 7)),
    ]


def gather_scratch(micro, seq, width):
    return [
        pltpu.VMEM((micro, seq, width), jnp.bfloat16),
        pltpu.SemaphoreType.DMA((micro, 7)),
        pltpu.SemaphoreType.DMA((micro, 7)),
    ]


def make_scatters(slab, refs, micro):
    terms, from_mate, outgoing, arrivals, send_sems, recv_sems = refs
    return [
        Scatter(
            slab,
            terms.at[m],
            from_mate.at[m],
            outgoing.at[m],
            arrivals.at[m],
            send_sems.at[m],
            recv_sems.at[m],
        )
        for m in range(micro)
    ]


def make_gathers(slab, refs, micro):
    whole, send_sems, recv_sems = refs
    return [
        Gather(slab, whole.at[m], send_sems.at[m], recv_sems.at[m]) for m in range(micro)
    ]


def step_from(start, i, size):
    return pl.ds(pl.multiple_of(start + i * size, size), size)


def step_rows(i, size):
    return pl.ds(pl.multiple_of(i * size, size), size)


def repeat(count, body):
    def one(i, carry):
        body(i)
        return carry

    lax.fori_loop(0, count, one, 0)


def shut_keys(length, own_rows, full_rows, shape, dimension):
    place = lax.broadcasted_iota(jnp.int32, shape, dimension)
    step = jnp.zeros(shape, jnp.int32)
    for t in range(1, 4):
        step += (place >= t * full_rows).astype(jnp.int32)
    live = (place - step * full_rows < own_rows) & (
        place - step * (full_rows - own_rows) < length
    )
    return jnp.where(live, 0.0, masked_score)


def stages(count, work, hooks):
    def body(k):
        work(k)
        for at, steps in hooks.items():

            @pl.when(k == at)
            def _():
                for step in steps:
                    step()

    repeat(count, body)


def chip_rows(slab, k):
    far, near = slab.far - slab.core, slab.near - slab.core
    start = (far + lax.rem(k, 2) * (near - far)) * (2 * slab.half_rows)
    return pl.multiple_of(start, 2 * slab.half_rows)


def open_gathers(gathers, fill, prepare):
    fill(0)
    gathers[0].start()
    fill(1)
    gathers[0].second()
    gathers[1].start()
    prepare()
    gathers[0].forward()
    gathers[1].second()


def widen(packed, wide):
    heads = packed.shape[1] // HEAD

    def block(i):
        rows = step_rows(i, 128)
        for h in range(heads):
            piece = packed[rows, h * HEAD : (h + 1) * HEAD]
            blank = jnp.zeros((128, LANES - HEAD), jnp.bfloat16)
            wide[rows, h * LANES : (h + 1) * LANES] = jnp.concatenate([piece, blank], axis=1)

    repeat(packed.shape[0] // 128, block)


def split_tail(packed, tails, up_cols):
    start = packed.shape[1] - LANES

    def block(i):
        rows = step_rows(i, 128)
        for j in range(2):
            piece = packed[rows, start + j * up_cols : start + (j + 1) * up_cols]
            blank = jnp.zeros((128, LANES - up_cols), jnp.bfloat16)
            tails[rows, j * LANES : (j + 1) * LANES] = jnp.concatenate([piece, blank], axis=1)

    repeat(packed.shape[0] // 128, block)


def up_dot(rows, packed, tails):
    main = (packed.shape[1] - LANES) // 2
    first = dot(rows, packed[:, :main], 1, 0)
    return jnp.concatenate([first, dot(rows, tails[:, :LANES], 1, 0)], axis=1)


def up_back(grads, packed, tails):
    main = (packed.shape[1] - LANES) // 2
    return dot(grads[:, :main], packed[:, :main], 1, 1) + dot(
        grads[:, main:], tails[:, :LANES], 1, 1
    )


def down_dot(active, packed, tails):
    main = (packed.shape[1] - LANES) // 2
    return dot(active[:, :main], packed[:, main : 2 * main], 1, 1) + dot(
        active[:, main:], tails[:, LANES:], 1, 1
    )


def down_back(rows, packed, tails):
    main = (packed.shape[1] - LANES) // 2
    first = dot(rows, packed[:, main : 2 * main], 1, 0)
    return jnp.concatenate([first, dot(rows, tails[:, LANES:], 1, 0)], axis=1)


def attn_forward_kernel(
    ready, at, layer, own_rows, rows_ref, vectors, bias_ref, lengths, packed_hbm, given_hbm, grads_ref,
    hidden_ref, lse_ref, normed_hbm, qkv_hbm, mixed_hbm, *rest
):
    micro, half_rows, width = rows_ref.shape
    gathered, gather_refs = rest[0], rest[0:3]
    scatter_refs = rest[3:9]
    terms = rest[3]
    packed, wide, qkv, mixed, load_sem, keep_sems, given_sems, all_grads, tile_send, tile_recv = rest[9:]
    vec, bias = vectors.at[layer], bias_ref[layer]
    seq = qkv.shape[1]
    pair = mixed.shape[2]
    heads = pair // LANES
    load = pltpu.make_async_copy(
        packed_hbm.at[:, at : at + packed.shape[1]], packed, load_sem
    )
    load.start()
    slab = Slab(half_rows)
    gathers = make_gathers(slab, gather_refs, micro)
    scatters = make_scatters(slab, scatter_refs, micro)
    given = [
        pltpu.make_async_copy(given_hbm.at[m], gathered.at[m], given_sems.at[m])
        for m in range(micro if ready else 0)
    ]
    for copy in given:
        copy.start()
    slab.greet()
    if ready:
        tiles = TileGather(all_grads, tile_send, tile_recv)
        for m in range(micro):
            own = tiles.tile(m, tiles.tensor)
            count = grads_ref.shape[1]
            own[:count] = grads_ref[m]
            own[count:] = jnp.zeros((tiles.tile_rows - count, width), jnp.bfloat16)
        tiles.start()

    def fill(m):
        own = slab.rows(gathered.at[m], slab.mine[0])
        for start in range(0, half_rows, 32):
            block = rows_ref[m, pl.ds(start, 32)].astype(jnp.float32)
            own[pl.ds(start, 32)] = low(layer_norm(block, vec[0:1], vec[2:3]))

    def prepare():
        load.wait()
        widen(packed, wide)

    if ready:
        prepare()
    else:
        open_gathers(gathers, fill, prepare)
    keeps = []

    def keep(src, dst, m, i):
        def copy():
            return pltpu.make_async_copy(src.at[m], dst.at[m], keep_sems.at[i])

        copy().start()
        keeps.append(copy)

    def project(m):
        def block(i):
            rows = step_rows(i, 4 * half_rows)
            out = dot(gathered[m, rows], wide[:, : 3 * pair], 1, 0)
            qkv[m, rows] = low(out + bias)

        repeat(seq // (4 * half_rows), block)

    def attend(m, rows):
        shut = shut_keys(lengths[m], own_rows, 2 * half_rows, (1, seq), 1)
        for h in range(heads):
            cols = slice(h * LANES, (h + 1) * LANES)
            q = qkv[m, rows, cols]
            k = qkv[m, :, pair + h * LANES : pair + (h + 1) * LANES]
            v = qkv[m, :, 2 * pair + h * LANES : 2 * pair + (h + 1) * LANES]
            scores = dot(q, k, 1, 1) * (score_scale * LOG2E) + shut
            top = jnp.max(scores, axis=-1, keepdims=True)
            exp_scores = jnp.exp2(scores - top)
            total = jnp.sum(exp_scores, axis=-1, keepdims=True)
            probs = low(exp_scores * (1.0 / total))
            mixed[m, rows, cols] = low(dot(probs, v, 1, 0))
            lse_ref[m, h, rows] = jnp.broadcast_to(
                top + jnp.log(total) * LOG2E, (2 * half_rows, LANES)
            )

    def output(m, rows):
        terms[m, rows] = low(dot(mixed[m, rows], wide[:, 3 * pair :], 1, 1))

    def close(m):
        scatters[m].finish()
        for rows in scatters[m].blocks():
            start = rows_ref[m, rows].astype(jnp.float32)
            hidden_ref[m, rows] = start + scatters[m].total(rows) + vec[5:6]

    def gathered_rows(m):
        if ready:
            given[m].wait()
            return
        gathers[m].to_mate()
        gathers[m].finish()
        keep(gathered, normed_hbm, m, m)

    def work(k):
        m = lax.div(k, 2)
        start = chip_rows(slab, k)
        pl.when(lax.rem(k, 2) == 0)(lambda: project(m))

        def piece(i):
            attend(m, step_from(start, i, 2 * half_rows))

        repeat(2, piece)
        output(m, pl.ds(start, 4 * half_rows))

    def keep_two(m):
        keep(qkv, qkv_hbm, m, 2 + 2 * m)
        keep(mixed, mixed_hbm, m, 3 + 2 * m)

    def grads_on():
        if ready:
            tiles.pass_on()

    def grads_in():
        if ready:
            tiles.finish()
            for m in range(micro):
                keep(all_grads, normed_hbm, m, m)

    gathered_rows(0)
    if not ready:
        gathers[1].forward()
    zero, one = scatters
    stages(
        4,
        work,
        {
            0: [zero.mate_far, lambda: gathered_rows(1), zero.far_hop],
            1: [zero.mate_near, lambda: keep_two(0), zero.second_hop, zero.first_hop, grads_on],
            2: [one.mate_far, lambda: close(0), one.far_hop, grads_in],
            3: [one.mate_near, lambda: keep_two(1), one.second_hop, one.first_hop],
        },
    )
    close(1)
    if ready:
        tiles.drain()
    for copy in keeps:
        copy().wait()


def ffn_forward_kernel(
    half_ff, at, layer, hidden_ref, vectors, up_biases, packed_hbm, out_ref, second_hbm, upper_hbm, *rest
):
    micro, half_rows, _ = hidden_ref.shape
    gathered, gather_refs = rest[0], rest[0:3]
    scatter_refs = rest[3:9]
    terms = rest[3]
    packed, tails, upper, load_sem, keep_sems = rest[9:]
    vec, up_bias = vectors.at[layer], up_biases.at[layer]
    _, ff = upper.shape[1:]
    load = pltpu.make_async_copy(
        packed_hbm.at[:, at : at + packed.shape[1]], packed, load_sem
    )
    load.start()
    slab = Slab(half_rows)
    gathers = make_gathers(slab, gather_refs, micro)
    scatters = make_scatters(slab, scatter_refs, micro)
    slab.greet()

    def fill(m):
        own = slab.rows(gathered.at[m], slab.mine[0])
        for start in range(0, half_rows, 32):
            block = hidden_ref[m, pl.ds(start, 32)]
            own[pl.ds(start, 32)] = low(layer_norm(block, vec[1:2], vec[6:7]))

    def prepare():
        load.wait()
        split_tail(packed, tails, half_ff - ff + LANES)

    open_gathers(gathers, fill, prepare)
    keeps = []

    def keep(src, dst, m, i):
        def copy():
            return pltpu.make_async_copy(src.at[m], dst.at[m], keep_sems.at[i])

        copy().start()
        keeps.append(copy)

    def compute(m, rows):
        value = up_dot(gathered[m, rows], packed, tails) + up_bias[...]
        upper[m, rows] = value
        active = low(gelu_tanh(value))
        terms[m, rows] = low(down_dot(active, packed, tails))

    def close(m):
        scatters[m].finish()
        for rows in scatters[m].blocks():
            out_ref[m, rows] = low(hidden_ref[m, rows] + scatters[m].total(rows) + vec[7:8])

    def work(k):
        compute(lax.div(k, 2), pl.ds(chip_rows(slab, k), 4 * half_rows))

    gathers[0].to_mate()
    gathers[0].finish()
    keep(gathered, second_hbm, 0, 0)
    zero, one = scatters
    stages(
        4,
        work,
        {
            0: [zero.mate_far, gathers[1].forward, zero.far_hop],
            1: [
                zero.mate_near,
                lambda: keep(upper, upper_hbm, 0, 1),
                gathers[1].to_mate,
                zero.second_hop,
                gathers[1].finish,
                lambda: keep(gathered, second_hbm, 1, 2),
            ],
            2: [one.mate_far, zero.first_hop, one.far_hop],
            3: [one.mate_near, lambda: keep(upper, upper_hbm, 1, 3), one.second_hop],
        },
    )
    close(0)
    one.first_hop()
    close(1)
    for copy in keeps:
        copy().wait()


def ffn_backward_kernel(
    half_ff, at, layer, grad_ref, hidden_ref, vectors, second_hbm, upper_hbm, packed_hbm,
    out_ref, grads_ref, small_ref, up_bias_ref, *rest
):
    micro, half_rows, width = hidden_ref.shape
    gathered, gather_refs = rest[0], rest[0:3]
    scatter_refs = rest[3:9]
    terms = rest[3]
    packed, tails, second, upper, grad_upper, active, load_sems = rest[9:]
    vec = vectors.at[layer]
    seq, ff = upper.shape[1:]
    main = ff - LANES
    extra = half_ff - main
    load_packed = pltpu.make_async_copy(
        packed_hbm.at[:, at : at + packed.shape[1]], packed, load_sems.at[0]
    )
    load_packed.start()
    load_upper, load_second = [], []
    for m in range(micro):
        load_upper.append(
            pltpu.make_async_copy(upper_hbm.at[m], upper.at[m], load_sems.at[1 + m])
        )
        load_upper[m].start()
    for m in range(micro):
        load_second.append(
            pltpu.make_async_copy(second_hbm.at[m], second.at[m], load_sems.at[1 + micro + m])
        )
        load_second[m].start()
    slab = Slab(half_rows)
    gathers = make_gathers(slab, gather_refs, micro)
    scatters = make_scatters(slab, scatter_refs, micro)
    slab.greet()

    def fill(m):
        own = slab.rows(gathered.at[m], slab.mine[0])
        for start in range(0, half_rows, 32):
            own[pl.ds(start, 32)] = grad_ref[m, pl.ds(start, 32)]

    def prepare():
        small_ref[...] = jnp.zeros_like(small_ref)
        up_bias_ref[...] = jnp.zeros_like(up_bias_ref)
        load_packed.wait()
        split_tail(packed, tails, extra)

    open_gathers(gathers, fill, prepare)

    def compute(m, rows):
        value = upper[m, rows]
        square = value * value
        bent = jnp.tanh(GELU_A * value * (1.0 + GELU_B * square))
        half = 0.5 * (1.0 + bent)
        active[m, rows] = low(value * half)
        slope = half + (0.5 * GELU_A) * value * (1.0 - bent * bent) * (1.0 + 3.0 * GELU_B * square)
        grad_active = down_back(gathered[m, rows], packed, tails)
        grad = low(grad_active * slope)
        grad_upper[m, rows] = grad
        up_bias_ref[0:1] += jnp.sum(grad.astype(jnp.float32), axis=0, keepdims=True)
        terms[m, rows] = low(up_back(grad, packed, tails))

    def stacked(ref, cols=slice(None)):
        return ref[:, :, cols].reshape(micro * seq, -1)

    def weight_grads(hooks):
        def block(i):
            cols = step_rows(i, WIDE)
            up = dot(stacked(second, cols), stacked(grad_upper), 0, 0)
            down = dot(stacked(gathered, cols), stacked(active), 0, 0)
            grads_ref[cols, :main] = low(up[:, :main])
            grads_ref[cols, main : 2 * main] = low(down[:, :main])
            blank = jnp.zeros((WIDE, LANES - 2 * extra), jnp.float32)
            rest_cols = [up[:, main : main + extra], down[:, main : main + extra], blank]
            grads_ref[cols, 2 * main :] = low(jnp.concatenate(rest_cols, axis=1))

        stages(width // WIDE, block, hooks)

    def close(m):
        scatters[m].finish()
        for rows in scatters[m].blocks():
            grad_normed = scatters[m].total(rows)
            back, gain_terms = norm_back(hidden_ref[m, rows], vec[1:2], grad_normed)
            grad_rows = grad_ref[m, rows].astype(jnp.float32)
            grad_hidden = grad_rows + back
            out_ref[m, rows] = grad_hidden
            branch = low(grad_hidden).astype(jnp.float32)
            for j, item in enumerate((gain_terms, grad_normed, grad_rows, branch)):
                small_ref[j : j + 1] += jnp.sum(item, axis=0, keepdims=True)

    def work(k):
        compute(lax.div(k, 2), pl.ds(chip_rows(slab, k), 4 * half_rows))

    gathers[0].to_mate()
    gathers[0].finish()
    load_upper[0].wait()
    zero, one = scatters
    stages(
        4,
        work,
        {
            0: [zero.mate_far, gathers[1].forward, zero.far_hop],
            1: [
                zero.mate_near,
                gathers[1].to_mate,
                zero.second_hop,
                gathers[1].finish,
                load_upper[1].wait,
            ],
            2: [one.mate_far, zero.first_hop, one.far_hop],
            3: [one.mate_near, one.second_hop],
        },
    )
    for load in load_second:
        load.wait()
    weight_grads({0: [one.first_hop, lambda: close(0)]})
    close(1)


def ffn_turn_kernel(
    half_ff, at, layer, hidden_ref, grad_ref, vectors, up_biases, given_hbm, packed_hbm,
    out_ref, grad_out_ref, grads_ref, small_ref, up_bias_ref, *rest
):
    micro, half_rows, width = hidden_ref.shape
    gathered, gather_refs = rest[0], rest[0:3]
    terms, back_terms = rest[3], rest[9]
    packed, tails, given, grad_upper, active, load_sem, given_sems = rest[15:]
    vec, up_bias = vectors.at[layer], up_biases.at[layer]
    seq, ff = active.shape[1:]
    main = ff - LANES
    extra = half_ff - main
    load = pltpu.make_async_copy(
        packed_hbm.at[:, at : at + packed.shape[1]], packed, load_sem
    )
    load.start()
    loads = [
        pltpu.make_async_copy(given_hbm.at[m], given.at[m], given_sems.at[m]) for m in range(micro)
    ]
    for copy in loads:
        copy.start()
    slab = Slab(half_rows)
    gathers = make_gathers(slab, gather_refs, micro)
    scatters = make_scatters(slab, rest[3:9], micro)
    backs = make_scatters(slab, rest[9:15], micro)
    slab.greet()

    def fill(m):
        own = slab.rows(gathered.at[m], slab.mine[0])
        for start in range(0, half_rows, 32):
            block = hidden_ref[m, pl.ds(start, 32)]
            own[pl.ds(start, 32)] = low(layer_norm(block, vec[1:2], vec[6:7]))

    def prepare():
        small_ref[...] = jnp.zeros_like(small_ref)
        up_bias_ref[...] = jnp.zeros_like(up_bias_ref)
        load.wait()
        split_tail(packed, tails, extra)

    open_gathers(gathers, fill, prepare)

    def compute(m, rows):
        value = up_dot(gathered[m, rows], packed, tails) + up_bias[...]
        square = value * value
        bent = jnp.tanh(GELU_A * value * (1.0 + GELU_B * square))
        half = 0.5 * (1.0 + bent)
        shown = low(value * half)
        active[m, rows] = shown
        slope = half + (0.5 * GELU_A) * value * (1.0 - bent * bent) * (1.0 + 3.0 * GELU_B * square)
        grad = low(down_back(given[m, rows], packed, tails) * slope)
        grad_upper[m, rows] = grad
        up_bias_ref[0:1] += jnp.sum(grad.astype(jnp.float32), axis=0, keepdims=True)
        back_terms[m, rows] = low(up_back(grad, packed, tails))
        terms[m, rows] = low(down_dot(shown, packed, tails))

    def stacked(ref, cols=slice(None)):
        return ref[:, :, cols].reshape(micro * seq, -1)

    def weight_grads(hooks):
        def block(i):
            cols = step_rows(i, WIDE)
            up = dot(stacked(gathered, cols), stacked(grad_upper), 0, 0)
            down = dot(stacked(given, cols), stacked(active), 0, 0)
            grads_ref[cols, :main] = low(up[:, :main])
            grads_ref[cols, main : 2 * main] = low(down[:, :main])
            blank = jnp.zeros((WIDE, LANES - 2 * extra), jnp.float32)
            rest_cols = [up[:, main : main + extra], down[:, main : main + extra], blank]
            grads_ref[cols, 2 * main :] = low(jnp.concatenate(rest_cols, axis=1))

        stages(width // WIDE, block, hooks)

    def close_back(m):
        backs[m].finish()
        for rows in backs[m].blocks():
            grad_normed = backs[m].total(rows)
            back, gain_terms = norm_back(hidden_ref[m, rows], vec[1:2], grad_normed)
            grad_rows = grad_ref[m, rows].astype(jnp.float32)
            grad_hidden = grad_rows + back
            grad_out_ref[m, rows] = grad_hidden
            branch = low(grad_hidden).astype(jnp.float32)
            for j, item in enumerate((gain_terms, grad_normed, grad_rows, branch)):
                small_ref[j : j + 1] += jnp.sum(item, axis=0, keepdims=True)

    def close(m):
        scatters[m].finish()
        for rows in scatters[m].blocks():
            out_ref[m, rows] = low(hidden_ref[m, rows] + scatters[m].total(rows) + vec[7:8])

    def work(k):
        compute(lax.div(k, 2), pl.ds(chip_rows(slab, k), 4 * half_rows))

    gathers[0].to_mate()
    gathers[0].finish()
    loads[0].wait()
    zero, one = scatters
    back_zero, back_one = backs
    stages(
        4,
        work,
        {
            0: [back_zero.mate_far, zero.mate_far, gathers[1].forward, back_zero.far_hop],
            1: [
                back_zero.mate_near,
                zero.mate_near,
                gathers[1].to_mate,
                back_zero.second_hop,
                gathers[1].finish,
                zero.far_hop,
                zero.second_hop,
                loads[1].wait,
            ],
            2: [
                back_one.mate_far,
                one.mate_far,
                back_zero.first_hop,
                back_one.far_hop,
                zero.first_hop,
            ],
            3: [
                back_one.mate_near,
                one.mate_near,
                back_one.second_hop,
                one.far_hop,
                one.second_hop,
            ],
        },
    )
    weight_grads({0: [back_one.first_hop, one.first_hop, lambda: close_back(0)]})
    close_back(1)
    for m in range(micro):
        close(m)


def attn_backward_kernel(
    at, layer, own_rows, both_ways, grad_ref, rows_ref, vectors, lse, lengths,
    normed_hbm, qkv_hbm, mixed_hbm, packed_hbm, errand_hbm,
    out_ref, grads_ref, small_ref, bias_ref, errand_got, *rest
):
    micro, half_rows, width = grad_ref.shape
    gathered, gather_refs = rest[0], rest[0:3]
    scatter_refs = rest[3:9]
    terms = rest[3]
    packed, wide, normed, qkv, mixed, grad_mixed, grad_qkv, turned, shut = rest[9:18]
    low_probs, grad_scores, high_probs, errand_sems, load_sems = rest[18:]
    vec = vectors.at[layer]
    seq, pair = mixed.shape[1:]
    heads = pair // LANES
    load_packed = pltpu.make_async_copy(
        packed_hbm.at[:, at : at + packed.shape[1]], packed, load_sems.at[0]
    )
    load_packed.start()
    load_qkv, load_rest = [], []
    for m in range(micro):
        load_qkv.append(pltpu.make_async_copy(qkv_hbm.at[m], qkv.at[m], load_sems.at[1 + 3 * m]))
        load_qkv[m].start()
    for m in range(micro):
        for k, (src, dst) in enumerate(((mixed_hbm, mixed), (normed_hbm, normed))):
            load = pltpu.make_async_copy(src.at[m], dst.at[m], load_sems.at[2 + k + 3 * m])
            load.start()
            load_rest.append(load)
    slab = Slab(half_rows)
    gathers = make_gathers(slab, gather_refs, micro)
    scatters = make_scatters(slab, scatter_refs, micro)
    slab.greet()

    def fill(m):
        own = slab.rows(gathered.at[m], slab.mine[0])
        for start in range(0, half_rows, 32):
            own[pl.ds(start, 32)] = low(grad_ref[m, pl.ds(start, 32)])

    def head(h, part=0):
        return pl.ds(pl.multiple_of(part * pair + h * LANES, LANES), LANES)

    def ready_qkv(m):
        load_qkv[m].wait()
        shut[m] = shut_keys(lengths[m], own_rows, 2 * half_rows, (seq, LANES), 0)
        for h in range(heads):
            turned[m, h] = low(qkv[m, :, head(h, 1)].astype(jnp.float32).T)

    def find_probs(m, h):
        def block(i):
            rows = step_rows(i, TILE)
            keys, queries = qkv[m, :, head(h, 1)], qkv[m, rows, head(h)]
            closed = jnp.concatenate([shut[m]] * (TILE // LANES), axis=1)
            scores = dot(keys, queries, 1, 1) * (score_scale * LOG2E) + closed
            high_probs[m, h, :, rows] = jnp.exp2(scores - lse[m, h, rows].T[0:1])

        repeat(seq // TILE, block)

    def find_all(k):
        find_probs(lax.div(k, heads), lax.rem(k, heads))

    span = errand_hbm.shape[0]
    cut = round_up(span // 2, 16) if span > 16 else span // 2
    errands = []
    for k, part in enumerate((pl.ds(0, cut), pl.ds(cut, span - cut))):
        errands.append(
            remote(
                errand_hbm.at[part],
                errand_got.at[part],
                errand_sems.at[0, k],
                errand_sems.at[1, k],
                {"section": 1 - lax.axis_index("section")},
            )
        )
    sends_errand = (lax.axis_index("section") == 0) | both_ways
    gets_errand = (lax.axis_index("section") == 1) | both_ways

    def prepare():
        small_ref[...] = jnp.zeros_like(small_ref)
        bias_ref[...] = jnp.zeros_like(bias_ref)
        load_packed.wait()
        widen(packed, wide)
        for m in range(micro):
            ready_qkv(m)

    fill(0)
    gathers[0].start()
    fill(1)
    gathers[0].second()
    gathers[1].start()
    prepare()

    def mix_grads(m):
        def block(i):
            rows = step_rows(i, 4 * half_rows)
            grad_mixed[m, rows] = low(dot(gathered[m, rows], wide[:, 3 * pair :], 1, 0))

        repeat(seq // (4 * half_rows), block)

    def attend(m, h):
        def block(i):
            rows = step_rows(i, TILE)
            grads = grad_mixed[m, rows, head(h)]
            probs = high_probs[m, h, :, rows]
            grad_probs = dot(qkv[m, :, head(h, 2)], grads, 1, 1)
            inner = jnp.sum(grad_probs * probs, axis=0, keepdims=True)
            low_probs[:, rows] = low(probs)
            grad_scores[:, rows] = low(probs * (grad_probs - inner))

        repeat(seq // TILE, block)
        grad_keys = dot(grad_scores[...], qkv[m, :, head(h)], 1, 0)
        grad_qkv[m, :, head(h, 1)] = low(grad_keys * score_scale)
        grad_qkv[m, :, head(h, 2)] = low(dot(low_probs[...], grad_mixed[m, :, head(h)], 1, 0))
        turn = dot(turned[m, h], grad_scores[...], 1, 0).T
        grad_qkv[m, :, head(h)] = low(turn * score_scale)

    def back_project(m, rows):
        grads = grad_qkv[m, rows]
        terms[m, rows] = low(dot(grads, wide[:, : 3 * pair], 1, 1))
        for j, part in enumerate((0, 2)):
            piece = grads[:, part * pair : (part + 1) * pair].astype(jnp.float32)
            bias_ref[j : j + 1] += jnp.sum(piece, axis=0, keepdims=True)

    def stacked(ref, cols=slice(None)):
        return ref[:, :, cols].reshape(micro * seq, -1)

    def weight_grads(hooks):
        def block(i):
            cols = step_rows(i, WIDE)
            front = dot(stacked(normed, cols), stacked(grad_qkv), 0, 0)
            back = dot(stacked(gathered, cols), stacked(mixed), 0, 0)
            total = low(jnp.concatenate([front, back], axis=1))
            pieces = [total[:, h * LANES : h * LANES + HEAD] for h in range(4 * heads)]
            grads_ref[cols] = jnp.concatenate(pieces, axis=1)

        stages(width // WIDE, block, hooks)

    def close(m):
        scatters[m].finish()
        for rows in scatters[m].blocks():
            grad_normed = scatters[m].total(rows)
            back, gain_terms = norm_back(
                rows_ref[m, rows].astype(jnp.float32), vec[0:1], grad_normed
            )
            out_ref[m, rows] = low(grad_ref[m, rows] + back)
            for j, item in enumerate((gain_terms, grad_normed)):
                small_ref[j : j + 1] += jnp.sum(item, axis=0, keepdims=True)

    def start_errand(k):
        pl.when(sends_errand)(errands[k].start)

    stages(
        2 * heads,
        find_all,
        {
            0: [gathers[0].forward, gathers[1].second],
            1: [gathers[1].forward, gathers[0].to_mate, lambda: start_errand(0)],
        },
    )
    gathers[0].finish()
    zero, one = scatters
    attend_hooks = {
        0: [gathers[1].to_mate],
        heads - 1: [gathers[1].finish],
        heads: [zero.first_hop, lambda: start_errand(1)],
    }
    project_hooks = {
        0: [zero.mate_far, zero.far_hop],
        1: [zero.mate_near, zero.second_hop],
        2: [one.mate_far, one.far_hop],
        3: [one.mate_near, lambda: close(0), one.second_hop],
    }

    def hooked(at, hooks):
        for k, steps in hooks.items():

            @pl.when(at == k)
            def _():
                for step in steps:
                    step()

    def image(m):
        mix_grads(m)

        def one_head(h):
            attend(m, h)
            hooked(m * heads + h, attend_hooks)

        repeat(heads, one_head)

        def one_chip(i):
            back_project(m, pl.ds(chip_rows(slab, i), 4 * half_rows))
            hooked(2 * m + i, project_hooks)

        repeat(2, one_chip)

    repeat(micro, image)
    for load in load_rest:
        load.wait()
    weight_grads({0: [one.first_hop]})
    close(1)

    for errand in errands:
        pl.when(sends_errand)(errand.wait_send)
        pl.when(gets_errand)(errand.wait_recv)


def any_spec():
    return pl.BlockSpec(memory_space=pl.ANY)


def vmem_spec():
    return pl.BlockSpec(memory_space=pltpu.VMEM)


def shape_of(shape, dtype):
    return jax.ShapeDtypeStruct(shape, dtype)


def params(collective):
    return pltpu.CompilerParams(
        collective_id=collective, has_side_effects=True, vmem_limit_bytes=VMEM_BYTES
    )


def smem_spec():
    return pl.BlockSpec(memory_space=pltpu.SMEM)


def attn_forward(rows_low, vectors, bias, packed, at, layer, lengths, own_rows, given=None, grads=None):
    micro, half_rows, width = rows_low.shape
    seq = 8 * half_rows
    pair = bias.shape[2] // 3
    heads = pair // LANES
    low_type, high_type = jnp.bfloat16, jnp.float32
    hidden, lse, normed, qkv, mixed = pl.pallas_call(
        functools.partial(attn_forward_kernel, given is not None, at, layer, own_rows),
        out_shape=[
            shape_of((micro, half_rows, width), high_type),
            shape_of((micro, heads, seq, LANES), high_type),
            shape_of((micro, seq, width), low_type),
            shape_of((micro, seq, 3 * pair), low_type),
            shape_of((micro, seq, pair), low_type),
        ],
        in_specs=[vmem_spec()] * 3 + [smem_spec(), any_spec(), any_spec(), vmem_spec()],
        out_specs=[vmem_spec()] * 2 + [any_spec()] * 3,
        scratch_shapes=gather_scratch(micro, seq, width)
        + scatter_scratch(micro, seq, half_rows, width)
        + [
            pltpu.VMEM((width, 4 * heads * HEAD), low_type),
            pltpu.VMEM((width, 4 * pair), low_type),
            pltpu.VMEM((micro, seq, 3 * pair), low_type),
            pltpu.VMEM((micro, seq, pair), low_type),
            pltpu.SemaphoreType.DMA,
            pltpu.SemaphoreType.DMA((6,)),
            pltpu.SemaphoreType.DMA((micro,)),
            pltpu.VMEM((micro, seq if given is not None else 32, width), low_type),
            pltpu.SemaphoreType.DMA((micro, 3)),
            pltpu.SemaphoreType.DMA((micro, 3)),
        ],
        compiler_params=params(0 if given is None else 6),
        cost_estimate=COST,
        name="attn_forward",
    )(
        rows_low,
        vectors,
        bias,
        lengths,
        packed,
        packed if given is None else given,
        rows_low if grads is None else grads,
    )
    if given is None:
        return hidden, (normed, qkv, lse, mixed)
    return hidden, (given, qkv, lse, mixed), normed


def ffn_forward(hidden, vectors, up_biases, packed, at, layer, half_ff):
    micro, half_rows, width = hidden.shape
    seq = 8 * half_rows
    ff = up_biases.shape[2]
    packed_cols = 2 * ff - LANES
    low_type, high_type = jnp.bfloat16, jnp.float32
    out, second, upper = pl.pallas_call(
        functools.partial(ffn_forward_kernel, half_ff, at, layer),
        out_shape=[
            shape_of((micro, half_rows, width), low_type),
            shape_of((micro, seq, width), low_type),
            shape_of((micro, seq, ff), high_type),
        ],
        in_specs=[vmem_spec()] * 3 + [any_spec()],
        out_specs=[vmem_spec()] + [any_spec()] * 2,
        scratch_shapes=gather_scratch(micro, seq, width)
        + scatter_scratch(micro, seq, half_rows, width)
        + [
            pltpu.VMEM((width, packed_cols), low_type),
            pltpu.VMEM((width, 2 * LANES), low_type),
            pltpu.VMEM((micro, seq, ff), high_type),
            pltpu.SemaphoreType.DMA,
            pltpu.SemaphoreType.DMA((4,)),
        ],
        compiler_params=params(1),
        cost_estimate=COST,
        name="ffn_forward",
    )(hidden, vectors, up_biases, packed)
    return out, (second, upper)


def ffn_turn(hidden, grad_low, given, vectors, up_biases, packed, at, layer, half_ff):
    micro, half_rows, width = hidden.shape
    seq = 8 * half_rows
    ff = up_biases.shape[2]
    low_type, high_type = jnp.bfloat16, jnp.float32
    out, grad_hidden, grads, small, up_bias = pl.pallas_call(
        functools.partial(ffn_turn_kernel, half_ff, at, layer),
        out_shape=[
            shape_of((micro, half_rows, width), low_type),
            shape_of((micro, half_rows, width), high_type),
            shape_of((width, 2 * ff - LANES), low_type),
            shape_of((8, width), high_type),
            shape_of((8, ff), high_type),
        ],
        in_specs=[vmem_spec()] * 4 + [any_spec()] * 2,
        out_specs=[vmem_spec()] * 5,
        scratch_shapes=gather_scratch(micro, seq, width)
        + scatter_scratch(micro, seq, half_rows, width)
        + scatter_scratch(micro, seq, half_rows, width)
        + [
            pltpu.VMEM((width, 2 * ff - LANES), low_type),
            pltpu.VMEM((width, 2 * LANES), low_type),
            pltpu.VMEM((micro, seq, width), low_type),
            pltpu.VMEM((micro, seq, ff), low_type),
            pltpu.VMEM((micro, seq, ff), low_type),
            pltpu.SemaphoreType.DMA,
            pltpu.SemaphoreType.DMA((micro,)),
        ],
        compiler_params=params(7),
        cost_estimate=COST,
        name="ffn_turn",
    )(hidden, grad_low, vectors, up_biases, given, packed)
    return out, grad_hidden, grads, small, up_bias[:1]


def ffn_backward(grad_low, hidden, kept, vectors, packed, at, layer, half_ff):
    second, upper = kept
    micro, half_rows, width = hidden.shape
    seq, ff = upper.shape[1:]
    low_type, high_type = jnp.bfloat16, jnp.float32
    grad_hidden, grads, small, up_bias = pl.pallas_call(
        functools.partial(ffn_backward_kernel, half_ff, at, layer),
        out_shape=[
            shape_of((micro, half_rows, width), high_type),
            shape_of((width, 2 * ff - LANES), low_type),
            shape_of((8, width), high_type),
            shape_of((8, ff), high_type),
        ],
        in_specs=[vmem_spec()] * 3 + [any_spec()] * 3,
        out_specs=[vmem_spec()] * 4,
        scratch_shapes=gather_scratch(micro, seq, width)
        + scatter_scratch(micro, seq, half_rows, width)
        + [
            pltpu.VMEM((width, 2 * ff - LANES), low_type),
            pltpu.VMEM((width, 2 * LANES), low_type),
            pltpu.VMEM((micro, seq, width), low_type),
            pltpu.VMEM((micro, seq, ff), high_type),
            pltpu.VMEM((micro, seq, ff), low_type),
            pltpu.VMEM((micro, seq, ff), low_type),
            pltpu.SemaphoreType.DMA((1 + 2 * micro,)),
        ],
        compiler_params=params(2),
        cost_estimate=COST,
        name="ffn_backward",
    )(grad_low, hidden, vectors, second, upper, packed)
    return grad_hidden, grads, small, up_bias[:1]


def attn_backward(
    grad_hidden, rows_low, kept, vectors, packed, at, layer, lengths, own_rows, errand, both_ways
):
    normed, qkv, lse, mixed = kept
    micro, half_rows, width = grad_hidden.shape
    seq, pair = mixed.shape[1:]
    heads = pair // LANES
    low_type, high_type = jnp.bfloat16, jnp.float32
    out, grads, small, bias, got = pl.pallas_call(
        functools.partial(attn_backward_kernel, at, layer, own_rows, both_ways),
        out_shape=[
            shape_of((micro, half_rows, width), low_type),
            shape_of((width, 4 * heads * HEAD), low_type),
            shape_of((8, width), high_type),
            shape_of((8, pair), high_type),
            shape_of(errand.shape, errand.dtype),
        ],
        in_specs=[vmem_spec()] * 4 + [smem_spec()] + [any_spec()] * 5,
        out_specs=[vmem_spec()] * 4 + [any_spec()],
        scratch_shapes=gather_scratch(micro, seq, width)
        + scatter_scratch(micro, seq, half_rows, width)
        + [
            pltpu.VMEM((width, 4 * heads * HEAD), low_type),
            pltpu.VMEM((width, 4 * pair), low_type),
            pltpu.VMEM((micro, seq, width), low_type),
            pltpu.VMEM((micro, seq, 3 * pair), low_type),
            pltpu.VMEM((micro, seq, pair), low_type),
            pltpu.VMEM((micro, seq, pair), low_type),
            pltpu.VMEM((micro, seq, 3 * pair), low_type),
            pltpu.VMEM((micro, heads, LANES, seq), low_type),
            pltpu.VMEM((micro, seq, LANES), high_type),
            pltpu.VMEM((seq, seq), low_type),
            pltpu.VMEM((seq, seq), low_type),
            pltpu.VMEM((micro, heads, seq, seq), high_type),
            pltpu.SemaphoreType.DMA((2, 2)),
            pltpu.SemaphoreType.DMA((1 + 3 * micro,)),
        ],
        compiler_params=params(3 + 5 * layer),
        cost_estimate=COST,
        name="attn_backward",
    )(grad_hidden, rows_low, vectors, lse, lengths, normed, qkv, mixed, packed, errand)
    return out, grads, small, bias, got


def slab_peers():
    section, tensor = lax.axis_index("section"), lax.axis_index("tensor")
    peers = []
    for role in range(1, 8):
        far, step = role // 4, role % 4
        other = section + far * (1 - 2 * section)
        to = (other, lax.rem(tensor + step, 4))
        source = (other, lax.rem(tensor + 4 - step, 4))
        peers.append((role, to, source))
    return peers


def column_peers(count):
    here = lax.axis_index("dp")
    return [
        (step, lax.rem(here + step, count), lax.rem(here + count - step, count))
        for step in range(1, count)
    ]


def greet_all(count):
    barrier = pltpu.get_barrier_semaphore()
    for _, to, _ in slab_peers():
        pl.semaphore_signal(barrier, inc=1, device_id=named(to), device_id_type=MESH)
    for _, to, _ in column_peers(count):
        pl.semaphore_signal(barrier, inc=1, device_id={"dp": to}, device_id_type=MESH)
    pl.semaphore_wait(barrier, 7 + count - 1)


def remote(src, dst, send_sem, recv_sem, peer):
    return pltpu.make_async_remote_copy(
        src_ref=src,
        dst_ref=dst,
        send_sem=send_sem,
        recv_sem=recv_sem,
        device_id=peer,
        device_id_type=MESH,
    )


def prologue_kernel(
    count, heads, qkv_ref, out_ref_in, up_ref_in, down_ref_t, gains_ref, shifts_ref, up_bias, rows_ref,
    first_hbm, normed_hbm, attn_ref, ff_zero_hbm, ff_one_hbm, out_ref, up_ref, bias_ref,
    attn_parts, ff_parts, up_halves, mine_ref, all_rows, line, ff_line, column, slab, up_got,
    rows_send, rows_recv, column_send, column_recv, slab_send, slab_recv, swap_send, swap_recv,
    right_send, right_recv, left_send, left_recv, out_sems,
):
    section, tensor, here = (lax.axis_index(name) for name in ("section", "tensor", "dp"))
    width = out_ref.shape[2]
    chunk = width // (4 * count)
    rows = attn_parts.shape[1]
    micro, own_rows = rows_ref.shape[:2]
    pieces = swap_send.shape[0] - 2
    size = rows // pieces
    other = {"section": 1 - section}
    pair = heads * LANES
    pair_cols = heads * HEAD
    half_ff = up_ref_in.shape[1] // 2
    main = half_ff // LANES * LANES
    extra = half_ff - main
    greet_all(count)
    out_turned = low(out_ref_in[...].astype(jnp.float32).T)
    for half in range(2):
        span = slice(half * pair_cols, (half + 1) * pair_cols)
        parts = [qkv_ref[k, :, span] for k in range(3)] + [out_turned[:, span]]
        attn_parts[half] = jnp.concatenate(parts, axis=1)
    keep_slot = jnp.where(section == 0, here, count)
    send_slot = jnp.where(section == 0, here, count)
    got_slot = jnp.where(section == 0, count, here)
    sent = []
    for p in range(pieces):
        span = pl.ds(p * size, size)
        copy = remote(
            attn_parts.at[1 - section, span],
            line.at[send_slot, span],
            swap_send.at[p],
            swap_recv.at[p],
            other,
        )
        copy.start()
        sent.append(copy)
    line[keep_slot] = attn_parts[section]
    mine_ref[...] = jnp.zeros_like(mine_ref)
    gains = gains_ref.shape[0]
    mine_ref[:gains, :chunk] = gains_ref[...]
    for i in range(shifts_ref.shape[0]):
        mine_ref[gains + i : gains + i + 1, :chunk] = shifts_ref[i]
    column[here] = mine_ref[...]
    for step, to, _ in column_peers(count):
        copy = remote(
            mine_ref, column.at[here], column_send.at[step], column_recv.at[step], {"dp": to}
        )
        copy.start()
        sent.append(copy)

    def swapped(p):
        got = line.at[got_slot, pl.ds(p * size, size)]
        remote(got, got, swap_send.at[p], swap_recv.at[p], other).wait_recv()

    def hop(step, p, way, finish=False):
        origin = here - way * step
        sends, recvs = (right_send, right_recv) if way == 1 else (left_send, left_recv)
        inside = (origin >= 0) if way == 1 else (origin < count)
        onward = (here + 1 < count) if way == 1 else (here > 0)
        slot = line.at[jnp.clip(origin, 0, count - 1), pl.ds(p * size, size)]
        target = jnp.clip(here + way, 0, count - 1)
        if step > 0 and not finish:

            @pl.when(inside)
            def _():
                remote(slot, slot, sends.at[step, p], recvs.at[step, p], {"dp": target}).wait_recv()

        if step + 1 < count:

            @pl.when(inside & onward)
            def _():
                copy = remote(
                    slot, slot, sends.at[step, p], recvs.at[step + 1, p], {"dp": target}
                )
                if finish:
                    copy.wait_send()
                else:
                    copy.start()

    def hops(step):
        for p in range(pieces):
            for way in (1, -1):
                hop(step, p, way)

    for step, _, source in column_peers(count):
        slot = column.at[source]
        remote(slot, slot, column_send.at[step], column_recv.at[step], {"dp": source}).wait_recv()
    for role, to, _ in slab_peers():
        copy = remote(
            column, slab.at[section, tensor], slab_send.at[role], slab_recv.at[role], named(to)
        )
        copy.start()
        sent.append(copy)
    slab[section, tensor] = column[...]
    for p in range(pieces):

        @pl.when(section == 1)
        def _():
            swapped(p)

        for way in (1, -1):
            hop(0, p, way)
    blank = jnp.zeros((rows, LANES - 2 * extra), jnp.bfloat16)
    up_halves[...] = jnp.zeros_like(up_halves)
    for half in range(2):
        start = half * half_ff
        up_halves[half, :, :half_ff] = up_bias[:, start : start + half_ff]
        ff_parts[half, :, :main] = up_ref_in[:, start : start + main]
        ff_parts[half, :, main : 2 * main] = down_ref_t[:, start : start + main]
        span = slice(start + main, start + half_ff)
        ff_parts[half, :, 2 * main :] = jnp.concatenate(
            [up_ref_in[:, span], down_ref_t[:, span], blank], axis=1
        )
    ff_swap = remote(
        ff_parts.at[1 - section],
        ff_line.at[section],
        swap_send.at[pieces],
        swap_recv.at[pieces],
        other,
    )
    up_swap = remote(
        up_halves.at[1 - section],
        up_got.at[section],
        swap_send.at[pieces + 1],
        swap_recv.at[pieces + 1],
        other,
    )
    up_swap.start()
    for role, _, source in slab_peers():
        slot = slab.at[source[0], source[1]]
        remote(slot, slot, slab_send.at[role], slab_recv.at[role], named(source)).wait_recv()
    ff_swap.start()
    for layer in range(2):
        for part in range(4 * count):
            piece = slab[layer, part % 4, part // 4]
            out_ref[layer, :, part * chunk : (part + 1) * chunk] = piece[:, :chunk]
    tiles = TileGather(all_rows, rows_send, rows_recv)
    for m in range(micro):
        own = tiles.tile(m, tensor)
        for begin in range(0, own_rows, 32):
            end = min(begin + 32, own_rows)
            block = rows_ref[m, begin:end].astype(jnp.float32)
            own[begin:end] = low(layer_norm(block, out_ref[0, 0:1], out_ref[0, 2:3]))
        own[own_rows:] = jnp.zeros((tiles.tile_rows - own_rows, width), jnp.bfloat16)
    tiles.start()
    hops(1)
    start = (2 * tensor + section) * pair_cols
    for layer in range(2):
        turned = pltpu.roll(out_ref[layer], lax.rem(width - start, width), 1)
        empty = jnp.zeros((1, LANES - HEAD), jnp.float32)
        for part, row in ((0, 3), (2, 4)):
            for h in range(heads):
                at = part * pair + h * LANES
                piece = turned[row : row + 1, h * HEAD : (h + 1) * HEAD]
                bias_ref[layer, :, at : at + LANES] = jnp.concatenate([piece, empty], 1)
        bias_ref[layer, :, pair : 2 * pair] = jnp.zeros((1, pair), jnp.float32)
    up_ref[section] = up_halves[section]
    outs = []

    def put(src, dst, i):
        copy = pltpu.make_async_copy(src, dst, out_sems.at[i])
        copy.start()
        outs.append(copy)

    def put_ff(src, section_of_first, i):
        for layer, dst in enumerate((ff_zero_hbm, ff_one_hbm)):
            here_too = layer if section_of_first == 0 else 1 - layer

            @pl.when(section == here_too)
            def _():
                pltpu.make_async_copy(src, dst, out_sems.at[i]).start()

        outs.append(pltpu.make_async_copy(src, ff_zero_hbm, out_sems.at[i]))

    put_ff(ff_parts.at[section], 0, count)
    for step in range(2, count):
        hops(step)
        if step == 2:
            tiles.pass_on()
    if count <= 2:
        tiles.pass_on()
    for p in range(pieces):

        @pl.when(section == 0)
        def _():
            swapped(p)

    for at in range(count):
        put(line.at[at], first_hbm.at[pl.ds(at * rows, rows)], at)
    attn_ref[...] = line[count]
    got = up_got.at[1 - section]
    remote(got, got, swap_send.at[pieces + 1], swap_recv.at[pieces + 1], other).wait_recv()
    up_ref[1 - section] = up_got[1 - section]
    tiles.finish()
    put(all_rows, normed_hbm, count + 2)
    ff_got = ff_line.at[1 - section]
    remote(ff_got, ff_got, swap_send.at[pieces], swap_recv.at[pieces], other).wait_recv()
    put_ff(ff_got, 1, count + 1)
    for step in range(count):
        for p in range(pieces):
            for way in (1, -1):
                hop(step, p, way, True)
    for copy in sent + [ff_swap, up_swap]:
        copy.wait_send()
    tiles.drain()
    for copy in outs:
        copy.wait()


def prologue(qkv, out, up, down_t, gains, shifts, up_bias, rows_low, count, heads, tile_rows):
    part_rows = qkv.shape[1]
    micro, _, width = rows_low.shape
    vector_rows = gains.shape[0] + shifts.shape[0]
    half_ff = up.shape[1] // 2
    ff_wide = round_up(half_ff, LANES)
    attn_shape = (part_rows, 4 * heads * HEAD)
    ff_shape = (2, part_rows, 2 * ff_wide - LANES)
    all_rows = (micro, 4 * tile_rows, width)
    pieces = 3 if part_rows % 96 == 0 else 1
    low_type, high_type = jnp.bfloat16, jnp.float32
    dma = pltpu.SemaphoreType.DMA
    return pl.pallas_call(
        functools.partial(prologue_kernel, count, heads),
        out_shape=[
            shape_of((count * part_rows, attn_shape[1]), low_type),
            shape_of(all_rows, low_type),
            shape_of(attn_shape, low_type),
            shape_of(ff_shape[1:], low_type),
            shape_of(ff_shape[1:], low_type),
            shape_of((2, vector_rows, width), high_type),
            shape_of((2, 1, ff_wide), high_type),
            shape_of((2, 1, 3 * heads * LANES), high_type),
        ],
        in_specs=[vmem_spec()] * 8,
        out_specs=[any_spec()] * 2 + [vmem_spec()] + [any_spec()] * 2 + [vmem_spec()] * 3,
        scratch_shapes=[
            pltpu.VMEM((2,) + attn_shape, low_type),
            pltpu.VMEM(ff_shape, low_type),
            pltpu.VMEM((2, 1, ff_wide), high_type),
            pltpu.VMEM((vector_rows, LANES), high_type),
            pltpu.VMEM(all_rows, low_type),
            pltpu.VMEM((count + 1,) + attn_shape, low_type),
            pltpu.VMEM(ff_shape, low_type),
            pltpu.VMEM((count, vector_rows, LANES), high_type),
            pltpu.VMEM((2, 4, count, vector_rows, LANES), high_type),
            pltpu.VMEM((2, 1, ff_wide), high_type),
            dma((micro, 3)),
            dma((micro, 3)),
            dma((count,)),
            dma((count,)),
            dma((8,)),
            dma((8,)),
            dma((pieces + 2,)),
            dma((pieces + 2,)),
            dma((count, pieces)),
            dma((count, pieces)),
            dma((count, pieces)),
            dma((count, pieces)),
            dma((count + 3,)),
        ],
        compiler_params=params(4),
        cost_estimate=COST,
        name="prologue",
    )(qkv, out, up, down_t, gains, shifts, up_bias, rows_low)


def home_kernel(
    count, chunk, attn_zero, attn_one, ff_zero, ff_one, biases_in, ups_in,
    ff_sum_hbm, attn_sum_hbm, rows_hbm,
    out_ref, up_ref, ff_got_hbm, attn_got_hbm, rows_got_hbm,
    parts, ups, slab, column, up_pair, up_column, total,
    column_send, column_recv, slab_send, slab_recv, up_sems, up_column_send, up_column_recv, far_send, far_recv,
):
    section, tensor, here = (lax.axis_index(name) for name in ("section", "tensor", "dp"))
    width = attn_zero.shape[1]
    heads = biases_in.shape[2] // LANES
    other = {"section": 1 - section}
    greet_all(count)
    parts[...] = jnp.zeros_like(parts)
    start = (2 * tensor + section) * (heads * HEAD)
    for layer, (attn, ff) in enumerate(((attn_zero, ff_zero), (attn_one, ff_one))):
        bias = biases_in[layer]
        blank = jnp.zeros((8, width - heads * HEAD), jnp.float32)
        pieces = [bias[:, h * LANES : h * LANES + HEAD] for h in range(heads)]
        placed = pltpu.roll(jnp.concatenate(pieces + [blank], 1), start, 1)
        whole = jnp.concatenate(
            [attn[0:1], ff[0:1], attn[1:2], placed[0:2], ff[3:4], ff[1:2], ff[2:3]], axis=0
        )
        for part in range(4 * count):
            piece = whole[:, part * chunk : (part + 1) * chunk]
            parts[layer, part % 4, part // 4, :, :chunk] = piece
        ups[layer] = ups_in[layer]
    sent = []

    def send(src, dst, send_sem, recv_sem, peer):
        copy = remote(src, dst, send_sem, recv_sem, peer)
        copy.start()
        sent.append(copy)

    send(ups.at[1 - section], up_pair.at[section], up_sems.at[0], up_sems.at[1], other)
    for role, to, _ in slab_peers():
        send(
            parts.at[to[0], to[1]], slab.at[role], slab_send.at[role], slab_recv.at[role], named(to)
        )
    far_rows = remote(rows_hbm, rows_got_hbm, far_send.at[0], far_recv.at[0], other)
    far_ff = remote(ff_sum_hbm, ff_got_hbm, far_send.at[1], far_recv.at[1], other)
    far_attn = remote(attn_sum_hbm, attn_got_hbm, far_send.at[2], far_recv.at[2], other)
    one_way = ((far_ff, 1), (far_attn, 0))
    far_rows.start()
    for copy, source in one_way:
        pl.when(section == source)(copy.start)
    up_pair[section] = ups[section]
    value = parts[section, tensor]
    for role, _, source in slab_peers():
        slot = slab.at[role]
        remote(slot, slot, slab_send.at[role], slab_recv.at[role], named(source)).wait_recv()
        value = value + slab[role]
    total[...] = value
    for step, to, _ in column_peers(count):
        send(total.at[to], column.at[step], column_send.at[step], column_recv.at[step], {"dp": to})
    got = up_pair.at[1 - section]
    remote(got, got, up_sems.at[0], up_sems.at[1], other).wait_recv()
    for step, to, _ in column_peers(count):
        send(
            up_pair, up_column.at[here], up_column_send.at[step], up_column_recv.at[step], {"dp": to}
        )
    up_column[here] = up_pair[...]
    result = total[here]
    for step, _, source in column_peers(count):
        slot = column.at[step]
        remote(slot, slot, column_send.at[step], column_recv.at[step], {"dp": source}).wait_recv()
        result = result + column[step]
    out_ref[...] = result
    for step, _, source in column_peers(count):
        slot = up_column.at[source]
        remote(
            slot, slot, up_column_send.at[step], up_column_recv.at[step], {"dp": source}
        ).wait_recv()
    value = up_column[0]
    for at in range(1, count):
        value = value + up_column[at]
    up_ref[...] = value
    far_rows.wait()
    for copy, source in one_way:
        pl.when(section == source)(copy.wait_send)
        pl.when(section != source)(copy.wait_recv)
    for copy in sent:
        copy.wait_send()


def home(attn_small, ff_small, bias_grads, up_grads, ff_sum, attn_sum, rows, count, chunk):
    vector_rows, lanes = 8, LANES
    up_shape = up_grads.shape[1:]
    dma = pltpu.SemaphoreType.DMA
    high_type = jnp.float32
    return pl.pallas_call(
        functools.partial(home_kernel, count, chunk),
        out_shape=[
            shape_of((vector_rows, lanes), high_type),
            shape_of((2,) + up_shape, high_type),
            shape_of(ff_sum.shape, ff_sum.dtype),
            shape_of(attn_sum.shape, attn_sum.dtype),
            shape_of(rows.shape, rows.dtype),
        ],
        in_specs=[vmem_spec()] * 6 + [any_spec()] * 3,
        out_specs=[vmem_spec()] * 2 + [any_spec()] * 3,
        scratch_shapes=[
            pltpu.VMEM((2, 4, count, vector_rows, lanes), high_type),
            pltpu.VMEM((2,) + up_shape, high_type),
            pltpu.VMEM((8, count, vector_rows, lanes), high_type),
            pltpu.VMEM((count, vector_rows, lanes), high_type),
            pltpu.VMEM((2,) + up_shape, high_type),
            pltpu.VMEM((count, 2) + up_shape, high_type),
            pltpu.VMEM((count, vector_rows, lanes), high_type),
            dma((count,)),
            dma((count,)),
            dma((8,)),
            dma((8,)),
            dma((2,)),
            dma((count,)),
            dma((count,)),
            dma((3,)),
            dma((3,)),
        ],
        compiler_params=params(5),
        cost_estimate=COST,
        name="home",
    )(*attn_small, *ff_small, bias_grads, up_grads, ff_sum, attn_sum, rows)


def ff_finish_kernel(zero, one, zero_got, one_got, up_ref, down_ref):
    first = lax.axis_index("section") == 0
    halves = (
        jnp.where(first, zero[...], one_got[...]),
        jnp.where(first, zero_got[...], one[...]),
    )
    half_ff = up_ref.shape[1] // 2
    main = half_ff // LANES * LANES
    extra = half_ff - main
    for k in range(2):
        pieces = []
        for half in halves:
            start = 2 * main + k * extra
            pieces += [half[:, k * main : (k + 1) * main], half[:, start : start + extra]]
        whole = jnp.concatenate(pieces, axis=1).astype(jnp.float32)
        (up_ref, down_ref)[k][...] = whole


def ff_finish(sums, got, ff_cols):
    rows = sums[0].shape[0]
    return pl.pallas_call(
        ff_finish_kernel,
        out_shape=[
            shape_of((rows, ff_cols), jnp.float32),
            shape_of((rows, ff_cols), jnp.float32),
        ],
        in_specs=[vmem_spec()] * 4,
        out_specs=[vmem_spec()] * 2,
        compiler_params=pltpu.CompilerParams(vmem_limit_bytes=VMEM_BYTES),
        cost_estimate=COST,
        name="ff_finish",
    )(*sums, *got)


def attn_finish_kernel(zero, one, zero_got, one_got, qkv_ref, out_ref):
    first = lax.axis_index("section") == 0
    halves = (
        jnp.where(first, zero[...], one_got[...]),
        jnp.where(first, zero_got[...], one[...]),
    )
    pair_cols = qkv_ref.shape[2] // 2
    for k in range(4):
        span = slice(k * pair_cols, (k + 1) * pair_cols)
        whole = jnp.concatenate([half[:, span] for half in halves], axis=1).astype(jnp.float32)
        if k < 3:
            qkv_ref[k] = whole
        else:
            out_ref[...] = whole.T


def attn_finish(sums, got, head_cols):
    rows = sums[0].shape[0]
    return pl.pallas_call(
        attn_finish_kernel,
        out_shape=[
            shape_of((3, rows, head_cols), jnp.float32),
            shape_of((head_cols, rows), jnp.float32),
        ],
        in_specs=[vmem_spec()] * 4,
        out_specs=[vmem_spec()] * 2,
        compiler_params=pltpu.CompilerParams(vmem_limit_bytes=VMEM_BYTES),
        name="attn_finish",
    )(*sums, *got)


def shards(
    section_input,
    final_cotangent,
    lengths,
    qkv_weight,
    out_weight,
    up_weight,
    down_weight,
    norm_gains,
    biases,
    up_bias,
):
    here = lax.axis_index("section")
    sections = lax.axis_size("section")
    micro, _, own_rows, _ = section_input.shape
    head_cols = qkv_weight.shape[3]
    pair_cols = head_cols // sections
    heads = pair_cols // HEAD
    ff_cols = up_weight.shape[2]
    half_ff = ff_cols // sections
    half_rows = round_up(-(-own_rows // sections), 32)
    full_rows = half_rows * sections

    def by_layer(mine, other):
        return [jnp.where(here == 0, mine, other), jnp.where(here == 0, other, mine)]

    count = lax.axis_size("dp")
    chunk = norm_gains.shape[2]
    first, normed, attn_part, ff_zero, ff_one, vectors, up_biases, bias_qv = prologue(
        qkv_weight[0],
        out_weight[0],
        up_weight[0],
        down_weight[0].T,
        norm_gains[0],
        biases.transpose(1, 0, 2),
        up_bias,
        section_input[:, 0],
        count,
        heads,
        full_rows,
    )

    def gather_column(part):
        return lax.all_gather(part, "dp", axis=0, tiled=True)

    ff_first = gather_column(ff_zero)
    attn_packed = [(first, 0), (gather_column(attn_part), 0)]
    ff_packed = [(ff_first, 0), (gather_column(ff_one), 0)]
    lengths_here = lengths.reshape(micro)

    def my_rows(value):
        padded = jnp.pad(value[:, 0], [(0, 0), (0, full_rows - own_rows), (0, 0)])
        return lax.dynamic_slice_in_dim(padded, here * half_rows, half_rows, 1)

    def whole_rows(first, second, got):
        low_half, high_half = by_layer(jnp.where(here == 0, first, second), got)
        return jnp.concatenate([low_half, high_half], 1)[:, None, :own_rows]

    rows = my_rows(section_input)
    inputs, hiddens, attn_kept = [], [], []
    for layer in range(2):
        inputs.append(rows)
        operands = (rows, vectors, bias_qv, *attn_packed[layer], layer, lengths_here, own_rows)
        if layer == 0:
            hidden, kept, grads_all = attn_forward(*operands, normed, final_cotangent[:, 0])
        else:
            hidden, kept = attn_forward(*operands)
        hiddens.append(hidden)
        attn_kept.append(kept)
        if layer == 0:
            rows, ff_kept = ffn_forward(hidden, vectors, up_biases, *ff_packed[0], 0, half_ff)

    attn_sums, ff_sums, up_sums, input_grads = {}, {}, {}, {}
    attn_small, ff_small, bias_grads, errands = {}, {}, {}, {}
    for layer in (1, 0):
        if layer == 1:
            last, grad_hidden, ff_grad, ff_small[1], up_sums[1] = ffn_turn(
                hiddens[1],
                my_rows(final_cotangent),
                grads_all,
                vectors,
                up_biases,
                *ff_packed[1],
                1,
                half_ff,
            )
        else:
            grad_hidden, ff_grad, ff_small[0], up_sums[0] = ffn_backward(
                grads, hiddens[0], ff_kept, vectors, *ff_packed[0], 0, half_ff
            )
        ff_sums[layer] = lax.psum_scatter(ff_grad, "dp", scatter_dimension=0, tiled=True)
        if layer == 1:
            errand, both_ways = jnp.where(here == 0, last, rows), True
        else:
            errand, both_ways = ff_sums[1], False
        grads, attn_grad, attn_small[layer], bias_grads[layer], got = attn_backward(
            grad_hidden,
            inputs[layer],
            attn_kept[layer],
            vectors,
            *attn_packed[layer],
            layer,
            lengths_here,
            own_rows,
            errand,
            both_ways,
        )
        errands[layer] = got
        attn_sums[layer] = lax.psum_scatter(attn_grad, "dp", scatter_dimension=0, tiled=True)
        input_grads[layer] = grads

    section_output = whole_rows(rows, last, errands[1])
    small_mine, up_total, ff_got, attn_got, rows_got = home(
        [attn_small[0], attn_small[1]],
        [ff_small[0], ff_small[1]],
        jnp.stack([bias_grads[0], bias_grads[1]]),
        jnp.stack([up_sums[0], up_sums[1]]),
        ff_sums[0],
        attn_sums[1],
        jnp.where(here == 0, input_grads[1], input_grads[0]),
        count,
        chunk,
    )
    attn_zero_got = lax.ppermute(attn_sums[0], "section", [(1, 0)])
    up_grad, down_grad = ff_finish([ff_sums[0], ff_sums[1]], [ff_got, errands[0]], ff_cols)
    small_mine, up_total, rows_got, up_grad = lax.optimization_barrier(
        (small_mine, up_total, rows_got, up_grad)
    )
    small_mine = small_mine[None, :, :chunk]
    up_total = up_total[:, :, :half_ff].reshape(1, ff_cols)
    input_grad = whole_rows(input_grads[0], input_grads[1], rows_got)

    qkv_total, out_total = attn_finish(
        [attn_sums[0], attn_sums[1]], [attn_zero_got, attn_got], head_cols
    )
    gains = norm_gains.shape[1]
    return (
        section_output[None],
        input_grad[None],
        qkv_total[None],
        out_total[None],
        up_grad[None],
        down_grad.T[None],
        small_mine[:, :gains],
        small_mine[:, gains:],
        up_total,
    )


def solution(mesh):
    in_specs = (
        P(None, "dp", "tensor", None),
        P(None, "dp", "tensor", None),
        P(None, "dp"),
        P("section", None, "dp", "tensor"),
        P("section", "tensor", "dp"),
        P("section", "dp", "tensor"),
        P("section", "tensor", "dp"),
        P("section", None, ("dp", "tensor")),
        P("section", None, ("dp", "tensor")),
        P("section", "tensor"),
    )
    out_specs = (
        P("section", None, "dp", "tensor", None),
        P("section", None, "dp", "tensor", None),
        P("section", None, "dp", "tensor"),
        P("section", "tensor", "dp"),
        P("section", "dp", "tensor"),
        P("section", "tensor", "dp"),
        P("section", None, ("dp", "tensor")),
        P("section", None, ("dp", "tensor")),
        P("section", "tensor"),
    )
    return jax.shard_map(shards, mesh=mesh, in_specs=in_specs, out_specs=out_specs, check_vma=False)
```

```python
import functools
import math

import jax
import jax.numpy as jnp
from jax import lax
from jax.experimental import pallas as pl
from jax.experimental.pallas import tpu as pltpu
from jax.sharding import PartitionSpec as P


HEAD = 72
LANES = 128
norm_eps = 1e-06
masked_score = -1000000000.0
score_scale = 1.0 / math.sqrt(HEAD)
GELU_A = math.sqrt(2.0 / math.pi)
GELU_B = 0.044715


def round_up(value, step):
    return -(-value // step) * step


def dot(left, right, left_dim, right_dim):
    return lax.dot_general(
        left, right, (((left_dim,), (right_dim,)), ((), ())), preferred_element_type=jnp.float32
    )


def low(value):
    return value.astype(jnp.bfloat16)


def layer_norm(rows, gain_vec, shift_vec):
    centred = rows - jnp.mean(rows, axis=-1, keepdims=True)
    spread = jnp.mean(centred * centred, axis=-1, keepdims=True)
    return centred * lax.rsqrt(spread + norm_eps) * gain_vec + shift_vec


def norm_back(rows, gain_vec, grads):
    centred = rows - jnp.mean(rows, axis=-1, keepdims=True)
    spread = jnp.mean(centred * centred, axis=-1, keepdims=True)
    inverse = lax.rsqrt(spread + norm_eps)
    xhat = centred * inverse
    e = grads * gain_vec
    back = inverse * (
        e
        - jnp.mean(e, axis=-1, keepdims=True)
        - xhat * jnp.mean(e * xhat, axis=-1, keepdims=True)
    )
    return back, grads * xhat


def gelu_tanh(value):
    return jax.nn.gelu(value, approximate=True)


MESH = pl.DeviceIdType.MESH
VMEM_BYTES = 64_000_000
COST = pl.CostEstimate(flops=20_000_000_000, transcendentals=0, bytes_accessed=100_000_000)
LOG2E = 1.0 / math.log(2.0)
TILE = 256
WIDE = 384


class Slab:
    def __init__(self, half_rows):
        self.half_rows = half_rows
        section = lax.axis_index("section")
        tensor = lax.axis_index("tensor")
        core = lax.rem(tensor, 2)
        self.core = core
        self.mine = self.around(section, tensor, core)
        self.theirs = self.around(section, tensor + 1 - 2 * core, 1 - core)
        self.far_role, self.near_role = 1 + core, 2 - core
        self.mate = self.theirs[0]
        over = lax.rem(tensor + 2, 4)
        self.near, self.far = tensor, over
        self.mate_near, self.mate_far = self.mate[1], lax.rem(self.mate[1] + 2, 4)
        self.grid = self.places(section, self.near, self.far)
        self.mate_grid = self.places(section, self.mate_near, self.mate_far)
        self.across_y = self.grid[2]
        self.first, self.second = self.mine[1], self.mine[2]

    def place(self, section, tensor):
        start = (2 * tensor + section) * self.half_rows
        return (section, tensor, pl.multiple_of(start, self.half_rows))

    def places(self, section, near, far):
        flip = 1 - section
        return [self.place(*at) for at in ((section, near), (flip, near), (section, far), (flip, far))]

    def around(self, section, tensor, core):
        over = lax.rem(tensor + 2, 4)
        turn = 1 - 2 * section
        first = (section + (1 - core) * turn, tensor + core * (over - tensor))
        second = (section + core * turn, tensor + (1 - core) * (over - tensor))
        places = ((section, tensor), first, second, (1 - section, over))
        return [self.place(*at) for at in places]

    def rows(self, ref, at):
        return ref.at[pl.ds(at[2], self.half_rows)]

    def greet(self):
        barrier = pltpu.get_barrier_semaphore()
        for peer in (self.first, self.second, self.mate):
            pl.semaphore_signal(barrier, inc=1, device_id=named(peer), device_id_type=MESH)
        pl.semaphore_wait(barrier, 3)


def named(at):
    return {"section": at[0], "tensor": at[1]}


class Moves:
    def __init__(self, slab, send_sems, recv_sems):
        self.slab, self.send_sems, self.recv_sems = slab, send_sems, recv_sems
        self.sent = []

    def copy(self, src, dst, role, peer):
        return pltpu.make_async_remote_copy(
            src_ref=src,
            dst_ref=dst,
            send_sem=self.send_sems.at[role],
            recv_sem=self.recv_sems.at[role],
            device_id=named(peer),
            device_id_type=MESH,
        )

    def send(self, ends, role, peer):
        self.copy(*ends(), role, peer).start()
        self.sent.append(lambda: self.copy(*ends(), role, peer))

    def arrived(self, dst, role):
        self.copy(dst, dst, role, self.slab.mate).wait_recv()

    def drain(self):
        for copy in self.sent:
            copy().wait_send()


class Gather(Moves):
    def __init__(self, slab, whole, send_sems, recv_sems):
        super().__init__(slab, send_sems, recv_sems)
        self.whole = whole

    def pass_on(self, at, role, peer):
        self.send(lambda: (self.slab.rows(self.whole, at),) * 2, role, peer)

    def arrive(self, at, role):
        self.arrived(self.slab.rows(self.whole, at), role)

    def start(self):
        mine = self.slab.mine
        self.pass_on(mine[0], 0, mine[1])
        self.pass_on(mine[0], 3, self.slab.mate)

    def second(self):
        self.sent.pop(0)().wait_send()
        self.pass_on(self.slab.mine[0], 1, self.slab.mine[2])

    def forward(self):
        mine, mate = self.slab.mine, self.slab.mate
        self.arrive(mine[1], 0)
        self.pass_on(mine[1], 2, mine[2])
        self.pass_on(mine[1], 4, mate)

    def to_mate(self):
        mine, mate = self.slab.mine, self.slab.mate
        self.arrive(mine[2], 1)
        self.pass_on(mine[2], 5, mate)
        self.arrive(mine[3], 2)
        self.pass_on(mine[3], 6, mate)

    def finish(self):
        for k in range(4):
            self.arrive(self.slab.theirs[k], 3 + k)
        self.drain()


class TileGather:
    def __init__(self, whole, send_sems, recv_sems):
        self.whole, self.send_sems, self.recv_sems = whole, send_sems, recv_sems
        self.tensor = lax.axis_index("tensor")
        self.over = lax.rem(self.tensor + 2, 4)
        self.mate = self.tensor + 1 - 2 * lax.rem(self.tensor, 2)
        self.micro, rows = whole.shape[0], whole.shape[1] // 4
        self.tile_rows = rows
        self.sent = []

    def tile(self, m, index):
        start = pl.multiple_of(index * self.tile_rows, self.tile_rows)
        return self.whole.at[m, pl.ds(start, self.tile_rows)]

    def copy(self, m, index, role, peer):
        part = self.tile(m, index)
        return remote(
            part, part, self.send_sems.at[m, role], self.recv_sems.at[m, role], {"tensor": peer}
        )

    def send(self, m, index, role, peer):
        self.copy(m, index, role, peer).start()
        self.sent.append(lambda: self.copy(m, index, role, peer))

    def start(self, m):
        self.send(m, self.tensor, 0, self.over)
        self.send(m, self.tensor, 1, self.mate)

    def pass_on(self):
        for m in range(self.micro):
            self.copy(m, self.over, 0, self.over).wait_recv()
            self.send(m, self.over, 2, self.mate)

    def finish(self):
        for m in range(self.micro):
            self.copy(m, self.mate, 1, self.mate).wait_recv()
            self.copy(m, lax.rem(self.mate + 2, 4), 2, self.mate).wait_recv()

    def drain(self):
        for copy in self.sent:
            copy().wait_send()


class Scatter(Moves):
    def __init__(self, slab, terms, from_mate, outgoing, arrivals, send_sems, recv_sems):
        super().__init__(slab, send_sems, recv_sems)
        self.terms, self.from_mate, self.outgoing = terms, from_mate, outgoing
        self.relay, self.from_second, self.from_first = (arrivals.at[k] for k in range(3))

    def to_mate(self, at, role):
        self.send(
            lambda: (self.slab.rows(self.terms, at), self.from_mate.at[role]), role, self.slab.mate
        )

    def mate_far(self):
        self.to_mate(self.slab.mate_grid[3], 3)
        self.to_mate(self.slab.mate_grid[2], self.slab.far_role)

    def mate_near(self):
        self.to_mate(self.slab.mate_grid[1], self.slab.near_role)
        self.to_mate(self.slab.mate_grid[0], 0)

    def chip_sum(self, k, rows):
        part = self.slab.rows(self.terms, self.slab.mine[k])
        return part[rows].astype(jnp.float32) + self.from_mate[k, rows].astype(jnp.float32)

    def blocks(self):
        return [pl.ds(start, 32) for start in range(0, self.slab.half_rows, 32)]

    def hop(self, k, slot, dst, role, peer, ride=None):
        self.arrived(self.from_mate.at[k], k)
        if ride is not None:
            self.arrived(ride, 4)
        for rows in self.blocks():
            value = self.chip_sum(k, rows)
            if ride is not None:
                value = value + ride[rows].astype(jnp.float32)
            self.outgoing[slot, rows] = low(value)
        self.send(lambda: (self.outgoing.at[slot], dst), role, peer)

    def far_hop(self):
        self.hop(3, 0, self.relay, 4, self.slab.second)

    def second_hop(self):
        self.hop(2, 1, self.from_second, 5, self.slab.second)

    def first_hop(self):
        self.hop(1, 2, self.from_first, 6, self.slab.first, self.relay)

    def finish(self):
        self.arrived(self.from_mate.at[0], 0)
        self.arrived(self.from_second, 5)
        self.arrived(self.from_first, 6)
        self.drain()

    def total(self, rows):
        other = self.from_second[rows].astype(jnp.float32) + self.from_first[rows].astype(
            jnp.float32
        )
        return self.chip_sum(0, rows) + other


def scatter_scratch(micro, seq, half_rows, width):
    return [
        pltpu.VMEM((micro, seq, width), jnp.bfloat16),
        pltpu.VMEM((micro, 4, half_rows, width), jnp.bfloat16),
        pltpu.VMEM((micro, 3, half_rows, width), jnp.bfloat16),
        pltpu.VMEM((micro, 3, half_rows, width), jnp.bfloat16),
        pltpu.SemaphoreType.DMA((micro, 7)),
        pltpu.SemaphoreType.DMA((micro, 7)),
    ]


def gather_scratch(micro, seq, width):
    return [
        pltpu.VMEM((micro, seq, width), jnp.bfloat16),
        pltpu.SemaphoreType.DMA((micro, 7)),
        pltpu.SemaphoreType.DMA((micro, 7)),
    ]


def make_scatters(slab, refs, micro):
    terms, from_mate, outgoing, arrivals, send_sems, recv_sems = refs
    return [
        Scatter(
            slab,
            terms.at[m],
            from_mate.at[m],
            outgoing.at[m],
            arrivals.at[m],
            send_sems.at[m],
            recv_sems.at[m],
        )
        for m in range(micro)
    ]


def make_gathers(slab, refs, micro):
    whole, send_sems, recv_sems = refs
    return [
        Gather(slab, whole.at[m], send_sems.at[m], recv_sems.at[m]) for m in range(micro)
    ]


def step_from(start, i, size):
    return pl.ds(pl.multiple_of(start + i * size, size), size)


def step_rows(i, size):
    return pl.ds(pl.multiple_of(i * size, size), size)


def repeat(count, body):
    def one(i, carry):
        body(i)
        return carry

    lax.fori_loop(0, count, one, 0)


def shut_keys(length, own_rows, full_rows, shape, dimension):
    place = lax.broadcasted_iota(jnp.int32, shape, dimension)
    step = jnp.zeros(shape, jnp.int32)
    for t in range(1, 4):
        step += (place >= t * full_rows).astype(jnp.int32)
    live = (place - step * full_rows < own_rows) & (
        place - step * (full_rows - own_rows) < length
    )
    return jnp.where(live, 0.0, masked_score)


def stages(count, work, hooks):
    def body(k):
        work(k)
        for at, steps in hooks.items():

            @pl.when(k == at)
            def _():
                for step in steps:
                    step()

    repeat(count, body)


def chip_rows(slab, k):
    far, near = slab.far - slab.core, slab.near - slab.core
    start = (far + lax.rem(k, 2) * (near - far)) * (2 * slab.half_rows)
    return pl.multiple_of(start, 2 * slab.half_rows)


def open_gathers(gathers, fill, prepare):
    fill(0)
    gathers[0].start()
    fill(1)
    gathers[0].second()
    gathers[1].start()
    prepare()
    gathers[0].forward()
    gathers[1].second()


def widen(packed, wide):
    heads = packed.shape[1] // HEAD

    def block(i):
        rows = step_rows(i, 128)
        for h in range(heads):
            piece = packed[rows, h * HEAD : (h + 1) * HEAD]
            blank = jnp.zeros((128, LANES - HEAD), jnp.bfloat16)
            wide[rows, h * LANES : (h + 1) * LANES] = jnp.concatenate([piece, blank], axis=1)

    repeat(packed.shape[0] // 128, block)


def split_tail(packed, tails, up_cols):
    start = packed.shape[1] - LANES

    def block(i):
        rows = step_rows(i, 128)
        for j in range(2):
            piece = packed[rows, start + j * up_cols : start + (j + 1) * up_cols]
            blank = jnp.zeros((128, LANES - up_cols), jnp.bfloat16)
            tails[rows, j * LANES : (j + 1) * LANES] = jnp.concatenate([piece, blank], axis=1)

    repeat(packed.shape[0] // 128, block)


def up_dot(rows, packed, tails):
    main = (packed.shape[1] - LANES) // 2
    first = dot(rows, packed[:, :main], 1, 0)
    return jnp.concatenate([first, dot(rows, tails[:, :LANES], 1, 0)], axis=1)


def up_back(grads, packed, tails):
    main = (packed.shape[1] - LANES) // 2
    return dot(grads[:, :main], packed[:, :main], 1, 1) + dot(
        grads[:, main:], tails[:, :LANES], 1, 1
    )


def down_dot(active, packed, tails):
    main = (packed.shape[1] - LANES) // 2
    return dot(active[:, :main], packed[:, main : 2 * main], 1, 1) + dot(
        active[:, main:], tails[:, LANES:], 1, 1
    )


def down_back(rows, packed, tails):
    main = (packed.shape[1] - LANES) // 2
    first = dot(rows, packed[:, main : 2 * main], 1, 0)
    return jnp.concatenate([first, dot(rows, tails[:, LANES:], 1, 0)], axis=1)


def attn_forward_kernel(
    ready, at, layer, own_rows, rows_ref, vectors, bias_ref, lengths, packed_hbm, given_hbm, grads_ref,
    hidden_ref, lse_ref, normed_hbm, qkv_hbm, mixed_hbm, *rest
):
    micro, half_rows, width = rows_ref.shape
    gathered, gather_refs = rest[0], rest[0:3]
    scatter_refs = rest[3:9]
    terms = rest[3]
    packed, wide, qkv, mixed, load_sem, keep_sems, given_sems, all_grads, tile_send, tile_recv = rest[9:]
    vec, bias = vectors.at[layer], bias_ref[layer]
    seq = qkv.shape[1]
    pair = mixed.shape[2]
    heads = pair // LANES
    load = pltpu.make_async_copy(
        packed_hbm.at[:, at : at + packed.shape[1]], packed, load_sem
    )
    load.start()
    slab = Slab(half_rows)
    gathers = make_gathers(slab, gather_refs, micro)
    scatters = make_scatters(slab, scatter_refs, micro)
    given = [
        pltpu.make_async_copy(given_hbm.at[m], gathered.at[m], given_sems.at[m])
        for m in range(micro if ready else 0)
    ]
    for copy in given:
        copy.start()
    slab.greet()
    if ready:
        tiles = TileGather(all_grads, tile_send, tile_recv)
        for m in range(micro):
            own = tiles.tile(m, tiles.tensor)
            count = grads_ref.shape[1]
            own[:count] = grads_ref[m]
            own[count:] = jnp.zeros((tiles.tile_rows - count, width), jnp.bfloat16)
            tiles.start(m)

    def fill(m):
        own = slab.rows(gathered.at[m], slab.mine[0])
        for start in range(0, half_rows, 32):
            block = rows_ref[m, pl.ds(start, 32)].astype(jnp.float32)
            own[pl.ds(start, 32)] = low(layer_norm(block, vec[0:1], vec[2:3]))

    def prepare():
        load.wait()
        widen(packed, wide)

    if ready:
        prepare()
    else:
        open_gathers(gathers, fill, prepare)
    keeps = []

    def keep(src, dst, m, i):
        def copy():
            return pltpu.make_async_copy(src.at[m], dst.at[m], keep_sems.at[i])

        copy().start()
        keeps.append(copy)

    def project(m):
        def block(i):
            rows = step_rows(i, 4 * half_rows)
            out = dot(gathered[m, rows], wide[:, : 3 * pair], 1, 0)
            qkv[m, rows] = low(out + bias)

        repeat(seq // (4 * half_rows), block)

    def attend(m, rows):
        shut = shut_keys(lengths[m], own_rows, 2 * half_rows, (1, seq), 1)
        for h in range(heads):
            cols = slice(h * LANES, (h + 1) * LANES)
            q = qkv[m, rows, cols]
            k = qkv[m, :, pair + h * LANES : pair + (h + 1) * LANES]
            v = qkv[m, :, 2 * pair + h * LANES : 2 * pair + (h + 1) * LANES]
            scores = dot(q, k, 1, 1) * (score_scale * LOG2E) + shut
            top = jnp.max(scores, axis=-1, keepdims=True)
            exp_scores = jnp.exp2(scores - top)
            total = jnp.sum(exp_scores, axis=-1, keepdims=True)
            probs = low(exp_scores * (1.0 / total))
            mixed[m, rows, cols] = low(dot(probs, v, 1, 0))
            lse_ref[m, h, rows] = jnp.broadcast_to(
                top + jnp.log(total) * LOG2E, (2 * half_rows, LANES)
            )

    def output(m, rows):
        terms[m, rows] = low(dot(mixed[m, rows], wide[:, 3 * pair :], 1, 1))

    def close(m):
        scatters[m].finish()
        for rows in scatters[m].blocks():
            start = rows_ref[m, rows].astype(jnp.float32)
            hidden_ref[m, rows] = start + scatters[m].total(rows) + vec[5:6]

    def gathered_rows(m):
        if ready:
            given[m].wait()
            return
        gathers[m].to_mate()
        gathers[m].finish()
        keep(gathered, normed_hbm, m, m)

    def work(k):
        m = lax.div(k, 2)
        start = chip_rows(slab, k)
        pl.when(lax.rem(k, 2) == 0)(lambda: project(m))

        def piece(i):
            attend(m, step_from(start, i, 2 * half_rows))

        repeat(2, piece)
        output(m, pl.ds(start, 4 * half_rows))

    def keep_two(m):
        keep(qkv, qkv_hbm, m, 2 + 2 * m)
        keep(mixed, mixed_hbm, m, 3 + 2 * m)

    def grads_on():
        if ready:
            tiles.pass_on()

    def grads_in():
        if ready:
            tiles.finish()
            for m in range(micro):
                keep(all_grads, normed_hbm, m, m)

    gathered_rows(0)
    if not ready:
        gathers[1].forward()
    zero, one = scatters
    stages(
        4,
        work,
        {
            0: [zero.mate_far, lambda: gathered_rows(1), zero.far_hop],
            1: [zero.mate_near, lambda: keep_two(0), zero.second_hop, zero.first_hop, grads_on],
            2: [one.mate_far, lambda: close(0), one.far_hop, grads_in],
            3: [one.mate_near, lambda: keep_two(1), one.second_hop, one.first_hop],
        },
    )
    close(1)
    if ready:
        tiles.drain()
    for copy in keeps:
        copy().wait()


def ffn_forward_kernel(
    half_ff, at, layer, hidden_ref, vectors, up_biases, packed_hbm, out_ref, second_hbm, upper_hbm, *rest
):
    micro, half_rows, _ = hidden_ref.shape
    gathered, gather_refs = rest[0], rest[0:3]
    scatter_refs = rest[3:9]
    terms = rest[3]
    packed, tails, upper, load_sem, keep_sems = rest[9:]
    vec, up_bias = vectors.at[layer], up_biases.at[layer]
    _, ff = upper.shape[1:]
    load = pltpu.make_async_copy(
        packed_hbm.at[:, at : at + packed.shape[1]], packed, load_sem
    )
    load.start()
    slab = Slab(half_rows)
    gathers = make_gathers(slab, gather_refs, micro)
    scatters = make_scatters(slab, scatter_refs, micro)
    slab.greet()

    def fill(m):
        own = slab.rows(gathered.at[m], slab.mine[0])
        for start in range(0, half_rows, 32):
            block = hidden_ref[m, pl.ds(start, 32)]
            own[pl.ds(start, 32)] = low(layer_norm(block, vec[1:2], vec[6:7]))

    def prepare():
        load.wait()
        split_tail(packed, tails, half_ff - ff + LANES)

    open_gathers(gathers, fill, prepare)
    keeps = []

    def keep(src, dst, m, i):
        def copy():
            return pltpu.make_async_copy(src.at[m], dst.at[m], keep_sems.at[i])

        copy().start()
        keeps.append(copy)

    def compute(m, rows):
        value = up_dot(gathered[m, rows], packed, tails) + up_bias[...]
        upper[m, rows] = value
        active = low(gelu_tanh(value))
        terms[m, rows] = low(down_dot(active, packed, tails))

    def close(m):
        scatters[m].finish()
        for rows in scatters[m].blocks():
            out_ref[m, rows] = low(hidden_ref[m, rows] + scatters[m].total(rows) + vec[7:8])

    def work(k):
        compute(lax.div(k, 2), pl.ds(chip_rows(slab, k), 4 * half_rows))

    gathers[0].to_mate()
    gathers[0].finish()
    keep(gathered, second_hbm, 0, 0)
    zero, one = scatters
    stages(
        4,
        work,
        {
            0: [zero.mate_far, gathers[1].forward, zero.far_hop],
            1: [
                zero.mate_near,
                lambda: keep(upper, upper_hbm, 0, 1),
                gathers[1].to_mate,
                zero.second_hop,
                gathers[1].finish,
                lambda: keep(gathered, second_hbm, 1, 2),
            ],
            2: [one.mate_far, zero.first_hop, one.far_hop],
            3: [one.mate_near, lambda: keep(upper, upper_hbm, 1, 3), one.second_hop],
        },
    )
    close(0)
    one.first_hop()
    close(1)
    for copy in keeps:
        copy().wait()


def ffn_backward_kernel(
    half_ff, at, layer, grad_ref, hidden_ref, vectors, second_hbm, upper_hbm, packed_hbm,
    out_ref, grads_ref, small_ref, up_bias_ref, *rest
):
    micro, half_rows, width = hidden_ref.shape
    gathered, gather_refs = rest[0], rest[0:3]
    scatter_refs = rest[3:9]
    terms = rest[3]
    packed, tails, second, upper, grad_upper, active, load_sems = rest[9:]
    vec = vectors.at[layer]
    seq, ff = upper.shape[1:]
    main = ff - LANES
    extra = half_ff - main
    load_packed = pltpu.make_async_copy(
        packed_hbm.at[:, at : at + packed.shape[1]], packed, load_sems.at[0]
    )
    load_packed.start()
    load_upper, load_second = [], []
    for m in range(micro):
        load_upper.append(
            pltpu.make_async_copy(upper_hbm.at[m], upper.at[m], load_sems.at[1 + m])
        )
        load_upper[m].start()
    for m in range(micro):
        load_second.append(
            pltpu.make_async_copy(second_hbm.at[m], second.at[m], load_sems.at[1 + micro + m])
        )
        load_second[m].start()
    slab = Slab(half_rows)
    gathers = make_gathers(slab, gather_refs, micro)
    scatters = make_scatters(slab, scatter_refs, micro)
    slab.greet()

    def fill(m):
        own = slab.rows(gathered.at[m], slab.mine[0])
        for start in range(0, half_rows, 32):
            own[pl.ds(start, 32)] = grad_ref[m, pl.ds(start, 32)]

    def prepare():
        small_ref[...] = jnp.zeros_like(small_ref)
        up_bias_ref[...] = jnp.zeros_like(up_bias_ref)
        load_packed.wait()
        split_tail(packed, tails, extra)

    open_gathers(gathers, fill, prepare)

    def compute(m, rows):
        value = upper[m, rows]
        square = value * value
        bent = jnp.tanh(GELU_A * value * (1.0 + GELU_B * square))
        half = 0.5 * (1.0 + bent)
        active[m, rows] = low(value * half)
        slope = half + (0.5 * GELU_A) * value * (1.0 - bent * bent) * (1.0 + 3.0 * GELU_B * square)
        grad_active = down_back(gathered[m, rows], packed, tails)
        grad = low(grad_active * slope)
        grad_upper[m, rows] = grad
        up_bias_ref[0:1] += jnp.sum(grad.astype(jnp.float32), axis=0, keepdims=True)
        terms[m, rows] = low(up_back(grad, packed, tails))

    def stacked(ref, cols=slice(None)):
        return ref[:, :, cols].reshape(micro * seq, -1)

    def weight_grads(hooks):
        def block(i):
            cols = step_rows(i, WIDE)
            up = dot(stacked(second, cols), stacked(grad_upper), 0, 0)
            down = dot(stacked(gathered, cols), stacked(active), 0, 0)
            grads_ref[cols, :main] = low(up[:, :main])
            grads_ref[cols, main : 2 * main] = low(down[:, :main])
            blank = jnp.zeros((WIDE, LANES - 2 * extra), jnp.float32)
            rest_cols = [up[:, main : main + extra], down[:, main : main + extra], blank]
            grads_ref[cols, 2 * main :] = low(jnp.concatenate(rest_cols, axis=1))

        stages(width // WIDE, block, hooks)

    def close(m):
        scatters[m].finish()
        for rows in scatters[m].blocks():
            grad_normed = scatters[m].total(rows)
            back, gain_terms = norm_back(hidden_ref[m, rows], vec[1:2], grad_normed)
            grad_rows = grad_ref[m, rows].astype(jnp.float32)
            grad_hidden = grad_rows + back
            out_ref[m, rows] = grad_hidden
            branch = low(grad_hidden).astype(jnp.float32)
            for j, item in enumerate((gain_terms, grad_normed, grad_rows, branch)):
                small_ref[j : j + 1] += jnp.sum(item, axis=0, keepdims=True)

    def work(k):
        compute(lax.div(k, 2), pl.ds(chip_rows(slab, k), 4 * half_rows))

    gathers[0].to_mate()
    gathers[0].finish()
    load_upper[0].wait()
    zero, one = scatters
    stages(
        4,
        work,
        {
            0: [zero.mate_far, gathers[1].forward, zero.far_hop],
            1: [
                zero.mate_near,
                gathers[1].to_mate,
                zero.second_hop,
                gathers[1].finish,
                load_upper[1].wait,
            ],
            2: [one.mate_far, zero.first_hop, one.far_hop],
            3: [one.mate_near, one.second_hop],
        },
    )
    for load in load_second:
        load.wait()
    weight_grads({0: [one.first_hop, lambda: close(0)]})
    close(1)


def ffn_turn_kernel(
    half_ff, at, layer, hidden_ref, grad_ref, vectors, up_biases, given_hbm, packed_hbm,
    out_ref, grad_out_ref, grads_ref, small_ref, up_bias_ref, *rest
):
    micro, half_rows, width = hidden_ref.shape
    gathered, gather_refs = rest[0], rest[0:3]
    terms, back_terms = rest[3], rest[9]
    packed, tails, given, grad_upper, active, load_sem, given_sems = rest[15:]
    vec, up_bias = vectors.at[layer], up_biases.at[layer]
    seq, ff = active.shape[1:]
    main = ff - LANES
    extra = half_ff - main
    load = pltpu.make_async_copy(
        packed_hbm.at[:, at : at + packed.shape[1]], packed, load_sem
    )
    load.start()
    loads = [
        pltpu.make_async_copy(given_hbm.at[m], given.at[m], given_sems.at[m]) for m in range(micro)
    ]
    for copy in loads:
        copy.start()
    slab = Slab(half_rows)
    gathers = make_gathers(slab, gather_refs, micro)
    scatters = make_scatters(slab, rest[3:9], micro)
    backs = make_scatters(slab, rest[9:15], micro)
    slab.greet()

    def fill(m):
        own = slab.rows(gathered.at[m], slab.mine[0])
        for start in range(0, half_rows, 32):
            block = hidden_ref[m, pl.ds(start, 32)]
            own[pl.ds(start, 32)] = low(layer_norm(block, vec[1:2], vec[6:7]))

    def prepare():
        small_ref[...] = jnp.zeros_like(small_ref)
        up_bias_ref[...] = jnp.zeros_like(up_bias_ref)
        load.wait()
        split_tail(packed, tails, extra)

    open_gathers(gathers, fill, prepare)

    def compute(m, rows):
        value = up_dot(gathered[m, rows], packed, tails) + up_bias[...]
        square = value * value
        bent = jnp.tanh(GELU_A * value * (1.0 + GELU_B * square))
        half = 0.5 * (1.0 + bent)
        shown = low(value * half)
        active[m, rows] = shown
        slope = half + (0.5 * GELU_A) * value * (1.0 - bent * bent) * (1.0 + 3.0 * GELU_B * square)
        grad = low(down_back(given[m, rows], packed, tails) * slope)
        grad_upper[m, rows] = grad
        up_bias_ref[0:1] += jnp.sum(grad.astype(jnp.float32), axis=0, keepdims=True)
        back_terms[m, rows] = low(up_back(grad, packed, tails))
        terms[m, rows] = low(down_dot(shown, packed, tails))

    def stacked(ref, cols=slice(None)):
        return ref[:, :, cols].reshape(micro * seq, -1)

    def weight_grads(hooks):
        def block(i):
            cols = step_rows(i, WIDE)
            up = dot(stacked(gathered, cols), stacked(grad_upper), 0, 0)
            down = dot(stacked(given, cols), stacked(active), 0, 0)
            grads_ref[cols, :main] = low(up[:, :main])
            grads_ref[cols, main : 2 * main] = low(down[:, :main])
            blank = jnp.zeros((WIDE, LANES - 2 * extra), jnp.float32)
            rest_cols = [up[:, main : main + extra], down[:, main : main + extra], blank]
            grads_ref[cols, 2 * main :] = low(jnp.concatenate(rest_cols, axis=1))

        stages(width // WIDE, block, hooks)

    def close_back(m):
        backs[m].finish()
        for rows in backs[m].blocks():
            grad_normed = backs[m].total(rows)
            back, gain_terms = norm_back(hidden_ref[m, rows], vec[1:2], grad_normed)
            grad_rows = grad_ref[m, rows].astype(jnp.float32)
            grad_hidden = grad_rows + back
            grad_out_ref[m, rows] = grad_hidden
            branch = low(grad_hidden).astype(jnp.float32)
            for j, item in enumerate((gain_terms, grad_normed, grad_rows, branch)):
                small_ref[j : j + 1] += jnp.sum(item, axis=0, keepdims=True)

    def close(m):
        scatters[m].finish()
        for rows in scatters[m].blocks():
            out_ref[m, rows] = low(hidden_ref[m, rows] + scatters[m].total(rows) + vec[7:8])

    def work(k):
        compute(lax.div(k, 2), pl.ds(chip_rows(slab, k), 4 * half_rows))

    gathers[0].to_mate()
    gathers[0].finish()
    loads[0].wait()
    zero, one = scatters
    back_zero, back_one = backs
    stages(
        4,
        work,
        {
            0: [back_zero.mate_far, zero.mate_far, gathers[1].forward, back_zero.far_hop],
            1: [
                back_zero.mate_near,
                zero.mate_near,
                gathers[1].to_mate,
                back_zero.second_hop,
                gathers[1].finish,
                zero.far_hop,
                zero.second_hop,
                loads[1].wait,
            ],
            2: [
                back_one.mate_far,
                one.mate_far,
                back_zero.first_hop,
                back_one.far_hop,
                zero.first_hop,
            ],
            3: [
                back_one.mate_near,
                one.mate_near,
                back_one.second_hop,
                one.far_hop,
                one.second_hop,
            ],
        },
    )
    weight_grads({0: [back_one.first_hop, one.first_hop, lambda: close_back(0)]})
    close_back(1)
    for m in range(micro):
        close(m)


def attn_backward_kernel(
    at, layer, own_rows, both_ways, grad_ref, rows_ref, vectors, lse, lengths,
    normed_hbm, qkv_hbm, mixed_hbm, packed_hbm, errand_hbm, errand_one_hbm,
    out_ref, grads_ref, small_ref, bias_ref, errand_got, *rest
):
    micro, half_rows, width = grad_ref.shape
    gathered, gather_refs = rest[0], rest[0:3]
    scatter_refs = rest[3:9]
    terms = rest[3]
    packed, wide, normed, qkv, mixed, grad_mixed, grad_qkv, turned, shut = rest[9:18]
    low_probs, grad_scores, high_probs, errand_sems, load_sems = rest[18:]
    vec = vectors.at[layer]
    seq, pair = mixed.shape[1:]
    heads = pair // LANES
    load_packed = pltpu.make_async_copy(
        packed_hbm.at[:, at : at + packed.shape[1]], packed, load_sems.at[0]
    )
    load_packed.start()
    load_qkv, load_rest = [], []
    for m in range(micro):
        load_qkv.append(pltpu.make_async_copy(qkv_hbm.at[m], qkv.at[m], load_sems.at[1 + 3 * m]))
        load_qkv[m].start()
    for m in range(micro):
        for k, (src, dst) in enumerate(((mixed_hbm, mixed), (normed_hbm, normed))):
            load = pltpu.make_async_copy(src.at[m], dst.at[m], load_sems.at[2 + k + 3 * m])
            load.start()
            load_rest.append(load)
    slab = Slab(half_rows)
    gathers = make_gathers(slab, gather_refs, micro)
    scatters = make_scatters(slab, scatter_refs, micro)
    slab.greet()

    def fill(m):
        own = slab.rows(gathered.at[m], slab.mine[0])
        for start in range(0, half_rows, 32):
            own[pl.ds(start, 32)] = low(grad_ref[m, pl.ds(start, 32)])

    def head(h, part=0):
        return pl.ds(pl.multiple_of(part * pair + h * LANES, LANES), LANES)

    def ready_qkv(m):
        load_qkv[m].wait()
        shut[m] = shut_keys(lengths[m], own_rows, 2 * half_rows, (seq, LANES), 0)
        for h in range(heads):
            turned[m, h] = low(qkv[m, :, head(h, 1)].astype(jnp.float32).T)

    def find_probs(m, h):
        def block(i):
            rows = step_rows(i, TILE)
            keys, queries = qkv[m, :, head(h, 1)], qkv[m, rows, head(h)]
            closed = jnp.concatenate([shut[m]] * (TILE // LANES), axis=1)
            scores = dot(keys, queries, 1, 1) * (score_scale * LOG2E) + closed
            high_probs[m, h, :, rows] = jnp.exp2(scores - lse[m, h, rows].T[0:1])

        repeat(seq // TILE, block)

    def find_all(k):
        find_probs(lax.div(k, heads), lax.rem(k, heads))

    span = errand_hbm.shape[0]
    cut = round_up(span // 2, 16) if span > 16 else span // 2
    errands = []
    for k, part in enumerate((pl.ds(0, cut), pl.ds(cut, span - cut))):
        errands.append(
            [
                remote(
                    source.at[part],
                    errand_got.at[part],
                    errand_sems.at[0, k],
                    errand_sems.at[1, k],
                    {"section": 1 - lax.axis_index("section")},
                )
                for source in (errand_hbm, errand_one_hbm)
            ]
        )
    first_section = lax.axis_index("section") == 0
    sends_errand, gets_errand = first_section | both_ways, ~first_section | both_ways

    def prepare():
        small_ref[...] = jnp.zeros_like(small_ref)
        bias_ref[...] = jnp.zeros_like(bias_ref)
        load_packed.wait()
        widen(packed, wide)
        for m in range(micro):
            ready_qkv(m)

    fill(0)
    gathers[0].start()
    fill(1)
    gathers[0].second()
    gathers[1].start()
    prepare()

    def mix_grads(m):
        def block(i):
            rows = step_rows(i, 4 * half_rows)
            grad_mixed[m, rows] = low(dot(gathered[m, rows], wide[:, 3 * pair :], 1, 0))

        repeat(seq // (4 * half_rows), block)

    def attend(m, h):
        def block(i):
            rows = step_rows(i, TILE)
            grads = grad_mixed[m, rows, head(h)]
            probs = high_probs[m, h, :, rows]
            grad_probs = dot(qkv[m, :, head(h, 2)], grads, 1, 1)
            inner = jnp.sum(grad_probs * probs, axis=0, keepdims=True)
            low_probs[:, rows] = low(probs)
            grad_scores[:, rows] = low(probs * (grad_probs - inner))

        repeat(seq // TILE, block)
        grad_keys = dot(grad_scores[...], qkv[m, :, head(h)], 1, 0)
        grad_qkv[m, :, head(h, 1)] = low(grad_keys * score_scale)
        grad_qkv[m, :, head(h, 2)] = low(dot(low_probs[...], grad_mixed[m, :, head(h)], 1, 0))
        turn = dot(turned[m, h], grad_scores[...], 1, 0).T
        grad_qkv[m, :, head(h)] = low(turn * score_scale)

    def back_project(m, rows):
        grads = grad_qkv[m, rows]
        terms[m, rows] = low(dot(grads, wide[:, : 3 * pair], 1, 1))
        for j, part in enumerate((0, 2)):
            piece = grads[:, part * pair : (part + 1) * pair].astype(jnp.float32)
            bias_ref[j : j + 1] += jnp.sum(piece, axis=0, keepdims=True)

    def stacked(ref, cols=slice(None)):
        return ref[:, :, cols].reshape(micro * seq, -1)

    def weight_grads(hooks):
        def block(i):
            cols = step_rows(i, WIDE)
            front = dot(stacked(normed, cols), stacked(grad_qkv), 0, 0)
            back = dot(stacked(gathered, cols), stacked(mixed), 0, 0)
            total = low(jnp.concatenate([front, back], axis=1))
            pieces = [total[:, h * LANES : h * LANES + HEAD] for h in range(4 * heads)]
            grads_ref[cols] = jnp.concatenate(pieces, axis=1)

        stages(width // WIDE, block, hooks)

    def close(m):
        scatters[m].finish()
        for rows in scatters[m].blocks():
            grad_normed = scatters[m].total(rows)
            back, gain_terms = norm_back(
                rows_ref[m, rows].astype(jnp.float32), vec[0:1], grad_normed
            )
            out_ref[m, rows] = low(grad_ref[m, rows] + back)
            for j, item in enumerate((gain_terms, grad_normed)):
                small_ref[j : j + 1] += jnp.sum(item, axis=0, keepdims=True)

    def start_errand(k):
        pl.when(first_section)(errands[k][0].start)
        if both_ways:
            pl.when(~first_section)(errands[k][1].start)

    stages(
        2 * heads,
        find_all,
        {
            0: [gathers[0].forward, gathers[1].second],
            1: [gathers[1].forward, gathers[0].to_mate, lambda: start_errand(0)],
        },
    )
    gathers[0].finish()
    zero, one = scatters
    attend_hooks = {
        0: [gathers[1].to_mate],
        heads - 1: [gathers[1].finish],
        heads: [zero.first_hop, lambda: start_errand(1)],
    }
    project_hooks = {
        0: [zero.mate_far, zero.far_hop],
        1: [zero.mate_near, zero.second_hop],
        2: [one.mate_far, one.far_hop],
        3: [one.mate_near, lambda: close(0), one.second_hop],
    }

    def hooked(at, hooks):
        for k, steps in hooks.items():

            @pl.when(at == k)
            def _():
                for step in steps:
                    step()

    def image(m):
        mix_grads(m)

        def one_head(h):
            attend(m, h)
            hooked(m * heads + h, attend_hooks)

        repeat(heads, one_head)

        def one_chip(i):
            back_project(m, pl.ds(chip_rows(slab, i), 4 * half_rows))
            hooked(2 * m + i, project_hooks)

        repeat(2, one_chip)

    repeat(micro, image)
    for load in load_rest:
        load.wait()
    weight_grads({0: [one.first_hop]})
    close(1)

    for errand, _ in errands:
        pl.when(sends_errand)(errand.wait_send)
        pl.when(gets_errand)(errand.wait_recv)


def any_spec():
    return pl.BlockSpec(memory_space=pl.ANY)


def vmem_spec():
    return pl.BlockSpec(memory_space=pltpu.VMEM)


def shape_of(shape, dtype):
    return jax.ShapeDtypeStruct(shape, dtype)


def params(collective):
    return pltpu.CompilerParams(
        collective_id=collective, has_side_effects=True, vmem_limit_bytes=VMEM_BYTES
    )


def smem_spec():
    return pl.BlockSpec(memory_space=pltpu.SMEM)


def attn_forward(rows_low, vectors, bias, packed, at, layer, lengths, own_rows, given=None, grads=None):
    micro, half_rows, width = rows_low.shape
    seq = 8 * half_rows
    pair = bias.shape[2] // 3
    heads = pair // LANES
    low_type, high_type = jnp.bfloat16, jnp.float32
    hidden, lse, normed, qkv, mixed = pl.pallas_call(
        functools.partial(attn_forward_kernel, given is not None, at, layer, own_rows),
        out_shape=[
            shape_of((micro, half_rows, width), high_type),
            shape_of((micro, heads, seq, LANES), high_type),
            shape_of((micro, seq, width), low_type),
            shape_of((micro, seq, 3 * pair), low_type),
            shape_of((micro, seq, pair), low_type),
        ],
        in_specs=[vmem_spec()] * 3 + [smem_spec(), any_spec(), any_spec(), vmem_spec()],
        out_specs=[vmem_spec()] * 2 + [any_spec()] * 3,
        scratch_shapes=gather_scratch(micro, seq, width)
        + scatter_scratch(micro, seq, half_rows, width)
        + [
            pltpu.VMEM((width, 4 * heads * HEAD), low_type),
            pltpu.VMEM((width, 4 * pair), low_type),
            pltpu.VMEM((micro, seq, 3 * pair), low_type),
            pltpu.VMEM((micro, seq, pair), low_type),
            pltpu.SemaphoreType.DMA,
            pltpu.SemaphoreType.DMA((6,)),
            pltpu.SemaphoreType.DMA((micro,)),
            pltpu.VMEM((micro, seq if given is not None else 32, width), low_type),
            pltpu.SemaphoreType.DMA((micro, 3)),
            pltpu.SemaphoreType.DMA((micro, 3)),
        ],
        compiler_params=params(0 if given is None else 6),
        cost_estimate=COST,
        name="attn_forward",
    )(
        rows_low,
        vectors,
        bias,
        lengths,
        packed,
        packed if given is None else given,
        rows_low if grads is None else grads,
    )
    if given is None:
        return hidden, (normed, qkv, lse, mixed)
    return hidden, (given, qkv, lse, mixed), normed


def ffn_forward(hidden, vectors, up_biases, packed, at, layer, half_ff):
    micro, half_rows, width = hidden.shape
    seq = 8 * half_rows
    ff = up_biases.shape[2]
    packed_cols = 2 * ff - LANES
    low_type, high_type = jnp.bfloat16, jnp.float32
    out, second, upper = pl.pallas_call(
        functools.partial(ffn_forward_kernel, half_ff, at, layer),
        out_shape=[
            shape_of((micro, half_rows, width), low_type),
            shape_of((micro, seq, width), low_type),
            shape_of((micro, seq, ff), high_type),
        ],
        in_specs=[vmem_spec()] * 3 + [any_spec()],
        out_specs=[vmem_spec()] + [any_spec()] * 2,
        scratch_shapes=gather_scratch(micro, seq, width)
        + scatter_scratch(micro, seq, half_rows, width)
        + [
            pltpu.VMEM((width, packed_cols), low_type),
            pltpu.VMEM((width, 2 * LANES), low_type),
            pltpu.VMEM((micro, seq, ff), high_type),
            pltpu.SemaphoreType.DMA,
            pltpu.SemaphoreType.DMA((4,)),
        ],
        compiler_params=params(1),
        cost_estimate=COST,
        name="ffn_forward",
    )(hidden, vectors, up_biases, packed)
    return out, (second, upper)


def ffn_turn(hidden, grad_low, given, vectors, up_biases, packed, at, layer, half_ff):
    micro, half_rows, width = hidden.shape
    seq = 8 * half_rows
    ff = up_biases.shape[2]
    low_type, high_type = jnp.bfloat16, jnp.float32
    out, grad_hidden, grads, small, up_bias = pl.pallas_call(
        functools.partial(ffn_turn_kernel, half_ff, at, layer),
        out_shape=[
            shape_of((micro, half_rows, width), low_type),
            shape_of((micro, half_rows, width), high_type),
            shape_of((width, 2 * ff - LANES), low_type),
            shape_of((8, width), high_type),
            shape_of((8, ff), high_type),
        ],
        in_specs=[vmem_spec()] * 4 + [any_spec()] * 2,
        out_specs=[vmem_spec()] * 5,
        scratch_shapes=gather_scratch(micro, seq, width)
        + scatter_scratch(micro, seq, half_rows, width)
        + scatter_scratch(micro, seq, half_rows, width)
        + [
            pltpu.VMEM((width, 2 * ff - LANES), low_type),
            pltpu.VMEM((width, 2 * LANES), low_type),
            pltpu.VMEM((micro, seq, width), low_type),
            pltpu.VMEM((micro, seq, ff), low_type),
            pltpu.VMEM((micro, seq, ff), low_type),
            pltpu.SemaphoreType.DMA,
            pltpu.SemaphoreType.DMA((micro,)),
        ],
        compiler_params=params(7),
        cost_estimate=COST,
        name="ffn_turn",
    )(hidden, grad_low, vectors, up_biases, given, packed)
    return out, grad_hidden, grads, small, up_bias


def ffn_backward(grad_low, hidden, kept, vectors, packed, at, layer, half_ff):
    second, upper = kept
    micro, half_rows, width = hidden.shape
    seq, ff = upper.shape[1:]
    low_type, high_type = jnp.bfloat16, jnp.float32
    grad_hidden, grads, small, up_bias = pl.pallas_call(
        functools.partial(ffn_backward_kernel, half_ff, at, layer),
        out_shape=[
            shape_of((micro, half_rows, width), high_type),
            shape_of((width, 2 * ff - LANES), low_type),
            shape_of((8, width), high_type),
            shape_of((8, ff), high_type),
        ],
        in_specs=[vmem_spec()] * 3 + [any_spec()] * 3,
        out_specs=[vmem_spec()] * 4,
        scratch_shapes=gather_scratch(micro, seq, width)
        + scatter_scratch(micro, seq, half_rows, width)
        + [
            pltpu.VMEM((width, 2 * ff - LANES), low_type),
            pltpu.VMEM((width, 2 * LANES), low_type),
            pltpu.VMEM((micro, seq, width), low_type),
            pltpu.VMEM((micro, seq, ff), high_type),
            pltpu.VMEM((micro, seq, ff), low_type),
            pltpu.VMEM((micro, seq, ff), low_type),
            pltpu.SemaphoreType.DMA((1 + 2 * micro,)),
        ],
        compiler_params=params(2),
        cost_estimate=COST,
        name="ffn_backward",
    )(grad_low, hidden, vectors, second, upper, packed)
    return grad_hidden, grads, small, up_bias


def attn_backward(
    grad_hidden, rows_low, kept, vectors, packed, at, layer, lengths, own_rows, errand, both_ways
):
    normed, qkv, lse, mixed = kept
    micro, half_rows, width = grad_hidden.shape
    seq, pair = mixed.shape[1:]
    heads = pair // LANES
    low_type, high_type = jnp.bfloat16, jnp.float32
    out, grads, small, bias, got = pl.pallas_call(
        functools.partial(attn_backward_kernel, at, layer, own_rows, both_ways),
        out_shape=[
            shape_of((micro, half_rows, width), low_type),
            shape_of((width, 4 * heads * HEAD), low_type),
            shape_of((8, width), high_type),
            shape_of((8, pair), high_type),
            shape_of(errand[0].shape, errand[0].dtype),
        ],
        in_specs=[vmem_spec()] * 4 + [smem_spec()] + [any_spec()] * 6,
        out_specs=[vmem_spec()] * 4 + [any_spec()],
        scratch_shapes=gather_scratch(micro, seq, width)
        + scatter_scratch(micro, seq, half_rows, width)
        + [
            pltpu.VMEM((width, 4 * heads * HEAD), low_type),
            pltpu.VMEM((width, 4 * pair), low_type),
            pltpu.VMEM((micro, seq, width), low_type),
            pltpu.VMEM((micro, seq, 3 * pair), low_type),
            pltpu.VMEM((micro, seq, pair), low_type),
            pltpu.VMEM((micro, seq, pair), low_type),
            pltpu.VMEM((micro, seq, 3 * pair), low_type),
            pltpu.VMEM((micro, heads, LANES, seq), low_type),
            pltpu.VMEM((micro, seq, LANES), high_type),
            pltpu.VMEM((seq, seq), low_type),
            pltpu.VMEM((seq, seq), low_type),
            pltpu.VMEM((micro, heads, seq, seq), high_type),
            pltpu.SemaphoreType.DMA((2, 2)),
            pltpu.SemaphoreType.DMA((1 + 3 * micro,)),
        ],
        compiler_params=params(3 + 5 * layer),
        cost_estimate=COST,
        name="attn_backward",
    )(grad_hidden, rows_low, vectors, lse, lengths, normed, qkv, mixed, packed, *errand)
    return out, grads, small, bias, got


def slab_peers():
    section, tensor = lax.axis_index("section"), lax.axis_index("tensor")
    peers = []
    for role in range(1, 8):
        far, step = role // 4, role % 4
        other = section + far * (1 - 2 * section)
        to = (other, lax.rem(tensor + step, 4))
        source = (other, lax.rem(tensor + 4 - step, 4))
        peers.append((role, to, source))
    return peers


def column_peers(count):
    here = lax.axis_index("dp")
    return [
        (step, lax.rem(here + step, count), lax.rem(here + count - step, count))
        for step in range(1, count)
    ]


def greet_all(count):
    barrier = pltpu.get_barrier_semaphore()
    for _, to, _ in slab_peers():
        pl.semaphore_signal(barrier, inc=1, device_id=named(to), device_id_type=MESH)
    for _, to, _ in column_peers(count):
        pl.semaphore_signal(barrier, inc=1, device_id={"dp": to}, device_id_type=MESH)
    pl.semaphore_wait(barrier, 7 + count - 1)


def remote(src, dst, send_sem, recv_sem, peer):
    return pltpu.make_async_remote_copy(
        src_ref=src,
        dst_ref=dst,
        send_sem=send_sem,
        recv_sem=recv_sem,
        device_id=peer,
        device_id_type=MESH,
    )


def prologue_kernel(
    count, heads, qkv_ref, out_ref_in, up_ref_in, down_ref_t, gains_ref, shifts_ref, up_bias, rows_ref,
    first_hbm, normed_hbm, attn_ref, ff_zero_hbm, ff_one_hbm, out_ref, up_ref, bias_ref,
    attn_parts, ff_parts, up_halves, mine_ref, all_rows, line, ff_line, column, slab, up_got,
    rows_send, rows_recv, column_send, column_recv, slab_send, slab_recv, swap_send, swap_recv,
    right_send, right_recv, left_send, left_recv, out_sems,
):
    section, tensor, here = (lax.axis_index(name) for name in ("section", "tensor", "dp"))
    width = out_ref.shape[2]
    chunk = width // (4 * count)
    rows = attn_parts.shape[1]
    micro, own_rows = rows_ref.shape[:2]
    pieces = swap_send.shape[0] - 2
    size = rows // pieces
    other = {"section": 1 - section}
    pair = heads * LANES
    pair_cols = heads * HEAD
    half_ff = up_ref_in.shape[1] // 2
    main = half_ff // LANES * LANES
    extra = half_ff - main
    greet_all(count)
    out_turned = low(out_ref_in[...].astype(jnp.float32).T)
    for half in range(2):
        span = slice(half * pair_cols, (half + 1) * pair_cols)
        parts = [qkv_ref[k, :, span] for k in range(3)] + [out_turned[:, span]]
        attn_parts[half] = jnp.concatenate(parts, axis=1)
    keep_slot = jnp.where(section == 0, here, count)
    send_slot = jnp.where(section == 0, here, count)
    got_slot = jnp.where(section == 0, count, here)
    sent = []
    for p in range(pieces):
        span = pl.ds(p * size, size)
        copy = remote(
            attn_parts.at[1 - section, span],
            line.at[send_slot, span],
            swap_send.at[p],
            swap_recv.at[p],
            other,
        )
        copy.start()
        sent.append(copy)
    line[keep_slot] = attn_parts[section]
    mine_ref[...] = jnp.zeros_like(mine_ref)
    gains = gains_ref.shape[0]
    mine_ref[:gains, :chunk] = gains_ref[...]
    for i in range(shifts_ref.shape[0]):
        mine_ref[gains + i : gains + i + 1, :chunk] = shifts_ref[i]
    column[here] = mine_ref[...]
    for step, to, _ in column_peers(count):
        copy = remote(
            mine_ref, column.at[here], column_send.at[step], column_recv.at[step], {"dp": to}
        )
        copy.start()
        sent.append(copy)

    def swapped(p):
        got = line.at[got_slot, pl.ds(p * size, size)]
        remote(got, got, swap_send.at[p], swap_recv.at[p], other).wait_recv()

    def hop(step, p, way, finish=False):
        origin = here - way * step
        sends, recvs = (right_send, right_recv) if way == 1 else (left_send, left_recv)
        inside = (origin >= 0) if way == 1 else (origin < count)
        onward = (here + 1 < count) if way == 1 else (here > 0)
        slot = line.at[jnp.clip(origin, 0, count - 1), pl.ds(p * size, size)]
        target = jnp.clip(here + way, 0, count - 1)
        if step > 0 and not finish:

            @pl.when(inside)
            def _():
                remote(slot, slot, sends.at[step, p], recvs.at[step, p], {"dp": target}).wait_recv()

        if step + 1 < count:

            @pl.when(inside & onward)
            def _():
                copy = remote(
                    slot, slot, sends.at[step, p], recvs.at[step + 1, p], {"dp": target}
                )
                if finish:
                    copy.wait_send()
                else:
                    copy.start()

    def hops(step):
        for p in range(pieces):
            for way in (1, -1):
                hop(step, p, way)

    for step, _, source in column_peers(count):
        slot = column.at[source]
        remote(slot, slot, column_send.at[step], column_recv.at[step], {"dp": source}).wait_recv()
    for role, to, _ in slab_peers():
        copy = remote(
            column, slab.at[section, tensor], slab_send.at[role], slab_recv.at[role], named(to)
        )
        copy.start()
        sent.append(copy)
    slab[section, tensor] = column[...]

    def set_out(p):
        pl.when(section == 1)(lambda: swapped(p))
        for way in (1, -1):
            hop(0, p, way)

    set_out(0)
    for role, _, source in slab_peers():
        slot = slab.at[source[0], source[1]]
        remote(slot, slot, slab_send.at[role], slab_recv.at[role], named(source)).wait_recv()
    for layer in range(2):
        for part in range(4 * count):
            piece = slab[layer, part % 4, part // 4]
            out_ref[layer, :, part * chunk : (part + 1) * chunk] = piece[:, :chunk]
    tiles = TileGather(all_rows, rows_send, rows_recv)
    for m in range(micro):
        own = tiles.tile(m, tensor)
        for begin in range(0, own_rows, 32):
            end = min(begin + 32, own_rows)
            block = rows_ref[m, begin:end].astype(jnp.float32)
            own[begin:end] = low(layer_norm(block, out_ref[0, 0:1], out_ref[0, 2:3]))
        own[own_rows:] = jnp.zeros((tiles.tile_rows - own_rows, width), jnp.bfloat16)
        tiles.start(m)
    for p in range(1, pieces):
        set_out(p)
    blank = jnp.zeros((rows, LANES - 2 * extra), jnp.bfloat16)
    up_halves[...] = jnp.zeros_like(up_halves)
    for half in range(2):
        start = half * half_ff
        up_halves[half, :, :half_ff] = up_bias[:, start : start + half_ff]
        ff_parts[half, :, :main] = up_ref_in[:, start : start + main]
        ff_parts[half, :, main : 2 * main] = down_ref_t[:, start : start + main]
        span = slice(start + main, start + half_ff)
        ff_parts[half, :, 2 * main :] = jnp.concatenate(
            [up_ref_in[:, span], down_ref_t[:, span], blank], axis=1
        )
    ff_swap = remote(
        ff_parts.at[1 - section],
        ff_line.at[section],
        swap_send.at[pieces],
        swap_recv.at[pieces],
        other,
    )
    up_swap = remote(
        up_halves.at[1 - section],
        up_got.at[section],
        swap_send.at[pieces + 1],
        swap_recv.at[pieces + 1],
        other,
    )
    up_swap.start()
    ff_swap.start()
    hops(1)
    start = (2 * tensor + section) * pair_cols
    for layer in range(2):
        turned = pltpu.roll(out_ref[layer], lax.rem(width - start, width), 1)
        empty = jnp.zeros((1, LANES - HEAD), jnp.float32)
        for part, row in ((0, 3), (2, 4)):
            for h in range(heads):
                at = part * pair + h * LANES
                piece = turned[row : row + 1, h * HEAD : (h + 1) * HEAD]
                bias_ref[layer, :, at : at + LANES] = jnp.concatenate([piece, empty], 1)
        bias_ref[layer, :, pair : 2 * pair] = jnp.zeros((1, pair), jnp.float32)
    up_ref[section] = up_halves[section]
    outs = []

    def put(src, dst, i):
        copy = pltpu.make_async_copy(src, dst, out_sems.at[i])
        copy.start()
        outs.append(copy)

    def put_ff(src, section_of_first, i):
        for layer, dst in enumerate((ff_zero_hbm, ff_one_hbm)):
            here_too = layer if section_of_first == 0 else 1 - layer

            @pl.when(section == here_too)
            def _():
                pltpu.make_async_copy(src, dst, out_sems.at[i]).start()

        outs.append(pltpu.make_async_copy(src, ff_zero_hbm, out_sems.at[i]))

    put_ff(ff_parts.at[section], 0, count)
    for step in range(2, count):
        hops(step)
        if step == 2:
            tiles.pass_on()
    if count <= 2:
        tiles.pass_on()
    for p in range(pieces):

        @pl.when(section == 0)
        def _():
            swapped(p)

    for at in range(count):
        put(line.at[at], first_hbm.at[pl.ds(at * rows, rows)], at)
    attn_ref[...] = line[count]
    got = up_got.at[1 - section]
    remote(got, got, swap_send.at[pieces + 1], swap_recv.at[pieces + 1], other).wait_recv()
    up_ref[1 - section] = up_got[1 - section]
    tiles.finish()
    put(all_rows, normed_hbm, count + 2)
    ff_got = ff_line.at[1 - section]
    remote(ff_got, ff_got, swap_send.at[pieces], swap_recv.at[pieces], other).wait_recv()
    put_ff(ff_got, 1, count + 1)
    for step in range(count):
        for p in range(pieces):
            for way in (1, -1):
                hop(step, p, way, True)
    for copy in sent + [ff_swap, up_swap]:
        copy.wait_send()
    tiles.drain()
    for copy in outs:
        copy.wait()


def prologue(qkv, out, up, down_t, gains, shifts, up_bias, rows_low, count, heads, tile_rows):
    part_rows = qkv.shape[1]
    micro, _, width = rows_low.shape
    vector_rows = gains.shape[0] + shifts.shape[0]
    half_ff = up.shape[1] // 2
    ff_wide = round_up(half_ff, LANES)
    attn_shape = (part_rows, 4 * heads * HEAD)
    ff_shape = (2, part_rows, 2 * ff_wide - LANES)
    all_rows = (micro, 4 * tile_rows, width)
    pieces = 3 if part_rows % 96 == 0 else 1
    low_type, high_type = jnp.bfloat16, jnp.float32
    dma = pltpu.SemaphoreType.DMA
    return pl.pallas_call(
        functools.partial(prologue_kernel, count, heads),
        out_shape=[
            shape_of((count * part_rows, attn_shape[1]), low_type),
            shape_of(all_rows, low_type),
            shape_of(attn_shape, low_type),
            shape_of(ff_shape[1:], low_type),
            shape_of(ff_shape[1:], low_type),
            shape_of((2, vector_rows, width), high_type),
            shape_of((2, 1, ff_wide), high_type),
            shape_of((2, 1, 3 * heads * LANES), high_type),
        ],
        in_specs=[vmem_spec()] * 8,
        out_specs=[any_spec()] * 2 + [vmem_spec()] + [any_spec()] * 2 + [vmem_spec()] * 3,
        scratch_shapes=[
            pltpu.VMEM((2,) + attn_shape, low_type),
            pltpu.VMEM(ff_shape, low_type),
            pltpu.VMEM((2, 1, ff_wide), high_type),
            pltpu.VMEM((vector_rows, LANES), high_type),
            pltpu.VMEM(all_rows, low_type),
            pltpu.VMEM((count + 1,) + attn_shape, low_type),
            pltpu.VMEM(ff_shape, low_type),
            pltpu.VMEM((count, vector_rows, LANES), high_type),
            pltpu.VMEM((2, 4, count, vector_rows, LANES), high_type),
            pltpu.VMEM((2, 1, ff_wide), high_type),
            dma((micro, 3)),
            dma((micro, 3)),
            dma((count,)),
            dma((count,)),
            dma((8,)),
            dma((8,)),
            dma((pieces + 2,)),
            dma((pieces + 2,)),
            dma((count, pieces)),
            dma((count, pieces)),
            dma((count, pieces)),
            dma((count, pieces)),
            dma((count + 3,)),
        ],
        compiler_params=params(4),
        cost_estimate=COST,
        name="prologue",
    )(qkv, out, up, down_t, gains, shifts, up_bias, rows_low)


def home_kernel(
    count, chunk, attn_zero, attn_one, ff_zero, ff_one, bias_zero, bias_one, up_zero, up_one,
    ff_sum_hbm, attn_sum_hbm, rows_zero_hbm, rows_one_hbm,
    out_ref, up_ref, ff_got_hbm, attn_got_hbm, rows_got_hbm,
    parts, ups, slab, column, up_pair, up_column, total,
    column_send, column_recv, slab_send, slab_recv, up_sems, up_column_send, up_column_recv, far_send, far_recv,
):
    section, tensor, here = (lax.axis_index(name) for name in ("section", "tensor", "dp"))
    width = attn_zero.shape[1]
    heads = bias_zero.shape[1] // LANES
    biases_in, ups_in = (bias_zero, bias_one), (up_zero, up_one)
    other = {"section": 1 - section}
    greet_all(count)
    parts[...] = jnp.zeros_like(parts)
    start = (2 * tensor + section) * (heads * HEAD)
    for layer, (attn, ff) in enumerate(((attn_zero, ff_zero), (attn_one, ff_one))):
        bias = biases_in[layer][...]
        blank = jnp.zeros((8, width - heads * HEAD), jnp.float32)
        pieces = [bias[:, h * LANES : h * LANES + HEAD] for h in range(heads)]
        placed = pltpu.roll(jnp.concatenate(pieces + [blank], 1), start, 1)
        whole = jnp.concatenate(
            [attn[0:1], ff[0:1], attn[1:2], placed[0:2], ff[3:4], ff[1:2], ff[2:3]], axis=0
        )
        for part in range(4 * count):
            piece = whole[:, part * chunk : (part + 1) * chunk]
            parts[layer, part % 4, part // 4, :, :chunk] = piece
        ups[layer] = ups_in[layer][0:1]
    sent = []

    def send(src, dst, send_sem, recv_sem, peer):
        copy = remote(src, dst, send_sem, recv_sem, peer)
        copy.start()
        sent.append(copy)

    send(ups.at[1 - section], up_pair.at[section], up_sems.at[0], up_sems.at[1], other)
    for role, to, _ in slab_peers():
        send(
            parts.at[to[0], to[1]], slab.at[role], slab_send.at[role], slab_recv.at[role], named(to)
        )
    far_rows = remote(rows_zero_hbm, rows_got_hbm, far_send.at[0], far_recv.at[0], other)
    far_rows_one = remote(rows_one_hbm, rows_got_hbm, far_send.at[0], far_recv.at[0], other)
    far_ff = remote(ff_sum_hbm, ff_got_hbm, far_send.at[1], far_recv.at[1], other)
    far_attn = remote(attn_sum_hbm, attn_got_hbm, far_send.at[2], far_recv.at[2], other)
    one_way = ((far_ff, 1), (far_attn, 0))
    pl.when(section == 1)(far_rows.start)
    pl.when(section == 0)(far_rows_one.start)
    for copy, source in one_way:
        pl.when(section == source)(copy.start)
    up_pair[section] = ups[section]
    value = parts[section, tensor]
    for role, _, source in slab_peers():
        slot = slab.at[role]
        remote(slot, slot, slab_send.at[role], slab_recv.at[role], named(source)).wait_recv()
        value = value + slab[role]
    total[...] = value
    for step, to, _ in column_peers(count):
        send(total.at[to], column.at[step], column_send.at[step], column_recv.at[step], {"dp": to})
    got = up_pair.at[1 - section]
    remote(got, got, up_sems.at[0], up_sems.at[1], other).wait_recv()
    for step, to, _ in column_peers(count):
        send(
            up_pair, up_column.at[here], up_column_send.at[step], up_column_recv.at[step], {"dp": to}
        )
    up_column[here] = up_pair[...]
    result = total[here]
    for step, _, source in column_peers(count):
        slot = column.at[step]
        remote(slot, slot, column_send.at[step], column_recv.at[step], {"dp": source}).wait_recv()
        result = result + column[step]
    out_ref[...] = result
    for step, _, source in column_peers(count):
        slot = up_column.at[source]
        remote(
            slot, slot, up_column_send.at[step], up_column_recv.at[step], {"dp": source}
        ).wait_recv()
    value = up_column[0]
    for at in range(1, count):
        value = value + up_column[at]
    up_ref[...] = value
    far_rows.wait()
    for copy, source in one_way:
        pl.when(section == source)(copy.wait_send)
        pl.when(section != source)(copy.wait_recv)
    for copy in sent:
        copy.wait_send()


def home(attn_small, ff_small, bias_grads, up_grads, ff_sum, attn_sum, rows, count, chunk):
    vector_rows, lanes = 8, LANES
    up_shape = (1, up_grads[0].shape[1])
    dma = pltpu.SemaphoreType.DMA
    high_type = jnp.float32
    return pl.pallas_call(
        functools.partial(home_kernel, count, chunk),
        out_shape=[
            shape_of((vector_rows, lanes), high_type),
            shape_of((2,) + up_shape, high_type),
            shape_of(ff_sum.shape, ff_sum.dtype),
            shape_of(attn_sum.shape, attn_sum.dtype),
            shape_of(rows[0].shape, rows[0].dtype),
        ],
        in_specs=[vmem_spec()] * 8 + [any_spec()] * 4,
        out_specs=[vmem_spec()] * 2 + [any_spec()] * 3,
        scratch_shapes=[
            pltpu.VMEM((2, 4, count, vector_rows, lanes), high_type),
            pltpu.VMEM((2,) + up_shape, high_type),
            pltpu.VMEM((8, count, vector_rows, lanes), high_type),
            pltpu.VMEM((count, vector_rows, lanes), high_type),
            pltpu.VMEM((2,) + up_shape, high_type),
            pltpu.VMEM((count, 2) + up_shape, high_type),
            pltpu.VMEM((count, vector_rows, lanes), high_type),
            dma((count,)),
            dma((count,)),
            dma((8,)),
            dma((8,)),
            dma((2,)),
            dma((count,)),
            dma((count,)),
            dma((3,)),
            dma((3,)),
        ],
        compiler_params=params(5),
        cost_estimate=COST,
        name="home",
    )(*attn_small, *ff_small, *bias_grads, *up_grads, ff_sum, attn_sum, *rows)


def ff_finish_kernel(zero, one, zero_got, one_got, up_ref, down_ref):
    first = lax.axis_index("section") == 0
    halves = (
        jnp.where(first, zero[...], one_got[...]),
        jnp.where(first, zero_got[...], one[...]),
    )
    half_ff = up_ref.shape[1] // 2
    main = half_ff // LANES * LANES
    extra = half_ff - main
    for k in range(2):
        pieces = []
        for half in halves:
            start = 2 * main + k * extra
            pieces += [half[:, k * main : (k + 1) * main], half[:, start : start + extra]]
        whole = jnp.concatenate(pieces, axis=1).astype(jnp.float32)
        (up_ref, down_ref)[k][...] = whole


def ff_finish(sums, got, ff_cols):
    rows = sums[0].shape[0]
    return pl.pallas_call(
        ff_finish_kernel,
        out_shape=[
            shape_of((rows, ff_cols), jnp.float32),
            shape_of((rows, ff_cols), jnp.float32),
        ],
        in_specs=[vmem_spec()] * 4,
        out_specs=[vmem_spec()] * 2,
        compiler_params=pltpu.CompilerParams(vmem_limit_bytes=VMEM_BYTES),
        cost_estimate=COST,
        name="ff_finish",
    )(*sums, *got)


def attn_finish_kernel(zero, one, zero_got, one_got, qkv_ref, out_ref):
    first = lax.axis_index("section") == 0
    halves = (
        jnp.where(first, zero[...], one_got[...]),
        jnp.where(first, zero_got[...], one[...]),
    )
    pair_cols = qkv_ref.shape[2] // 2
    for k in range(4):
        span = slice(k * pair_cols, (k + 1) * pair_cols)
        whole = jnp.concatenate([half[:, span] for half in halves], axis=1).astype(jnp.float32)
        if k < 3:
            qkv_ref[k] = whole
        else:
            out_ref[...] = whole.T


def attn_finish(sums, got, head_cols):
    rows = sums[0].shape[0]
    return pl.pallas_call(
        attn_finish_kernel,
        out_shape=[
            shape_of((3, rows, head_cols), jnp.float32),
            shape_of((head_cols, rows), jnp.float32),
        ],
        in_specs=[vmem_spec()] * 4,
        out_specs=[vmem_spec()] * 2,
        compiler_params=pltpu.CompilerParams(vmem_limit_bytes=VMEM_BYTES),
        name="attn_finish",
    )(*sums, *got)


def shards(
    section_input,
    final_cotangent,
    lengths,
    qkv_weight,
    out_weight,
    up_weight,
    down_weight,
    norm_gains,
    biases,
    up_bias,
):
    here = lax.axis_index("section")
    sections = lax.axis_size("section")
    micro, _, own_rows, _ = section_input.shape
    head_cols = qkv_weight.shape[3]
    pair_cols = head_cols // sections
    heads = pair_cols // HEAD
    ff_cols = up_weight.shape[2]
    half_ff = ff_cols // sections
    half_rows = round_up(-(-own_rows // sections), 32)
    full_rows = half_rows * sections

    def by_layer(mine, other):
        return [jnp.where(here == 0, mine, other), jnp.where(here == 0, other, mine)]

    count = lax.axis_size("dp")
    chunk = norm_gains.shape[2]
    first, normed, attn_part, ff_zero, ff_one, vectors, up_biases, bias_qv = prologue(
        qkv_weight[0],
        out_weight[0],
        up_weight[0],
        down_weight[0].T,
        norm_gains[0],
        biases.transpose(1, 0, 2),
        up_bias,
        section_input[:, 0],
        count,
        heads,
        full_rows,
    )

    def gather_column(part):
        return lax.all_gather(part, "dp", axis=0, tiled=True)

    ff_first = gather_column(ff_zero)
    attn_packed = [(first, 0), (gather_column(attn_part), 0)]
    ff_packed = [(ff_first, 0), (gather_column(ff_one), 0)]
    lengths_here = lengths.reshape(micro)

    def my_rows(value):
        padded = jnp.pad(value[:, 0], [(0, 0), (0, full_rows - own_rows), (0, 0)])
        return lax.dynamic_slice_in_dim(padded, here * half_rows, half_rows, 1)

    def whole_rows(first, second, got):
        low_half, high_half = by_layer(jnp.where(here == 0, first, second), got)
        return jnp.concatenate([low_half, high_half], 1)[:, None, :own_rows]

    rows = my_rows(section_input)
    inputs, hiddens, attn_kept = [], [], []
    for layer in range(2):
        inputs.append(rows)
        operands = (rows, vectors, bias_qv, *attn_packed[layer], layer, lengths_here, own_rows)
        if layer == 0:
            hidden, kept, grads_all = attn_forward(*operands, normed, final_cotangent[:, 0])
        else:
            hidden, kept = attn_forward(*operands)
        hiddens.append(hidden)
        attn_kept.append(kept)
        if layer == 0:
            rows, ff_kept = ffn_forward(hidden, vectors, up_biases, *ff_packed[0], 0, half_ff)

    attn_sums, ff_sums, up_sums, input_grads = {}, {}, {}, {}
    attn_small, ff_small, bias_grads, errands = {}, {}, {}, {}
    for layer in (1, 0):
        if layer == 1:
            last, grad_hidden, ff_grad, ff_small[1], up_sums[1] = ffn_turn(
                hiddens[1],
                my_rows(final_cotangent),
                grads_all,
                vectors,
                up_biases,
                *ff_packed[1],
                1,
                half_ff,
            )
        else:
            grad_hidden, ff_grad, ff_small[0], up_sums[0] = ffn_backward(
                grads, hiddens[0], ff_kept, vectors, *ff_packed[0], 0, half_ff
            )
        ff_sums[layer] = lax.psum_scatter(ff_grad, "dp", scatter_dimension=0, tiled=True)
        if layer == 1:
            errand, both_ways = (last, rows), True
        else:
            errand, both_ways = (ff_sums[1], ff_sums[1]), False
        grads, attn_grad, attn_small[layer], bias_grads[layer], got = attn_backward(
            grad_hidden,
            inputs[layer],
            attn_kept[layer],
            vectors,
            *attn_packed[layer],
            layer,
            lengths_here,
            own_rows,
            errand,
            both_ways,
        )
        errands[layer] = got
        attn_sums[layer] = lax.psum_scatter(attn_grad, "dp", scatter_dimension=0, tiled=True)
        input_grads[layer] = grads

    small_mine, up_total, ff_got, attn_got, rows_got = home(
        [attn_small[0], attn_small[1]],
        [ff_small[0], ff_small[1]],
        [bias_grads[0], bias_grads[1]],
        [up_sums[0], up_sums[1]],
        ff_sums[0],
        attn_sums[1],
        [input_grads[0], input_grads[1]],
        count,
        chunk,
    )
    attn_zero_got = lax.ppermute(attn_sums[0], "section", [(1, 0)])
    up_grad, down_grad = ff_finish([ff_sums[0], ff_sums[1]], [ff_got, errands[0]], ff_cols)
    small_mine, up_total, rows_got, out_got, up_grad = lax.optimization_barrier(
        (small_mine, up_total, rows_got, errands[1], up_grad)
    )
    section_output = whole_rows(rows, last, out_got)
    small_mine = small_mine[None, :, :chunk]
    up_total = up_total[:, :, :half_ff].reshape(1, ff_cols)
    input_grad = whole_rows(input_grads[0], input_grads[1], rows_got)

    qkv_total, out_total = attn_finish(
        [attn_sums[0], attn_sums[1]], [attn_zero_got, attn_got], head_cols
    )
    gains = norm_gains.shape[1]
    return (
        section_output[None],
        input_grad[None],
        qkv_total[None],
        out_total[None],
        up_grad[None],
        down_grad.T[None],
        small_mine[:, :gains],
        small_mine[:, gains:],
        up_total,
    )


def solution(mesh):
    in_specs = (
        P(None, "dp", "tensor", None),
        P(None, "dp", "tensor", None),
        P(None, "dp"),
        P("section", None, "dp", "tensor"),
        P("section", "tensor", "dp"),
        P("section", "dp", "tensor"),
        P("section", "tensor", "dp"),
        P("section", None, ("dp", "tensor")),
        P("section", None, ("dp", "tensor")),
        P("section", "tensor"),
    )
    out_specs = (
        P("section", None, "dp", "tensor", None),
        P("section", None, "dp", "tensor", None),
        P("section", None, "dp", "tensor"),
        P("section", "tensor", "dp"),
        P("section", "dp", "tensor"),
        P("section", "tensor", "dp"),
        P("section", None, ("dp", "tensor")),
        P("section", None, ("dp", "tensor")),
        P("section", "tensor"),
    )
    return jax.shard_map(shards, mesh=mesh, in_specs=in_specs, out_specs=out_specs, check_vma=False)
```

```python
import functools
import math

import jax
import jax.numpy as jnp
from jax import lax
from jax.experimental import pallas as pl
from jax.experimental.pallas import tpu as pltpu
from jax.sharding import PartitionSpec as P


HEAD = 72
LANES = 128
norm_eps = 1e-06
masked_score = -1000000000.0
score_scale = 1.0 / math.sqrt(HEAD)
GELU_A = math.sqrt(2.0 / math.pi)
GELU_B = 0.044715


def round_up(value, step):
    return -(-value // step) * step


def dot(left, right, left_dim, right_dim):
    return lax.dot_general(
        left, right, (((left_dim,), (right_dim,)), ((), ())), preferred_element_type=jnp.float32
    )


def low(value):
    return value.astype(jnp.bfloat16)


def layer_norm(rows, gain_vec, shift_vec):
    centred = rows - jnp.mean(rows, axis=-1, keepdims=True)
    spread = jnp.mean(centred * centred, axis=-1, keepdims=True)
    return centred * lax.rsqrt(spread + norm_eps) * gain_vec + shift_vec


def norm_back(rows, gain_vec, grads):
    centred = rows - jnp.mean(rows, axis=-1, keepdims=True)
    spread = jnp.mean(centred * centred, axis=-1, keepdims=True)
    inverse = lax.rsqrt(spread + norm_eps)
    xhat = centred * inverse
    e = grads * gain_vec
    back = inverse * (
        e
        - jnp.mean(e, axis=-1, keepdims=True)
        - xhat * jnp.mean(e * xhat, axis=-1, keepdims=True)
    )
    return back, grads * xhat


def gelu_tanh(value):
    return jax.nn.gelu(value, approximate=True)


MESH = pl.DeviceIdType.MESH
VMEM_BYTES = 64_000_000
COST = pl.CostEstimate(flops=20_000_000_000, transcendentals=0, bytes_accessed=100_000_000)
LOG2E = 1.0 / math.log(2.0)
TILE = 256
WIDE = 384


class Slab:
    def __init__(self, half_rows):
        self.half_rows = half_rows
        section = lax.axis_index("section")
        tensor = lax.axis_index("tensor")
        core = lax.rem(tensor, 2)
        self.core = core
        self.mine = self.around(section, tensor, core)
        self.theirs = self.around(section, tensor + 1 - 2 * core, 1 - core)
        self.far_role, self.near_role = 1 + core, 2 - core
        self.mate = self.theirs[0]
        over = lax.rem(tensor + 2, 4)
        self.near, self.far = tensor, over
        self.mate_near, self.mate_far = self.mate[1], lax.rem(self.mate[1] + 2, 4)
        self.grid = self.places(section, self.near, self.far)
        self.mate_grid = self.places(section, self.mate_near, self.mate_far)
        self.across_y = self.grid[2]
        self.first, self.second = self.mine[1], self.mine[2]

    def place(self, section, tensor):
        start = (2 * tensor + section) * self.half_rows
        return (section, tensor, pl.multiple_of(start, self.half_rows))

    def places(self, section, near, far):
        flip = 1 - section
        return [self.place(*at) for at in ((section, near), (flip, near), (section, far), (flip, far))]

    def around(self, section, tensor, core):
        over = lax.rem(tensor + 2, 4)
        turn = 1 - 2 * section
        first = (section + (1 - core) * turn, tensor + core * (over - tensor))
        second = (section + core * turn, tensor + (1 - core) * (over - tensor))
        places = ((section, tensor), first, second, (1 - section, over))
        return [self.place(*at) for at in places]

    def rows(self, ref, at):
        return ref.at[pl.ds(at[2], self.half_rows)]

    def greet(self):
        barrier = pltpu.get_barrier_semaphore()
        for peer in (self.first, self.second, self.mate):
            pl.semaphore_signal(barrier, inc=1, device_id=named(peer), device_id_type=MESH)
        pl.semaphore_wait(barrier, 3)


def named(at):
    return {"section": at[0], "tensor": at[1]}


class Moves:
    def __init__(self, slab, send_sems, recv_sems):
        self.slab, self.send_sems, self.recv_sems = slab, send_sems, recv_sems
        self.sent = []

    def copy(self, src, dst, role, peer):
        return pltpu.make_async_remote_copy(
            src_ref=src,
            dst_ref=dst,
            send_sem=self.send_sems.at[role],
            recv_sem=self.recv_sems.at[role],
            device_id=named(peer),
            device_id_type=MESH,
        )

    def send(self, ends, role, peer):
        self.copy(*ends(), role, peer).start()
        self.sent.append(lambda: self.copy(*ends(), role, peer))

    def arrived(self, dst, role):
        self.copy(dst, dst, role, self.slab.mate).wait_recv()

    def drain(self):
        for copy in self.sent:
            copy().wait_send()


class Gather(Moves):
    def __init__(self, slab, whole, send_sems, recv_sems):
        super().__init__(slab, send_sems, recv_sems)
        self.whole = whole

    def pass_on(self, at, role, peer):
        self.send(lambda: (self.slab.rows(self.whole, at),) * 2, role, peer)

    def arrive(self, at, role):
        self.arrived(self.slab.rows(self.whole, at), role)

    def start(self):
        mine = self.slab.mine
        self.pass_on(mine[0], 0, mine[1])
        self.pass_on(mine[0], 3, self.slab.mate)

    def second(self):
        self.sent.pop(0)().wait_send()
        self.pass_on(self.slab.mine[0], 1, self.slab.mine[2])

    def forward(self):
        mine, mate = self.slab.mine, self.slab.mate
        self.arrive(mine[1], 0)
        self.pass_on(mine[1], 2, mine[2])
        self.pass_on(mine[1], 4, mate)

    def to_mate(self):
        mine, mate = self.slab.mine, self.slab.mate
        self.arrive(mine[2], 1)
        self.pass_on(mine[2], 5, mate)
        self.arrive(mine[3], 2)
        self.pass_on(mine[3], 6, mate)

    def finish(self):
        for k in range(4):
            self.arrive(self.slab.theirs[k], 3 + k)
        self.drain()


class TileGather:
    def __init__(self, whole, send_sems, recv_sems):
        self.whole, self.send_sems, self.recv_sems = whole, send_sems, recv_sems
        self.tensor = lax.axis_index("tensor")
        self.over = lax.rem(self.tensor + 2, 4)
        self.mate = self.tensor + 1 - 2 * lax.rem(self.tensor, 2)
        self.micro, rows = whole.shape[0], whole.shape[1] // 4
        self.tile_rows = rows
        self.sent = []

    def tile(self, m, index):
        start = pl.multiple_of(index * self.tile_rows, self.tile_rows)
        return self.whole.at[m, pl.ds(start, self.tile_rows)]

    def copy(self, m, index, role, peer):
        part = self.tile(m, index)
        return remote(
            part, part, self.send_sems.at[m, role], self.recv_sems.at[m, role], {"tensor": peer}
        )

    def send(self, m, index, role, peer):
        self.copy(m, index, role, peer).start()
        self.sent.append(lambda: self.copy(m, index, role, peer))

    def start(self, m):
        self.send(m, self.tensor, 0, self.over)
        self.send(m, self.tensor, 1, self.mate)

    def pass_on(self):
        for m in range(self.micro):
            self.copy(m, self.over, 0, self.over).wait_recv()
            self.send(m, self.over, 2, self.mate)

    def finish(self):
        for m in range(self.micro):
            self.copy(m, self.mate, 1, self.mate).wait_recv()
            self.copy(m, lax.rem(self.mate + 2, 4), 2, self.mate).wait_recv()

    def drain(self):
        for copy in self.sent:
            copy().wait_send()


class Scatter(Moves):
    def __init__(self, slab, terms, from_mate, outgoing, arrivals, send_sems, recv_sems):
        super().__init__(slab, send_sems, recv_sems)
        self.terms, self.from_mate, self.outgoing = terms, from_mate, outgoing
        self.relay, self.from_second, self.from_first = (arrivals.at[k] for k in range(3))

    def to_mate(self, at, role):
        self.send(
            lambda: (self.slab.rows(self.terms, at), self.from_mate.at[role]), role, self.slab.mate
        )

    def mate_far(self):
        self.to_mate(self.slab.mate_grid[3], 3)
        self.to_mate(self.slab.mate_grid[2], self.slab.far_role)

    def mate_near(self):
        self.to_mate(self.slab.mate_grid[1], self.slab.near_role)
        self.to_mate(self.slab.mate_grid[0], 0)

    def chip_sum(self, k, rows):
        part = self.slab.rows(self.terms, self.slab.mine[k])
        return part[rows].astype(jnp.float32) + self.from_mate[k, rows].astype(jnp.float32)

    def blocks(self):
        return [pl.ds(start, 32) for start in range(0, self.slab.half_rows, 32)]

    def hop(self, k, slot, dst, role, peer, ride=None):
        self.arrived(self.from_mate.at[k], k)
        if ride is not None:
            self.arrived(ride, 4)
        for rows in self.blocks():
            value = self.chip_sum(k, rows)
            if ride is not None:
                value = value + ride[rows].astype(jnp.float32)
            self.outgoing[slot, rows] = low(value)
        self.send(lambda: (self.outgoing.at[slot], dst), role, peer)

    def far_hop(self):
        self.hop(3, 0, self.relay, 4, self.slab.second)

    def second_hop(self):
        self.hop(2, 1, self.from_second, 5, self.slab.second)

    def first_hop(self):
        self.hop(1, 2, self.from_first, 6, self.slab.first, self.relay)

    def finish(self):
        self.arrived(self.from_mate.at[0], 0)
        self.arrived(self.from_second, 5)
        self.arrived(self.from_first, 6)
        self.drain()

    def total(self, rows):
        other = self.from_second[rows].astype(jnp.float32) + self.from_first[rows].astype(
            jnp.float32
        )
        return self.chip_sum(0, rows) + other


def scatter_scratch(micro, seq, half_rows, width):
    return [
        pltpu.VMEM((micro, seq, width), jnp.bfloat16),
        pltpu.VMEM((micro, 4, half_rows, width), jnp.bfloat16),
        pltpu.VMEM((micro, 3, half_rows, width), jnp.bfloat16),
        pltpu.VMEM((micro, 3, half_rows, width), jnp.bfloat16),
        pltpu.SemaphoreType.DMA((micro, 7)),
        pltpu.SemaphoreType.DMA((micro, 7)),
    ]


def gather_scratch(micro, seq, width):
    return [
        pltpu.VMEM((micro, seq, width), jnp.bfloat16),
        pltpu.SemaphoreType.DMA((micro, 7)),
        pltpu.SemaphoreType.DMA((micro, 7)),
    ]


def make_scatters(slab, refs, micro):
    terms, from_mate, outgoing, arrivals, send_sems, recv_sems = refs
    return [
        Scatter(
            slab,
            terms.at[m],
            from_mate.at[m],
            outgoing.at[m],
            arrivals.at[m],
            send_sems.at[m],
            recv_sems.at[m],
        )
        for m in range(micro)
    ]


def make_gathers(slab, refs, micro):
    whole, send_sems, recv_sems = refs
    return [
        Gather(slab, whole.at[m], send_sems.at[m], recv_sems.at[m]) for m in range(micro)
    ]


def step_from(start, i, size):
    return pl.ds(pl.multiple_of(start + i * size, size), size)


def step_rows(i, size):
    return pl.ds(pl.multiple_of(i * size, size), size)


def repeat(count, body):
    def one(i, carry):
        body(i)
        return carry

    lax.fori_loop(0, count, one, 0)


def shut_keys(length, own_rows, full_rows, shape, dimension):
    place = lax.broadcasted_iota(jnp.int32, shape, dimension)
    step = jnp.zeros(shape, jnp.int32)
    for t in range(1, 4):
        step += (place >= t * full_rows).astype(jnp.int32)
    live = (place - step * full_rows < own_rows) & (
        place - step * (full_rows - own_rows) < length
    )
    return jnp.where(live, 0.0, masked_score)


def stages(count, work, hooks):
    def body(k):
        work(k)
        for at, steps in hooks.items():

            @pl.when(k == at)
            def _():
                for step in steps:
                    step()

    repeat(count, body)


def chip_rows(slab, k):
    far, near = slab.far - slab.core, slab.near - slab.core
    start = (far + lax.rem(k, 2) * (near - far)) * (2 * slab.half_rows)
    return pl.multiple_of(start, 2 * slab.half_rows)


def open_gathers(gathers, fill, prepare):
    fill(0)
    gathers[0].start()
    fill(1)
    gathers[0].second()
    gathers[1].start()
    prepare()
    gathers[0].forward()
    gathers[1].second()


def widen(packed, wide):
    heads = packed.shape[1] // HEAD

    def block(i):
        rows = step_rows(i, 128)
        for h in range(heads):
            piece = packed[rows, h * HEAD : (h + 1) * HEAD]
            blank = jnp.zeros((128, LANES - HEAD), jnp.bfloat16)
            wide[rows, h * LANES : (h + 1) * LANES] = jnp.concatenate([piece, blank], axis=1)

    repeat(packed.shape[0] // 128, block)


def split_tail(packed, tails, up_cols):
    start = packed.shape[1] - LANES

    def block(i):
        rows = step_rows(i, 128)
        for j in range(2):
            piece = packed[rows, start + j * up_cols : start + (j + 1) * up_cols]
            blank = jnp.zeros((128, LANES - up_cols), jnp.bfloat16)
            tails[rows, j * LANES : (j + 1) * LANES] = jnp.concatenate([piece, blank], axis=1)

    repeat(packed.shape[0] // 128, block)


def up_dot(rows, packed, tails):
    main = (packed.shape[1] - LANES) // 2
    first = dot(rows, packed[:, :main], 1, 0)
    return jnp.concatenate([first, dot(rows, tails[:, :LANES], 1, 0)], axis=1)


def up_back(grads, packed, tails):
    main = (packed.shape[1] - LANES) // 2
    return dot(grads[:, :main], packed[:, :main], 1, 1) + dot(
        grads[:, main:], tails[:, :LANES], 1, 1
    )


def down_dot(active, packed, tails):
    main = (packed.shape[1] - LANES) // 2
    return dot(active[:, :main], packed[:, main : 2 * main], 1, 1) + dot(
        active[:, main:], tails[:, LANES:], 1, 1
    )


def down_back(rows, packed, tails):
    main = (packed.shape[1] - LANES) // 2
    first = dot(rows, packed[:, main : 2 * main], 1, 0)
    return jnp.concatenate([first, dot(rows, tails[:, LANES:], 1, 0)], axis=1)


def attn_forward_kernel(
    ready, at, layer, own_rows, rows_ref, vectors, bias_ref, lengths, packed_hbm, given_hbm, grads_ref,
    hidden_ref, lse_ref, normed_hbm, qkv_hbm, mixed_hbm, *rest
):
    micro, half_rows, width = rows_ref.shape
    gathered, gather_refs = rest[0], rest[0:3]
    scatter_refs = rest[3:9]
    terms = rest[3]
    packed, wide, qkv, mixed, load_sem, keep_sems, given_sems, all_grads, tile_send, tile_recv = rest[9:]
    vec, bias = vectors.at[layer], bias_ref[layer]
    seq = qkv.shape[1]
    pair = mixed.shape[2]
    heads = pair // LANES
    load = pltpu.make_async_copy(
        packed_hbm.at[:, at : at + packed.shape[1]], packed, load_sem
    )
    load.start()
    slab = Slab(half_rows)
    gathers = make_gathers(slab, gather_refs, micro)
    scatters = make_scatters(slab, scatter_refs, micro)
    given = [
        pltpu.make_async_copy(given_hbm.at[m], gathered.at[m], given_sems.at[m])
        for m in range(micro if ready else 0)
    ]
    for copy in given:
        copy.start()
    slab.greet()
    if ready:
        tiles = TileGather(all_grads, tile_send, tile_recv)
        for m in range(micro):
            own = tiles.tile(m, tiles.tensor)
            count = grads_ref.shape[1]
            own[:count] = grads_ref[m]
            own[count:] = jnp.zeros((tiles.tile_rows - count, width), jnp.bfloat16)
            tiles.start(m)

    def fill(m):
        own = slab.rows(gathered.at[m], slab.mine[0])
        for start in range(0, half_rows, 32):
            block = rows_ref[m, pl.ds(start, 32)].astype(jnp.float32)
            own[pl.ds(start, 32)] = low(layer_norm(block, vec[0:1], vec[2:3]))

    def prepare():
        load.wait()
        widen(packed, wide)

    if ready:
        prepare()
    else:
        open_gathers(gathers, fill, prepare)
    keeps = []

    def keep(src, dst, m, i):
        def copy():
            return pltpu.make_async_copy(src.at[m], dst.at[m], keep_sems.at[i])

        copy().start()
        keeps.append(copy)

    def project(m):
        def block(i):
            rows = step_rows(i, 4 * half_rows)
            out = dot(gathered[m, rows], wide[:, : 3 * pair], 1, 0)
            qkv[m, rows] = low(out + bias)

        repeat(seq // (4 * half_rows), block)

    def attend(m, rows):
        shut = shut_keys(lengths[m], own_rows, 2 * half_rows, (1, seq), 1)
        for h in range(heads):
            cols = slice(h * LANES, (h + 1) * LANES)
            q = qkv[m, rows, cols]
            k = qkv[m, :, pair + h * LANES : pair + (h + 1) * LANES]
            v = qkv[m, :, 2 * pair + h * LANES : 2 * pair + (h + 1) * LANES]
            scores = dot(q, k, 1, 1) * (score_scale * LOG2E) + shut
            top = jnp.max(scores, axis=-1, keepdims=True)
            exp_scores = jnp.exp2(scores - top)
            total = jnp.sum(exp_scores, axis=-1, keepdims=True)
            probs = low(exp_scores * (1.0 / total))
            mixed[m, rows, cols] = low(dot(probs, v, 1, 0))
            lse_ref[m, h, rows] = jnp.broadcast_to(
                top + jnp.log(total) * LOG2E, (2 * half_rows, LANES)
            )

    def output(m, rows):
        terms[m, rows] = low(dot(mixed[m, rows], wide[:, 3 * pair :], 1, 1))

    def close(m):
        scatters[m].finish()
        for rows in scatters[m].blocks():
            start = rows_ref[m, rows].astype(jnp.float32)
            hidden_ref[m, rows] = start + scatters[m].total(rows) + vec[5:6]

    def gathered_rows(m):
        if ready:
            given[m].wait()
            return
        gathers[m].to_mate()
        gathers[m].finish()
        keep(gathered, normed_hbm, m, m)

    def work(k):
        m = lax.div(k, 2)
        start = chip_rows(slab, k)
        pl.when(lax.rem(k, 2) == 0)(lambda: project(m))

        def piece(i):
            attend(m, step_from(start, i, 2 * half_rows))

        repeat(2, piece)
        output(m, pl.ds(start, 4 * half_rows))

    def keep_two(m):
        keep(qkv, qkv_hbm, m, 2 + 2 * m)
        keep(mixed, mixed_hbm, m, 3 + 2 * m)

    def grads_on():
        if ready:
            tiles.pass_on()

    def grads_in():
        if ready:
            tiles.finish()
            for m in range(micro):
                keep(all_grads, normed_hbm, m, m)

    gathered_rows(0)
    if not ready:
        gathers[1].forward()
    zero, one = scatters
    stages(
        4,
        work,
        {
            0: [zero.mate_far, lambda: gathered_rows(1), zero.far_hop],
            1: [zero.mate_near, lambda: keep_two(0), zero.second_hop, zero.first_hop, grads_on],
            2: [one.mate_far, lambda: close(0), one.far_hop, grads_in],
            3: [one.mate_near, lambda: keep_two(1), one.second_hop, one.first_hop],
        },
    )
    close(1)
    if ready:
        tiles.drain()
    for copy in keeps:
        copy().wait()


def ffn_forward_kernel(
    half_ff, at, layer, hidden_ref, vectors, up_biases, packed_hbm, out_ref, second_hbm, upper_hbm, *rest
):
    micro, half_rows, _ = hidden_ref.shape
    gathered, gather_refs = rest[0], rest[0:3]
    scatter_refs = rest[3:9]
    terms = rest[3]
    packed, tails, upper, load_sem, keep_sems = rest[9:]
    vec, up_bias = vectors.at[layer], up_biases.at[layer]
    _, ff = upper.shape[1:]
    load = pltpu.make_async_copy(
        packed_hbm.at[:, at : at + packed.shape[1]], packed, load_sem
    )
    load.start()
    slab = Slab(half_rows)
    gathers = make_gathers(slab, gather_refs, micro)
    scatters = make_scatters(slab, scatter_refs, micro)
    slab.greet()

    def fill(m):
        own = slab.rows(gathered.at[m], slab.mine[0])
        for start in range(0, half_rows, 32):
            block = hidden_ref[m, pl.ds(start, 32)]
            own[pl.ds(start, 32)] = low(layer_norm(block, vec[1:2], vec[6:7]))

    def prepare():
        load.wait()
        split_tail(packed, tails, half_ff - ff + LANES)

    open_gathers(gathers, fill, prepare)
    keeps = []

    def keep(src, dst, m, i):
        def copy():
            return pltpu.make_async_copy(src.at[m], dst.at[m], keep_sems.at[i])

        copy().start()
        keeps.append(copy)

    def compute(m, rows):
        value = up_dot(gathered[m, rows], packed, tails) + up_bias[...]
        upper[m, rows] = value
        active = low(gelu_tanh(value))
        terms[m, rows] = low(down_dot(active, packed, tails))

    def close(m):
        scatters[m].finish()
        for rows in scatters[m].blocks():
            out_ref[m, rows] = low(hidden_ref[m, rows] + scatters[m].total(rows) + vec[7:8])

    def work(k):
        compute(lax.div(k, 2), pl.ds(chip_rows(slab, k), 4 * half_rows))

    gathers[0].to_mate()
    gathers[0].finish()
    keep(gathered, second_hbm, 0, 0)
    zero, one = scatters
    stages(
        4,
        work,
        {
            0: [zero.mate_far, gathers[1].forward, zero.far_hop],
            1: [
                zero.mate_near,
                lambda: keep(upper, upper_hbm, 0, 1),
                gathers[1].to_mate,
                zero.second_hop,
                gathers[1].finish,
                lambda: keep(gathered, second_hbm, 1, 2),
            ],
            2: [one.mate_far, zero.first_hop, one.far_hop],
            3: [
                one.mate_near,
                lambda: keep(upper, upper_hbm, 1, 3),
                lambda: close(0),
                one.second_hop,
            ],
        },
    )
    one.first_hop()
    close(1)
    for copy in keeps:
        copy().wait()


def ffn_backward_kernel(
    half_ff, at, layer, grad_ref, hidden_ref, vectors, second_hbm, upper_hbm, packed_hbm,
    out_ref, grads_ref, small_ref, up_bias_ref, *rest
):
    micro, half_rows, width = hidden_ref.shape
    gathered, gather_refs = rest[0], rest[0:3]
    scatter_refs = rest[3:9]
    terms = rest[3]
    packed, tails, second, upper, grad_upper, active, load_sems = rest[9:]
    vec = vectors.at[layer]
    seq, ff = upper.shape[1:]
    main = ff - LANES
    extra = half_ff - main
    load_packed = pltpu.make_async_copy(
        packed_hbm.at[:, at : at + packed.shape[1]], packed, load_sems.at[0]
    )
    load_packed.start()
    load_upper, load_second = [], []
    for m in range(micro):
        load_upper.append(
            pltpu.make_async_copy(upper_hbm.at[m], upper.at[m], load_sems.at[1 + m])
        )
        load_upper[m].start()
    for m in range(micro):
        load_second.append(
            pltpu.make_async_copy(second_hbm.at[m], second.at[m], load_sems.at[1 + micro + m])
        )
        load_second[m].start()
    slab = Slab(half_rows)
    gathers = make_gathers(slab, gather_refs, micro)
    scatters = make_scatters(slab, scatter_refs, micro)
    slab.greet()

    def fill(m):
        own = slab.rows(gathered.at[m], slab.mine[0])
        for start in range(0, half_rows, 32):
            own[pl.ds(start, 32)] = grad_ref[m, pl.ds(start, 32)]

    def prepare():
        small_ref[...] = jnp.zeros_like(small_ref)
        up_bias_ref[...] = jnp.zeros_like(up_bias_ref)
        load_packed.wait()
        split_tail(packed, tails, extra)

    open_gathers(gathers, fill, prepare)

    def compute(m, rows):
        value = upper[m, rows]
        square = value * value
        bent = jnp.tanh(GELU_A * value * (1.0 + GELU_B * square))
        half = 0.5 * (1.0 + bent)
        active[m, rows] = low(value * half)
        slope = half + (0.5 * GELU_A) * value * (1.0 - bent * bent) * (1.0 + 3.0 * GELU_B * square)
        grad_active = down_back(gathered[m, rows], packed, tails)
        grad = low(grad_active * slope)
        grad_upper[m, rows] = grad
        up_bias_ref[0:1] += jnp.sum(grad.astype(jnp.float32), axis=0, keepdims=True)
        terms[m, rows] = low(up_back(grad, packed, tails))

    def stacked(ref, cols=slice(None)):
        return ref[:, :, cols].reshape(micro * seq, -1)

    def weight_grads(hooks):
        def block(i):
            cols = step_rows(i, WIDE)
            up = dot(stacked(second, cols), stacked(grad_upper), 0, 0)
            down = dot(stacked(gathered, cols), stacked(active), 0, 0)
            grads_ref[cols, :main] = low(up[:, :main])
            grads_ref[cols, main : 2 * main] = low(down[:, :main])
            blank = jnp.zeros((WIDE, LANES - 2 * extra), jnp.float32)
            rest_cols = [up[:, main : main + extra], down[:, main : main + extra], blank]
            grads_ref[cols, 2 * main :] = low(jnp.concatenate(rest_cols, axis=1))

        stages(width // WIDE, block, hooks)

    def close(m):
        scatters[m].finish()
        for rows in scatters[m].blocks():
            grad_normed = scatters[m].total(rows)
            back, gain_terms = norm_back(hidden_ref[m, rows], vec[1:2], grad_normed)
            grad_rows = grad_ref[m, rows].astype(jnp.float32)
            grad_hidden = grad_rows + back
            out_ref[m, rows] = grad_hidden
            branch = low(grad_hidden).astype(jnp.float32)
            for j, item in enumerate((gain_terms, grad_normed, grad_rows, branch)):
                small_ref[j : j + 1] += jnp.sum(item, axis=0, keepdims=True)

    def work(k):
        compute(lax.div(k, 2), pl.ds(chip_rows(slab, k), 4 * half_rows))

    gathers[0].to_mate()
    gathers[0].finish()
    load_upper[0].wait()
    zero, one = scatters
    stages(
        4,
        work,
        {
            0: [zero.mate_far, gathers[1].forward, zero.far_hop],
            1: [
                zero.mate_near,
                gathers[1].to_mate,
                zero.second_hop,
                gathers[1].finish,
                load_upper[1].wait,
            ],
            2: [one.mate_far, zero.first_hop, one.far_hop],
            3: [one.mate_near, lambda: close(0), one.second_hop],
        },
    )
    for load in load_second:
        load.wait()
    weight_grads({0: [one.first_hop]})
    close(1)


def ffn_turn_kernel(
    half_ff, at, layer, hidden_ref, grad_ref, vectors, up_biases, given_hbm, packed_hbm,
    out_ref, grad_out_ref, grads_ref, small_ref, up_bias_ref, *rest
):
    micro, half_rows, width = hidden_ref.shape
    gathered, gather_refs = rest[0], rest[0:3]
    terms, back_terms = rest[3], rest[9]
    packed, tails, given, grad_upper, active, load_sem, given_sems = rest[15:]
    vec, up_bias = vectors.at[layer], up_biases.at[layer]
    seq, ff = active.shape[1:]
    main = ff - LANES
    extra = half_ff - main
    load = pltpu.make_async_copy(
        packed_hbm.at[:, at : at + packed.shape[1]], packed, load_sem
    )
    load.start()
    loads = [
        pltpu.make_async_copy(given_hbm.at[m], given.at[m], given_sems.at[m]) for m in range(micro)
    ]
    for copy in loads:
        copy.start()
    slab = Slab(half_rows)
    gathers = make_gathers(slab, gather_refs, micro)
    scatters = make_scatters(slab, rest[3:9], micro)
    backs = make_scatters(slab, rest[9:15], micro)
    slab.greet()

    def fill(m):
        own = slab.rows(gathered.at[m], slab.mine[0])
        for start in range(0, half_rows, 32):
            block = hidden_ref[m, pl.ds(start, 32)]
            own[pl.ds(start, 32)] = low(layer_norm(block, vec[1:2], vec[6:7]))

    def prepare():
        small_ref[...] = jnp.zeros_like(small_ref)
        up_bias_ref[...] = jnp.zeros_like(up_bias_ref)
        load.wait()
        split_tail(packed, tails, extra)

    open_gathers(gathers, fill, prepare)

    def compute(m, rows):
        value = up_dot(gathered[m, rows], packed, tails) + up_bias[...]
        square = value * value
        bent = jnp.tanh(GELU_A * value * (1.0 + GELU_B * square))
        half = 0.5 * (1.0 + bent)
        shown = low(value * half)
        active[m, rows] = shown
        slope = half + (0.5 * GELU_A) * value * (1.0 - bent * bent) * (1.0 + 3.0 * GELU_B * square)
        grad = low(down_back(given[m, rows], packed, tails) * slope)
        grad_upper[m, rows] = grad
        up_bias_ref[0:1] += jnp.sum(grad.astype(jnp.float32), axis=0, keepdims=True)
        back_terms[m, rows] = low(up_back(grad, packed, tails))
        terms[m, rows] = low(down_dot(shown, packed, tails))

    def stacked(ref, cols=slice(None)):
        return ref[:, :, cols].reshape(micro * seq, -1)

    def weight_grads(hooks):
        def block(i):
            cols = step_rows(i, WIDE)
            up = dot(stacked(gathered, cols), stacked(grad_upper), 0, 0)
            down = dot(stacked(given, cols), stacked(active), 0, 0)
            grads_ref[cols, :main] = low(up[:, :main])
            grads_ref[cols, main : 2 * main] = low(down[:, :main])
            blank = jnp.zeros((WIDE, LANES - 2 * extra), jnp.float32)
            rest_cols = [up[:, main : main + extra], down[:, main : main + extra], blank]
            grads_ref[cols, 2 * main :] = low(jnp.concatenate(rest_cols, axis=1))

        stages(width // WIDE, block, hooks)

    def close_back(m):
        backs[m].finish()
        for rows in backs[m].blocks():
            grad_normed = backs[m].total(rows)
            back, gain_terms = norm_back(hidden_ref[m, rows], vec[1:2], grad_normed)
            grad_rows = grad_ref[m, rows].astype(jnp.float32)
            grad_hidden = grad_rows + back
            grad_out_ref[m, rows] = grad_hidden
            branch = low(grad_hidden).astype(jnp.float32)
            for j, item in enumerate((gain_terms, grad_normed, grad_rows, branch)):
                small_ref[j : j + 1] += jnp.sum(item, axis=0, keepdims=True)

    def close(m):
        scatters[m].finish()
        for rows in scatters[m].blocks():
            out_ref[m, rows] = low(hidden_ref[m, rows] + scatters[m].total(rows) + vec[7:8])

    def work(k):
        compute(lax.div(k, 2), pl.ds(chip_rows(slab, k), 4 * half_rows))

    gathers[0].to_mate()
    gathers[0].finish()
    loads[0].wait()
    zero, one = scatters
    back_zero, back_one = backs
    stages(
        4,
        work,
        {
            0: [back_zero.mate_far, zero.mate_far, gathers[1].forward, back_zero.far_hop],
            1: [
                back_zero.mate_near,
                zero.mate_near,
                gathers[1].to_mate,
                back_zero.second_hop,
                gathers[1].finish,
                zero.far_hop,
                zero.second_hop,
                loads[1].wait,
            ],
            2: [
                back_one.mate_far,
                one.mate_far,
                back_zero.first_hop,
                back_one.far_hop,
                zero.first_hop,
            ],
            3: [
                back_one.mate_near,
                one.mate_near,
                lambda: close_back(0),
                back_one.second_hop,
                one.far_hop,
                one.second_hop,
            ],
        },
    )
    weight_grads({0: [back_one.first_hop, one.first_hop]})
    close_back(1)
    for m in range(micro):
        close(m)


def attn_backward_kernel(
    at, layer, own_rows, both_ways, grad_ref, rows_ref, vectors, lse, lengths,
    normed_hbm, qkv_hbm, mixed_hbm, packed_hbm, errand_hbm, errand_one_hbm,
    out_ref, grads_ref, small_ref, bias_ref, errand_got, *rest
):
    micro, half_rows, width = grad_ref.shape
    gathered, gather_refs = rest[0], rest[0:3]
    scatter_refs = rest[3:9]
    terms = rest[3]
    packed, wide, normed, qkv, mixed, grad_mixed, grad_qkv, turned, shut = rest[9:18]
    low_probs, grad_scores, high_probs, errand_sems, load_sems = rest[18:]
    vec = vectors.at[layer]
    seq, pair = mixed.shape[1:]
    heads = pair // LANES
    load_packed = pltpu.make_async_copy(
        packed_hbm.at[:, at : at + packed.shape[1]], packed, load_sems.at[0]
    )
    load_packed.start()
    load_qkv, load_rest = [], []
    for m in range(micro):
        load_qkv.append(pltpu.make_async_copy(qkv_hbm.at[m], qkv.at[m], load_sems.at[1 + 3 * m]))
        load_qkv[m].start()
    for m in range(micro):
        for k, (src, dst) in enumerate(((mixed_hbm, mixed), (normed_hbm, normed))):
            load = pltpu.make_async_copy(src.at[m], dst.at[m], load_sems.at[2 + k + 3 * m])
            load.start()
            load_rest.append(load)
    slab = Slab(half_rows)
    gathers = make_gathers(slab, gather_refs, micro)
    scatters = make_scatters(slab, scatter_refs, micro)
    slab.greet()

    def fill(m):
        own = slab.rows(gathered.at[m], slab.mine[0])
        for start in range(0, half_rows, 32):
            own[pl.ds(start, 32)] = low(grad_ref[m, pl.ds(start, 32)])

    def head(h, part=0):
        return pl.ds(pl.multiple_of(part * pair + h * LANES, LANES), LANES)

    def ready_qkv(m):
        load_qkv[m].wait()
        shut[m] = shut_keys(lengths[m], own_rows, 2 * half_rows, (seq, LANES), 0)
        for h in range(heads):
            turned[m, h] = low(qkv[m, :, head(h, 1)].astype(jnp.float32).T)

    def find_probs(m, h):
        def block(i):
            rows = step_rows(i, TILE)
            keys, queries = qkv[m, :, head(h, 1)], qkv[m, rows, head(h)]
            closed = jnp.concatenate([shut[m]] * (TILE // LANES), axis=1)
            scores = dot(keys, queries, 1, 1) * (score_scale * LOG2E) + closed
            high_probs[m, h, :, rows] = jnp.exp2(scores - lse[m, h, rows].T[0:1])

        repeat(seq // TILE, block)

    def find_all(k):
        find_probs(lax.div(k, heads), lax.rem(k, heads))

    span = errand_hbm.shape[0]
    cut = round_up(span // 2, 16) if span > 16 else span // 2
    errands = []
    for k, part in enumerate((pl.ds(0, cut), pl.ds(cut, span - cut))):
        errands.append(
            [
                remote(
                    source.at[part],
                    errand_got.at[part],
                    errand_sems.at[0, k],
                    errand_sems.at[1, k],
                    {"section": 1 - lax.axis_index("section")},
                )
                for source in (errand_hbm, errand_one_hbm)
            ]
        )
    first_section = lax.axis_index("section") == 0
    sends_errand, gets_errand = first_section | both_ways, ~first_section | both_ways

    def prepare():
        small_ref[...] = jnp.zeros_like(small_ref)
        bias_ref[...] = jnp.zeros_like(bias_ref)
        load_packed.wait()
        widen(packed, wide)
        for m in range(micro):
            ready_qkv(m)

    fill(0)
    gathers[0].start()
    fill(1)
    gathers[0].second()
    gathers[1].start()
    prepare()

    def mix_grads(m):
        def block(i):
            rows = step_rows(i, 4 * half_rows)
            grad_mixed[m, rows] = low(dot(gathered[m, rows], wide[:, 3 * pair :], 1, 0))

        repeat(seq // (4 * half_rows), block)

    def attend(m, h):
        def block(i):
            rows = step_rows(i, TILE)
            grads = grad_mixed[m, rows, head(h)]
            probs = high_probs[m, h, :, rows]
            grad_probs = dot(qkv[m, :, head(h, 2)], grads, 1, 1)
            inner = jnp.sum(grad_probs * probs, axis=0, keepdims=True)
            low_probs[:, rows] = low(probs)
            grad_scores[:, rows] = low(probs * (grad_probs - inner))

        repeat(seq // TILE, block)
        grad_keys = dot(grad_scores[...], qkv[m, :, head(h)], 1, 0)
        grad_qkv[m, :, head(h, 1)] = low(grad_keys * score_scale)
        grad_qkv[m, :, head(h, 2)] = low(dot(low_probs[...], grad_mixed[m, :, head(h)], 1, 0))
        turn = dot(turned[m, h], grad_scores[...], 1, 0).T
        grad_qkv[m, :, head(h)] = low(turn * score_scale)

    def back_project(m, rows):
        grads = grad_qkv[m, rows]
        terms[m, rows] = low(dot(grads, wide[:, : 3 * pair], 1, 1))
        for j, part in enumerate((0, 2)):
            piece = grads[:, part * pair : (part + 1) * pair].astype(jnp.float32)
            bias_ref[j : j + 1] += jnp.sum(piece, axis=0, keepdims=True)

    def stacked(ref, cols=slice(None)):
        return ref[:, :, cols].reshape(micro * seq, -1)

    def weight_grads(hooks):
        def block(i):
            cols = step_rows(i, WIDE)
            front = dot(stacked(normed, cols), stacked(grad_qkv), 0, 0)
            back = dot(stacked(gathered, cols), stacked(mixed), 0, 0)
            total = low(jnp.concatenate([front, back], axis=1))
            pieces = [total[:, h * LANES : h * LANES + HEAD] for h in range(4 * heads)]
            grads_ref[cols] = jnp.concatenate(pieces, axis=1)

        stages(width // WIDE, block, hooks)

    def close(m):
        scatters[m].finish()
        for rows in scatters[m].blocks():
            grad_normed = scatters[m].total(rows)
            back, gain_terms = norm_back(
                rows_ref[m, rows].astype(jnp.float32), vec[0:1], grad_normed
            )
            out_ref[m, rows] = low(grad_ref[m, rows] + back)
            for j, item in enumerate((gain_terms, grad_normed)):
                small_ref[j : j + 1] += jnp.sum(item, axis=0, keepdims=True)

    def start_errand(k):
        pl.when(first_section)(errands[k][0].start)
        if both_ways:
            pl.when(~first_section)(errands[k][1].start)

    stages(
        2 * heads,
        find_all,
        {
            0: [gathers[0].forward, gathers[1].second],
            1: [gathers[1].forward, gathers[0].to_mate, lambda: start_errand(0)],
        },
    )
    gathers[0].finish()
    zero, one = scatters
    attend_hooks = {
        0: [gathers[1].to_mate],
        heads - 1: [gathers[1].finish],
        heads: [zero.second_hop, zero.first_hop, lambda: start_errand(1)],
    }
    project_hooks = {
        0: [zero.mate_far],
        1: [zero.far_hop, zero.mate_near],
        2: [one.mate_far],
        3: [one.far_hop, one.mate_near, lambda: close(0), one.second_hop],
    }

    def hooked(at, hooks):
        for k, steps in hooks.items():

            @pl.when(at == k)
            def _():
                for step in steps:
                    step()

    def image(m):
        mix_grads(m)

        def one_head(h):
            attend(m, h)
            hooked(m * heads + h, attend_hooks)

        repeat(heads, one_head)

        def one_chip(i):
            back_project(m, pl.ds(chip_rows(slab, i), 4 * half_rows))
            hooked(2 * m + i, project_hooks)

        repeat(2, one_chip)

    repeat(micro, image)
    for load in load_rest:
        load.wait()
    weight_grads({0: [one.first_hop]})
    close(1)

    for errand, _ in errands:
        pl.when(sends_errand)(errand.wait_send)
        pl.when(gets_errand)(errand.wait_recv)


def any_spec():
    return pl.BlockSpec(memory_space=pl.ANY)


def vmem_spec():
    return pl.BlockSpec(memory_space=pltpu.VMEM)


def shape_of(shape, dtype):
    return jax.ShapeDtypeStruct(shape, dtype)


def params(collective):
    return pltpu.CompilerParams(
        collective_id=collective, has_side_effects=True, vmem_limit_bytes=VMEM_BYTES
    )


def smem_spec():
    return pl.BlockSpec(memory_space=pltpu.SMEM)


def attn_forward(rows_low, vectors, bias, packed, at, layer, lengths, own_rows, given=None, grads=None):
    micro, half_rows, width = rows_low.shape
    seq = 8 * half_rows
    pair = bias.shape[2] // 3
    heads = pair // LANES
    low_type, high_type = jnp.bfloat16, jnp.float32
    hidden, lse, normed, qkv, mixed = pl.pallas_call(
        functools.partial(attn_forward_kernel, given is not None, at, layer, own_rows),
        out_shape=[
            shape_of((micro, half_rows, width), high_type),
            shape_of((micro, heads, seq, LANES), high_type),
            shape_of((micro, seq, width), low_type),
            shape_of((micro, seq, 3 * pair), low_type),
            shape_of((micro, seq, pair), low_type),
        ],
        in_specs=[vmem_spec()] * 3 + [smem_spec(), any_spec(), any_spec(), vmem_spec()],
        out_specs=[vmem_spec()] * 2 + [any_spec()] * 3,
        scratch_shapes=gather_scratch(micro, seq, width)
        + scatter_scratch(micro, seq, half_rows, width)
        + [
            pltpu.VMEM((width, 4 * heads * HEAD), low_type),
            pltpu.VMEM((width, 4 * pair), low_type),
            pltpu.VMEM((micro, seq, 3 * pair), low_type),
            pltpu.VMEM((micro, seq, pair), low_type),
            pltpu.SemaphoreType.DMA,
            pltpu.SemaphoreType.DMA((6,)),
            pltpu.SemaphoreType.DMA((micro,)),
            pltpu.VMEM((micro, seq if given is not None else 32, width), low_type),
            pltpu.SemaphoreType.DMA((micro, 3)),
            pltpu.SemaphoreType.DMA((micro, 3)),
        ],
        compiler_params=params(0 if given is None else 6),
        cost_estimate=COST,
        name="attn_forward",
    )(
        rows_low,
        vectors,
        bias,
        lengths,
        packed,
        packed if given is None else given,
        rows_low if grads is None else grads,
    )
    if given is None:
        return hidden, (normed, qkv, lse, mixed)
    return hidden, (given, qkv, lse, mixed), normed


def ffn_forward(hidden, vectors, up_biases, packed, at, layer, half_ff):
    micro, half_rows, width = hidden.shape
    seq = 8 * half_rows
    ff = up_biases.shape[2]
    packed_cols = 2 * ff - LANES
    low_type, high_type = jnp.bfloat16, jnp.float32
    out, second, upper = pl.pallas_call(
        functools.partial(ffn_forward_kernel, half_ff, at, layer),
        out_shape=[
            shape_of((micro, half_rows, width), low_type),
            shape_of((micro, seq, width), low_type),
            shape_of((micro, seq, ff), high_type),
        ],
        in_specs=[vmem_spec()] * 3 + [any_spec()],
        out_specs=[vmem_spec()] + [any_spec()] * 2,
        scratch_shapes=gather_scratch(micro, seq, width)
        + scatter_scratch(micro, seq, half_rows, width)
        + [
            pltpu.VMEM((width, packed_cols), low_type),
            pltpu.VMEM((width, 2 * LANES), low_type),
            pltpu.VMEM((micro, seq, ff), high_type),
            pltpu.SemaphoreType.DMA,
            pltpu.SemaphoreType.DMA((4,)),
        ],
        compiler_params=params(1),
        cost_estimate=COST,
        name="ffn_forward",
    )(hidden, vectors, up_biases, packed)
    return out, (second, upper)


def ffn_turn(hidden, grad_low, given, vectors, up_biases, packed, at, layer, half_ff):
    micro, half_rows, width = hidden.shape
    seq = 8 * half_rows
    ff = up_biases.shape[2]
    low_type, high_type = jnp.bfloat16, jnp.float32
    out, grad_hidden, grads, small, up_bias = pl.pallas_call(
        functools.partial(ffn_turn_kernel, half_ff, at, layer),
        out_shape=[
            shape_of((micro, half_rows, width), low_type),
            shape_of((micro, half_rows, width), high_type),
            shape_of((width, 2 * ff - LANES), low_type),
            shape_of((8, width), high_type),
            shape_of((8, ff), high_type),
        ],
        in_specs=[vmem_spec()] * 4 + [any_spec()] * 2,
        out_specs=[vmem_spec()] * 5,
        scratch_shapes=gather_scratch(micro, seq, width)
        + scatter_scratch(micro, seq, half_rows, width)
        + scatter_scratch(micro, seq, half_rows, width)
        + [
            pltpu.VMEM((width, 2 * ff - LANES), low_type),
            pltpu.VMEM((width, 2 * LANES), low_type),
            pltpu.VMEM((micro, seq, width), low_type),
            pltpu.VMEM((micro, seq, ff), low_type),
            pltpu.VMEM((micro, seq, ff), low_type),
            pltpu.SemaphoreType.DMA,
            pltpu.SemaphoreType.DMA((micro,)),
        ],
        compiler_params=params(7),
        cost_estimate=COST,
        name="ffn_turn",
    )(hidden, grad_low, vectors, up_biases, given, packed)
    return out, grad_hidden, grads, small, up_bias


def ffn_backward(grad_low, hidden, kept, vectors, packed, at, layer, half_ff):
    second, upper = kept
    micro, half_rows, width = hidden.shape
    seq, ff = upper.shape[1:]
    low_type, high_type = jnp.bfloat16, jnp.float32
    grad_hidden, grads, small, up_bias = pl.pallas_call(
        functools.partial(ffn_backward_kernel, half_ff, at, layer),
        out_shape=[
            shape_of((micro, half_rows, width), high_type),
            shape_of((width, 2 * ff - LANES), low_type),
            shape_of((8, width), high_type),
            shape_of((8, ff), high_type),
        ],
        in_specs=[vmem_spec()] * 3 + [any_spec()] * 3,
        out_specs=[vmem_spec()] * 4,
        scratch_shapes=gather_scratch(micro, seq, width)
        + scatter_scratch(micro, seq, half_rows, width)
        + [
            pltpu.VMEM((width, 2 * ff - LANES), low_type),
            pltpu.VMEM((width, 2 * LANES), low_type),
            pltpu.VMEM((micro, seq, width), low_type),
            pltpu.VMEM((micro, seq, ff), high_type),
            pltpu.VMEM((micro, seq, ff), low_type),
            pltpu.VMEM((micro, seq, ff), low_type),
            pltpu.SemaphoreType.DMA((1 + 2 * micro,)),
        ],
        compiler_params=params(2),
        cost_estimate=COST,
        name="ffn_backward",
    )(grad_low, hidden, vectors, second, upper, packed)
    return grad_hidden, grads, small, up_bias


def attn_backward(
    grad_hidden, rows_low, kept, vectors, packed, at, layer, lengths, own_rows, errand, both_ways
):
    normed, qkv, lse, mixed = kept
    micro, half_rows, width = grad_hidden.shape
    seq, pair = mixed.shape[1:]
    heads = pair // LANES
    low_type, high_type = jnp.bfloat16, jnp.float32
    out, grads, small, bias, got = pl.pallas_call(
        functools.partial(attn_backward_kernel, at, layer, own_rows, both_ways),
        out_shape=[
            shape_of((micro, half_rows, width), low_type),
            shape_of((width, 4 * heads * HEAD), low_type),
            shape_of((8, width), high_type),
            shape_of((8, pair), high_type),
            shape_of(errand[0].shape, errand[0].dtype),
        ],
        in_specs=[vmem_spec()] * 4 + [smem_spec()] + [any_spec()] * 6,
        out_specs=[vmem_spec()] * 4 + [any_spec()],
        scratch_shapes=gather_scratch(micro, seq, width)
        + scatter_scratch(micro, seq, half_rows, width)
        + [
            pltpu.VMEM((width, 4 * heads * HEAD), low_type),
            pltpu.VMEM((width, 4 * pair), low_type),
            pltpu.VMEM((micro, seq, width), low_type),
            pltpu.VMEM((micro, seq, 3 * pair), low_type),
            pltpu.VMEM((micro, seq, pair), low_type),
            pltpu.VMEM((micro, seq, pair), low_type),
            pltpu.VMEM((micro, seq, 3 * pair), low_type),
            pltpu.VMEM((micro, heads, LANES, seq), low_type),
            pltpu.VMEM((micro, seq, LANES), high_type),
            pltpu.VMEM((seq, seq), low_type),
            pltpu.VMEM((seq, seq), low_type),
            pltpu.VMEM((micro, heads, seq, seq), high_type),
            pltpu.SemaphoreType.DMA((2, 2)),
            pltpu.SemaphoreType.DMA((1 + 3 * micro,)),
        ],
        compiler_params=params(3 + 5 * layer),
        cost_estimate=COST,
        name="attn_backward",
    )(grad_hidden, rows_low, vectors, lse, lengths, normed, qkv, mixed, packed, *errand)
    return out, grads, small, bias, got


def slab_peers():
    section, tensor = lax.axis_index("section"), lax.axis_index("tensor")
    peers = []
    for role in range(1, 8):
        far, step = role // 4, role % 4
        other = section + far * (1 - 2 * section)
        to = (other, lax.rem(tensor + step, 4))
        source = (other, lax.rem(tensor + 4 - step, 4))
        peers.append((role, to, source))
    return peers


def column_peers(count):
    here = lax.axis_index("dp")
    return [
        (step, lax.rem(here + step, count), lax.rem(here + count - step, count))
        for step in range(1, count)
    ]


def greet_all(count):
    barrier = pltpu.get_barrier_semaphore()
    for _, to, _ in slab_peers():
        pl.semaphore_signal(barrier, inc=1, device_id=named(to), device_id_type=MESH)
    for _, to, _ in column_peers(count):
        pl.semaphore_signal(barrier, inc=1, device_id={"dp": to}, device_id_type=MESH)
    pl.semaphore_wait(barrier, 7 + count - 1)


def remote(src, dst, send_sem, recv_sem, peer):
    return pltpu.make_async_remote_copy(
        src_ref=src,
        dst_ref=dst,
        send_sem=send_sem,
        recv_sem=recv_sem,
        device_id=peer,
        device_id_type=MESH,
    )


def prologue_kernel(
    count, heads, qkv_ref, out_ref_in, up_ref_in, down_ref_t, gains_ref, shifts_ref, up_bias, rows_ref,
    first_hbm, normed_hbm, attn_ref, ff_zero_hbm, ff_one_hbm, out_ref, up_ref, bias_ref,
    attn_parts, ff_parts, up_halves, mine_ref, all_rows, line, ff_line, column, slab, up_got,
    rows_send, rows_recv, column_send, column_recv, slab_send, slab_recv, swap_send, swap_recv,
    right_send, right_recv, left_send, left_recv, out_sems,
):
    section, tensor, here = (lax.axis_index(name) for name in ("section", "tensor", "dp"))
    width = out_ref.shape[2]
    chunk = width // (4 * count)
    rows = attn_parts.shape[1]
    micro, own_rows = rows_ref.shape[:2]
    pieces = swap_send.shape[0] - 2
    size = rows // pieces
    other = {"section": 1 - section}
    pair = heads * LANES
    pair_cols = heads * HEAD
    half_ff = up_ref_in.shape[1] // 2
    main = half_ff // LANES * LANES
    extra = half_ff - main
    greet_all(count)
    out_turned = low(out_ref_in[...].astype(jnp.float32).T)
    for half in range(2):
        span = slice(half * pair_cols, (half + 1) * pair_cols)
        parts = [qkv_ref[k, :, span] for k in range(3)] + [out_turned[:, span]]
        attn_parts[half] = jnp.concatenate(parts, axis=1)
    keep_slot = jnp.where(section == 0, here, count)
    send_slot = jnp.where(section == 0, here, count)
    got_slot = jnp.where(section == 0, count, here)
    sent = []
    for p in range(pieces):
        span = pl.ds(p * size, size)
        copy = remote(
            attn_parts.at[1 - section, span],
            line.at[send_slot, span],
            swap_send.at[p],
            swap_recv.at[p],
            other,
        )
        copy.start()
        sent.append(copy)
    line[keep_slot] = attn_parts[section]
    mine_ref[...] = jnp.zeros_like(mine_ref)
    gains = gains_ref.shape[0]
    mine_ref[:gains, :chunk] = gains_ref[...]
    for i in range(shifts_ref.shape[0]):
        mine_ref[gains + i : gains + i + 1, :chunk] = shifts_ref[i]
    column[here] = mine_ref[...]
    for step, to, _ in column_peers(count):
        copy = remote(
            mine_ref, column.at[here], column_send.at[step], column_recv.at[step], {"dp": to}
        )
        copy.start()
        sent.append(copy)

    def swapped(p):
        got = line.at[got_slot, pl.ds(p * size, size)]
        remote(got, got, swap_send.at[p], swap_recv.at[p], other).wait_recv()

    def hop(step, p, way, finish=False):
        origin = here - way * step
        sends, recvs = (right_send, right_recv) if way == 1 else (left_send, left_recv)
        inside = (origin >= 0) if way == 1 else (origin < count)
        onward = (here + 1 < count) if way == 1 else (here > 0)
        slot = line.at[jnp.clip(origin, 0, count - 1), pl.ds(p * size, size)]
        target = jnp.clip(here + way, 0, count - 1)
        if step > 0 and not finish:

            @pl.when(inside)
            def _():
                remote(slot, slot, sends.at[step, p], recvs.at[step, p], {"dp": target}).wait_recv()

        if step + 1 < count:

            @pl.when(inside & onward)
            def _():
                copy = remote(
                    slot, slot, sends.at[step, p], recvs.at[step + 1, p], {"dp": target}
                )
                if finish:
                    copy.wait_send()
                else:
                    copy.start()

    def hops(step):
        for p in range(pieces):
            for way in (1, -1):
                hop(step, p, way)

    for step, _, source in column_peers(count):
        slot = column.at[source]
        remote(slot, slot, column_send.at[step], column_recv.at[step], {"dp": source}).wait_recv()
    for role, to, _ in slab_peers():
        copy = remote(
            column, slab.at[section, tensor], slab_send.at[role], slab_recv.at[role], named(to)
        )
        copy.start()
        sent.append(copy)
    slab[section, tensor] = column[...]

    def set_out(p):
        pl.when(section == 1)(lambda: swapped(p))
        for way in (1, -1):
            hop(0, p, way)

    set_out(0)
    for role, _, source in slab_peers():
        slot = slab.at[source[0], source[1]]
        remote(slot, slot, slab_send.at[role], slab_recv.at[role], named(source)).wait_recv()
    for layer in range(2):
        for part in range(4 * count):
            piece = slab[layer, part % 4, part // 4]
            out_ref[layer, :, part * chunk : (part + 1) * chunk] = piece[:, :chunk]
    tiles = TileGather(all_rows, rows_send, rows_recv)
    for m in range(micro):
        own = tiles.tile(m, tensor)
        for begin in range(0, own_rows, 32):
            end = min(begin + 32, own_rows)
            block = rows_ref[m, begin:end].astype(jnp.float32)
            own[begin:end] = low(layer_norm(block, out_ref[0, 0:1], out_ref[0, 2:3]))
        own[own_rows:] = jnp.zeros((tiles.tile_rows - own_rows, width), jnp.bfloat16)
        tiles.start(m)
    for p in range(1, pieces):
        set_out(p)
    blank = jnp.zeros((rows, LANES - 2 * extra), jnp.bfloat16)
    up_halves[...] = jnp.zeros_like(up_halves)
    for half in range(2):
        start = half * half_ff
        up_halves[half, :, :half_ff] = up_bias[:, start : start + half_ff]
        ff_parts[half, :, :main] = up_ref_in[:, start : start + main]
        ff_parts[half, :, main : 2 * main] = down_ref_t[:, start : start + main]
        span = slice(start + main, start + half_ff)
        ff_parts[half, :, 2 * main :] = jnp.concatenate(
            [up_ref_in[:, span], down_ref_t[:, span], blank], axis=1
        )
    ff_swap = remote(
        ff_parts.at[1 - section],
        ff_line.at[section],
        swap_send.at[pieces],
        swap_recv.at[pieces],
        other,
    )
    up_swap = remote(
        up_halves.at[1 - section],
        up_got.at[section],
        swap_send.at[pieces + 1],
        swap_recv.at[pieces + 1],
        other,
    )
    up_swap.start()
    ff_swap.start()
    hops(1)
    start = (2 * tensor + section) * pair_cols
    for layer in range(2):
        turned = pltpu.roll(out_ref[layer], lax.rem(width - start, width), 1)
        empty = jnp.zeros((1, LANES - HEAD), jnp.float32)
        for part, row in ((0, 3), (2, 4)):
            for h in range(heads):
                at = part * pair + h * LANES
                piece = turned[row : row + 1, h * HEAD : (h + 1) * HEAD]
                bias_ref[layer, :, at : at + LANES] = jnp.concatenate([piece, empty], 1)
        bias_ref[layer, :, pair : 2 * pair] = jnp.zeros((1, pair), jnp.float32)
    up_ref[section] = up_halves[section]
    outs = []

    def put(src, dst, i):
        copy = pltpu.make_async_copy(src, dst, out_sems.at[i])
        copy.start()
        outs.append(copy)

    def put_ff(src, section_of_first, i):
        for layer, dst in enumerate((ff_zero_hbm, ff_one_hbm)):
            here_too = layer if section_of_first == 0 else 1 - layer

            @pl.when(section == here_too)
            def _():
                pltpu.make_async_copy(src, dst, out_sems.at[i]).start()

        outs.append(pltpu.make_async_copy(src, ff_zero_hbm, out_sems.at[i]))

    put_ff(ff_parts.at[section], 0, count)
    for step in range(2, count):
        hops(step)
        if step == 2:
            tiles.pass_on()
    if count <= 2:
        tiles.pass_on()
    for p in range(pieces):

        @pl.when(section == 0)
        def _():
            swapped(p)

    for at in range(count):
        put(line.at[at], first_hbm.at[pl.ds(at * rows, rows)], at)
    attn_ref[...] = line[count]
    got = up_got.at[1 - section]
    remote(got, got, swap_send.at[pieces + 1], swap_recv.at[pieces + 1], other).wait_recv()
    up_ref[1 - section] = up_got[1 - section]
    tiles.finish()
    put(all_rows, normed_hbm, count + 2)
    ff_got = ff_line.at[1 - section]
    remote(ff_got, ff_got, swap_send.at[pieces], swap_recv.at[pieces], other).wait_recv()
    put_ff(ff_got, 1, count + 1)
    for step in range(count):
        for p in range(pieces):
            for way in (1, -1):
                hop(step, p, way, True)
    for copy in sent + [ff_swap, up_swap]:
        copy.wait_send()
    tiles.drain()
    for copy in outs:
        copy.wait()


def prologue(qkv, out, up, down_t, gains, shifts, up_bias, rows_low, count, heads, tile_rows):
    part_rows = qkv.shape[1]
    micro, _, width = rows_low.shape
    vector_rows = gains.shape[0] + shifts.shape[0]
    half_ff = up.shape[1] // 2
    ff_wide = round_up(half_ff, LANES)
    attn_shape = (part_rows, 4 * heads * HEAD)
    ff_shape = (2, part_rows, 2 * ff_wide - LANES)
    all_rows = (micro, 4 * tile_rows, width)
    pieces = 3 if part_rows % 96 == 0 else 1
    low_type, high_type = jnp.bfloat16, jnp.float32
    dma = pltpu.SemaphoreType.DMA
    return pl.pallas_call(
        functools.partial(prologue_kernel, count, heads),
        out_shape=[
            shape_of((count * part_rows, attn_shape[1]), low_type),
            shape_of(all_rows, low_type),
            shape_of(attn_shape, low_type),
            shape_of(ff_shape[1:], low_type),
            shape_of(ff_shape[1:], low_type),
            shape_of((2, vector_rows, width), high_type),
            shape_of((2, 1, ff_wide), high_type),
            shape_of((2, 1, 3 * heads * LANES), high_type),
        ],
        in_specs=[vmem_spec()] * 8,
        out_specs=[any_spec()] * 2 + [vmem_spec()] + [any_spec()] * 2 + [vmem_spec()] * 3,
        scratch_shapes=[
            pltpu.VMEM((2,) + attn_shape, low_type),
            pltpu.VMEM(ff_shape, low_type),
            pltpu.VMEM((2, 1, ff_wide), high_type),
            pltpu.VMEM((vector_rows, LANES), high_type),
            pltpu.VMEM(all_rows, low_type),
            pltpu.VMEM((count + 1,) + attn_shape, low_type),
            pltpu.VMEM(ff_shape, low_type),
            pltpu.VMEM((count, vector_rows, LANES), high_type),
            pltpu.VMEM((2, 4, count, vector_rows, LANES), high_type),
            pltpu.VMEM((2, 1, ff_wide), high_type),
            dma((micro, 3)),
            dma((micro, 3)),
            dma((count,)),
            dma((count,)),
            dma((8,)),
            dma((8,)),
            dma((pieces + 2,)),
            dma((pieces + 2,)),
            dma((count, pieces)),
            dma((count, pieces)),
            dma((count, pieces)),
            dma((count, pieces)),
            dma((count + 3,)),
        ],
        compiler_params=params(4),
        cost_estimate=COST,
        name="prologue",
    )(qkv, out, up, down_t, gains, shifts, up_bias, rows_low)


def home_kernel(
    count, chunk, attn_zero, attn_one, ff_zero, ff_one, bias_zero, bias_one, up_zero, up_one,
    ff_sum_hbm, attn_sum_hbm, rows_zero_hbm, rows_one_hbm,
    out_ref, up_ref, ff_got_hbm, attn_got_hbm, rows_got_hbm,
    parts, ups, slab, column, up_pair, up_column, total,
    column_send, column_recv, slab_send, slab_recv, up_sems, up_column_send, up_column_recv, far_send, far_recv,
):
    section, tensor, here = (lax.axis_index(name) for name in ("section", "tensor", "dp"))
    width = attn_zero.shape[1]
    heads = bias_zero.shape[1] // LANES
    biases_in, ups_in = (bias_zero, bias_one), (up_zero, up_one)
    other = {"section": 1 - section}
    greet_all(count)
    parts[...] = jnp.zeros_like(parts)
    start = (2 * tensor + section) * (heads * HEAD)
    for layer, (attn, ff) in enumerate(((attn_zero, ff_zero), (attn_one, ff_one))):
        bias = biases_in[layer][...]
        blank = jnp.zeros((8, width - heads * HEAD), jnp.float32)
        pieces = [bias[:, h * LANES : h * LANES + HEAD] for h in range(heads)]
        placed = pltpu.roll(jnp.concatenate(pieces + [blank], 1), start, 1)
        whole = jnp.concatenate(
            [attn[0:1], ff[0:1], attn[1:2], placed[0:2], ff[3:4], ff[1:2], ff[2:3]], axis=0
        )
        for part in range(4 * count):
            piece = whole[:, part * chunk : (part + 1) * chunk]
            parts[layer, part % 4, part // 4, :, :chunk] = piece
        ups[layer] = ups_in[layer][0:1]
    sent = []

    def send(src, dst, send_sem, recv_sem, peer):
        copy = remote(src, dst, send_sem, recv_sem, peer)
        copy.start()
        sent.append(copy)

    send(ups.at[1 - section], up_pair.at[section], up_sems.at[0], up_sems.at[1], other)
    for role, to, _ in slab_peers():
        send(
            parts.at[to[0], to[1]], slab.at[role], slab_send.at[role], slab_recv.at[role], named(to)
        )
    far_rows = remote(rows_zero_hbm, rows_got_hbm, far_send.at[0], far_recv.at[0], other)
    far_rows_one = remote(rows_one_hbm, rows_got_hbm, far_send.at[0], far_recv.at[0], other)
    far_ff = remote(ff_sum_hbm, ff_got_hbm, far_send.at[1], far_recv.at[1], other)
    far_attn = remote(attn_sum_hbm, attn_got_hbm, far_send.at[2], far_recv.at[2], other)
    one_way = ((far_ff, 1), (far_attn, 0))
    pl.when(section == 1)(far_rows.start)
    pl.when(section == 0)(far_rows_one.start)
    for copy, source in one_way:
        pl.when(section == source)(copy.start)
    up_pair[section] = ups[section]
    value = parts[section, tensor]
    for role, _, source in slab_peers():
        slot = slab.at[role]
        remote(slot, slot, slab_send.at[role], slab_recv.at[role], named(source)).wait_recv()
        value = value + slab[role]
    total[...] = value
    for step, to, _ in column_peers(count):
        send(total.at[to], column.at[step], column_send.at[step], column_recv.at[step], {"dp": to})
    got = up_pair.at[1 - section]
    remote(got, got, up_sems.at[0], up_sems.at[1], other).wait_recv()
    for step, to, _ in column_peers(count):
        send(
            up_pair, up_column.at[here], up_column_send.at[step], up_column_recv.at[step], {"dp": to}
        )
    up_column[here] = up_pair[...]
    result = total[here]
    for step, _, source in column_peers(count):
        slot = column.at[step]
        remote(slot, slot, column_send.at[step], column_recv.at[step], {"dp": source}).wait_recv()
        result = result + column[step]
    out_ref[...] = result
    for step, _, source in column_peers(count):
        slot = up_column.at[source]
        remote(
            slot, slot, up_column_send.at[step], up_column_recv.at[step], {"dp": source}
        ).wait_recv()
    value = up_column[0]
    for at in range(1, count):
        value = value + up_column[at]
    up_ref[...] = value
    far_rows.wait()
    for copy, source in one_way:
        pl.when(section == source)(copy.wait_send)
        pl.when(section != source)(copy.wait_recv)
    for copy in sent:
        copy.wait_send()


def home(attn_small, ff_small, bias_grads, up_grads, ff_sum, attn_sum, rows, count, chunk):
    vector_rows, lanes = 8, LANES
    up_shape = (1, up_grads[0].shape[1])
    dma = pltpu.SemaphoreType.DMA
    high_type = jnp.float32
    return pl.pallas_call(
        functools.partial(home_kernel, count, chunk),
        out_shape=[
            shape_of((vector_rows, lanes), high_type),
            shape_of((2,) + up_shape, high_type),
            shape_of(ff_sum.shape, ff_sum.dtype),
            shape_of(attn_sum.shape, attn_sum.dtype),
            shape_of(rows[0].shape, rows[0].dtype),
        ],
        in_specs=[vmem_spec()] * 8 + [any_spec()] * 4,
        out_specs=[vmem_spec()] * 2 + [any_spec()] * 3,
        scratch_shapes=[
            pltpu.VMEM((2, 4, count, vector_rows, lanes), high_type),
            pltpu.VMEM((2,) + up_shape, high_type),
            pltpu.VMEM((8, count, vector_rows, lanes), high_type),
            pltpu.VMEM((count, vector_rows, lanes), high_type),
            pltpu.VMEM((2,) + up_shape, high_type),
            pltpu.VMEM((count, 2) + up_shape, high_type),
            pltpu.VMEM((count, vector_rows, lanes), high_type),
            dma((count,)),
            dma((count,)),
            dma((8,)),
            dma((8,)),
            dma((2,)),
            dma((count,)),
            dma((count,)),
            dma((3,)),
            dma((3,)),
        ],
        compiler_params=params(5),
        cost_estimate=COST,
        name="home",
    )(*attn_small, *ff_small, *bias_grads, *up_grads, ff_sum, attn_sum, *rows)


def ff_finish_kernel(zero, one, zero_got, one_got, up_ref, down_ref):
    first = lax.axis_index("section") == 0
    halves = (
        jnp.where(first, zero[...], one_got[...]),
        jnp.where(first, zero_got[...], one[...]),
    )
    half_ff = up_ref.shape[1] // 2
    main = half_ff // LANES * LANES
    extra = half_ff - main
    for k in range(2):
        pieces = []
        for half in halves:
            start = 2 * main + k * extra
            pieces += [half[:, k * main : (k + 1) * main], half[:, start : start + extra]]
        whole = jnp.concatenate(pieces, axis=1).astype(jnp.float32)
        (up_ref, down_ref)[k][...] = whole


def ff_finish(sums, got, ff_cols):
    rows = sums[0].shape[0]
    return pl.pallas_call(
        ff_finish_kernel,
        out_shape=[
            shape_of((rows, ff_cols), jnp.float32),
            shape_of((rows, ff_cols), jnp.float32),
        ],
        in_specs=[vmem_spec()] * 4,
        out_specs=[vmem_spec()] * 2,
        compiler_params=pltpu.CompilerParams(vmem_limit_bytes=VMEM_BYTES),
        cost_estimate=COST,
        name="ff_finish",
    )(*sums, *got)


def attn_finish_kernel(zero, one, zero_got, one_got, qkv_ref, out_ref):
    first = lax.axis_index("section") == 0
    halves = (
        jnp.where(first, zero[...], one_got[...]),
        jnp.where(first, zero_got[...], one[...]),
    )
    pair_cols = qkv_ref.shape[2] // 2
    for k in range(4):
        span = slice(k * pair_cols, (k + 1) * pair_cols)
        whole = jnp.concatenate([half[:, span] for half in halves], axis=1).astype(jnp.float32)
        if k < 3:
            qkv_ref[k] = whole
        else:
            out_ref[...] = whole.T


def attn_finish(sums, got, head_cols):
    rows = sums[0].shape[0]
    return pl.pallas_call(
        attn_finish_kernel,
        out_shape=[
            shape_of((3, rows, head_cols), jnp.float32),
            shape_of((head_cols, rows), jnp.float32),
        ],
        in_specs=[vmem_spec()] * 4,
        out_specs=[vmem_spec()] * 2,
        compiler_params=pltpu.CompilerParams(vmem_limit_bytes=VMEM_BYTES),
        name="attn_finish",
    )(*sums, *got)


def shards(
    section_input,
    final_cotangent,
    lengths,
    qkv_weight,
    out_weight,
    up_weight,
    down_weight,
    norm_gains,
    biases,
    up_bias,
):
    here = lax.axis_index("section")
    sections = lax.axis_size("section")
    micro, _, own_rows, _ = section_input.shape
    head_cols = qkv_weight.shape[3]
    pair_cols = head_cols // sections
    heads = pair_cols // HEAD
    ff_cols = up_weight.shape[2]
    half_ff = ff_cols // sections
    half_rows = round_up(-(-own_rows // sections), 32)
    full_rows = half_rows * sections

    def by_layer(mine, other):
        return [jnp.where(here == 0, mine, other), jnp.where(here == 0, other, mine)]

    count = lax.axis_size("dp")
    chunk = norm_gains.shape[2]
    first, normed, attn_part, ff_zero, ff_one, vectors, up_biases, bias_qv = prologue(
        qkv_weight[0],
        out_weight[0],
        up_weight[0],
        down_weight[0].T,
        norm_gains[0],
        biases.transpose(1, 0, 2),
        up_bias,
        section_input[:, 0],
        count,
        heads,
        full_rows,
    )

    def gather_column(part):
        return lax.all_gather(part, "dp", axis=0, tiled=True)

    ff_first = gather_column(ff_zero)
    attn_packed = [(first, 0), (gather_column(attn_part), 0)]
    ff_packed = [(ff_first, 0), (gather_column(ff_one), 0)]
    lengths_here = lengths.reshape(micro)

    def my_rows(value):
        padded = jnp.pad(value[:, 0], [(0, 0), (0, full_rows - own_rows), (0, 0)])
        return lax.dynamic_slice_in_dim(padded, here * half_rows, half_rows, 1)

    def whole_rows(first, second, got):
        low_half, high_half = by_layer(jnp.where(here == 0, first, second), got)
        return jnp.concatenate([low_half, high_half], 1)[:, None, :own_rows]

    rows = my_rows(section_input)
    inputs, hiddens, attn_kept = [], [], []
    for layer in range(2):
        inputs.append(rows)
        operands = (rows, vectors, bias_qv, *attn_packed[layer], layer, lengths_here, own_rows)
        if layer == 0:
            hidden, kept, grads_all = attn_forward(*operands, normed, final_cotangent[:, 0])
        else:
            hidden, kept = attn_forward(*operands)
        hiddens.append(hidden)
        attn_kept.append(kept)
        if layer == 0:
            rows, ff_kept = ffn_forward(hidden, vectors, up_biases, *ff_packed[0], 0, half_ff)

    attn_sums, ff_sums, up_sums, input_grads = {}, {}, {}, {}
    attn_small, ff_small, bias_grads, errands = {}, {}, {}, {}
    for layer in (1, 0):
        if layer == 1:
            last, grad_hidden, ff_grad, ff_small[1], up_sums[1] = ffn_turn(
                hiddens[1],
                my_rows(final_cotangent),
                grads_all,
                vectors,
                up_biases,
                *ff_packed[1],
                1,
                half_ff,
            )
        else:
            grad_hidden, ff_grad, ff_small[0], up_sums[0] = ffn_backward(
                grads, hiddens[0], ff_kept, vectors, *ff_packed[0], 0, half_ff
            )
        ff_sums[layer] = lax.psum_scatter(ff_grad, "dp", scatter_dimension=0, tiled=True)
        if layer == 1:
            errand, both_ways = (last, rows), True
        else:
            errand, both_ways = (ff_sums[1], ff_sums[1]), False
        grads, attn_grad, attn_small[layer], bias_grads[layer], got = attn_backward(
            grad_hidden,
            inputs[layer],
            attn_kept[layer],
            vectors,
            *attn_packed[layer],
            layer,
            lengths_here,
            own_rows,
            errand,
            both_ways,
        )
        errands[layer] = got
        attn_sums[layer] = lax.psum_scatter(attn_grad, "dp", scatter_dimension=0, tiled=True)
        input_grads[layer] = grads

    small_mine, up_total, ff_got, attn_got, rows_got = home(
        [attn_small[0], attn_small[1]],
        [ff_small[0], ff_small[1]],
        [bias_grads[0], bias_grads[1]],
        [up_sums[0], up_sums[1]],
        ff_sums[0],
        attn_sums[1],
        [input_grads[0], input_grads[1]],
        count,
        chunk,
    )
    attn_zero_got = lax.ppermute(attn_sums[0], "section", [(1, 0)])
    up_grad, down_grad = ff_finish([ff_sums[0], ff_sums[1]], [ff_got, errands[0]], ff_cols)
    small_mine, up_total, rows_got, out_got, up_grad = lax.optimization_barrier(
        (small_mine, up_total, rows_got, errands[1], up_grad)
    )
    section_output = whole_rows(rows, last, out_got)
    small_mine = small_mine[None, :, :chunk]
    up_total = up_total[:, :, :half_ff].reshape(1, ff_cols)
    input_grad = whole_rows(input_grads[0], input_grads[1], rows_got)

    qkv_total, out_total = attn_finish(
        [attn_sums[0], attn_sums[1]], [attn_zero_got, attn_got], head_cols
    )
    gains = norm_gains.shape[1]
    return (
        section_output[None],
        input_grad[None],
        qkv_total[None],
        out_total[None],
        up_grad[None],
        down_grad.T[None],
        small_mine[:, :gains],
        small_mine[:, gains:],
        up_total,
    )


def solution(mesh):
    in_specs = (
        P(None, "dp", "tensor", None),
        P(None, "dp", "tensor", None),
        P(None, "dp"),
        P("section", None, "dp", "tensor"),
        P("section", "tensor", "dp"),
        P("section", "dp", "tensor"),
        P("section", "tensor", "dp"),
        P("section", None, ("dp", "tensor")),
        P("section", None, ("dp", "tensor")),
        P("section", "tensor"),
    )
    out_specs = (
        P("section", None, "dp", "tensor", None),
        P("section", None, "dp", "tensor", None),
        P("section", None, "dp", "tensor"),
        P("section", "tensor", "dp"),
        P("section", "dp", "tensor"),
        P("section", "tensor", "dp"),
        P("section", None, ("dp", "tensor")),
        P("section", None, ("dp", "tensor")),
        P("section", "tensor"),
    )
    return jax.shard_map(shards, mesh=mesh, in_specs=in_specs, out_specs=out_specs, check_vma=False)
```

```python
import functools
import math

import jax
import jax.numpy as jnp
from jax import lax
from jax.experimental import pallas as pl
from jax.experimental.pallas import tpu as pltpu
from jax.sharding import PartitionSpec as P


HEAD = 72
LANES = 128
norm_eps = 1e-06
masked_score = -1000000000.0
score_scale = 1.0 / math.sqrt(HEAD)
GELU_A = math.sqrt(2.0 / math.pi)
GELU_B = 0.044715


def round_up(value, step):
    return -(-value // step) * step


def dot(left, right, left_dim, right_dim):
    return lax.dot_general(
        left, right, (((left_dim,), (right_dim,)), ((), ())), preferred_element_type=jnp.float32
    )


def low(value):
    return value.astype(jnp.bfloat16)


def layer_norm(rows, gain_vec, shift_vec):
    centred = rows - jnp.mean(rows, axis=-1, keepdims=True)
    spread = jnp.mean(centred * centred, axis=-1, keepdims=True)
    return centred * lax.rsqrt(spread + norm_eps) * gain_vec + shift_vec


def norm_back(rows, gain_vec, grads):
    centred = rows - jnp.mean(rows, axis=-1, keepdims=True)
    spread = jnp.mean(centred * centred, axis=-1, keepdims=True)
    inverse = lax.rsqrt(spread + norm_eps)
    xhat = centred * inverse
    e = grads * gain_vec
    back = inverse * (
        e
        - jnp.mean(e, axis=-1, keepdims=True)
        - xhat * jnp.mean(e * xhat, axis=-1, keepdims=True)
    )
    return back, grads * xhat


def gelu_tanh(value):
    return jax.nn.gelu(value, approximate=True)


MESH = pl.DeviceIdType.MESH
VMEM_BYTES = 64_000_000
COST = pl.CostEstimate(flops=20_000_000_000, transcendentals=0, bytes_accessed=100_000_000)
LOG2E = 1.0 / math.log(2.0)
TILE = 256
WIDE = 384


class Slab:
    def __init__(self, half_rows):
        self.half_rows = half_rows
        section = lax.axis_index("section")
        tensor = lax.axis_index("tensor")
        core = lax.rem(tensor, 2)
        self.core = core
        self.mine = self.around(section, tensor, core)
        self.theirs = self.around(section, tensor + 1 - 2 * core, 1 - core)
        self.far_role, self.near_role = 1 + core, 2 - core
        self.mate = self.theirs[0]
        over = lax.rem(tensor + 2, 4)
        self.near, self.far = tensor, over
        self.mate_near, self.mate_far = self.mate[1], lax.rem(self.mate[1] + 2, 4)
        self.grid = self.places(section, self.near, self.far)
        self.mate_grid = self.places(section, self.mate_near, self.mate_far)
        self.across_y = self.grid[2]
        self.first, self.second = self.mine[1], self.mine[2]

    def place(self, section, tensor):
        start = (2 * tensor + section) * self.half_rows
        return (section, tensor, pl.multiple_of(start, self.half_rows))

    def places(self, section, near, far):
        flip = 1 - section
        return [self.place(*at) for at in ((section, near), (flip, near), (section, far), (flip, far))]

    def around(self, section, tensor, core):
        over = lax.rem(tensor + 2, 4)
        turn = 1 - 2 * section
        first = (section + (1 - core) * turn, tensor + core * (over - tensor))
        second = (section + core * turn, tensor + (1 - core) * (over - tensor))
        places = ((section, tensor), first, second, (1 - section, over))
        return [self.place(*at) for at in places]

    def rows(self, ref, at):
        return ref.at[pl.ds(at[2], self.half_rows)]

    def greet(self):
        barrier = pltpu.get_barrier_semaphore()
        for peer in (self.first, self.second, self.mate):
            pl.semaphore_signal(barrier, inc=1, device_id=named(peer), device_id_type=MESH)
        pl.semaphore_wait(barrier, 3)


def named(at):
    return {"section": at[0], "tensor": at[1]}


class Moves:
    def __init__(self, slab, send_sems, recv_sems):
        self.slab, self.send_sems, self.recv_sems = slab, send_sems, recv_sems
        self.sent = []

    def copy(self, src, dst, role, peer):
        return pltpu.make_async_remote_copy(
            src_ref=src,
            dst_ref=dst,
            send_sem=self.send_sems.at[role],
            recv_sem=self.recv_sems.at[role],
            device_id=named(peer),
            device_id_type=MESH,
        )

    def send(self, ends, role, peer):
        self.copy(*ends(), role, peer).start()
        self.sent.append(lambda: self.copy(*ends(), role, peer))

    def arrived(self, dst, role):
        self.copy(dst, dst, role, self.slab.mate).wait_recv()

    def drain(self):
        for copy in self.sent:
            copy().wait_send()


class Gather(Moves):
    def __init__(self, slab, whole, send_sems, recv_sems):
        super().__init__(slab, send_sems, recv_sems)
        self.whole = whole

    def pass_on(self, at, role, peer):
        self.send(lambda: (self.slab.rows(self.whole, at),) * 2, role, peer)

    def arrive(self, at, role):
        self.arrived(self.slab.rows(self.whole, at), role)

    def start(self):
        mine = self.slab.mine
        self.pass_on(mine[0], 0, mine[1])
        self.pass_on(mine[0], 3, self.slab.mate)

    def second(self):
        self.sent.pop(0)().wait_send()
        self.pass_on(self.slab.mine[0], 1, self.slab.mine[2])

    def forward(self):
        mine, mate = self.slab.mine, self.slab.mate
        self.arrive(mine[1], 0)
        self.pass_on(mine[1], 2, mine[2])
        self.pass_on(mine[1], 4, mate)

    def to_mate(self):
        mine, mate = self.slab.mine, self.slab.mate
        self.arrive(mine[2], 1)
        self.pass_on(mine[2], 5, mate)
        self.arrive(mine[3], 2)
        self.pass_on(mine[3], 6, mate)

    def finish(self):
        for k in range(4):
            self.arrive(self.slab.theirs[k], 3 + k)
        self.drain()


class TileGather:
    def __init__(self, whole, send_sems, recv_sems):
        self.whole, self.send_sems, self.recv_sems = whole, send_sems, recv_sems
        self.tensor = lax.axis_index("tensor")
        self.over = lax.rem(self.tensor + 2, 4)
        self.mate = self.tensor + 1 - 2 * lax.rem(self.tensor, 2)
        self.micro, rows = whole.shape[0], whole.shape[1] // 4
        self.tile_rows = rows
        self.sent = []

    def tile(self, m, index):
        start = pl.multiple_of(index * self.tile_rows, self.tile_rows)
        return self.whole.at[m, pl.ds(start, self.tile_rows)]

    def copy(self, m, index, role, peer):
        part = self.tile(m, index)
        return remote(
            part, part, self.send_sems.at[m, role], self.recv_sems.at[m, role], {"tensor": peer}
        )

    def send(self, m, index, role, peer):
        self.copy(m, index, role, peer).start()
        self.sent.append(lambda: self.copy(m, index, role, peer))

    def start(self, m):
        self.send(m, self.tensor, 0, self.over)
        self.send(m, self.tensor, 1, self.mate)

    def pass_on(self):
        for m in range(self.micro):
            self.copy(m, self.over, 0, self.over).wait_recv()
            self.send(m, self.over, 2, self.mate)

    def finish(self):
        for m in range(self.micro):
            self.copy(m, self.mate, 1, self.mate).wait_recv()
            self.copy(m, lax.rem(self.mate + 2, 4), 2, self.mate).wait_recv()

    def drain(self):
        for copy in self.sent:
            copy().wait_send()


class Scatter(Moves):
    def __init__(self, slab, terms, from_mate, outgoing, arrivals, send_sems, recv_sems):
        super().__init__(slab, send_sems, recv_sems)
        self.terms, self.from_mate, self.outgoing = terms, from_mate, outgoing
        self.relay, self.from_second, self.from_first = (arrivals.at[k] for k in range(3))

    def to_mate(self, at, role):
        self.send(
            lambda: (self.slab.rows(self.terms, at), self.from_mate.at[role]), role, self.slab.mate
        )

    def mate_far(self):
        self.to_mate(self.slab.mate_grid[3], 3)
        self.to_mate(self.slab.mate_grid[2], self.slab.far_role)

    def mate_near(self):
        self.to_mate(self.slab.mate_grid[1], self.slab.near_role)
        self.to_mate(self.slab.mate_grid[0], 0)

    def chip_sum(self, k, rows):
        part = self.slab.rows(self.terms, self.slab.mine[k])
        return part[rows].astype(jnp.float32) + self.from_mate[k, rows].astype(jnp.float32)

    def blocks(self):
        return [pl.ds(start, 32) for start in range(0, self.slab.half_rows, 32)]

    def hop(self, k, slot, dst, role, peer, ride=None):
        self.arrived(self.from_mate.at[k], k)
        if ride is not None:
            self.arrived(ride, 4)
        for rows in self.blocks():
            value = self.chip_sum(k, rows)
            if ride is not None:
                value = value + ride[rows].astype(jnp.float32)
            self.outgoing[slot, rows] = low(value)
        self.send(lambda: (self.outgoing.at[slot], dst), role, peer)

    def far_hop(self):
        self.hop(3, 0, self.relay, 4, self.slab.second)

    def second_hop(self):
        self.hop(2, 1, self.from_second, 5, self.slab.second)

    def first_hop(self):
        self.hop(1, 2, self.from_first, 6, self.slab.first, self.relay)

    def finish(self):
        self.arrived(self.from_mate.at[0], 0)
        self.arrived(self.from_second, 5)
        self.arrived(self.from_first, 6)
        self.drain()

    def total(self, rows):
        other = self.from_second[rows].astype(jnp.float32) + self.from_first[rows].astype(
            jnp.float32
        )
        return self.chip_sum(0, rows) + other


def scatter_scratch(micro, seq, half_rows, width):
    return [
        pltpu.VMEM((micro, seq, width), jnp.bfloat16),
        pltpu.VMEM((micro, 4, half_rows, width), jnp.bfloat16),
        pltpu.VMEM((micro, 3, half_rows, width), jnp.bfloat16),
        pltpu.VMEM((micro, 3, half_rows, width), jnp.bfloat16),
        pltpu.SemaphoreType.DMA((micro, 7)),
        pltpu.SemaphoreType.DMA((micro, 7)),
    ]


def gather_scratch(micro, seq, width):
    return [
        pltpu.VMEM((micro, seq, width), jnp.bfloat16),
        pltpu.SemaphoreType.DMA((micro, 7)),
        pltpu.SemaphoreType.DMA((micro, 7)),
    ]


def make_scatters(slab, refs, micro):
    terms, from_mate, outgoing, arrivals, send_sems, recv_sems = refs
    return [
        Scatter(
            slab,
            terms.at[m],
            from_mate.at[m],
            outgoing.at[m],
            arrivals.at[m],
            send_sems.at[m],
            recv_sems.at[m],
        )
        for m in range(micro)
    ]


def make_gathers(slab, refs, micro):
    whole, send_sems, recv_sems = refs
    return [
        Gather(slab, whole.at[m], send_sems.at[m], recv_sems.at[m]) for m in range(micro)
    ]


def step_from(start, i, size):
    return pl.ds(pl.multiple_of(start + i * size, size), size)


def step_rows(i, size):
    return pl.ds(pl.multiple_of(i * size, size), size)


def repeat(count, body):
    def one(i, carry):
        body(i)
        return carry

    lax.fori_loop(0, count, one, 0)


def shut_keys(length, own_rows, full_rows, shape, dimension):
    place = lax.broadcasted_iota(jnp.int32, shape, dimension)
    step = jnp.zeros(shape, jnp.int32)
    for t in range(1, 4):
        step += (place >= t * full_rows).astype(jnp.int32)
    live = (place - step * full_rows < own_rows) & (
        place - step * (full_rows - own_rows) < length
    )
    return jnp.where(live, 0.0, masked_score)


def stages(count, work, hooks):
    def body(k):
        work(k)
        for at, steps in hooks.items():

            @pl.when(k == at)
            def _():
                for step in steps:
                    step()

    repeat(count, body)


def chip_rows(slab, k):
    far, near = slab.far - slab.core, slab.near - slab.core
    start = (far + lax.rem(k, 2) * (near - far)) * (2 * slab.half_rows)
    return pl.multiple_of(start, 2 * slab.half_rows)


def open_gathers(gathers, fill, prepare):
    fill(0)
    gathers[0].start()
    fill(1)
    gathers[0].second()
    gathers[1].start()
    prepare()
    gathers[0].forward()
    gathers[1].second()


def block_out(src, dst, sems, i):
    rows = step_rows(i, WIDE)
    return pltpu.make_async_copy(src.at[rows], dst.at[rows], sems.at[i])


def widen(packed, wide):
    heads = packed.shape[1] // HEAD

    def block(i):
        rows = step_rows(i, 128)
        for h in range(heads):
            piece = packed[rows, h * HEAD : (h + 1) * HEAD]
            blank = jnp.zeros((128, LANES - HEAD), jnp.bfloat16)
            wide[rows, h * LANES : (h + 1) * LANES] = jnp.concatenate([piece, blank], axis=1)

    repeat(packed.shape[0] // 128, block)


def split_tail(packed, tails, up_cols):
    start = packed.shape[1] - LANES

    def block(i):
        rows = step_rows(i, 128)
        for j in range(2):
            piece = packed[rows, start + j * up_cols : start + (j + 1) * up_cols]
            blank = jnp.zeros((128, LANES - up_cols), jnp.bfloat16)
            tails[rows, j * LANES : (j + 1) * LANES] = jnp.concatenate([piece, blank], axis=1)

    repeat(packed.shape[0] // 128, block)


def up_dot(rows, packed, tails):
    main = (packed.shape[1] - LANES) // 2
    first = dot(rows, packed[:, :main], 1, 0)
    return jnp.concatenate([first, dot(rows, tails[:, :LANES], 1, 0)], axis=1)


def up_back(grads, packed, tails):
    main = (packed.shape[1] - LANES) // 2
    return dot(grads[:, :main], packed[:, :main], 1, 1) + dot(
        grads[:, main:], tails[:, :LANES], 1, 1
    )


def down_dot(active, packed, tails):
    main = (packed.shape[1] - LANES) // 2
    return dot(active[:, :main], packed[:, main : 2 * main], 1, 1) + dot(
        active[:, main:], tails[:, LANES:], 1, 1
    )


def down_back(rows, packed, tails):
    main = (packed.shape[1] - LANES) // 2
    first = dot(rows, packed[:, main : 2 * main], 1, 0)
    return jnp.concatenate([first, dot(rows, tails[:, LANES:], 1, 0)], axis=1)


def attn_forward_kernel(
    ready, at, layer, own_rows, rows_ref, vectors, bias_ref, lengths, packed_hbm, given_hbm, grads_ref,
    hidden_ref, lse_ref, normed_hbm, qkv_hbm, mixed_hbm, *rest
):
    micro, half_rows, width = rows_ref.shape
    gathered, gather_refs = rest[0], rest[0:3]
    scatter_refs = rest[3:9]
    terms = rest[3]
    packed, wide, qkv, mixed, load_sem, keep_sems, given_sems, all_grads, tile_send, tile_recv = rest[9:]
    vec, bias = vectors.at[layer], bias_ref[layer]
    seq = qkv.shape[1]
    pair = mixed.shape[2]
    heads = pair // LANES
    load = pltpu.make_async_copy(
        packed_hbm.at[:, at : at + packed.shape[1]], packed, load_sem
    )
    load.start()
    slab = Slab(half_rows)
    gathers = make_gathers(slab, gather_refs, micro)
    scatters = make_scatters(slab, scatter_refs, micro)
    given = [
        pltpu.make_async_copy(given_hbm.at[m], gathered.at[m], given_sems.at[m])
        for m in range(micro if ready else 0)
    ]
    for copy in given:
        copy.start()
    slab.greet()
    if ready:
        tiles = TileGather(all_grads, tile_send, tile_recv)
        for m in range(micro):
            own = tiles.tile(m, tiles.tensor)
            count = grads_ref.shape[1]
            own[:count] = grads_ref[m]
            own[count:] = jnp.zeros((tiles.tile_rows - count, width), jnp.bfloat16)
            tiles.start(m)

    def fill(m):
        own = slab.rows(gathered.at[m], slab.mine[0])
        for start in range(0, half_rows, 32):
            block = rows_ref[m, pl.ds(start, 32)].astype(jnp.float32)
            own[pl.ds(start, 32)] = low(layer_norm(block, vec[0:1], vec[2:3]))

    def prepare():
        load.wait()
        widen(packed, wide)

    if ready:
        prepare()
    else:
        open_gathers(gathers, fill, prepare)
    keeps = []

    def keep(src, dst, m, i):
        def copy():
            return pltpu.make_async_copy(src.at[m], dst.at[m], keep_sems.at[i])

        copy().start()
        keeps.append(copy)

    def project(m):
        def block(i):
            rows = step_rows(i, 4 * half_rows)
            out = dot(gathered[m, rows], wide[:, : 3 * pair], 1, 0)
            qkv[m, rows] = low(out + bias)

        repeat(seq // (4 * half_rows), block)

    def attend(m, rows):
        shut = shut_keys(lengths[m], own_rows, 2 * half_rows, (1, seq), 1)
        for h in range(heads):
            cols = slice(h * LANES, (h + 1) * LANES)
            q = qkv[m, rows, cols]
            k = qkv[m, :, pair + h * LANES : pair + (h + 1) * LANES]
            v = qkv[m, :, 2 * pair + h * LANES : 2 * pair + (h + 1) * LANES]
            scores = dot(q, k, 1, 1) * (score_scale * LOG2E) + shut
            top = jnp.max(scores, axis=-1, keepdims=True)
            exp_scores = jnp.exp2(scores - top)
            total = jnp.sum(exp_scores, axis=-1, keepdims=True)
            probs = low(exp_scores * (1.0 / total))
            mixed[m, rows, cols] = low(dot(probs, v, 1, 0))
            lse_ref[m, h, rows] = jnp.broadcast_to(
                top + jnp.log(total) * LOG2E, (2 * half_rows, LANES)
            )

    def output(m, rows):
        terms[m, rows] = low(dot(mixed[m, rows], wide[:, 3 * pair :], 1, 1))

    def close(m):
        scatters[m].finish()
        for rows in scatters[m].blocks():
            start = rows_ref[m, rows].astype(jnp.float32)
            hidden_ref[m, rows] = start + scatters[m].total(rows) + vec[5:6]

    def gathered_rows(m):
        if ready:
            given[m].wait()
            return
        gathers[m].to_mate()
        gathers[m].finish()
        keep(gathered, normed_hbm, m, m)

    def work(k):
        m = lax.div(k, 2)
        start = chip_rows(slab, k)
        pl.when(lax.rem(k, 2) == 0)(lambda: project(m))

        def piece(i):
            attend(m, step_from(start, i, 2 * half_rows))

        repeat(2, piece)
        output(m, pl.ds(start, 4 * half_rows))

    def keep_two(m):
        keep(qkv, qkv_hbm, m, 2 + 2 * m)
        keep(mixed, mixed_hbm, m, 3 + 2 * m)

    def grads_on():
        if ready:
            tiles.pass_on()

    def grads_in():
        if ready:
            tiles.finish()
            for m in range(micro):
                keep(all_grads, normed_hbm, m, m)

    gathered_rows(0)
    if not ready:
        gathers[1].forward()
    zero, one = scatters
    stages(
        4,
        work,
        {
            0: [zero.mate_far, lambda: gathered_rows(1), zero.far_hop],
            1: [zero.mate_near, lambda: keep_two(0), zero.second_hop, zero.first_hop, grads_on],
            2: [one.mate_far, lambda: close(0), one.far_hop, grads_in],
            3: [one.mate_near, lambda: keep_two(1), one.second_hop, one.first_hop],
        },
    )
    close(1)
    if ready:
        tiles.drain()
    for copy in keeps:
        copy().wait()


def ffn_forward_kernel(
    half_ff, at, layer, hidden_ref, vectors, up_biases, packed_hbm, out_ref, second_hbm, upper_hbm, *rest
):
    micro, half_rows, _ = hidden_ref.shape
    gathered, gather_refs = rest[0], rest[0:3]
    scatter_refs = rest[3:9]
    terms = rest[3]
    packed, tails, upper, load_sem, keep_sems = rest[9:]
    vec, up_bias = vectors.at[layer], up_biases.at[layer]
    _, ff = upper.shape[1:]
    load = pltpu.make_async_copy(
        packed_hbm.at[:, at : at + packed.shape[1]], packed, load_sem
    )
    load.start()
    slab = Slab(half_rows)
    gathers = make_gathers(slab, gather_refs, micro)
    scatters = make_scatters(slab, scatter_refs, micro)
    slab.greet()

    def fill(m):
        own = slab.rows(gathered.at[m], slab.mine[0])
        for start in range(0, half_rows, 32):
            block = hidden_ref[m, pl.ds(start, 32)]
            own[pl.ds(start, 32)] = low(layer_norm(block, vec[1:2], vec[6:7]))

    def prepare():
        load.wait()
        split_tail(packed, tails, half_ff - ff + LANES)

    open_gathers(gathers, fill, prepare)
    keeps = []

    def keep(src, dst, m, i):
        def copy():
            return pltpu.make_async_copy(src.at[m], dst.at[m], keep_sems.at[i])

        copy().start()
        keeps.append(copy)

    def compute(m, rows):
        value = up_dot(gathered[m, rows], packed, tails) + up_bias[...]
        upper[m, rows] = value
        active = low(gelu_tanh(value))
        terms[m, rows] = low(down_dot(active, packed, tails))

    def close(m):
        scatters[m].finish()
        for rows in scatters[m].blocks():
            out_ref[m, rows] = low(hidden_ref[m, rows] + scatters[m].total(rows) + vec[7:8])

    def work(k):
        compute(lax.div(k, 2), pl.ds(chip_rows(slab, k), 4 * half_rows))

    gathers[0].to_mate()
    gathers[0].finish()
    keep(gathered, second_hbm, 0, 0)
    zero, one = scatters
    stages(
        4,
        work,
        {
            0: [zero.mate_far, gathers[1].forward, zero.far_hop],
            1: [
                zero.mate_near,
                lambda: keep(upper, upper_hbm, 0, 1),
                gathers[1].to_mate,
                zero.second_hop,
                gathers[1].finish,
                lambda: keep(gathered, second_hbm, 1, 2),
            ],
            2: [one.mate_far, zero.first_hop, one.far_hop],
            3: [one.mate_near, lambda: keep(upper, upper_hbm, 1, 3), one.second_hop],
        },
    )
    close(0)
    one.first_hop()
    close(1)
    for copy in keeps:
        copy().wait()


def ffn_backward_kernel(
    half_ff, at, layer, grad_ref, hidden_ref, vectors, second_hbm, upper_hbm, packed_hbm,
    out_ref, grads_hbm, small_ref, up_bias_ref, *rest
):
    micro, half_rows, width = hidden_ref.shape
    gathered, gather_refs = rest[0], rest[0:3]
    scatter_refs = rest[3:9]
    terms = rest[3]
    packed, tails, second, upper, grad_upper, active, load_sems, grads_ref, grads_sems = rest[9:]
    vec = vectors.at[layer]
    seq, ff = upper.shape[1:]
    main = ff - LANES
    extra = half_ff - main
    load_packed = pltpu.make_async_copy(
        packed_hbm.at[:, at : at + packed.shape[1]], packed, load_sems.at[0]
    )
    load_packed.start()
    load_upper, load_second = [], []
    for m in range(micro):
        load_upper.append(
            pltpu.make_async_copy(upper_hbm.at[m], upper.at[m], load_sems.at[1 + m])
        )
        load_upper[m].start()
    for m in range(micro):
        load_second.append(
            pltpu.make_async_copy(second_hbm.at[m], second.at[m], load_sems.at[1 + micro + m])
        )
        load_second[m].start()
    slab = Slab(half_rows)
    gathers = make_gathers(slab, gather_refs, micro)
    scatters = make_scatters(slab, scatter_refs, micro)
    slab.greet()

    def fill(m):
        own = slab.rows(gathered.at[m], slab.mine[0])
        for start in range(0, half_rows, 32):
            own[pl.ds(start, 32)] = grad_ref[m, pl.ds(start, 32)]

    def prepare():
        small_ref[...] = jnp.zeros_like(small_ref)
        up_bias_ref[...] = jnp.zeros_like(up_bias_ref)
        load_packed.wait()
        split_tail(packed, tails, extra)

    open_gathers(gathers, fill, prepare)

    def compute(m, rows):
        value = upper[m, rows]
        square = value * value
        bent = jnp.tanh(GELU_A * value * (1.0 + GELU_B * square))
        half = 0.5 * (1.0 + bent)
        active[m, rows] = low(value * half)
        slope = half + (0.5 * GELU_A) * value * (1.0 - bent * bent) * (1.0 + 3.0 * GELU_B * square)
        grad_active = down_back(gathered[m, rows], packed, tails)
        grad = low(grad_active * slope)
        grad_upper[m, rows] = grad
        up_bias_ref[0:1] += jnp.sum(grad.astype(jnp.float32), axis=0, keepdims=True)
        terms[m, rows] = low(up_back(grad, packed, tails))

    def stacked(ref, cols=slice(None)):
        return ref[:, :, cols].reshape(micro * seq, -1)

    def weight_grads(hooks):
        def block(i):
            cols = step_rows(i, WIDE)
            up = dot(stacked(second, cols), stacked(grad_upper), 0, 0)
            down = dot(stacked(gathered, cols), stacked(active), 0, 0)
            grads_ref[cols, :main] = low(up[:, :main])
            grads_ref[cols, main : 2 * main] = low(down[:, :main])
            blank = jnp.zeros((WIDE, LANES - 2 * extra), jnp.float32)
            rest_cols = [up[:, main : main + extra], down[:, main : main + extra], blank]
            grads_ref[cols, 2 * main :] = low(jnp.concatenate(rest_cols, axis=1))
            block_out(grads_ref, grads_hbm, grads_sems, i).start()

        stages(width // WIDE, block, hooks)

    def grads_out():
        for i in range(width // WIDE):
            block_out(grads_ref, grads_hbm, grads_sems, i).wait()

    def close(m):
        scatters[m].finish()
        for rows in scatters[m].blocks():
            grad_normed = scatters[m].total(rows)
            back, gain_terms = norm_back(hidden_ref[m, rows], vec[1:2], grad_normed)
            grad_rows = grad_ref[m, rows].astype(jnp.float32)
            grad_hidden = grad_rows + back
            out_ref[m, rows] = grad_hidden
            branch = low(grad_hidden).astype(jnp.float32)
            for j, item in enumerate((gain_terms, grad_normed, grad_rows, branch)):
                small_ref[j : j + 1] += jnp.sum(item, axis=0, keepdims=True)

    def work(k):
        compute(lax.div(k, 2), pl.ds(chip_rows(slab, k), 4 * half_rows))

    gathers[0].to_mate()
    gathers[0].finish()
    load_upper[0].wait()
    zero, one = scatters
    stages(
        4,
        work,
        {
            0: [zero.mate_far, gathers[1].forward, zero.far_hop],
            1: [
                zero.mate_near,
                gathers[1].to_mate,
                zero.second_hop,
                gathers[1].finish,
                load_upper[1].wait,
            ],
            2: [one.mate_far, zero.first_hop, one.far_hop],
            3: [one.mate_near, one.second_hop],
        },
    )
    for load in load_second:
        load.wait()
    weight_grads({0: [one.first_hop, lambda: close(0)]})
    close(1)
    grads_out()


def ffn_turn_kernel(
    half_ff, at, layer, hidden_ref, grad_ref, vectors, up_biases, given_hbm, packed_hbm,
    out_ref, grad_out_ref, grads_hbm, small_ref, up_bias_ref, *rest
):
    micro, half_rows, width = hidden_ref.shape
    gathered, gather_refs = rest[0], rest[0:3]
    terms, back_terms = rest[3], rest[9]
    packed, tails, given, grad_upper, active, load_sem, given_sems, grads_ref, grads_sems = rest[15:]
    vec, up_bias = vectors.at[layer], up_biases.at[layer]
    seq, ff = active.shape[1:]
    main = ff - LANES
    extra = half_ff - main
    load = pltpu.make_async_copy(
        packed_hbm.at[:, at : at + packed.shape[1]], packed, load_sem
    )
    load.start()
    loads = [
        pltpu.make_async_copy(given_hbm.at[m], given.at[m], given_sems.at[m]) for m in range(micro)
    ]
    for copy in loads:
        copy.start()
    slab = Slab(half_rows)
    gathers = make_gathers(slab, gather_refs, micro)
    scatters = make_scatters(slab, rest[3:9], micro)
    backs = make_scatters(slab, rest[9:15], micro)
    slab.greet()

    def fill(m):
        own = slab.rows(gathered.at[m], slab.mine[0])
        for start in range(0, half_rows, 32):
            block = hidden_ref[m, pl.ds(start, 32)]
            own[pl.ds(start, 32)] = low(layer_norm(block, vec[1:2], vec[6:7]))

    def prepare():
        small_ref[...] = jnp.zeros_like(small_ref)
        up_bias_ref[...] = jnp.zeros_like(up_bias_ref)
        load.wait()
        split_tail(packed, tails, extra)

    open_gathers(gathers, fill, prepare)

    def compute(m, rows):
        value = up_dot(gathered[m, rows], packed, tails) + up_bias[...]
        square = value * value
        bent = jnp.tanh(GELU_A * value * (1.0 + GELU_B * square))
        half = 0.5 * (1.0 + bent)
        shown = low(value * half)
        active[m, rows] = shown
        slope = half + (0.5 * GELU_A) * value * (1.0 - bent * bent) * (1.0 + 3.0 * GELU_B * square)
        grad = low(down_back(given[m, rows], packed, tails) * slope)
        grad_upper[m, rows] = grad
        up_bias_ref[0:1] += jnp.sum(grad.astype(jnp.float32), axis=0, keepdims=True)
        back_terms[m, rows] = low(up_back(grad, packed, tails))
        terms[m, rows] = low(down_dot(shown, packed, tails))

    def stacked(ref, cols=slice(None)):
        return ref[:, :, cols].reshape(micro * seq, -1)

    def weight_grads(hooks):
        def block(i):
            cols = step_rows(i, WIDE)
            up = dot(stacked(gathered, cols), stacked(grad_upper), 0, 0)
            down = dot(stacked(given, cols), stacked(active), 0, 0)
            grads_ref[cols, :main] = low(up[:, :main])
            grads_ref[cols, main : 2 * main] = low(down[:, :main])
            blank = jnp.zeros((WIDE, LANES - 2 * extra), jnp.float32)
            rest_cols = [up[:, main : main + extra], down[:, main : main + extra], blank]
            grads_ref[cols, 2 * main :] = low(jnp.concatenate(rest_cols, axis=1))
            block_out(grads_ref, grads_hbm, grads_sems, i).start()

        stages(width // WIDE, block, hooks)

    def grads_out():
        for i in range(width // WIDE):
            block_out(grads_ref, grads_hbm, grads_sems, i).wait()

    def close_back(m):
        backs[m].finish()
        for rows in backs[m].blocks():
            grad_normed = backs[m].total(rows)
            back, gain_terms = norm_back(hidden_ref[m, rows], vec[1:2], grad_normed)
            grad_rows = grad_ref[m, rows].astype(jnp.float32)
            grad_hidden = grad_rows + back
            grad_out_ref[m, rows] = grad_hidden
            branch = low(grad_hidden).astype(jnp.float32)
            for j, item in enumerate((gain_terms, grad_normed, grad_rows, branch)):
                small_ref[j : j + 1] += jnp.sum(item, axis=0, keepdims=True)

    def close(m):
        scatters[m].finish()
        for rows in scatters[m].blocks():
            out_ref[m, rows] = low(hidden_ref[m, rows] + scatters[m].total(rows) + vec[7:8])

    def work(k):
        compute(lax.div(k, 2), pl.ds(chip_rows(slab, k), 4 * half_rows))

    gathers[0].to_mate()
    gathers[0].finish()
    loads[0].wait()
    zero, one = scatters
    back_zero, back_one = backs
    stages(
        4,
        work,
        {
            0: [back_zero.mate_far, zero.mate_far, gathers[1].forward, back_zero.far_hop],
            1: [
                back_zero.mate_near,
                zero.mate_near,
                gathers[1].to_mate,
                back_zero.second_hop,
                gathers[1].finish,
                zero.far_hop,
                zero.second_hop,
                loads[1].wait,
            ],
            2: [
                back_one.mate_far,
                one.mate_far,
                back_zero.first_hop,
                back_one.far_hop,
                zero.first_hop,
            ],
            3: [
                back_one.mate_near,
                one.mate_near,
                lambda: close_back(0),
                back_one.second_hop,
                one.far_hop,
                one.second_hop,
            ],
        },
    )
    weight_grads({0: [back_one.first_hop, one.first_hop]})
    close_back(1)
    for m in range(micro):
        close(m)
    grads_out()


def attn_backward_kernel(
    at, layer, own_rows, both_ways, grad_ref, rows_ref, vectors, lse_hbm, lengths,
    normed_hbm, qkv_hbm, mixed_hbm, packed_hbm, errand_hbm, errand_one_hbm,
    out_ref, grads_hbm, small_ref, bias_ref, errand_got, *rest
):
    micro, half_rows, width = grad_ref.shape
    gathered, gather_refs = rest[0], rest[0:3]
    scatter_refs = rest[3:9]
    terms = rest[3]
    packed, wide, normed, qkv, mixed, grad_mixed, grad_qkv, turned, shut = rest[9:18]
    low_probs, grad_scores, high_probs, errand_sems, load_sems = rest[18:23]
    grads_ref, grads_sems, lse, lse_sem = rest[23:]
    load_lse = pltpu.make_async_copy(lse_hbm, lse, lse_sem)
    load_lse.start()
    vec = vectors.at[layer]
    seq, pair = mixed.shape[1:]
    heads = pair // LANES
    load_packed = pltpu.make_async_copy(
        packed_hbm.at[:, at : at + packed.shape[1]], packed, load_sems.at[0]
    )
    load_packed.start()
    load_qkv, load_rest = [], []
    for m in range(micro):
        load_qkv.append(pltpu.make_async_copy(qkv_hbm.at[m], qkv.at[m], load_sems.at[1 + 3 * m]))
        load_qkv[m].start()
    for m in range(micro):
        for k, (src, dst) in enumerate(((mixed_hbm, mixed), (normed_hbm, normed))):
            load = pltpu.make_async_copy(src.at[m], dst.at[m], load_sems.at[2 + k + 3 * m])
            load.start()
            load_rest.append(load)
    slab = Slab(half_rows)
    gathers = make_gathers(slab, gather_refs, micro)
    scatters = make_scatters(slab, scatter_refs, micro)
    slab.greet()

    def fill(m):
        own = slab.rows(gathered.at[m], slab.mine[0])
        for start in range(0, half_rows, 32):
            own[pl.ds(start, 32)] = low(grad_ref[m, pl.ds(start, 32)])

    def head(h, part=0):
        return pl.ds(pl.multiple_of(part * pair + h * LANES, LANES), LANES)

    def ready_qkv(m):
        load_qkv[m].wait()
        shut[m] = shut_keys(lengths[m], own_rows, 2 * half_rows, (seq, LANES), 0)
        for h in range(heads):
            turned[m, h] = low(qkv[m, :, head(h, 1)].astype(jnp.float32).T)

    def find_probs(m, h):
        def block(i):
            rows = step_rows(i, TILE)
            keys, queries = qkv[m, :, head(h, 1)], qkv[m, rows, head(h)]
            closed = jnp.concatenate([shut[m]] * (TILE // LANES), axis=1)
            scores = dot(keys, queries, 1, 1) * (score_scale * LOG2E) + closed
            high_probs[m, h, :, rows] = jnp.exp2(scores - lse[m, h, rows].T[0:1])

        repeat(seq // TILE, block)

    def find_all(k):
        find_probs(lax.div(k, heads), lax.rem(k, heads))

    span = errand_hbm.shape[0]
    cut = round_up(span // 2, 16) if span > 16 else span // 2
    errands = []
    for k, part in enumerate((pl.ds(0, cut), pl.ds(cut, span - cut))):
        errands.append(
            [
                remote(
                    source.at[part],
                    errand_got.at[part],
                    errand_sems.at[0, k],
                    errand_sems.at[1, k],
                    {"section": 1 - lax.axis_index("section")},
                )
                for source in (errand_hbm, errand_one_hbm)
            ]
        )
    first_section = lax.axis_index("section") == 0
    sends_errand, gets_errand = first_section | both_ways, ~first_section | both_ways

    def prepare():
        small_ref[...] = jnp.zeros_like(small_ref)
        bias_ref[...] = jnp.zeros_like(bias_ref)
        load_packed.wait()
        widen(packed, wide)
        for m in range(micro):
            ready_qkv(m)
        load_lse.wait()

    fill(0)
    gathers[0].start()
    fill(1)
    gathers[0].second()
    gathers[1].start()
    prepare()

    def mix_grads(m):
        def block(i):
            rows = step_rows(i, 4 * half_rows)
            grad_mixed[m, rows] = low(dot(gathered[m, rows], wide[:, 3 * pair :], 1, 0))

        repeat(seq // (4 * half_rows), block)

    def attend(m, h):
        def block(i):
            rows = step_rows(i, TILE)
            grads = grad_mixed[m, rows, head(h)]
            probs = high_probs[m, h, :, rows]
            grad_probs = dot(qkv[m, :, head(h, 2)], grads, 1, 1)
            inner = jnp.sum(grad_probs * probs, axis=0, keepdims=True)
            low_probs[:, rows] = low(probs)
            grad_scores[:, rows] = low(probs * (grad_probs - inner))

        repeat(seq // TILE, block)
        grad_keys = dot(grad_scores[...], qkv[m, :, head(h)], 1, 0)
        grad_qkv[m, :, head(h, 1)] = low(grad_keys * score_scale)
        grad_qkv[m, :, head(h, 2)] = low(dot(low_probs[...], grad_mixed[m, :, head(h)], 1, 0))
        turn = dot(turned[m, h], grad_scores[...], 1, 0).T
        grad_qkv[m, :, head(h)] = low(turn * score_scale)

    def back_project(m, rows):
        grads = grad_qkv[m, rows]
        terms[m, rows] = low(dot(grads, wide[:, : 3 * pair], 1, 1))
        for j, part in enumerate((0, 2)):
            piece = grads[:, part * pair : (part + 1) * pair].astype(jnp.float32)
            bias_ref[j : j + 1] += jnp.sum(piece, axis=0, keepdims=True)

    def stacked(ref, cols=slice(None)):
        return ref[:, :, cols].reshape(micro * seq, -1)

    def weight_grads(hooks):
        def block(i):
            cols = step_rows(i, WIDE)
            front = dot(stacked(normed, cols), stacked(grad_qkv), 0, 0)
            back = dot(stacked(gathered, cols), stacked(mixed), 0, 0)
            total = low(jnp.concatenate([front, back], axis=1))
            pieces = [total[:, h * LANES : h * LANES + HEAD] for h in range(4 * heads)]
            grads_ref[cols] = jnp.concatenate(pieces, axis=1)
            block_out(grads_ref, grads_hbm, grads_sems, i).start()

        stages(width // WIDE, block, hooks)

    def close(m):
        scatters[m].finish()
        for rows in scatters[m].blocks():
            grad_normed = scatters[m].total(rows)
            back, gain_terms = norm_back(
                rows_ref[m, rows].astype(jnp.float32), vec[0:1], grad_normed
            )
            out_ref[m, rows] = low(grad_ref[m, rows] + back)
            for j, item in enumerate((gain_terms, grad_normed)):
                small_ref[j : j + 1] += jnp.sum(item, axis=0, keepdims=True)

    def start_errand(k):
        pl.when(first_section)(errands[k][0].start)
        if both_ways:
            pl.when(~first_section)(errands[k][1].start)

    stages(
        2 * heads,
        find_all,
        {
            0: [gathers[0].forward, gathers[1].second],
            1: [gathers[1].forward, gathers[0].to_mate, lambda: start_errand(0)],
        },
    )
    gathers[0].finish()
    zero, one = scatters
    attend_hooks = {
        0: [gathers[1].to_mate],
        heads - 1: [gathers[1].finish],
        heads: [zero.first_hop, lambda: start_errand(1)],
    }
    project_hooks = {
        0: [zero.mate_far, zero.far_hop],
        1: [zero.mate_near, zero.second_hop],
        2: [one.mate_far, one.far_hop],
        3: [one.mate_near, lambda: close(0), one.second_hop],
    }

    def hooked(at, hooks):
        for k, steps in hooks.items():

            @pl.when(at == k)
            def _():
                for step in steps:
                    step()

    def image(m):
        mix_grads(m)

        def one_head(h):
            attend(m, h)
            hooked(m * heads + h, attend_hooks)

        repeat(heads, one_head)

        def one_chip(i):
            back_project(m, pl.ds(chip_rows(slab, i), 4 * half_rows))
            hooked(2 * m + i, project_hooks)

        repeat(2, one_chip)

    repeat(micro, image)
    for load in load_rest:
        load.wait()
    weight_grads({0: [one.first_hop]})
    close(1)
    for i in range(width // WIDE):
        block_out(grads_ref, grads_hbm, grads_sems, i).wait()

    for errand, _ in errands:
        pl.when(sends_errand)(errand.wait_send)
        pl.when(gets_errand)(errand.wait_recv)


def any_spec():
    return pl.BlockSpec(memory_space=pl.ANY)


def vmem_spec():
    return pl.BlockSpec(memory_space=pltpu.VMEM)


def shape_of(shape, dtype):
    return jax.ShapeDtypeStruct(shape, dtype)


def params(collective):
    return pltpu.CompilerParams(
        collective_id=collective, has_side_effects=True, vmem_limit_bytes=VMEM_BYTES
    )


def smem_spec():
    return pl.BlockSpec(memory_space=pltpu.SMEM)


def attn_forward(rows_low, vectors, bias, packed, at, layer, lengths, own_rows, given=None, grads=None):
    micro, half_rows, width = rows_low.shape
    seq = 8 * half_rows
    pair = bias.shape[2] // 3
    heads = pair // LANES
    low_type, high_type = jnp.bfloat16, jnp.float32
    hidden, lse, normed, qkv, mixed = pl.pallas_call(
        functools.partial(attn_forward_kernel, given is not None, at, layer, own_rows),
        out_shape=[
            shape_of((micro, half_rows, width), high_type),
            shape_of((micro, heads, seq, LANES), high_type),
            shape_of((micro, seq, width), low_type),
            shape_of((micro, seq, 3 * pair), low_type),
            shape_of((micro, seq, pair), low_type),
        ],
        in_specs=[vmem_spec()] * 3 + [smem_spec(), any_spec(), any_spec(), vmem_spec()],
        out_specs=[vmem_spec()] * 2 + [any_spec()] * 3,
        scratch_shapes=gather_scratch(micro, seq, width)
        + scatter_scratch(micro, seq, half_rows, width)
        + [
            pltpu.VMEM((width, 4 * heads * HEAD), low_type),
            pltpu.VMEM((width, 4 * pair), low_type),
            pltpu.VMEM((micro, seq, 3 * pair), low_type),
            pltpu.VMEM((micro, seq, pair), low_type),
            pltpu.SemaphoreType.DMA,
            pltpu.SemaphoreType.DMA((6,)),
            pltpu.SemaphoreType.DMA((micro,)),
            pltpu.VMEM((micro, seq if given is not None else 32, width), low_type),
            pltpu.SemaphoreType.DMA((micro, 3)),
            pltpu.SemaphoreType.DMA((micro, 3)),
        ],
        compiler_params=params(0 if given is None else 6),
        cost_estimate=COST,
        name="attn_forward",
    )(
        rows_low,
        vectors,
        bias,
        lengths,
        packed,
        packed if given is None else given,
        rows_low if grads is None else grads,
    )
    if given is None:
        return hidden, (normed, qkv, lse, mixed)
    return hidden, (given, qkv, lse, mixed), normed


def ffn_forward(hidden, vectors, up_biases, packed, at, layer, half_ff):
    micro, half_rows, width = hidden.shape
    seq = 8 * half_rows
    ff = up_biases.shape[2]
    packed_cols = 2 * ff - LANES
    low_type, high_type = jnp.bfloat16, jnp.float32
    out, second, upper = pl.pallas_call(
        functools.partial(ffn_forward_kernel, half_ff, at, layer),
        out_shape=[
            shape_of((micro, half_rows, width), low_type),
            shape_of((micro, seq, width), low_type),
            shape_of((micro, seq, ff), high_type),
        ],
        in_specs=[vmem_spec()] * 3 + [any_spec()],
        out_specs=[vmem_spec()] + [any_spec()] * 2,
        scratch_shapes=gather_scratch(micro, seq, width)
        + scatter_scratch(micro, seq, half_rows, width)
        + [
            pltpu.VMEM((width, packed_cols), low_type),
            pltpu.VMEM((width, 2 * LANES), low_type),
            pltpu.VMEM((micro, seq, ff), high_type),
            pltpu.SemaphoreType.DMA,
            pltpu.SemaphoreType.DMA((4,)),
        ],
        compiler_params=params(1),
        cost_estimate=COST,
        name="ffn_forward",
    )(hidden, vectors, up_biases, packed)
    return out, (second, upper)


def ffn_turn(hidden, grad_low, given, vectors, up_biases, packed, at, layer, half_ff):
    micro, half_rows, width = hidden.shape
    seq = 8 * half_rows
    ff = up_biases.shape[2]
    low_type, high_type = jnp.bfloat16, jnp.float32
    out, grad_hidden, grads, small, up_bias = pl.pallas_call(
        functools.partial(ffn_turn_kernel, half_ff, at, layer),
        out_shape=[
            shape_of((micro, half_rows, width), low_type),
            shape_of((micro, half_rows, width), high_type),
            shape_of((width, 2 * ff - LANES), low_type),
            shape_of((8, width), high_type),
            shape_of((8, ff), high_type),
        ],
        in_specs=[vmem_spec()] * 4 + [any_spec()] * 2,
        out_specs=[vmem_spec()] * 2 + [any_spec()] + [vmem_spec()] * 2,
        scratch_shapes=gather_scratch(micro, seq, width)
        + scatter_scratch(micro, seq, half_rows, width)
        + scatter_scratch(micro, seq, half_rows, width)
        + [
            pltpu.VMEM((width, 2 * ff - LANES), low_type),
            pltpu.VMEM((width, 2 * LANES), low_type),
            pltpu.VMEM((micro, seq, width), low_type),
            pltpu.VMEM((micro, seq, ff), low_type),
            pltpu.VMEM((micro, seq, ff), low_type),
            pltpu.SemaphoreType.DMA,
            pltpu.SemaphoreType.DMA((micro,)),
            pltpu.VMEM((width, 2 * ff - LANES), low_type),
            pltpu.SemaphoreType.DMA((width // WIDE,)),
        ],
        compiler_params=params(7),
        cost_estimate=COST,
        name="ffn_turn",
    )(hidden, grad_low, vectors, up_biases, given, packed)
    return out, grad_hidden, grads, small, up_bias


def ffn_backward(grad_low, hidden, kept, vectors, packed, at, layer, half_ff):
    second, upper = kept
    micro, half_rows, width = hidden.shape
    seq, ff = upper.shape[1:]
    low_type, high_type = jnp.bfloat16, jnp.float32
    grad_hidden, grads, small, up_bias = pl.pallas_call(
        functools.partial(ffn_backward_kernel, half_ff, at, layer),
        out_shape=[
            shape_of((micro, half_rows, width), high_type),
            shape_of((width, 2 * ff - LANES), low_type),
            shape_of((8, width), high_type),
            shape_of((8, ff), high_type),
        ],
        in_specs=[vmem_spec()] * 3 + [any_spec()] * 3,
        out_specs=[vmem_spec(), any_spec()] + [vmem_spec()] * 2,
        scratch_shapes=gather_scratch(micro, seq, width)
        + scatter_scratch(micro, seq, half_rows, width)
        + [
            pltpu.VMEM((width, 2 * ff - LANES), low_type),
            pltpu.VMEM((width, 2 * LANES), low_type),
            pltpu.VMEM((micro, seq, width), low_type),
            pltpu.VMEM((micro, seq, ff), high_type),
            pltpu.VMEM((micro, seq, ff), low_type),
            pltpu.VMEM((micro, seq, ff), low_type),
            pltpu.SemaphoreType.DMA((1 + 2 * micro,)),
            pltpu.VMEM((width, 2 * ff - LANES), low_type),
            pltpu.SemaphoreType.DMA((width // WIDE,)),
        ],
        compiler_params=params(2),
        cost_estimate=COST,
        name="ffn_backward",
    )(grad_low, hidden, vectors, second, upper, packed)
    return grad_hidden, grads, small, up_bias


def attn_backward(
    grad_hidden, rows_low, kept, vectors, packed, at, layer, lengths, own_rows, errand, both_ways
):
    normed, qkv, lse, mixed = kept
    micro, half_rows, width = grad_hidden.shape
    seq, pair = mixed.shape[1:]
    heads = pair // LANES
    low_type, high_type = jnp.bfloat16, jnp.float32
    out, grads, small, bias, got = pl.pallas_call(
        functools.partial(attn_backward_kernel, at, layer, own_rows, both_ways),
        out_shape=[
            shape_of((micro, half_rows, width), low_type),
            shape_of((width, 4 * heads * HEAD), low_type),
            shape_of((8, width), high_type),
            shape_of((8, pair), high_type),
            shape_of(errand[0].shape, errand[0].dtype),
        ],
        in_specs=[vmem_spec()] * 3 + [any_spec(), smem_spec()] + [any_spec()] * 6,
        out_specs=[vmem_spec(), any_spec()] + [vmem_spec()] * 2 + [any_spec()],
        scratch_shapes=gather_scratch(micro, seq, width)
        + scatter_scratch(micro, seq, half_rows, width)
        + [
            pltpu.VMEM((width, 4 * heads * HEAD), low_type),
            pltpu.VMEM((width, 4 * pair), low_type),
            pltpu.VMEM((micro, seq, width), low_type),
            pltpu.VMEM((micro, seq, 3 * pair), low_type),
            pltpu.VMEM((micro, seq, pair), low_type),
            pltpu.VMEM((micro, seq, pair), low_type),
            pltpu.VMEM((micro, seq, 3 * pair), low_type),
            pltpu.VMEM((micro, heads, LANES, seq), low_type),
            pltpu.VMEM((micro, seq, LANES), high_type),
            pltpu.VMEM((seq, seq), low_type),
            pltpu.VMEM((seq, seq), low_type),
            pltpu.VMEM((micro, heads, seq, seq), high_type),
            pltpu.SemaphoreType.DMA((2, 2)),
            pltpu.SemaphoreType.DMA((1 + 3 * micro,)),
            pltpu.VMEM((width, 4 * heads * HEAD), low_type),
            pltpu.SemaphoreType.DMA((width // WIDE,)),
            pltpu.VMEM(lse.shape, high_type),
            pltpu.SemaphoreType.DMA,
        ],
        compiler_params=params(3 + 5 * layer),
        cost_estimate=COST,
        name="attn_backward",
    )(grad_hidden, rows_low, vectors, lse, lengths, normed, qkv, mixed, packed, *errand)
    return out, grads, small, bias, got


def slab_peers():
    section, tensor = lax.axis_index("section"), lax.axis_index("tensor")
    peers = []
    for role in range(1, 8):
        far, step = role // 4, role % 4
        other = section + far * (1 - 2 * section)
        to = (other, lax.rem(tensor + step, 4))
        source = (other, lax.rem(tensor + 4 - step, 4))
        peers.append((role, to, source))
    return peers


def column_peers(count):
    here = lax.axis_index("dp")
    return [
        (step, lax.rem(here + step, count), lax.rem(here + count - step, count))
        for step in range(1, count)
    ]


def greet_all(count):
    barrier = pltpu.get_barrier_semaphore()
    for _, to, _ in slab_peers():
        pl.semaphore_signal(barrier, inc=1, device_id=named(to), device_id_type=MESH)
    for _, to, _ in column_peers(count):
        pl.semaphore_signal(barrier, inc=1, device_id={"dp": to}, device_id_type=MESH)
    pl.semaphore_wait(barrier, 7 + count - 1)


def remote(src, dst, send_sem, recv_sem, peer):
    return pltpu.make_async_remote_copy(
        src_ref=src,
        dst_ref=dst,
        send_sem=send_sem,
        recv_sem=recv_sem,
        device_id=peer,
        device_id_type=MESH,
    )


def prologue_kernel(
    count, heads, qkv_ref, out_ref_in, up_ref_in, down_ref_t, gains_ref, shifts_ref, up_bias, rows_ref,
    first_hbm, normed_hbm, attn_ref, ff_zero_hbm, ff_one_hbm, out_ref, up_ref, bias_ref,
    attn_parts, ff_parts, up_halves, mine_ref, all_rows, line, ff_line, column, slab, up_got,
    rows_send, rows_recv, column_send, column_recv, slab_send, slab_recv, swap_send, swap_recv,
    right_send, right_recv, left_send, left_recv, out_sems,
):
    section, tensor, here = (lax.axis_index(name) for name in ("section", "tensor", "dp"))
    width = out_ref.shape[2]
    chunk = width // (4 * count)
    rows = attn_parts.shape[1]
    micro, own_rows = rows_ref.shape[:2]
    pieces = swap_send.shape[0] - 2
    size = rows // pieces
    other = {"section": 1 - section}
    pair = heads * LANES
    pair_cols = heads * HEAD
    half_ff = up_ref_in.shape[1] // 2
    main = half_ff // LANES * LANES
    extra = half_ff - main
    greet_all(count)
    out_turned = low(out_ref_in[...].astype(jnp.float32).T)
    for half in range(2):
        span = slice(half * pair_cols, (half + 1) * pair_cols)
        parts = [qkv_ref[k, :, span] for k in range(3)] + [out_turned[:, span]]
        attn_parts[half] = jnp.concatenate(parts, axis=1)
    keep_slot = jnp.where(section == 0, here, count)
    send_slot = jnp.where(section == 0, here, count)
    got_slot = jnp.where(section == 0, count, here)
    sent = []
    for p in range(pieces):
        span = pl.ds(p * size, size)
        copy = remote(
            attn_parts.at[1 - section, span],
            line.at[send_slot, span],
            swap_send.at[p],
            swap_recv.at[p],
            other,
        )
        copy.start()
        sent.append(copy)
    line[keep_slot] = attn_parts[section]
    mine_ref[...] = jnp.zeros_like(mine_ref)
    gains = gains_ref.shape[0]
    mine_ref[:gains, :chunk] = gains_ref[...]
    for i in range(shifts_ref.shape[0]):
        mine_ref[gains + i : gains + i + 1, :chunk] = shifts_ref[i]
    column[here] = mine_ref[...]
    for step, to, _ in column_peers(count):
        copy = remote(
            mine_ref, column.at[here], column_send.at[step], column_recv.at[step], {"dp": to}
        )
        copy.start()
        sent.append(copy)

    def swapped(p):
        got = line.at[got_slot, pl.ds(p * size, size)]
        remote(got, got, swap_send.at[p], swap_recv.at[p], other).wait_recv()

    def hop(step, p, way, finish=False):
        origin = here - way * step
        sends, recvs = (right_send, right_recv) if way == 1 else (left_send, left_recv)
        inside = (origin >= 0) if way == 1 else (origin < count)
        onward = (here + 1 < count) if way == 1 else (here > 0)
        slot = line.at[jnp.clip(origin, 0, count - 1), pl.ds(p * size, size)]
        target = jnp.clip(here + way, 0, count - 1)
        if step > 0 and not finish:

            @pl.when(inside)
            def _():
                remote(slot, slot, sends.at[step, p], recvs.at[step, p], {"dp": target}).wait_recv()

        if step + 1 < count:

            @pl.when(inside & onward)
            def _():
                copy = remote(
                    slot, slot, sends.at[step, p], recvs.at[step + 1, p], {"dp": target}
                )
                if finish:
                    copy.wait_send()
                else:
                    copy.start()

    def hops(step):
        for p in range(pieces):
            for way in (1, -1):
                hop(step, p, way)

    for step, _, source in column_peers(count):
        slot = column.at[source]
        remote(slot, slot, column_send.at[step], column_recv.at[step], {"dp": source}).wait_recv()
    for role, to, _ in slab_peers():
        copy = remote(
            column, slab.at[section, tensor], slab_send.at[role], slab_recv.at[role], named(to)
        )
        copy.start()
        sent.append(copy)
    slab[section, tensor] = column[...]

    def set_out(p):
        pl.when(section == 1)(lambda: swapped(p))
        for way in (1, -1):
            hop(0, p, way)

    set_out(0)
    for role, _, source in slab_peers():
        slot = slab.at[source[0], source[1]]
        remote(slot, slot, slab_send.at[role], slab_recv.at[role], named(source)).wait_recv()
    for layer in range(2):
        for part in range(4 * count):
            piece = slab[layer, part % 4, part // 4]
            out_ref[layer, :, part * chunk : (part + 1) * chunk] = piece[:, :chunk]
    tiles = TileGather(all_rows, rows_send, rows_recv)
    for m in range(micro):
        own = tiles.tile(m, tensor)
        for begin in range(0, own_rows, 32):
            end = min(begin + 32, own_rows)
            block = rows_ref[m, begin:end].astype(jnp.float32)
            own[begin:end] = low(layer_norm(block, out_ref[0, 0:1], out_ref[0, 2:3]))
        own[own_rows:] = jnp.zeros((tiles.tile_rows - own_rows, width), jnp.bfloat16)
        tiles.start(m)
    for p in range(1, pieces):
        set_out(p)
    blank = jnp.zeros((rows, LANES - 2 * extra), jnp.bfloat16)
    up_halves[...] = jnp.zeros_like(up_halves)
    for half in range(2):
        start = half * half_ff
        up_halves[half, :, :half_ff] = up_bias[:, start : start + half_ff]
        ff_parts[half, :, :main] = up_ref_in[:, start : start + main]
        ff_parts[half, :, main : 2 * main] = down_ref_t[:, start : start + main]
        span = slice(start + main, start + half_ff)
        ff_parts[half, :, 2 * main :] = jnp.concatenate(
            [up_ref_in[:, span], down_ref_t[:, span], blank], axis=1
        )
    ff_swap = remote(
        ff_parts.at[1 - section],
        ff_line.at[section],
        swap_send.at[pieces],
        swap_recv.at[pieces],
        other,
    )
    up_swap = remote(
        up_halves.at[1 - section],
        up_got.at[section],
        swap_send.at[pieces + 1],
        swap_recv.at[pieces + 1],
        other,
    )
    up_swap.start()
    ff_swap.start()
    hops(1)
    start = (2 * tensor + section) * pair_cols
    for layer in range(2):
        turned = pltpu.roll(out_ref[layer], lax.rem(width - start, width), 1)
        empty = jnp.zeros((1, LANES - HEAD), jnp.float32)
        for part, row in ((0, 3), (2, 4)):
            for h in range(heads):
                at = part * pair + h * LANES
                piece = turned[row : row + 1, h * HEAD : (h + 1) * HEAD]
                bias_ref[layer, :, at : at + LANES] = jnp.concatenate([piece, empty], 1)
        bias_ref[layer, :, pair : 2 * pair] = jnp.zeros((1, pair), jnp.float32)
    up_ref[section] = up_halves[section]
    outs = []

    def put(src, dst, i):
        copy = pltpu.make_async_copy(src, dst, out_sems.at[i])
        copy.start()
        outs.append(copy)

    def put_ff(src, section_of_first, i):
        for layer, dst in enumerate((ff_zero_hbm, ff_one_hbm)):
            here_too = layer if section_of_first == 0 else 1 - layer

            @pl.when(section == here_too)
            def _():
                pltpu.make_async_copy(src, dst, out_sems.at[i]).start()

        outs.append(pltpu.make_async_copy(src, ff_zero_hbm, out_sems.at[i]))

    put_ff(ff_parts.at[section], 0, count)
    for step in range(2, count):
        hops(step)
        if step == 2:
            tiles.pass_on()
    if count <= 2:
        tiles.pass_on()
    for p in range(pieces):

        @pl.when(section == 0)
        def _():
            swapped(p)

    for at in range(count):
        put(line.at[at], first_hbm.at[pl.ds(at * rows, rows)], at)
    attn_ref[...] = line[count]
    got = up_got.at[1 - section]
    remote(got, got, swap_send.at[pieces + 1], swap_recv.at[pieces + 1], other).wait_recv()
    up_ref[1 - section] = up_got[1 - section]
    tiles.finish()
    put(all_rows, normed_hbm, count + 2)
    ff_got = ff_line.at[1 - section]
    remote(ff_got, ff_got, swap_send.at[pieces], swap_recv.at[pieces], other).wait_recv()
    put_ff(ff_got, 1, count + 1)
    for step in range(count):
        for p in range(pieces):
            for way in (1, -1):
                hop(step, p, way, True)
    for copy in sent + [ff_swap, up_swap]:
        copy.wait_send()
    tiles.drain()
    for copy in outs:
        copy.wait()


def prologue(qkv, out, up, down_t, gains, shifts, up_bias, rows_low, count, heads, tile_rows):
    part_rows = qkv.shape[1]
    micro, _, width = rows_low.shape
    vector_rows = gains.shape[0] + shifts.shape[0]
    half_ff = up.shape[1] // 2
    ff_wide = round_up(half_ff, LANES)
    attn_shape = (part_rows, 4 * heads * HEAD)
    ff_shape = (2, part_rows, 2 * ff_wide - LANES)
    all_rows = (micro, 4 * tile_rows, width)
    pieces = 3 if part_rows % 96 == 0 else 1
    low_type, high_type = jnp.bfloat16, jnp.float32
    dma = pltpu.SemaphoreType.DMA
    return pl.pallas_call(
        functools.partial(prologue_kernel, count, heads),
        out_shape=[
            shape_of((count * part_rows, attn_shape[1]), low_type),
            shape_of(all_rows, low_type),
            shape_of(attn_shape, low_type),
            shape_of(ff_shape[1:], low_type),
            shape_of(ff_shape[1:], low_type),
            shape_of((2, vector_rows, width), high_type),
            shape_of((2, 1, ff_wide), high_type),
            shape_of((2, 1, 3 * heads * LANES), high_type),
        ],
        in_specs=[vmem_spec()] * 8,
        out_specs=[any_spec()] * 2 + [vmem_spec()] + [any_spec()] * 2 + [vmem_spec()] * 3,
        scratch_shapes=[
            pltpu.VMEM((2,) + attn_shape, low_type),
            pltpu.VMEM(ff_shape, low_type),
            pltpu.VMEM((2, 1, ff_wide), high_type),
            pltpu.VMEM((vector_rows, LANES), high_type),
            pltpu.VMEM(all_rows, low_type),
            pltpu.VMEM((count + 1,) + attn_shape, low_type),
            pltpu.VMEM(ff_shape, low_type),
            pltpu.VMEM((count, vector_rows, LANES), high_type),
            pltpu.VMEM((2, 4, count, vector_rows, LANES), high_type),
            pltpu.VMEM((2, 1, ff_wide), high_type),
            dma((micro, 3)),
            dma((micro, 3)),
            dma((count,)),
            dma((count,)),
            dma((8,)),
            dma((8,)),
            dma((pieces + 2,)),
            dma((pieces + 2,)),
            dma((count, pieces)),
            dma((count, pieces)),
            dma((count, pieces)),
            dma((count, pieces)),
            dma((count + 3,)),
        ],
        compiler_params=params(4),
        cost_estimate=COST,
        name="prologue",
    )(qkv, out, up, down_t, gains, shifts, up_bias, rows_low)


def home_kernel(
    count, chunk, attn_zero, attn_one, ff_zero, ff_one, bias_zero, bias_one, up_zero, up_one,
    ff_sum_hbm, attn_sum_hbm, rows_zero_hbm, rows_one_hbm,
    out_ref, up_ref, ff_got_hbm, attn_got_hbm, rows_got_hbm,
    parts, ups, slab, column, up_pair, up_column, total,
    column_send, column_recv, slab_send, slab_recv, up_sems, up_column_send, up_column_recv, far_send, far_recv,
):
    section, tensor, here = (lax.axis_index(name) for name in ("section", "tensor", "dp"))
    width = attn_zero.shape[1]
    heads = bias_zero.shape[1] // LANES
    biases_in, ups_in = (bias_zero, bias_one), (up_zero, up_one)
    other = {"section": 1 - section}
    greet_all(count)
    parts[...] = jnp.zeros_like(parts)
    start = (2 * tensor + section) * (heads * HEAD)
    for layer, (attn, ff) in enumerate(((attn_zero, ff_zero), (attn_one, ff_one))):
        bias = biases_in[layer][...]
        blank = jnp.zeros((8, width - heads * HEAD), jnp.float32)
        pieces = [bias[:, h * LANES : h * LANES + HEAD] for h in range(heads)]
        placed = pltpu.roll(jnp.concatenate(pieces + [blank], 1), start, 1)
        whole = jnp.concatenate(
            [attn[0:1], ff[0:1], attn[1:2], placed[0:2], ff[3:4], ff[1:2], ff[2:3]], axis=0
        )
        for part in range(4 * count):
            piece = whole[:, part * chunk : (part + 1) * chunk]
            parts[layer, part % 4, part // 4, :, :chunk] = piece
        ups[layer] = ups_in[layer][0:1]
    sent = []

    def send(src, dst, send_sem, recv_sem, peer):
        copy = remote(src, dst, send_sem, recv_sem, peer)
        copy.start()
        sent.append(copy)

    send(ups.at[1 - section], up_pair.at[section], up_sems.at[0], up_sems.at[1], other)
    for role, to, _ in slab_peers():
        send(
            parts.at[to[0], to[1]], slab.at[role], slab_send.at[role], slab_recv.at[role], named(to)
        )
    far_rows = remote(rows_zero_hbm, rows_got_hbm, far_send.at[0], far_recv.at[0], other)
    far_rows_one = remote(rows_one_hbm, rows_got_hbm, far_send.at[0], far_recv.at[0], other)
    far_ff = remote(ff_sum_hbm, ff_got_hbm, far_send.at[1], far_recv.at[1], other)
    far_attn = remote(attn_sum_hbm, attn_got_hbm, far_send.at[2], far_recv.at[2], other)
    one_way = ((far_ff, 1), (far_attn, 0))
    pl.when(section == 1)(far_rows.start)
    pl.when(section == 0)(far_rows_one.start)
    for copy, source in one_way:
        pl.when(section == source)(copy.start)
    up_pair[section] = ups[section]
    value = parts[section, tensor]
    for role, _, source in slab_peers():
        slot = slab.at[role]
        remote(slot, slot, slab_send.at[role], slab_recv.at[role], named(source)).wait_recv()
        value = value + slab[role]
    total[...] = value
    for step, to, _ in column_peers(count):
        send(total.at[to], column.at[step], column_send.at[step], column_recv.at[step], {"dp": to})
    got = up_pair.at[1 - section]
    remote(got, got, up_sems.at[0], up_sems.at[1], other).wait_recv()
    for step, to, _ in column_peers(count):
        send(
            up_pair, up_column.at[here], up_column_send.at[step], up_column_recv.at[step], {"dp": to}
        )
    up_column[here] = up_pair[...]
    result = total[here]
    for step, _, source in column_peers(count):
        slot = column.at[step]
        remote(slot, slot, column_send.at[step], column_recv.at[step], {"dp": source}).wait_recv()
        result = result + column[step]
    out_ref[...] = result
    for step, _, source in column_peers(count):
        slot = up_column.at[source]
        remote(
            slot, slot, up_column_send.at[step], up_column_recv.at[step], {"dp": source}
        ).wait_recv()
    value = up_column[0]
    for at in range(1, count):
        value = value + up_column[at]
    up_ref[...] = value
    far_rows.wait()
    for copy, source in one_way:
        pl.when(section == source)(copy.wait_send)
        pl.when(section != source)(copy.wait_recv)
    for copy in sent:
        copy.wait_send()


def home(attn_small, ff_small, bias_grads, up_grads, ff_sum, attn_sum, rows, count, chunk):
    vector_rows, lanes = 8, LANES
    up_shape = (1, up_grads[0].shape[1])
    dma = pltpu.SemaphoreType.DMA
    high_type = jnp.float32
    return pl.pallas_call(
        functools.partial(home_kernel, count, chunk),
        out_shape=[
            shape_of((vector_rows, lanes), high_type),
            shape_of((2,) + up_shape, high_type),
            shape_of(ff_sum.shape, ff_sum.dtype),
            shape_of(attn_sum.shape, attn_sum.dtype),
            shape_of(rows[0].shape, rows[0].dtype),
        ],
        in_specs=[vmem_spec()] * 8 + [any_spec()] * 4,
        out_specs=[vmem_spec()] * 2 + [any_spec()] * 3,
        scratch_shapes=[
            pltpu.VMEM((2, 4, count, vector_rows, lanes), high_type),
            pltpu.VMEM((2,) + up_shape, high_type),
            pltpu.VMEM((8, count, vector_rows, lanes), high_type),
            pltpu.VMEM((count, vector_rows, lanes), high_type),
            pltpu.VMEM((2,) + up_shape, high_type),
            pltpu.VMEM((count, 2) + up_shape, high_type),
            pltpu.VMEM((count, vector_rows, lanes), high_type),
            dma((count,)),
            dma((count,)),
            dma((8,)),
            dma((8,)),
            dma((2,)),
            dma((count,)),
            dma((count,)),
            dma((3,)),
            dma((3,)),
        ],
        compiler_params=params(5),
        cost_estimate=COST,
        name="home",
    )(*attn_small, *ff_small, *bias_grads, *up_grads, ff_sum, attn_sum, *rows)


def ff_finish_kernel(zero, one, zero_got, one_got, up_ref, down_ref):
    first = lax.axis_index("section") == 0
    halves = (
        jnp.where(first, zero[...], one_got[...]),
        jnp.where(first, zero_got[...], one[...]),
    )
    half_ff = up_ref.shape[1] // 2
    main = half_ff // LANES * LANES
    extra = half_ff - main
    for k in range(2):
        pieces = []
        for half in halves:
            start = 2 * main + k * extra
            pieces += [half[:, k * main : (k + 1) * main], half[:, start : start + extra]]
        whole = jnp.concatenate(pieces, axis=1).astype(jnp.float32)
        (up_ref, down_ref)[k][...] = whole


def ff_finish(sums, got, ff_cols):
    rows = sums[0].shape[0]
    return pl.pallas_call(
        ff_finish_kernel,
        out_shape=[
            shape_of((rows, ff_cols), jnp.float32),
            shape_of((rows, ff_cols), jnp.float32),
        ],
        in_specs=[vmem_spec()] * 4,
        out_specs=[vmem_spec()] * 2,
        compiler_params=pltpu.CompilerParams(vmem_limit_bytes=VMEM_BYTES),
        cost_estimate=COST,
        name="ff_finish",
    )(*sums, *got)


def attn_finish_kernel(zero, one, zero_got, one_got, qkv_ref, out_ref):
    first = lax.axis_index("section") == 0
    halves = (
        jnp.where(first, zero[...], one_got[...]),
        jnp.where(first, zero_got[...], one[...]),
    )
    pair_cols = qkv_ref.shape[2] // 2
    for k in range(4):
        span = slice(k * pair_cols, (k + 1) * pair_cols)
        whole = jnp.concatenate([half[:, span] for half in halves], axis=1).astype(jnp.float32)
        if k < 3:
            qkv_ref[k] = whole
        else:
            out_ref[...] = whole.T


def attn_finish(sums, got, head_cols):
    rows = sums[0].shape[0]
    return pl.pallas_call(
        attn_finish_kernel,
        out_shape=[
            shape_of((3, rows, head_cols), jnp.float32),
            shape_of((head_cols, rows), jnp.float32),
        ],
        in_specs=[vmem_spec()] * 4,
        out_specs=[vmem_spec()] * 2,
        compiler_params=pltpu.CompilerParams(vmem_limit_bytes=VMEM_BYTES),
        name="attn_finish",
    )(*sums, *got)


def shards(
    section_input,
    final_cotangent,
    lengths,
    qkv_weight,
    out_weight,
    up_weight,
    down_weight,
    norm_gains,
    biases,
    up_bias,
):
    here = lax.axis_index("section")
    sections = lax.axis_size("section")
    micro, _, own_rows, _ = section_input.shape
    head_cols = qkv_weight.shape[3]
    pair_cols = head_cols // sections
    heads = pair_cols // HEAD
    ff_cols = up_weight.shape[2]
    half_ff = ff_cols // sections
    half_rows = round_up(-(-own_rows // sections), 32)
    full_rows = half_rows * sections

    def by_layer(mine, other):
        return [jnp.where(here == 0, mine, other), jnp.where(here == 0, other, mine)]

    count = lax.axis_size("dp")
    chunk = norm_gains.shape[2]
    first, normed, attn_part, ff_zero, ff_one, vectors, up_biases, bias_qv = prologue(
        qkv_weight[0],
        out_weight[0],
        up_weight[0],
        down_weight[0].T,
        norm_gains[0],
        biases.transpose(1, 0, 2),
        up_bias,
        section_input[:, 0],
        count,
        heads,
        full_rows,
    )

    def gather_column(part):
        return lax.all_gather(part, "dp", axis=0, tiled=True)

    ff_first = gather_column(ff_zero)
    attn_packed = [(first, 0), (gather_column(attn_part), 0)]
    ff_packed = [(ff_first, 0), (gather_column(ff_one), 0)]
    lengths_here = lengths.reshape(micro)

    def my_rows(value):
        padded = jnp.pad(value[:, 0], [(0, 0), (0, full_rows - own_rows), (0, 0)])
        return lax.dynamic_slice_in_dim(padded, here * half_rows, half_rows, 1)

    def whole_rows(first, second, got):
        low_half, high_half = by_layer(jnp.where(here == 0, first, second), got)
        return jnp.concatenate([low_half, high_half], 1)[:, None, :own_rows]

    rows = my_rows(section_input)
    inputs, hiddens, attn_kept = [], [], []
    for layer in range(2):
        inputs.append(rows)
        operands = (rows, vectors, bias_qv, *attn_packed[layer], layer, lengths_here, own_rows)
        if layer == 0:
            hidden, kept, grads_all = attn_forward(*operands, normed, final_cotangent[:, 0])
        else:
            hidden, kept = attn_forward(*operands)
        hiddens.append(hidden)
        attn_kept.append(kept)
        if layer == 0:
            rows, ff_kept = ffn_forward(hidden, vectors, up_biases, *ff_packed[0], 0, half_ff)

    attn_sums, ff_sums, up_sums, input_grads = {}, {}, {}, {}
    attn_small, ff_small, bias_grads, errands = {}, {}, {}, {}
    for layer in (1, 0):
        if layer == 1:
            last, grad_hidden, ff_grad, ff_small[1], up_sums[1] = ffn_turn(
                hiddens[1],
                my_rows(final_cotangent),
                grads_all,
                vectors,
                up_biases,
                *ff_packed[1],
                1,
                half_ff,
            )
        else:
            grad_hidden, ff_grad, ff_small[0], up_sums[0] = ffn_backward(
                grads, hiddens[0], ff_kept, vectors, *ff_packed[0], 0, half_ff
            )
        ff_sums[layer] = lax.psum_scatter(ff_grad, "dp", scatter_dimension=0, tiled=True)
        if layer == 1:
            errand, both_ways = (last, rows), True
        else:
            errand, both_ways = (ff_sums[1], ff_sums[1]), False
        grads, attn_grad, attn_small[layer], bias_grads[layer], got = attn_backward(
            grad_hidden,
            inputs[layer],
            attn_kept[layer],
            vectors,
            *attn_packed[layer],
            layer,
            lengths_here,
            own_rows,
            errand,
            both_ways,
        )
        errands[layer] = got
        attn_sums[layer] = lax.psum_scatter(attn_grad, "dp", scatter_dimension=0, tiled=True)
        input_grads[layer] = grads

    small_mine, up_total, ff_got, attn_got, rows_got = home(
        [attn_small[0], attn_small[1]],
        [ff_small[0], ff_small[1]],
        [bias_grads[0], bias_grads[1]],
        [up_sums[0], up_sums[1]],
        ff_sums[0],
        attn_sums[1],
        [input_grads[0], input_grads[1]],
        count,
        chunk,
    )
    attn_zero_got = lax.ppermute(attn_sums[0], "section", [(1, 0)])
    up_grad, down_grad = ff_finish([ff_sums[0], ff_sums[1]], [ff_got, errands[0]], ff_cols)
    small_mine, up_total, rows_got, out_got, up_grad = lax.optimization_barrier(
        (small_mine, up_total, rows_got, errands[1], up_grad)
    )
    section_output = whole_rows(rows, last, out_got)
    small_mine = small_mine[None, :, :chunk]
    up_total = up_total[:, :, :half_ff].reshape(1, ff_cols)
    input_grad = whole_rows(input_grads[0], input_grads[1], rows_got)

    qkv_total, out_total = attn_finish(
        [attn_sums[0], attn_sums[1]], [attn_zero_got, attn_got], head_cols
    )
    gains = norm_gains.shape[1]
    return (
        section_output[None],
        input_grad[None],
        qkv_total[None],
        out_total[None],
        up_grad[None],
        down_grad.T[None],
        small_mine[:, :gains],
        small_mine[:, gains:],
        up_total,
    )


def solution(mesh):
    in_specs = (
        P(None, "dp", "tensor", None),
        P(None, "dp", "tensor", None),
        P(None, "dp"),
        P("section", None, "dp", "tensor"),
        P("section", "tensor", "dp"),
        P("section", "dp", "tensor"),
        P("section", "tensor", "dp"),
        P("section", None, ("dp", "tensor")),
        P("section", None, ("dp", "tensor")),
        P("section", "tensor"),
    )
    out_specs = (
        P("section", None, "dp", "tensor", None),
        P("section", None, "dp", "tensor", None),
        P("section", None, "dp", "tensor"),
        P("section", "tensor", "dp"),
        P("section", "dp", "tensor"),
        P("section", "tensor", "dp"),
        P("section", None, ("dp", "tensor")),
        P("section", None, ("dp", "tensor")),
        P("section", "tensor"),
    )
    return jax.shard_map(shards, mesh=mesh, in_specs=in_specs, out_specs=out_specs, check_vma=False)
```

```python
import functools
import math

import jax
import jax.numpy as jnp
from jax import lax
from jax.experimental import pallas as pl
from jax.experimental.pallas import tpu as pltpu
from jax.sharding import PartitionSpec as P


HEAD = 72
LANES = 128
norm_eps = 1e-06
masked_score = -1000000000.0
score_scale = 1.0 / math.sqrt(HEAD)
GELU_A = math.sqrt(2.0 / math.pi)
GELU_B = 0.044715


def round_up(value, step):
    return -(-value // step) * step


def dot(left, right, left_dim, right_dim):
    return lax.dot_general(
        left, right, (((left_dim,), (right_dim,)), ((), ())), preferred_element_type=jnp.float32
    )


def low(value):
    return value.astype(jnp.bfloat16)


def layer_norm(rows, gain_vec, shift_vec):
    centred = rows - jnp.mean(rows, axis=-1, keepdims=True)
    spread = jnp.mean(centred * centred, axis=-1, keepdims=True)
    return centred * lax.rsqrt(spread + norm_eps) * gain_vec + shift_vec


def norm_back(rows, gain_vec, grads):
    centred = rows - jnp.mean(rows, axis=-1, keepdims=True)
    spread = jnp.mean(centred * centred, axis=-1, keepdims=True)
    inverse = lax.rsqrt(spread + norm_eps)
    xhat = centred * inverse
    e = grads * gain_vec
    back = inverse * (
        e
        - jnp.mean(e, axis=-1, keepdims=True)
        - xhat * jnp.mean(e * xhat, axis=-1, keepdims=True)
    )
    return back, grads * xhat


def gelu_tanh(value):
    return jax.nn.gelu(value, approximate=True)


MESH = pl.DeviceIdType.MESH
VMEM_BYTES = 64_000_000
COST = pl.CostEstimate(flops=20_000_000_000, transcendentals=0, bytes_accessed=100_000_000)
LOG2E = 1.0 / math.log(2.0)
TILE = 256
WIDE = 128


class Slab:
    def __init__(self, half_rows):
        self.half_rows = half_rows
        section = lax.axis_index("section")
        tensor = lax.axis_index("tensor")
        core = lax.rem(tensor, 2)
        self.core = core
        self.mine = self.around(section, tensor, core)
        self.theirs = self.around(section, tensor + 1 - 2 * core, 1 - core)
        self.far_role, self.near_role = 1 + core, 2 - core
        self.mate = self.theirs[0]
        over = lax.rem(tensor + 2, 4)
        self.near, self.far = tensor, over
        self.mate_near, self.mate_far = self.mate[1], lax.rem(self.mate[1] + 2, 4)
        self.grid = self.places(section, self.near, self.far)
        self.mate_grid = self.places(section, self.mate_near, self.mate_far)
        self.across_y = self.grid[2]
        self.first, self.second = self.mine[1], self.mine[2]

    def place(self, section, tensor):
        start = (2 * tensor + section) * self.half_rows
        return (section, tensor, pl.multiple_of(start, self.half_rows))

    def places(self, section, near, far):
        flip = 1 - section
        return [self.place(*at) for at in ((section, near), (flip, near), (section, far), (flip, far))]

    def around(self, section, tensor, core):
        over = lax.rem(tensor + 2, 4)
        turn = 1 - 2 * section
        first = (section + (1 - core) * turn, tensor + core * (over - tensor))
        second = (section + core * turn, tensor + (1 - core) * (over - tensor))
        places = ((section, tensor), first, second, (1 - section, over))
        return [self.place(*at) for at in places]

    def rows(self, ref, at):
        return ref.at[pl.ds(at[2], self.half_rows)]

    def greet(self):
        barrier = pltpu.get_barrier_semaphore()
        for peer in (self.first, self.second, self.mate):
            pl.semaphore_signal(barrier, inc=1, device_id=named(peer), device_id_type=MESH)
        pl.semaphore_wait(barrier, 3)


def named(at):
    return {"section": at[0], "tensor": at[1]}


class Moves:
    def __init__(self, slab, send_sems, recv_sems):
        self.slab, self.send_sems, self.recv_sems = slab, send_sems, recv_sems
        self.sent = []

    def copy(self, src, dst, role, peer):
        return pltpu.make_async_remote_copy(
            src_ref=src,
            dst_ref=dst,
            send_sem=self.send_sems.at[role],
            recv_sem=self.recv_sems.at[role],
            device_id=named(peer),
            device_id_type=MESH,
        )

    def send(self, ends, role, peer):
        self.copy(*ends(), role, peer).start()
        self.sent.append(lambda: self.copy(*ends(), role, peer))

    def arrived(self, dst, role):
        self.copy(dst, dst, role, self.slab.mate).wait_recv()

    def drain(self):
        for copy in self.sent:
            copy().wait_send()


class Gather(Moves):
    def __init__(self, slab, whole, send_sems, recv_sems):
        super().__init__(slab, send_sems, recv_sems)
        self.whole = whole

    def pass_on(self, at, role, peer):
        self.send(lambda: (self.slab.rows(self.whole, at),) * 2, role, peer)

    def arrive(self, at, role):
        self.arrived(self.slab.rows(self.whole, at), role)

    def start(self):
        mine = self.slab.mine
        self.pass_on(mine[0], 0, mine[1])
        self.pass_on(mine[0], 3, self.slab.mate)

    def second(self):
        self.sent.pop(0)().wait_send()
        self.pass_on(self.slab.mine[0], 1, self.slab.mine[2])

    def forward(self):
        mine, mate = self.slab.mine, self.slab.mate
        self.arrive(mine[1], 0)
        self.pass_on(mine[1], 2, mine[2])
        self.pass_on(mine[1], 4, mate)

    def to_mate(self):
        mine, mate = self.slab.mine, self.slab.mate
        self.arrive(mine[2], 1)
        self.pass_on(mine[2], 5, mate)
        self.arrive(mine[3], 2)
        self.pass_on(mine[3], 6, mate)

    def finish(self):
        for k in range(4):
            self.arrive(self.slab.theirs[k], 3 + k)
        self.drain()


class TileGather:
    def __init__(self, whole, send_sems, recv_sems):
        self.whole, self.send_sems, self.recv_sems = whole, send_sems, recv_sems
        self.tensor = lax.axis_index("tensor")
        self.over = lax.rem(self.tensor + 2, 4)
        self.mate = self.tensor + 1 - 2 * lax.rem(self.tensor, 2)
        self.micro, rows = whole.shape[0], whole.shape[1] // 4
        self.tile_rows = rows
        self.sent = []

    def tile(self, m, index):
        start = pl.multiple_of(index * self.tile_rows, self.tile_rows)
        return self.whole.at[m, pl.ds(start, self.tile_rows)]

    def copy(self, m, index, role, peer):
        part = self.tile(m, index)
        return remote(
            part, part, self.send_sems.at[m, role], self.recv_sems.at[m, role], {"tensor": peer}
        )

    def send(self, m, index, role, peer):
        self.copy(m, index, role, peer).start()
        self.sent.append(lambda: self.copy(m, index, role, peer))

    def start(self, m):
        self.send(m, self.tensor, 0, self.over)
        self.send(m, self.tensor, 1, self.mate)

    def pass_on(self):
        for m in range(self.micro):
            self.copy(m, self.over, 0, self.over).wait_recv()
            self.send(m, self.over, 2, self.mate)

    def finish(self):
        for m in range(self.micro):
            self.copy(m, self.mate, 1, self.mate).wait_recv()
            self.copy(m, lax.rem(self.mate + 2, 4), 2, self.mate).wait_recv()

    def drain(self):
        for copy in self.sent:
            copy().wait_send()


class Scatter(Moves):
    def __init__(self, slab, terms, from_mate, outgoing, arrivals, send_sems, recv_sems):
        super().__init__(slab, send_sems, recv_sems)
        self.terms, self.from_mate, self.outgoing = terms, from_mate, outgoing
        self.relay, self.from_second, self.from_first = (arrivals.at[k] for k in range(3))

    def to_mate(self, at, role):
        self.send(
            lambda: (self.slab.rows(self.terms, at), self.from_mate.at[role]), role, self.slab.mate
        )

    def mate_far(self):
        self.to_mate(self.slab.mate_grid[3], 3)
        self.to_mate(self.slab.mate_grid[2], self.slab.far_role)

    def mate_near(self):
        self.to_mate(self.slab.mate_grid[1], self.slab.near_role)
        self.to_mate(self.slab.mate_grid[0], 0)

    def chip_sum(self, k, rows):
        part = self.slab.rows(self.terms, self.slab.mine[k])
        return part[rows].astype(jnp.float32) + self.from_mate[k, rows].astype(jnp.float32)

    def blocks(self):
        return [pl.ds(start, 32) for start in range(0, self.slab.half_rows, 32)]

    def hop(self, k, slot, dst, role, peer, ride=None):
        self.arrived(self.from_mate.at[k], k)
        if ride is not None:
            self.arrived(ride, 4)
        for rows in self.blocks():
            value = self.chip_sum(k, rows)
            if ride is not None:
                value = value + ride[rows].astype(jnp.float32)
            self.outgoing[slot, rows] = low(value)
        self.send(lambda: (self.outgoing.at[slot], dst), role, peer)

    def far_hop(self):
        self.hop(3, 0, self.relay, 4, self.slab.second)

    def second_hop(self):
        self.hop(2, 1, self.from_second, 5, self.slab.second)

    def first_hop(self):
        self.hop(1, 2, self.from_first, 6, self.slab.first, self.relay)

    def finish(self):
        self.arrived(self.from_mate.at[0], 0)
        self.arrived(self.from_second, 5)
        self.arrived(self.from_first, 6)
        self.drain()

    def total(self, rows):
        other = self.from_second[rows].astype(jnp.float32) + self.from_first[rows].astype(
            jnp.float32
        )
        return self.chip_sum(0, rows) + other


def scatter_scratch(micro, seq, half_rows, width):
    return [
        pltpu.VMEM((micro, seq, width), jnp.bfloat16),
        pltpu.VMEM((micro, 4, half_rows, width), jnp.bfloat16),
        pltpu.VMEM((micro, 3, half_rows, width), jnp.bfloat16),
        pltpu.VMEM((micro, 3, half_rows, width), jnp.bfloat16),
        pltpu.SemaphoreType.DMA((micro, 7)),
        pltpu.SemaphoreType.DMA((micro, 7)),
    ]


def gather_scratch(micro, seq, width):
    return [
        pltpu.VMEM((micro, seq, width), jnp.bfloat16),
        pltpu.SemaphoreType.DMA((micro, 7)),
        pltpu.SemaphoreType.DMA((micro, 7)),
    ]


def make_scatters(slab, refs, micro):
    terms, from_mate, outgoing, arrivals, send_sems, recv_sems = refs
    return [
        Scatter(
            slab,
            terms.at[m],
            from_mate.at[m],
            outgoing.at[m],
            arrivals.at[m],
            send_sems.at[m],
            recv_sems.at[m],
        )
        for m in range(micro)
    ]


def make_gathers(slab, refs, micro):
    whole, send_sems, recv_sems = refs
    return [
        Gather(slab, whole.at[m], send_sems.at[m], recv_sems.at[m]) for m in range(micro)
    ]


def step_from(start, i, size):
    return pl.ds(pl.multiple_of(start + i * size, size), size)


def step_rows(i, size):
    return pl.ds(pl.multiple_of(i * size, size), size)


def repeat(count, body):
    def one(i, carry):
        body(i)
        return carry

    lax.fori_loop(0, count, one, 0)


def shut_keys(length, own_rows, full_rows, shape, dimension):
    place = lax.broadcasted_iota(jnp.int32, shape, dimension)
    step = jnp.zeros(shape, jnp.int32)
    for t in range(1, 4):
        step += (place >= t * full_rows).astype(jnp.int32)
    live = (place - step * full_rows < own_rows) & (
        place - step * (full_rows - own_rows) < length
    )
    return jnp.where(live, 0.0, masked_score)


def stages(count, work, hooks):
    def body(k):
        work(k)
        for at, steps in hooks.items():

            @pl.when(k == at)
            def _():
                for step in steps:
                    step()

    repeat(count, body)


def chip_rows(slab, k):
    far, near = slab.far - slab.core, slab.near - slab.core
    start = (far + lax.rem(k, 2) * (near - far)) * (2 * slab.half_rows)
    return pl.multiple_of(start, 2 * slab.half_rows)


def open_gathers(gathers, fill, prepare):
    fill(0)
    gathers[0].start()
    fill(1)
    gathers[0].second()
    gathers[1].start()
    prepare()
    gathers[0].forward()
    gathers[1].second()


def block_out(src, dst, sems, i):
    rows = step_rows(i, WIDE)
    return pltpu.make_async_copy(src.at[rows], dst.at[rows], sems.at[i])


def widen(packed, wide):
    heads = packed.shape[1] // HEAD

    def block(i):
        rows = step_rows(i, 128)
        for h in range(heads):
            piece = packed[rows, h * HEAD : (h + 1) * HEAD]
            blank = jnp.zeros((128, LANES - HEAD), jnp.bfloat16)
            wide[rows, h * LANES : (h + 1) * LANES] = jnp.concatenate([piece, blank], axis=1)

    repeat(packed.shape[0] // 128, block)


def split_tail(packed, tails, up_cols):
    start = packed.shape[1] - LANES

    def block(i):
        rows = step_rows(i, 128)
        for j in range(2):
            piece = packed[rows, start + j * up_cols : start + (j + 1) * up_cols]
            blank = jnp.zeros((128, LANES - up_cols), jnp.bfloat16)
            tails[rows, j * LANES : (j + 1) * LANES] = jnp.concatenate([piece, blank], axis=1)

    repeat(packed.shape[0] // 128, block)


def up_dot(rows, packed, tails):
    main = (packed.shape[1] - LANES) // 2
    first = dot(rows, packed[:, :main], 1, 0)
    return jnp.concatenate([first, dot(rows, tails[:, :LANES], 1, 0)], axis=1)


def up_back(grads, packed, tails):
    main = (packed.shape[1] - LANES) // 2
    return dot(grads[:, :main], packed[:, :main], 1, 1) + dot(
        grads[:, main:], tails[:, :LANES], 1, 1
    )


def down_dot(active, packed, tails):
    main = (packed.shape[1] - LANES) // 2
    return dot(active[:, :main], packed[:, main : 2 * main], 1, 1) + dot(
        active[:, main:], tails[:, LANES:], 1, 1
    )


def down_back(rows, packed, tails):
    main = (packed.shape[1] - LANES) // 2
    first = dot(rows, packed[:, main : 2 * main], 1, 0)
    return jnp.concatenate([first, dot(rows, tails[:, LANES:], 1, 0)], axis=1)


def attn_forward_kernel(
    ready, at, layer, own_rows, rows_ref, vectors, bias_ref, lengths, packed_hbm, given_hbm, grads_ref,
    hidden_ref, lse_ref, normed_hbm, qkv_hbm, mixed_hbm, *rest
):
    micro, half_rows, width = rows_ref.shape
    gathered, gather_refs = rest[0], rest[0:3]
    scatter_refs = rest[3:9]
    terms = rest[3]
    packed, wide, qkv, mixed, load_sem, keep_sems, given_sems, all_grads, tile_send, tile_recv = rest[9:]
    vec, bias = vectors.at[layer], bias_ref[layer]
    seq = qkv.shape[1]
    pair = mixed.shape[2]
    heads = pair // LANES
    load = pltpu.make_async_copy(
        packed_hbm.at[:, at : at + packed.shape[1]], packed, load_sem
    )
    load.start()
    slab = Slab(half_rows)
    gathers = make_gathers(slab, gather_refs, micro)
    scatters = make_scatters(slab, scatter_refs, micro)
    given = [
        pltpu.make_async_copy(given_hbm.at[m], gathered.at[m], given_sems.at[m])
        for m in range(micro if ready else 0)
    ]
    for copy in given:
        copy.start()
    slab.greet()
    if ready:
        tiles = TileGather(all_grads, tile_send, tile_recv)
        for m in range(micro):
            own = tiles.tile(m, tiles.tensor)
            count = grads_ref.shape[1]
            own[:count] = grads_ref[m]
            own[count:] = jnp.zeros((tiles.tile_rows - count, width), jnp.bfloat16)
            tiles.start(m)

    def fill(m):
        own = slab.rows(gathered.at[m], slab.mine[0])
        for start in range(0, half_rows, 32):
            block = rows_ref[m, pl.ds(start, 32)].astype(jnp.float32)
            own[pl.ds(start, 32)] = low(layer_norm(block, vec[0:1], vec[2:3]))

    def prepare():
        load.wait()
        widen(packed, wide)

    if ready:
        prepare()
    else:
        open_gathers(gathers, fill, prepare)
    keeps = []

    def keep(src, dst, m, i):
        def copy():
            return pltpu.make_async_copy(src.at[m], dst.at[m], keep_sems.at[i])

        copy().start()
        keeps.append(copy)

    def project(m):
        def block(i):
            rows = step_rows(i, 4 * half_rows)
            out = dot(gathered[m, rows], wide[:, : 3 * pair], 1, 0)
            qkv[m, rows] = low(out + bias)

        repeat(seq // (4 * half_rows), block)

    def attend(m, rows):
        shut = shut_keys(lengths[m], own_rows, 2 * half_rows, (1, seq), 1)
        for h in range(heads):
            cols = slice(h * LANES, (h + 1) * LANES)
            q = qkv[m, rows, cols]
            k = qkv[m, :, pair + h * LANES : pair + (h + 1) * LANES]
            v = qkv[m, :, 2 * pair + h * LANES : 2 * pair + (h + 1) * LANES]
            scores = dot(q, k, 1, 1) * (score_scale * LOG2E) + shut
            top = jnp.max(scores, axis=-1, keepdims=True)
            exp_scores = jnp.exp2(scores - top)
            total = jnp.sum(exp_scores, axis=-1, keepdims=True)
            probs = low(exp_scores * (1.0 / total))
            mixed[m, rows, cols] = low(dot(probs, v, 1, 0))
            lse_ref[m, h, rows] = jnp.broadcast_to(
                top + jnp.log(total) * LOG2E, (2 * half_rows, LANES)
            )

    def output(m, rows):
        terms[m, rows] = low(dot(mixed[m, rows], wide[:, 3 * pair :], 1, 1))

    def close(m):
        scatters[m].finish()
        for rows in scatters[m].blocks():
            start = rows_ref[m, rows].astype(jnp.float32)
            hidden_ref[m, rows] = start + scatters[m].total(rows) + vec[5:6]

    def gathered_rows(m):
        if ready:
            given[m].wait()
            return
        gathers[m].to_mate()
        gathers[m].finish()
        keep(gathered, normed_hbm, m, m)

    def work(k):
        m = lax.div(k, 2)
        start = chip_rows(slab, k)
        pl.when(lax.rem(k, 2) == 0)(lambda: project(m))

        def piece(i):
            attend(m, step_from(start, i, 2 * half_rows))

        repeat(2, piece)
        output(m, pl.ds(start, 4 * half_rows))

    def keep_two(m):
        keep(qkv, qkv_hbm, m, 2 + 2 * m)
        keep(mixed, mixed_hbm, m, 3 + 2 * m)

    def grads_on():
        if ready:
            tiles.pass_on()

    def grads_in():
        if ready:
            tiles.finish()
            for m in range(micro):
                keep(all_grads, normed_hbm, m, m)

    gathered_rows(0)
    if not ready:
        gathers[1].forward()
    zero, one = scatters
    stages(
        4,
        work,
        {
            0: [zero.mate_far, lambda: gathered_rows(1), zero.far_hop],
            1: [zero.mate_near, lambda: keep_two(0), zero.second_hop, zero.first_hop, grads_on],
            2: [one.mate_far, lambda: close(0), one.far_hop, grads_in],
            3: [one.mate_near, lambda: keep_two(1), one.second_hop, one.first_hop],
        },
    )
    close(1)
    if ready:
        tiles.drain()
    for copy in keeps:
        copy().wait()


def ffn_forward_kernel(
    half_ff, at, layer, hidden_ref, vectors, up_biases, packed_hbm, out_ref, second_hbm, upper_hbm, *rest
):
    micro, half_rows, _ = hidden_ref.shape
    gathered, gather_refs = rest[0], rest[0:3]
    scatter_refs = rest[3:9]
    terms = rest[3]
    packed, tails, upper, load_sem, keep_sems = rest[9:]
    vec, up_bias = vectors.at[layer], up_biases.at[layer]
    _, ff = upper.shape[1:]
    load = pltpu.make_async_copy(
        packed_hbm.at[:, at : at + packed.shape[1]], packed, load_sem
    )
    load.start()
    slab = Slab(half_rows)
    gathers = make_gathers(slab, gather_refs, micro)
    scatters = make_scatters(slab, scatter_refs, micro)
    slab.greet()

    def fill(m):
        own = slab.rows(gathered.at[m], slab.mine[0])
        for start in range(0, half_rows, 32):
            block = hidden_ref[m, pl.ds(start, 32)]
            own[pl.ds(start, 32)] = low(layer_norm(block, vec[1:2], vec[6:7]))

    def prepare():
        load.wait()
        split_tail(packed, tails, half_ff - ff + LANES)

    open_gathers(gathers, fill, prepare)
    keeps = []

    def keep(src, dst, m, i):
        def copy():
            return pltpu.make_async_copy(src.at[m], dst.at[m], keep_sems.at[i])

        copy().start()
        keeps.append(copy)

    def compute(m, rows):
        value = up_dot(gathered[m, rows], packed, tails) + up_bias[...]
        upper[m, rows] = value
        active = low(gelu_tanh(value))
        terms[m, rows] = low(down_dot(active, packed, tails))

    def close(m):
        scatters[m].finish()
        for rows in scatters[m].blocks():
            out_ref[m, rows] = low(hidden_ref[m, rows] + scatters[m].total(rows) + vec[7:8])

    def work(k):
        compute(lax.div(k, 2), pl.ds(chip_rows(slab, k), 4 * half_rows))

    gathers[0].to_mate()
    gathers[0].finish()
    keep(gathered, second_hbm, 0, 0)
    zero, one = scatters
    stages(
        4,
        work,
        {
            0: [zero.mate_far, gathers[1].forward, zero.far_hop],
            1: [
                zero.mate_near,
                lambda: keep(upper, upper_hbm, 0, 1),
                gathers[1].to_mate,
                zero.second_hop,
                gathers[1].finish,
                lambda: keep(gathered, second_hbm, 1, 2),
            ],
            2: [one.mate_far, zero.first_hop, one.far_hop],
            3: [one.mate_near, lambda: keep(upper, upper_hbm, 1, 3), one.second_hop],
        },
    )
    close(0)
    one.first_hop()
    close(1)
    for copy in keeps:
        copy().wait()


def ffn_backward_kernel(
    half_ff, at, layer, grad_ref, hidden_ref, vectors, second_hbm, upper_hbm, packed_hbm,
    out_ref, grads_hbm, small_ref, up_bias_ref, *rest
):
    micro, half_rows, width = hidden_ref.shape
    gathered, gather_refs = rest[0], rest[0:3]
    scatter_refs = rest[3:9]
    terms = rest[3]
    packed, tails, second, upper, grad_upper, active, load_sems, grads_ref, grads_sems = rest[9:]
    vec = vectors.at[layer]
    seq, ff = upper.shape[1:]
    main = ff - LANES
    extra = half_ff - main
    load_packed = pltpu.make_async_copy(
        packed_hbm.at[:, at : at + packed.shape[1]], packed, load_sems.at[0]
    )
    load_packed.start()
    load_upper, load_second = [], []
    for m in range(micro):
        load_upper.append(
            pltpu.make_async_copy(upper_hbm.at[m], upper.at[m], load_sems.at[1 + m])
        )
        load_upper[m].start()
    for m in range(micro):
        load_second.append(
            pltpu.make_async_copy(second_hbm.at[m], second.at[m], load_sems.at[1 + micro + m])
        )
        load_second[m].start()
    slab = Slab(half_rows)
    gathers = make_gathers(slab, gather_refs, micro)
    scatters = make_scatters(slab, scatter_refs, micro)
    slab.greet()

    def fill(m):
        own = slab.rows(gathered.at[m], slab.mine[0])
        for start in range(0, half_rows, 32):
            own[pl.ds(start, 32)] = grad_ref[m, pl.ds(start, 32)]

    def prepare():
        small_ref[...] = jnp.zeros_like(small_ref)
        up_bias_ref[...] = jnp.zeros_like(up_bias_ref)
        load_packed.wait()
        split_tail(packed, tails, extra)

    open_gathers(gathers, fill, prepare)

    def compute(m, rows):
        value = upper[m, rows]
        square = value * value
        bent = jnp.tanh(GELU_A * value * (1.0 + GELU_B * square))
        half = 0.5 * (1.0 + bent)
        active[m, rows] = low(value * half)
        slope = half + (0.5 * GELU_A) * value * (1.0 - bent * bent) * (1.0 + 3.0 * GELU_B * square)
        grad_active = down_back(gathered[m, rows], packed, tails)
        grad = low(grad_active * slope)
        grad_upper[m, rows] = grad
        up_bias_ref[0:1] += jnp.sum(grad.astype(jnp.float32), axis=0, keepdims=True)
        terms[m, rows] = low(up_back(grad, packed, tails))

    def stacked(ref, cols=slice(None)):
        return ref[:, :, cols].reshape(micro * seq, -1)

    def weight_grads(hooks):
        def block(i):
            cols = step_rows(i, WIDE)
            up = dot(stacked(second, cols), stacked(grad_upper), 0, 0)
            down = dot(stacked(gathered, cols), stacked(active), 0, 0)
            grads_ref[cols, :main] = low(up[:, :main])
            grads_ref[cols, main : 2 * main] = low(down[:, :main])
            blank = jnp.zeros((WIDE, LANES - 2 * extra), jnp.float32)
            rest_cols = [up[:, main : main + extra], down[:, main : main + extra], blank]
            grads_ref[cols, 2 * main :] = low(jnp.concatenate(rest_cols, axis=1))
            block_out(grads_ref, grads_hbm, grads_sems, i).start()

        stages(width // WIDE, block, hooks)

    def grads_out():
        for i in range(width // WIDE):
            block_out(grads_ref, grads_hbm, grads_sems, i).wait()

    def close(m):
        scatters[m].finish()
        for rows in scatters[m].blocks():
            grad_normed = scatters[m].total(rows)
            back, gain_terms = norm_back(hidden_ref[m, rows], vec[1:2], grad_normed)
            grad_rows = grad_ref[m, rows].astype(jnp.float32)
            grad_hidden = grad_rows + back
            out_ref[m, rows] = grad_hidden
            branch = low(grad_hidden).astype(jnp.float32)
            for j, item in enumerate((gain_terms, grad_normed, grad_rows, branch)):
                small_ref[j : j + 1] += jnp.sum(item, axis=0, keepdims=True)

    def work(k):
        compute(lax.div(k, 2), pl.ds(chip_rows(slab, k), 4 * half_rows))

    gathers[0].to_mate()
    gathers[0].finish()
    load_upper[0].wait()
    zero, one = scatters
    stages(
        4,
        work,
        {
            0: [zero.mate_far, gathers[1].forward, zero.far_hop],
            1: [
                zero.mate_near,
                gathers[1].to_mate,
                zero.second_hop,
                gathers[1].finish,
                load_upper[1].wait,
            ],
            2: [one.mate_far, zero.first_hop, one.far_hop],
            3: [one.mate_near, one.second_hop],
        },
    )
    for load in load_second:
        load.wait()
    weight_grads({0: [one.first_hop, lambda: close(0)]})
    close(1)
    grads_out()


def ffn_turn_kernel(
    half_ff, at, layer, hidden_ref, grad_ref, vectors, up_biases, given_hbm, packed_hbm,
    out_ref, grad_out_ref, grads_hbm, small_ref, up_bias_ref, *rest
):
    micro, half_rows, width = hidden_ref.shape
    gathered, gather_refs = rest[0], rest[0:3]
    terms, back_terms = rest[3], rest[9]
    packed, tails, given, grad_upper, active, load_sem, given_sems, grads_ref, grads_sems = rest[15:]
    vec, up_bias = vectors.at[layer], up_biases.at[layer]
    seq, ff = active.shape[1:]
    main = ff - LANES
    extra = half_ff - main
    load = pltpu.make_async_copy(
        packed_hbm.at[:, at : at + packed.shape[1]], packed, load_sem
    )
    load.start()
    loads = [
        pltpu.make_async_copy(given_hbm.at[m], given.at[m], given_sems.at[m]) for m in range(micro)
    ]
    for copy in loads:
        copy.start()
    slab = Slab(half_rows)
    gathers = make_gathers(slab, gather_refs, micro)
    scatters = make_scatters(slab, rest[3:9], micro)
    backs = make_scatters(slab, rest[9:15], micro)
    slab.greet()

    def fill(m):
        own = slab.rows(gathered.at[m], slab.mine[0])
        for start in range(0, half_rows, 32):
            block = hidden_ref[m, pl.ds(start, 32)]
            own[pl.ds(start, 32)] = low(layer_norm(block, vec[1:2], vec[6:7]))

    def prepare():
        small_ref[...] = jnp.zeros_like(small_ref)
        up_bias_ref[...] = jnp.zeros_like(up_bias_ref)
        load.wait()
        split_tail(packed, tails, extra)

    open_gathers(gathers, fill, prepare)

    def compute(m, rows):
        value = up_dot(gathered[m, rows], packed, tails) + up_bias[...]
        square = value * value
        bent = jnp.tanh(GELU_A * value * (1.0 + GELU_B * square))
        half = 0.5 * (1.0 + bent)
        shown = low(value * half)
        active[m, rows] = shown
        slope = half + (0.5 * GELU_A) * value * (1.0 - bent * bent) * (1.0 + 3.0 * GELU_B * square)
        grad = low(down_back(given[m, rows], packed, tails) * slope)
        grad_upper[m, rows] = grad
        up_bias_ref[0:1] += jnp.sum(grad.astype(jnp.float32), axis=0, keepdims=True)
        back_terms[m, rows] = low(up_back(grad, packed, tails))
        terms[m, rows] = low(down_dot(shown, packed, tails))

    def stacked(ref, cols=slice(None)):
        return ref[:, :, cols].reshape(micro * seq, -1)

    def weight_grads(hooks):
        def block(i):
            cols = step_rows(i, WIDE)
            up = dot(stacked(gathered, cols), stacked(grad_upper), 0, 0)
            down = dot(stacked(given, cols), stacked(active), 0, 0)
            grads_ref[cols, :main] = low(up[:, :main])
            grads_ref[cols, main : 2 * main] = low(down[:, :main])
            blank = jnp.zeros((WIDE, LANES - 2 * extra), jnp.float32)
            rest_cols = [up[:, main : main + extra], down[:, main : main + extra], blank]
            grads_ref[cols, 2 * main :] = low(jnp.concatenate(rest_cols, axis=1))
            block_out(grads_ref, grads_hbm, grads_sems, i).start()

        stages(width // WIDE, block, hooks)

    def grads_out():
        for i in range(width // WIDE):
            block_out(grads_ref, grads_hbm, grads_sems, i).wait()

    def close_back(m):
        backs[m].finish()
        for rows in backs[m].blocks():
            grad_normed = backs[m].total(rows)
            back, gain_terms = norm_back(hidden_ref[m, rows], vec[1:2], grad_normed)
            grad_rows = grad_ref[m, rows].astype(jnp.float32)
            grad_hidden = grad_rows + back
            grad_out_ref[m, rows] = grad_hidden
            branch = low(grad_hidden).astype(jnp.float32)
            for j, item in enumerate((gain_terms, grad_normed, grad_rows, branch)):
                small_ref[j : j + 1] += jnp.sum(item, axis=0, keepdims=True)

    def close(m):
        scatters[m].finish()
        for rows in scatters[m].blocks():
            out_ref[m, rows] = low(hidden_ref[m, rows] + scatters[m].total(rows) + vec[7:8])

    def work(k):
        compute(lax.div(k, 2), pl.ds(chip_rows(slab, k), 4 * half_rows))

    gathers[0].to_mate()
    gathers[0].finish()
    loads[0].wait()
    zero, one = scatters
    back_zero, back_one = backs
    stages(
        4,
        work,
        {
            0: [back_zero.mate_far, zero.mate_far, gathers[1].forward, back_zero.far_hop],
            1: [
                back_zero.mate_near,
                zero.mate_near,
                gathers[1].to_mate,
                back_zero.second_hop,
                gathers[1].finish,
                zero.far_hop,
                zero.second_hop,
                loads[1].wait,
            ],
            2: [
                back_one.mate_far,
                one.mate_far,
                back_zero.first_hop,
                back_one.far_hop,
                zero.first_hop,
            ],
            3: [
                back_one.mate_near,
                one.mate_near,
                lambda: close_back(0),
                back_one.second_hop,
                one.far_hop,
                one.second_hop,
            ],
        },
    )
    weight_grads({0: [back_one.first_hop, one.first_hop]})
    close_back(1)
    for m in range(micro):
        close(m)
    grads_out()


def attn_backward_kernel(
    at, layer, own_rows, both_ways, grad_ref, rows_ref, vectors, lse_hbm, lengths,
    normed_hbm, qkv_hbm, mixed_hbm, packed_hbm, errand_hbm, errand_one_hbm,
    out_ref, grads_hbm, small_ref, bias_ref, errand_got, *rest
):
    micro, half_rows, width = grad_ref.shape
    gathered, gather_refs = rest[0], rest[0:3]
    scatter_refs = rest[3:9]
    terms = rest[3]
    packed, wide, normed, qkv, mixed, grad_mixed, grad_qkv, turned, shut = rest[9:18]
    low_probs, grad_scores, high_probs, errand_sems, load_sems = rest[18:23]
    grads_ref, grads_sems, lse, lse_sem = rest[23:]
    load_lse = pltpu.make_async_copy(lse_hbm, lse, lse_sem)
    load_lse.start()
    vec = vectors.at[layer]
    seq, pair = mixed.shape[1:]
    heads = pair // LANES
    load_packed = pltpu.make_async_copy(
        packed_hbm.at[:, at : at + packed.shape[1]], packed, load_sems.at[0]
    )
    load_packed.start()
    load_qkv, load_rest = [], []
    for m in range(micro):
        load_qkv.append(pltpu.make_async_copy(qkv_hbm.at[m], qkv.at[m], load_sems.at[1 + 3 * m]))
        load_qkv[m].start()
    for m in range(micro):
        for k, (src, dst) in enumerate(((mixed_hbm, mixed), (normed_hbm, normed))):
            load = pltpu.make_async_copy(src.at[m], dst.at[m], load_sems.at[2 + k + 3 * m])
            load.start()
            load_rest.append(load)
    slab = Slab(half_rows)
    gathers = make_gathers(slab, gather_refs, micro)
    scatters = make_scatters(slab, scatter_refs, micro)
    slab.greet()

    def fill(m):
        own = slab.rows(gathered.at[m], slab.mine[0])
        for start in range(0, half_rows, 32):
            own[pl.ds(start, 32)] = low(grad_ref[m, pl.ds(start, 32)])

    def head(h, part=0):
        return pl.ds(pl.multiple_of(part * pair + h * LANES, LANES), LANES)

    def ready_qkv(m):
        load_qkv[m].wait()
        shut[m] = shut_keys(lengths[m], own_rows, 2 * half_rows, (seq, LANES), 0)
        for h in range(heads):
            turned[m, h] = low(qkv[m, :, head(h, 1)].astype(jnp.float32).T)

    def find_probs(m, h):
        def block(i):
            rows = step_rows(i, TILE)
            keys, queries = qkv[m, :, head(h, 1)], qkv[m, rows, head(h)]
            closed = jnp.concatenate([shut[m]] * (TILE // LANES), axis=1)
            scores = dot(keys, queries, 1, 1) * (score_scale * LOG2E) + closed
            high_probs[m, h, :, rows] = jnp.exp2(scores - lse[m, h, rows].T[0:1])

        repeat(seq // TILE, block)

    def find_all(k):
        find_probs(lax.div(k, heads), lax.rem(k, heads))

    span = errand_hbm.shape[0]
    cut = round_up(span // 2, 16) if span > 16 else span // 2
    errands = []
    for k, part in enumerate((pl.ds(0, cut), pl.ds(cut, span - cut))):
        errands.append(
            [
                remote(
                    source.at[part],
                    errand_got.at[part],
                    errand_sems.at[0, k],
                    errand_sems.at[1, k],
                    {"section": 1 - lax.axis_index("section")},
                )
                for source in (errand_hbm, errand_one_hbm)
            ]
        )
    first_section = lax.axis_index("section") == 0
    sends_errand, gets_errand = first_section | both_ways, ~first_section | both_ways

    def prepare():
        small_ref[...] = jnp.zeros_like(small_ref)
        bias_ref[...] = jnp.zeros_like(bias_ref)
        load_packed.wait()
        widen(packed, wide)
        for m in range(micro):
            ready_qkv(m)
        load_lse.wait()

    fill(0)
    gathers[0].start()
    fill(1)
    gathers[0].second()
    gathers[1].start()
    prepare()

    def mix_grads(m):
        def block(i):
            rows = step_rows(i, 4 * half_rows)
            grad_mixed[m, rows] = low(dot(gathered[m, rows], wide[:, 3 * pair :], 1, 0))

        repeat(seq // (4 * half_rows), block)

    def attend(m, h):
        def block(i):
            rows = step_rows(i, TILE)
            grads = grad_mixed[m, rows, head(h)]
            probs = high_probs[m, h, :, rows]
            grad_probs = dot(qkv[m, :, head(h, 2)], grads, 1, 1)
            inner = jnp.sum(grad_probs * probs, axis=0, keepdims=True)
            low_probs[:, rows] = low(probs)
            grad_scores[:, rows] = low(probs * (grad_probs - inner))

        repeat(seq // TILE, block)
        grad_keys = dot(grad_scores[...], qkv[m, :, head(h)], 1, 0)
        grad_qkv[m, :, head(h, 1)] = low(grad_keys * score_scale)
        grad_qkv[m, :, head(h, 2)] = low(dot(low_probs[...], grad_mixed[m, :, head(h)], 1, 0))
        turn = dot(turned[m, h], grad_scores[...], 1, 0).T
        grad_qkv[m, :, head(h)] = low(turn * score_scale)

    def back_project(m, rows):
        grads = grad_qkv[m, rows]
        terms[m, rows] = low(dot(grads, wide[:, : 3 * pair], 1, 1))
        for j, part in enumerate((0, 2)):
            piece = grads[:, part * pair : (part + 1) * pair].astype(jnp.float32)
            bias_ref[j : j + 1] += jnp.sum(piece, axis=0, keepdims=True)

    def stacked(ref, cols=slice(None)):
        return ref[:, :, cols].reshape(micro * seq, -1)

    def weight_grads(hooks):
        def block(i):
            cols = step_rows(i, WIDE)
            front = dot(stacked(normed, cols), stacked(grad_qkv), 0, 0)
            back = dot(stacked(gathered, cols), stacked(mixed), 0, 0)
            total = low(jnp.concatenate([front, back], axis=1))
            pieces = [total[:, h * LANES : h * LANES + HEAD] for h in range(4 * heads)]
            grads_ref[cols] = jnp.concatenate(pieces, axis=1)
            block_out(grads_ref, grads_hbm, grads_sems, i).start()

        stages(width // WIDE, block, hooks)

    def close(m):
        scatters[m].finish()
        for rows in scatters[m].blocks():
            grad_normed = scatters[m].total(rows)
            back, gain_terms = norm_back(
                rows_ref[m, rows].astype(jnp.float32), vec[0:1], grad_normed
            )
            out_ref[m, rows] = low(grad_ref[m, rows] + back)
            for j, item in enumerate((gain_terms, grad_normed)):
                small_ref[j : j + 1] += jnp.sum(item, axis=0, keepdims=True)

    def start_errand(k):
        pl.when(first_section)(errands[k][0].start)
        if both_ways:
            pl.when(~first_section)(errands[k][1].start)

    stages(
        2 * heads,
        find_all,
        {
            0: [gathers[0].forward, gathers[1].second],
            1: [gathers[1].forward, gathers[0].to_mate, lambda: start_errand(0)],
        },
    )
    gathers[0].finish()
    zero, one = scatters
    attend_hooks = {
        0: [gathers[1].to_mate],
        heads - 1: [gathers[1].finish],
        heads: [zero.first_hop, lambda: start_errand(1)],
    }
    project_hooks = {
        0: [zero.mate_far, zero.far_hop],
        1: [zero.mate_near, zero.second_hop],
        2: [one.mate_far, one.far_hop],
        3: [one.mate_near, lambda: close(0), one.second_hop],
    }

    def hooked(at, hooks):
        for k, steps in hooks.items():

            @pl.when(at == k)
            def _():
                for step in steps:
                    step()

    def image(m):
        mix_grads(m)

        def one_head(h):
            attend(m, h)
            hooked(m * heads + h, attend_hooks)

        repeat(heads, one_head)

        def one_chip(i):
            back_project(m, pl.ds(chip_rows(slab, i), 4 * half_rows))
            hooked(2 * m + i, project_hooks)

        repeat(2, one_chip)

    repeat(micro, image)
    for load in load_rest:
        load.wait()
    weight_grads({0: [one.first_hop]})
    close(1)
    for i in range(width // WIDE):
        block_out(grads_ref, grads_hbm, grads_sems, i).wait()

    for errand, _ in errands:
        pl.when(sends_errand)(errand.wait_send)
        pl.when(gets_errand)(errand.wait_recv)


def any_spec():
    return pl.BlockSpec(memory_space=pl.ANY)


def vmem_spec():
    return pl.BlockSpec(memory_space=pltpu.VMEM)


def shape_of(shape, dtype):
    return jax.ShapeDtypeStruct(shape, dtype)


def params(collective):
    return pltpu.CompilerParams(
        collective_id=collective, has_side_effects=True, vmem_limit_bytes=VMEM_BYTES
    )


def smem_spec():
    return pl.BlockSpec(memory_space=pltpu.SMEM)


def attn_forward(rows_low, vectors, bias, packed, at, layer, lengths, own_rows, given=None, grads=None):
    micro, half_rows, width = rows_low.shape
    seq = 8 * half_rows
    pair = bias.shape[2] // 3
    heads = pair // LANES
    low_type, high_type = jnp.bfloat16, jnp.float32
    hidden, lse, normed, qkv, mixed = pl.pallas_call(
        functools.partial(attn_forward_kernel, given is not None, at, layer, own_rows),
        out_shape=[
            shape_of((micro, half_rows, width), high_type),
            shape_of((micro, heads, seq, LANES), high_type),
            shape_of((micro, seq, width), low_type),
            shape_of((micro, seq, 3 * pair), low_type),
            shape_of((micro, seq, pair), low_type),
        ],
        in_specs=[vmem_spec()] * 3 + [smem_spec(), any_spec(), any_spec(), vmem_spec()],
        out_specs=[vmem_spec()] * 2 + [any_spec()] * 3,
        scratch_shapes=gather_scratch(micro, seq, width)
        + scatter_scratch(micro, seq, half_rows, width)
        + [
            pltpu.VMEM((width, 4 * heads * HEAD), low_type),
            pltpu.VMEM((width, 4 * pair), low_type),
            pltpu.VMEM((micro, seq, 3 * pair), low_type),
            pltpu.VMEM((micro, seq, pair), low_type),
            pltpu.SemaphoreType.DMA,
            pltpu.SemaphoreType.DMA((6,)),
            pltpu.SemaphoreType.DMA((micro,)),
            pltpu.VMEM((micro, seq if given is not None else 32, width), low_type),
            pltpu.SemaphoreType.DMA((micro, 3)),
            pltpu.SemaphoreType.DMA((micro, 3)),
        ],
        compiler_params=params(0 if given is None else 6),
        cost_estimate=COST,
        name="attn_forward",
    )(
        rows_low,
        vectors,
        bias,
        lengths,
        packed,
        packed if given is None else given,
        rows_low if grads is None else grads,
    )
    if given is None:
        return hidden, (normed, qkv, lse, mixed)
    return hidden, (given, qkv, lse, mixed), normed


def ffn_forward(hidden, vectors, up_biases, packed, at, layer, half_ff):
    micro, half_rows, width = hidden.shape
    seq = 8 * half_rows
    ff = up_biases.shape[2]
    packed_cols = 2 * ff - LANES
    low_type, high_type = jnp.bfloat16, jnp.float32
    out, second, upper = pl.pallas_call(
        functools.partial(ffn_forward_kernel, half_ff, at, layer),
        out_shape=[
            shape_of((micro, half_rows, width), low_type),
            shape_of((micro, seq, width), low_type),
            shape_of((micro, seq, ff), high_type),
        ],
        in_specs=[vmem_spec()] * 3 + [any_spec()],
        out_specs=[vmem_spec()] + [any_spec()] * 2,
        scratch_shapes=gather_scratch(micro, seq, width)
        + scatter_scratch(micro, seq, half_rows, width)
        + [
            pltpu.VMEM((width, packed_cols), low_type),
            pltpu.VMEM((width, 2 * LANES), low_type),
            pltpu.VMEM((micro, seq, ff), high_type),
            pltpu.SemaphoreType.DMA,
            pltpu.SemaphoreType.DMA((4,)),
        ],
        compiler_params=params(1),
        cost_estimate=COST,
        name="ffn_forward",
    )(hidden, vectors, up_biases, packed)
    return out, (second, upper)


def ffn_turn(hidden, grad_low, given, vectors, up_biases, packed, at, layer, half_ff):
    micro, half_rows, width = hidden.shape
    seq = 8 * half_rows
    ff = up_biases.shape[2]
    low_type, high_type = jnp.bfloat16, jnp.float32
    out, grad_hidden, grads, small, up_bias = pl.pallas_call(
        functools.partial(ffn_turn_kernel, half_ff, at, layer),
        out_shape=[
            shape_of((micro, half_rows, width), low_type),
            shape_of((micro, half_rows, width), high_type),
            shape_of((width, 2 * ff - LANES), low_type),
            shape_of((8, width), high_type),
            shape_of((8, ff), high_type),
        ],
        in_specs=[vmem_spec()] * 4 + [any_spec()] * 2,
        out_specs=[vmem_spec()] * 2 + [any_spec()] + [vmem_spec()] * 2,
        scratch_shapes=gather_scratch(micro, seq, width)
        + scatter_scratch(micro, seq, half_rows, width)
        + scatter_scratch(micro, seq, half_rows, width)
        + [
            pltpu.VMEM((width, 2 * ff - LANES), low_type),
            pltpu.VMEM((width, 2 * LANES), low_type),
            pltpu.VMEM((micro, seq, width), low_type),
            pltpu.VMEM((micro, seq, ff), low_type),
            pltpu.VMEM((micro, seq, ff), low_type),
            pltpu.SemaphoreType.DMA,
            pltpu.SemaphoreType.DMA((micro,)),
            pltpu.VMEM((width, 2 * ff - LANES), low_type),
            pltpu.SemaphoreType.DMA((width // WIDE,)),
        ],
        compiler_params=params(7),
        cost_estimate=COST,
        name="ffn_turn",
    )(hidden, grad_low, vectors, up_biases, given, packed)
    return out, grad_hidden, grads, small, up_bias


def ffn_backward(grad_low, hidden, kept, vectors, packed, at, layer, half_ff):
    second, upper = kept
    micro, half_rows, width = hidden.shape
    seq, ff = upper.shape[1:]
    low_type, high_type = jnp.bfloat16, jnp.float32
    grad_hidden, grads, small, up_bias = pl.pallas_call(
        functools.partial(ffn_backward_kernel, half_ff, at, layer),
        out_shape=[
            shape_of((micro, half_rows, width), high_type),
            shape_of((width, 2 * ff - LANES), low_type),
            shape_of((8, width), high_type),
            shape_of((8, ff), high_type),
        ],
        in_specs=[vmem_spec()] * 3 + [any_spec()] * 3,
        out_specs=[vmem_spec(), any_spec()] + [vmem_spec()] * 2,
        scratch_shapes=gather_scratch(micro, seq, width)
        + scatter_scratch(micro, seq, half_rows, width)
        + [
            pltpu.VMEM((width, 2 * ff - LANES), low_type),
            pltpu.VMEM((width, 2 * LANES), low_type),
            pltpu.VMEM((micro, seq, width), low_type),
            pltpu.VMEM((micro, seq, ff), high_type),
            pltpu.VMEM((micro, seq, ff), low_type),
            pltpu.VMEM((micro, seq, ff), low_type),
            pltpu.SemaphoreType.DMA((1 + 2 * micro,)),
            pltpu.VMEM((width, 2 * ff - LANES), low_type),
            pltpu.SemaphoreType.DMA((width // WIDE,)),
        ],
        compiler_params=params(2),
        cost_estimate=COST,
        name="ffn_backward",
    )(grad_low, hidden, vectors, second, upper, packed)
    return grad_hidden, grads, small, up_bias


def attn_backward(
    grad_hidden, rows_low, kept, vectors, packed, at, layer, lengths, own_rows, errand, both_ways
):
    normed, qkv, lse, mixed = kept
    micro, half_rows, width = grad_hidden.shape
    seq, pair = mixed.shape[1:]
    heads = pair // LANES
    low_type, high_type = jnp.bfloat16, jnp.float32
    out, grads, small, bias, got = pl.pallas_call(
        functools.partial(attn_backward_kernel, at, layer, own_rows, both_ways),
        out_shape=[
            shape_of((micro, half_rows, width), low_type),
            shape_of((width, 4 * heads * HEAD), low_type),
            shape_of((8, width), high_type),
            shape_of((8, pair), high_type),
            shape_of(errand[0].shape, errand[0].dtype),
        ],
        in_specs=[vmem_spec()] * 3 + [any_spec(), smem_spec()] + [any_spec()] * 6,
        out_specs=[vmem_spec(), any_spec()] + [vmem_spec()] * 2 + [any_spec()],
        scratch_shapes=gather_scratch(micro, seq, width)
        + scatter_scratch(micro, seq, half_rows, width)
        + [
            pltpu.VMEM((width, 4 * heads * HEAD), low_type),
            pltpu.VMEM((width, 4 * pair), low_type),
            pltpu.VMEM((micro, seq, width), low_type),
            pltpu.VMEM((micro, seq, 3 * pair), low_type),
            pltpu.VMEM((micro, seq, pair), low_type),
            pltpu.VMEM((micro, seq, pair), low_type),
            pltpu.VMEM((micro, seq, 3 * pair), low_type),
            pltpu.VMEM((micro, heads, LANES, seq), low_type),
            pltpu.VMEM((micro, seq, LANES), high_type),
            pltpu.VMEM((seq, seq), low_type),
            pltpu.VMEM((seq, seq), low_type),
            pltpu.VMEM((micro, heads, seq, seq), high_type),
            pltpu.SemaphoreType.DMA((2, 2)),
            pltpu.SemaphoreType.DMA((1 + 3 * micro,)),
            pltpu.VMEM((width, 4 * heads * HEAD), low_type),
            pltpu.SemaphoreType.DMA((width // WIDE,)),
            pltpu.VMEM(lse.shape, high_type),
            pltpu.SemaphoreType.DMA,
        ],
        compiler_params=params(3 + 5 * layer),
        cost_estimate=COST,
        name="attn_backward",
    )(grad_hidden, rows_low, vectors, lse, lengths, normed, qkv, mixed, packed, *errand)
    return out, grads, small, bias, got


def slab_peers():
    section, tensor = lax.axis_index("section"), lax.axis_index("tensor")
    peers = []
    for role in range(1, 8):
        far, step = role // 4, role % 4
        other = section + far * (1 - 2 * section)
        to = (other, lax.rem(tensor + step, 4))
        source = (other, lax.rem(tensor + 4 - step, 4))
        peers.append((role, to, source))
    return peers


def column_peers(count):
    here = lax.axis_index("dp")
    return [
        (step, lax.rem(here + step, count), lax.rem(here + count - step, count))
        for step in range(1, count)
    ]


def greet_all(count):
    barrier = pltpu.get_barrier_semaphore()
    for _, to, _ in slab_peers():
        pl.semaphore_signal(barrier, inc=1, device_id=named(to), device_id_type=MESH)
    for _, to, _ in column_peers(count):
        pl.semaphore_signal(barrier, inc=1, device_id={"dp": to}, device_id_type=MESH)
    pl.semaphore_wait(barrier, 7 + count - 1)


def remote(src, dst, send_sem, recv_sem, peer):
    return pltpu.make_async_remote_copy(
        src_ref=src,
        dst_ref=dst,
        send_sem=send_sem,
        recv_sem=recv_sem,
        device_id=peer,
        device_id_type=MESH,
    )


def prologue_kernel(
    count, heads, qkv_ref, out_ref_in, up_ref_in, down_ref_t, gains_ref, shifts_ref, up_bias, rows_ref,
    first_hbm, normed_hbm, attn_ref, ff_zero_hbm, ff_one_hbm, out_ref, up_ref, bias_ref,
    attn_parts, ff_parts, up_halves, mine_ref, all_rows, line, ff_line, column, slab, up_got,
    rows_send, rows_recv, column_send, column_recv, slab_send, slab_recv, swap_send, swap_recv,
    right_send, right_recv, left_send, left_recv, out_sems,
):
    section, tensor, here = (lax.axis_index(name) for name in ("section", "tensor", "dp"))
    width = out_ref.shape[2]
    chunk = width // (4 * count)
    rows = attn_parts.shape[1]
    micro, own_rows = rows_ref.shape[:2]
    pieces = swap_send.shape[0] - 2
    size = rows // pieces
    other = {"section": 1 - section}
    pair = heads * LANES
    pair_cols = heads * HEAD
    half_ff = up_ref_in.shape[1] // 2
    main = half_ff // LANES * LANES
    extra = half_ff - main
    greet_all(count)
    out_turned = low(out_ref_in[...].astype(jnp.float32).T)
    for half in range(2):
        span = slice(half * pair_cols, (half + 1) * pair_cols)
        parts = [qkv_ref[k, :, span] for k in range(3)] + [out_turned[:, span]]
        attn_parts[half] = jnp.concatenate(parts, axis=1)
    keep_slot = jnp.where(section == 0, here, count)
    send_slot = jnp.where(section == 0, here, count)
    got_slot = jnp.where(section == 0, count, here)
    sent = []
    for p in range(pieces):
        span = pl.ds(p * size, size)
        copy = remote(
            attn_parts.at[1 - section, span],
            line.at[send_slot, span],
            swap_send.at[p],
            swap_recv.at[p],
            other,
        )
        copy.start()
        sent.append(copy)
    line[keep_slot] = attn_parts[section]
    mine_ref[...] = jnp.zeros_like(mine_ref)
    gains = gains_ref.shape[0]
    mine_ref[:gains, :chunk] = gains_ref[...]
    for i in range(shifts_ref.shape[0]):
        mine_ref[gains + i : gains + i + 1, :chunk] = shifts_ref[i]
    column[here] = mine_ref[...]
    for step, to, _ in column_peers(count):
        copy = remote(
            mine_ref, column.at[here], column_send.at[step], column_recv.at[step], {"dp": to}
        )
        copy.start()
        sent.append(copy)

    def swapped(p):
        got = line.at[got_slot, pl.ds(p * size, size)]
        remote(got, got, swap_send.at[p], swap_recv.at[p], other).wait_recv()

    def hop(step, p, way, finish=False):
        origin = here - way * step
        sends, recvs = (right_send, right_recv) if way == 1 else (left_send, left_recv)
        inside = (origin >= 0) if way == 1 else (origin < count)
        onward = (here + 1 < count) if way == 1 else (here > 0)
        slot = line.at[jnp.clip(origin, 0, count - 1), pl.ds(p * size, size)]
        target = jnp.clip(here + way, 0, count - 1)
        if step > 0 and not finish:

            @pl.when(inside)
            def _():
                remote(slot, slot, sends.at[step, p], recvs.at[step, p], {"dp": target}).wait_recv()

        if step + 1 < count:

            @pl.when(inside & onward)
            def _():
                copy = remote(
                    slot, slot, sends.at[step, p], recvs.at[step + 1, p], {"dp": target}
                )
                if finish:
                    copy.wait_send()
                else:
                    copy.start()

    def hops(step):
        for p in range(pieces):
            for way in (1, -1):
                hop(step, p, way)

    for step, _, source in column_peers(count):
        slot = column.at[source]
        remote(slot, slot, column_send.at[step], column_recv.at[step], {"dp": source}).wait_recv()
    for role, to, _ in slab_peers():
        copy = remote(
            column, slab.at[section, tensor], slab_send.at[role], slab_recv.at[role], named(to)
        )
        copy.start()
        sent.append(copy)
    slab[section, tensor] = column[...]
    for p in range(pieces):

        @pl.when(section == 1)
        def _():
            swapped(p)

        for way in (1, -1):
            hop(0, p, way)
    blank = jnp.zeros((rows, LANES - 2 * extra), jnp.bfloat16)
    up_halves[...] = jnp.zeros_like(up_halves)
    for half in range(2):
        start = half * half_ff
        up_halves[half, :, :half_ff] = up_bias[:, start : start + half_ff]
        ff_parts[half, :, :main] = up_ref_in[:, start : start + main]
        ff_parts[half, :, main : 2 * main] = down_ref_t[:, start : start + main]
        span = slice(start + main, start + half_ff)
        ff_parts[half, :, 2 * main :] = jnp.concatenate(
            [up_ref_in[:, span], down_ref_t[:, span], blank], axis=1
        )
    ff_swap = remote(
        ff_parts.at[1 - section],
        ff_line.at[section],
        swap_send.at[pieces],
        swap_recv.at[pieces],
        other,
    )
    up_swap = remote(
        up_halves.at[1 - section],
        up_got.at[section],
        swap_send.at[pieces + 1],
        swap_recv.at[pieces + 1],
        other,
    )
    up_swap.start()
    for role, _, source in slab_peers():
        slot = slab.at[source[0], source[1]]
        remote(slot, slot, slab_send.at[role], slab_recv.at[role], named(source)).wait_recv()
    ff_swap.start()
    for layer in range(2):
        for part in range(4 * count):
            piece = slab[layer, part % 4, part // 4]
            out_ref[layer, :, part * chunk : (part + 1) * chunk] = piece[:, :chunk]
    tiles = TileGather(all_rows, rows_send, rows_recv)
    for m in range(micro):
        own = tiles.tile(m, tensor)
        for begin in range(0, own_rows, 32):
            end = min(begin + 32, own_rows)
            block = rows_ref[m, begin:end].astype(jnp.float32)
            own[begin:end] = low(layer_norm(block, out_ref[0, 0:1], out_ref[0, 2:3]))
        own[own_rows:] = jnp.zeros((tiles.tile_rows - own_rows, width), jnp.bfloat16)
    for m in range(micro):
        tiles.start(m)
    hops(1)
    start = (2 * tensor + section) * pair_cols
    for layer in range(2):
        turned = pltpu.roll(out_ref[layer], lax.rem(width - start, width), 1)
        empty = jnp.zeros((1, LANES - HEAD), jnp.float32)
        for part, row in ((0, 3), (2, 4)):
            for h in range(heads):
                at = part * pair + h * LANES
                piece = turned[row : row + 1, h * HEAD : (h + 1) * HEAD]
                bias_ref[layer, :, at : at + LANES] = jnp.concatenate([piece, empty], 1)
        bias_ref[layer, :, pair : 2 * pair] = jnp.zeros((1, pair), jnp.float32)
    up_ref[section] = up_halves[section]
    outs = []

    def put(src, dst, i):
        copy = pltpu.make_async_copy(src, dst, out_sems.at[i])
        copy.start()
        outs.append(copy)

    def put_ff(src, section_of_first, i):
        for layer, dst in enumerate((ff_zero_hbm, ff_one_hbm)):
            here_too = layer if section_of_first == 0 else 1 - layer

            @pl.when(section == here_too)
            def _():
                pltpu.make_async_copy(src, dst, out_sems.at[i]).start()

        outs.append(pltpu.make_async_copy(src, ff_zero_hbm, out_sems.at[i]))

    put_ff(ff_parts.at[section], 0, count)
    for step in range(2, count):
        hops(step)
        if step == 2:
            tiles.pass_on()
    if count <= 2:
        tiles.pass_on()
    for p in range(pieces):

        @pl.when(section == 0)
        def _():
            swapped(p)

    for at in range(count):
        put(line.at[at], first_hbm.at[pl.ds(at * rows, rows)], at)
    attn_ref[...] = line[count]
    got = up_got.at[1 - section]
    remote(got, got, swap_send.at[pieces + 1], swap_recv.at[pieces + 1], other).wait_recv()
    up_ref[1 - section] = up_got[1 - section]
    tiles.finish()
    put(all_rows, normed_hbm, count + 2)
    ff_got = ff_line.at[1 - section]
    remote(ff_got, ff_got, swap_send.at[pieces], swap_recv.at[pieces], other).wait_recv()
    put_ff(ff_got, 1, count + 1)
    for step in range(count):
        for p in range(pieces):
            for way in (1, -1):
                hop(step, p, way, True)
    for copy in sent + [ff_swap, up_swap]:
        copy.wait_send()
    tiles.drain()
    for copy in outs:
        copy.wait()


def prologue(qkv, out, up, down_t, gains, shifts, up_bias, rows_low, count, heads, tile_rows):
    part_rows = qkv.shape[1]
    micro, _, width = rows_low.shape
    vector_rows = gains.shape[0] + shifts.shape[0]
    half_ff = up.shape[1] // 2
    ff_wide = round_up(half_ff, LANES)
    attn_shape = (part_rows, 4 * heads * HEAD)
    ff_shape = (2, part_rows, 2 * ff_wide - LANES)
    all_rows = (micro, 4 * tile_rows, width)
    pieces = 3 if part_rows % 96 == 0 else 1
    low_type, high_type = jnp.bfloat16, jnp.float32
    dma = pltpu.SemaphoreType.DMA
    return pl.pallas_call(
        functools.partial(prologue_kernel, count, heads),
        out_shape=[
            shape_of((count * part_rows, attn_shape[1]), low_type),
            shape_of(all_rows, low_type),
            shape_of(attn_shape, low_type),
            shape_of(ff_shape[1:], low_type),
            shape_of(ff_shape[1:], low_type),
            shape_of((2, vector_rows, width), high_type),
            shape_of((2, 1, ff_wide), high_type),
            shape_of((2, 1, 3 * heads * LANES), high_type),
        ],
        in_specs=[vmem_spec()] * 8,
        out_specs=[any_spec()] * 2 + [vmem_spec()] + [any_spec()] * 2 + [vmem_spec()] * 3,
        scratch_shapes=[
            pltpu.VMEM((2,) + attn_shape, low_type),
            pltpu.VMEM(ff_shape, low_type),
            pltpu.VMEM((2, 1, ff_wide), high_type),
            pltpu.VMEM((vector_rows, LANES), high_type),
            pltpu.VMEM(all_rows, low_type),
            pltpu.VMEM((count + 1,) + attn_shape, low_type),
            pltpu.VMEM(ff_shape, low_type),
            pltpu.VMEM((count, vector_rows, LANES), high_type),
            pltpu.VMEM((2, 4, count, vector_rows, LANES), high_type),
            pltpu.VMEM((2, 1, ff_wide), high_type),
            dma((micro, 3)),
            dma((micro, 3)),
            dma((count,)),
            dma((count,)),
            dma((8,)),
            dma((8,)),
            dma((pieces + 2,)),
            dma((pieces + 2,)),
            dma((count, pieces)),
            dma((count, pieces)),
            dma((count, pieces)),
            dma((count, pieces)),
            dma((count + 3,)),
        ],
        compiler_params=params(4),
        cost_estimate=COST,
        name="prologue",
    )(qkv, out, up, down_t, gains, shifts, up_bias, rows_low)


def home_kernel(
    count, chunk, attn_zero, attn_one, ff_zero, ff_one, bias_zero, bias_one, up_zero, up_one,
    ff_sum_hbm, attn_sum_hbm, rows_zero_hbm, rows_one_hbm,
    out_ref, up_ref, ff_got_hbm, attn_got_hbm, rows_got_hbm,
    parts, ups, slab, column, up_pair, up_column, total,
    column_send, column_recv, slab_send, slab_recv, up_sems, up_column_send, up_column_recv, far_send, far_recv,
):
    section, tensor, here = (lax.axis_index(name) for name in ("section", "tensor", "dp"))
    width = attn_zero.shape[1]
    heads = bias_zero.shape[1] // LANES
    biases_in, ups_in = (bias_zero, bias_one), (up_zero, up_one)
    other = {"section": 1 - section}
    greet_all(count)
    parts[...] = jnp.zeros_like(parts)
    start = (2 * tensor + section) * (heads * HEAD)
    for layer, (attn, ff) in enumerate(((attn_zero, ff_zero), (attn_one, ff_one))):
        bias = biases_in[layer][...]
        blank = jnp.zeros((8, width - heads * HEAD), jnp.float32)
        pieces = [bias[:, h * LANES : h * LANES + HEAD] for h in range(heads)]
        placed = pltpu.roll(jnp.concatenate(pieces + [blank], 1), start, 1)
        whole = jnp.concatenate(
            [attn[0:1], ff[0:1], attn[1:2], placed[0:2], ff[3:4], ff[1:2], ff[2:3]], axis=0
        )
        for part in range(4 * count):
            piece = whole[:, part * chunk : (part + 1) * chunk]
            parts[layer, part % 4, part // 4, :, :chunk] = piece
        ups[layer] = ups_in[layer][0:1]
    sent = []

    def send(src, dst, send_sem, recv_sem, peer):
        copy = remote(src, dst, send_sem, recv_sem, peer)
        copy.start()
        sent.append(copy)

    send(ups.at[1 - section], up_pair.at[section], up_sems.at[0], up_sems.at[1], other)
    for role, to, _ in slab_peers():
        send(
            parts.at[to[0], to[1]], slab.at[role], slab_send.at[role], slab_recv.at[role], named(to)
        )
    far_rows = remote(rows_zero_hbm, rows_got_hbm, far_send.at[0], far_recv.at[0], other)
    far_rows_one = remote(rows_one_hbm, rows_got_hbm, far_send.at[0], far_recv.at[0], other)
    far_ff = remote(ff_sum_hbm, ff_got_hbm, far_send.at[1], far_recv.at[1], other)
    far_attn = remote(attn_sum_hbm, attn_got_hbm, far_send.at[2], far_recv.at[2], other)
    one_way = ((far_ff, 1), (far_attn, 0))
    pl.when(section == 1)(far_rows.start)
    pl.when(section == 0)(far_rows_one.start)
    for copy, source in one_way:
        pl.when(section == source)(copy.start)
    up_pair[section] = ups[section]
    value = parts[section, tensor]
    for role, _, source in slab_peers():
        slot = slab.at[role]
        remote(slot, slot, slab_send.at[role], slab_recv.at[role], named(source)).wait_recv()
        value = value + slab[role]
    total[...] = value
    for step, to, _ in column_peers(count):
        send(total.at[to], column.at[step], column_send.at[step], column_recv.at[step], {"dp": to})
    got = up_pair.at[1 - section]
    remote(got, got, up_sems.at[0], up_sems.at[1], other).wait_recv()
    for step, to, _ in column_peers(count):
        send(
            up_pair, up_column.at[here], up_column_send.at[step], up_column_recv.at[step], {"dp": to}
        )
    up_column[here] = up_pair[...]
    result = total[here]
    for step, _, source in column_peers(count):
        slot = column.at[step]
        remote(slot, slot, column_send.at[step], column_recv.at[step], {"dp": source}).wait_recv()
        result = result + column[step]
    out_ref[...] = result
    for step, _, source in column_peers(count):
        slot = up_column.at[source]
        remote(
            slot, slot, up_column_send.at[step], up_column_recv.at[step], {"dp": source}
        ).wait_recv()
    value = up_column[0]
    for at in range(1, count):
        value = value + up_column[at]
    up_ref[...] = value
    far_rows.wait()
    for copy, source in one_way:
        pl.when(section == source)(copy.wait_send)
        pl.when(section != source)(copy.wait_recv)
    for copy in sent:
        copy.wait_send()


def home(attn_small, ff_small, bias_grads, up_grads, ff_sum, attn_sum, rows, count, chunk):
    vector_rows, lanes = 8, LANES
    up_shape = (1, up_grads[0].shape[1])
    dma = pltpu.SemaphoreType.DMA
    high_type = jnp.float32
    return pl.pallas_call(
        functools.partial(home_kernel, count, chunk),
        out_shape=[
            shape_of((vector_rows, lanes), high_type),
            shape_of((2,) + up_shape, high_type),
            shape_of(ff_sum.shape, ff_sum.dtype),
            shape_of(attn_sum.shape, attn_sum.dtype),
            shape_of(rows[0].shape, rows[0].dtype),
        ],
        in_specs=[vmem_spec()] * 8 + [any_spec()] * 4,
        out_specs=[vmem_spec()] * 2 + [any_spec()] * 3,
        scratch_shapes=[
            pltpu.VMEM((2, 4, count, vector_rows, lanes), high_type),
            pltpu.VMEM((2,) + up_shape, high_type),
            pltpu.VMEM((8, count, vector_rows, lanes), high_type),
            pltpu.VMEM((count, vector_rows, lanes), high_type),
            pltpu.VMEM((2,) + up_shape, high_type),
            pltpu.VMEM((count, 2) + up_shape, high_type),
            pltpu.VMEM((count, vector_rows, lanes), high_type),
            dma((count,)),
            dma((count,)),
            dma((8,)),
            dma((8,)),
            dma((2,)),
            dma((count,)),
            dma((count,)),
            dma((3,)),
            dma((3,)),
        ],
        compiler_params=params(5),
        cost_estimate=COST,
        name="home",
    )(*attn_small, *ff_small, *bias_grads, *up_grads, ff_sum, attn_sum, *rows)


def ff_finish_kernel(zero, one, zero_got, one_got, up_ref, down_ref):
    first = lax.axis_index("section") == 0
    halves = (
        jnp.where(first, zero[...], one_got[...]),
        jnp.where(first, zero_got[...], one[...]),
    )
    half_ff = up_ref.shape[1] // 2
    main = half_ff // LANES * LANES
    extra = half_ff - main
    for k in range(2):
        pieces = []
        for half in halves:
            start = 2 * main + k * extra
            pieces += [half[:, k * main : (k + 1) * main], half[:, start : start + extra]]
        whole = jnp.concatenate(pieces, axis=1).astype(jnp.float32)
        (up_ref, down_ref)[k][...] = whole


def ff_finish(sums, got, ff_cols):
    rows = sums[0].shape[0]
    return pl.pallas_call(
        ff_finish_kernel,
        out_shape=[
            shape_of((rows, ff_cols), jnp.float32),
            shape_of((rows, ff_cols), jnp.float32),
        ],
        in_specs=[vmem_spec()] * 4,
        out_specs=[vmem_spec()] * 2,
        compiler_params=pltpu.CompilerParams(vmem_limit_bytes=VMEM_BYTES),
        cost_estimate=COST,
        name="ff_finish",
    )(*sums, *got)


def attn_finish_kernel(zero, one, zero_got, one_got, qkv_ref, out_ref):
    first = lax.axis_index("section") == 0
    halves = (
        jnp.where(first, zero[...], one_got[...]),
        jnp.where(first, zero_got[...], one[...]),
    )
    pair_cols = qkv_ref.shape[2] // 2
    for k in range(4):
        span = slice(k * pair_cols, (k + 1) * pair_cols)
        whole = jnp.concatenate([half[:, span] for half in halves], axis=1).astype(jnp.float32)
        if k < 3:
            qkv_ref[k] = whole
        else:
            out_ref[...] = whole.T


def attn_finish(sums, got, head_cols):
    rows = sums[0].shape[0]
    return pl.pallas_call(
        attn_finish_kernel,
        out_shape=[
            shape_of((3, rows, head_cols), jnp.float32),
            shape_of((head_cols, rows), jnp.float32),
        ],
        in_specs=[vmem_spec()] * 4,
        out_specs=[vmem_spec()] * 2,
        compiler_params=pltpu.CompilerParams(vmem_limit_bytes=VMEM_BYTES),
        name="attn_finish",
    )(*sums, *got)


def shards(
    section_input,
    final_cotangent,
    lengths,
    qkv_weight,
    out_weight,
    up_weight,
    down_weight,
    norm_gains,
    biases,
    up_bias,
):
    here = lax.axis_index("section")
    sections = lax.axis_size("section")
    micro, _, own_rows, _ = section_input.shape
    head_cols = qkv_weight.shape[3]
    pair_cols = head_cols // sections
    heads = pair_cols // HEAD
    ff_cols = up_weight.shape[2]
    half_ff = ff_cols // sections
    half_rows = round_up(-(-own_rows // sections), 32)
    full_rows = half_rows * sections

    def by_layer(mine, other):
        return [jnp.where(here == 0, mine, other), jnp.where(here == 0, other, mine)]

    count = lax.axis_size("dp")
    chunk = norm_gains.shape[2]
    first, normed, attn_part, ff_zero, ff_one, vectors, up_biases, bias_qv = prologue(
        qkv_weight[0],
        out_weight[0],
        up_weight[0],
        down_weight[0].T,
        norm_gains[0],
        biases.transpose(1, 0, 2),
        up_bias,
        section_input[:, 0],
        count,
        heads,
        full_rows,
    )

    def gather_column(part):
        return lax.all_gather(part, "dp", axis=0, tiled=True)

    ff_first = gather_column(ff_zero)
    attn_packed = [(first, 0), (gather_column(attn_part), 0)]
    ff_packed = [(ff_first, 0), (gather_column(ff_one), 0)]
    lengths_here = lengths.reshape(micro)

    def my_rows(value):
        padded = jnp.pad(value[:, 0], [(0, 0), (0, full_rows - own_rows), (0, 0)])
        return lax.dynamic_slice_in_dim(padded, here * half_rows, half_rows, 1)

    def whole_rows(first, second, got):
        low_half, high_half = by_layer(jnp.where(here == 0, first, second), got)
        return jnp.concatenate([low_half, high_half], 1)[:, None, :own_rows]

    rows = my_rows(section_input)
    inputs, hiddens, attn_kept = [], [], []
    for layer in range(2):
        inputs.append(rows)
        operands = (rows, vectors, bias_qv, *attn_packed[layer], layer, lengths_here, own_rows)
        if layer == 0:
            hidden, kept, grads_all = attn_forward(*operands, normed, final_cotangent[:, 0])
        else:
            hidden, kept = attn_forward(*operands)
        hiddens.append(hidden)
        attn_kept.append(kept)
        if layer == 0:
            rows, ff_kept = ffn_forward(hidden, vectors, up_biases, *ff_packed[0], 0, half_ff)

    attn_sums, ff_sums, up_sums, input_grads = {}, {}, {}, {}
    attn_small, ff_small, bias_grads, errands = {}, {}, {}, {}
    for layer in (1, 0):
        if layer == 1:
            last, grad_hidden, ff_grad, ff_small[1], up_sums[1] = ffn_turn(
                hiddens[1],
                my_rows(final_cotangent),
                grads_all,
                vectors,
                up_biases,
                *ff_packed[1],
                1,
                half_ff,
            )
        else:
            grad_hidden, ff_grad, ff_small[0], up_sums[0] = ffn_backward(
                grads, hiddens[0], ff_kept, vectors, *ff_packed[0], 0, half_ff
            )
        ff_sums[layer] = lax.psum_scatter(ff_grad, "dp", scatter_dimension=0, tiled=True)
        if layer == 1:
            errand, both_ways = (last, rows), True
        else:
            errand, both_ways = (ff_sums[1], ff_sums[1]), False
        grads, attn_grad, attn_small[layer], bias_grads[layer], got = attn_backward(
            grad_hidden,
            inputs[layer],
            attn_kept[layer],
            vectors,
            *attn_packed[layer],
            layer,
            lengths_here,
            own_rows,
            errand,
            both_ways,
        )
        errands[layer] = got
        attn_sums[layer] = lax.psum_scatter(attn_grad, "dp", scatter_dimension=0, tiled=True)
        input_grads[layer] = grads

    small_mine, up_total, ff_got, attn_got, rows_got = home(
        [attn_small[0], attn_small[1]],
        [ff_small[0], ff_small[1]],
        [bias_grads[0], bias_grads[1]],
        [up_sums[0], up_sums[1]],
        ff_sums[0],
        attn_sums[1],
        [input_grads[0], input_grads[1]],
        count,
        chunk,
    )
    attn_zero_got = lax.ppermute(attn_sums[0], "section", [(1, 0)])
    up_grad, down_grad = ff_finish([ff_sums[0], ff_sums[1]], [ff_got, errands[0]], ff_cols)
    small_mine, up_total, rows_got, out_got, up_grad = lax.optimization_barrier(
        (small_mine, up_total, rows_got, errands[1], up_grad)
    )
    section_output = whole_rows(rows, last, out_got)
    small_mine = small_mine[None, :, :chunk]
    up_total = up_total[:, :, :half_ff].reshape(1, ff_cols)
    input_grad = whole_rows(input_grads[0], input_grads[1], rows_got)

    qkv_total, out_total = attn_finish(
        [attn_sums[0], attn_sums[1]], [attn_zero_got, attn_got], head_cols
    )
    gains = norm_gains.shape[1]
    return (
        section_output[None],
        input_grad[None],
        qkv_total[None],
        out_total[None],
        up_grad[None],
        down_grad.T[None],
        small_mine[:, :gains],
        small_mine[:, gains:],
        up_total,
    )


def solution(mesh):
    in_specs = (
        P(None, "dp", "tensor", None),
        P(None, "dp", "tensor", None),
        P(None, "dp"),
        P("section", None, "dp", "tensor"),
        P("section", "tensor", "dp"),
        P("section", "dp", "tensor"),
        P("section", "tensor", "dp"),
        P("section", None, ("dp", "tensor")),
        P("section", None, ("dp", "tensor")),
        P("section", "tensor"),
    )
    out_specs = (
        P("section", None, "dp", "tensor", None),
        P("section", None, "dp", "tensor", None),
        P("section", None, "dp", "tensor"),
        P("section", "tensor", "dp"),
        P("section", "dp", "tensor"),
        P("section", "tensor", "dp"),
        P("section", None, ("dp", "tensor")),
        P("section", None, ("dp", "tensor")),
        P("section", "tensor"),
    )
    return jax.shard_map(shards, mesh=mesh, in_specs=in_specs, out_specs=out_specs, check_vma=False)
```
